32 devices in a mesh: dp: 1 (over z), ty: 4 (over y), tx: 8 (over x, core).
Axes of the slice: x: 4, y: 4, z: 1, core: 2. Of those that a mesh axis runs over, the one named last changes fastest.
The devices are a block of a 4x4x8 slice.
Arguments:
- x_in: bfloat16 [128, 6144], P('dp', 'tx')
- seq_lens: int32 [128], P('dp')
- k_cache: bfloat16 [128, 4096, 128], P(('dp', 'ty', 'tx'))
- v_cache: bfloat16 [128, 4096, 128], P(('dp', 'ty', 'tx'))
- ln_gamma: float32 [6144], P('tx')
- w_query: bfloat16 [6144, 6144], P('tx', 'ty')
- w_key: bfloat16 [6144, 128], P('tx')
- w_value: bfloat16 [6144, 128], P('tx')
- w_gate: bfloat16 [6144, 24576], P('tx', 'ty')
- w_up: bfloat16 [6144, 24576], P('tx', 'ty')
- w_out: bfloat16 [6144, 6144], P('ty', 'tx')
- w_down: bfloat16 [24576, 6144], P('ty', 'tx')
Outputs:
- output 1: bfloat16 [128, 6144], P('dp', 'tx')
- output 2: bfloat16 [128, 4096, 128], P(('dp', 'ty', 'tx'))
- output 3: bfloat16 [128, 4096, 128], P(('dp', 'ty', 'tx'))
All inputs are finite; a program needn't handle non-finite values.
Results may differ from the reference program's by a relative error of at most 0.0159228.
Values are sent between devices in bfloat16 or wider.
A program may use at most 768 MiB of HBM per device.

```python
import jax
import jax.numpy as jnp
from jax import lax

D_MODEL = 6144
NUM_HEADS = 48
HEAD_DIM = 128
FFN_DIM = 24576
BATCH = 128
SEQ_BLOCK = 4
CTX_LEN = 4096

EPSILON = 1e-6
ROPE_BASE = 10000.0


def setup_inputs(seed: int = 0, part: int = 0) -> dict:
    part_keys = jax.random.split(jax.random.fold_in(jax.random.key(seed), part), 6)
    shared_keys = jax.random.split(jax.random.key(seed + 1), 8)
    x_in = jax.random.normal(part_keys[0], (BATCH, D_MODEL), jnp.float32).astype(jnp.bfloat16)
    block_caps = jax.random.randint(part_keys[1], (BATCH // SEQ_BLOCK,), 1, CTX_LEN + 1)
    raw_lens = jax.random.randint(part_keys[2], (BATCH,), 0, jnp.repeat(block_caps, SEQ_BLOCK))
    pick_order = jax.random.permutation(part_keys[3], BATCH)
    seq_lens = raw_lens.at[pick_order[0]].set(CTX_LEN - 1).at[pick_order[1]].set(0).astype(jnp.int32)
    k_cache = jax.random.normal(part_keys[4], (BATCH, CTX_LEN, HEAD_DIM), jnp.float32).astype(jnp.bfloat16)
    v_cache = jax.random.normal(part_keys[5], (BATCH, CTX_LEN, HEAD_DIM), jnp.float32).astype(jnp.bfloat16)
    ln_gamma = 1.0 + 0.4 * jax.random.normal(shared_keys[0], (D_MODEL,), jnp.float32)
    w_query = (jax.random.normal(shared_keys[1], (D_MODEL, NUM_HEADS * HEAD_DIM), jnp.float32) * (2.0 * D_MODEL ** -0.5)).astype(jnp.bfloat16)
    w_key = (jax.random.normal(shared_keys[2], (D_MODEL, HEAD_DIM), jnp.float32) * D_MODEL ** -0.5).astype(jnp.bfloat16)
    w_value = (jax.random.normal(shared_keys[3], (D_MODEL, HEAD_DIM), jnp.float32) * D_MODEL ** -0.5).astype(jnp.bfloat16)
    w_gate = (jax.random.normal(shared_keys[4], (D_MODEL, FFN_DIM), jnp.float32) * D_MODEL ** -0.5).astype(jnp.bfloat16)
    w_up = (jax.random.normal(shared_keys[5], (D_MODEL, FFN_DIM), jnp.float32) * D_MODEL ** -0.5).astype(jnp.bfloat16)
    w_out = (jax.random.normal(shared_keys[6], (NUM_HEADS * HEAD_DIM, D_MODEL), jnp.float32) * (NUM_HEADS * HEAD_DIM) ** -0.5).astype(jnp.bfloat16)
    w_down = (jax.random.normal(shared_keys[7], (FFN_DIM, D_MODEL), jnp.float32) * FFN_DIM ** -0.5).astype(jnp.bfloat16)
    return {"x_in": x_in, "seq_lens": seq_lens, "k_cache": k_cache, "v_cache": v_cache, "ln_gamma": ln_gamma, "w_query": w_query, "w_key": w_key, "w_value": w_value, "w_gate": w_gate, "w_up": w_up, "w_out": w_out, "w_down": w_down}


def rope_tables(positions, head_dim):
    half_dim = head_dim // 2
    inv_freqs = ROPE_BASE ** (-(jnp.arange(half_dim, dtype=jnp.float32) * 2.0) / head_dim)
    angles = positions.astype(jnp.float32)[:, None] * inv_freqs[None, :]
    return jnp.cos(angles), jnp.sin(angles)


def rope_apply(vals, cosines, sines):
    half_dim = vals.shape[-1] // 2
    first = vals[..., :half_dim]
    second = vals[..., half_dim:]
    return jnp.concatenate([first * cosines - second * sines, second * cosines + first * sines], axis=-1)


def reference(x_in, seq_lens, k_cache, v_cache, ln_gamma, w_query, w_key, w_value, w_gate, w_up, w_out, w_down):
    x_f32 = x_in.astype(jnp.float32)
    row_mean = jnp.sum(x_f32, axis=-1) / D_MODEL
    row_var = jnp.sum(x_f32 * x_f32, axis=-1) / D_MODEL - row_mean * row_mean
    normed = ((x_f32 - row_mean[:, None]) * lax.rsqrt(row_var[:, None] + EPSILON) * ln_gamma[None, :]).astype(jnp.bfloat16)
    q_proj = jnp.dot(normed, w_query, preferred_element_type=jnp.float32).reshape(BATCH, NUM_HEADS, HEAD_DIM)
    k_proj = jnp.dot(normed, w_key, preferred_element_type=jnp.float32)
    v_new = jnp.dot(normed, w_value, preferred_element_type=jnp.float32).astype(jnp.bfloat16)
    gate = jnp.dot(normed, w_gate, preferred_element_type=jnp.float32).astype(jnp.bfloat16)
    up_proj = jnp.dot(normed, w_up, preferred_element_type=jnp.float32).astype(jnp.bfloat16)
    cosines, sines = rope_tables(seq_lens, HEAD_DIM)
    queries = rope_apply(q_proj, cosines[:, None, :], sines[:, None, :]).astype(jnp.bfloat16)
    k_new = rope_apply(k_proj, cosines, sines).astype(jnp.bfloat16)
    positions = jnp.arange(CTX_LEN)
    at_slot = positions[None, :, None] == seq_lens[:, None, None]
    k_out = jnp.where(at_slot, k_new[:, None, :], k_cache)
    v_out = jnp.where(at_slot, v_new[:, None, :], v_cache)

    def one_sequence(item):
        q_row, k_rows, v_rows, length = item
        scores = jnp.dot(q_row, k_rows.T, preferred_element_type=jnp.float32) * (HEAD_DIM ** -0.5)
        in_range = positions[None, :] <= length
        scores = jnp.where(in_range, scores, -1e30)
        att_probs = jax.nn.softmax(scores, axis=-1).astype(jnp.bfloat16)
        return jnp.dot(att_probs, v_rows, preferred_element_type=jnp.float32).astype(jnp.bfloat16)

    att_heads = lax.map(one_sequence, (queries, k_out, v_out, seq_lens))
    mlp_act = (jax.nn.silu(gate.astype(jnp.float32)) * up_proj.astype(jnp.float32)).astype(jnp.bfloat16)
    attn_part = jnp.dot(att_heads.reshape(BATCH, NUM_HEADS * HEAD_DIM), w_out, preferred_element_type=jnp.float32)
    mlp_part = jnp.dot(mlp_act, w_down, preferred_element_type=jnp.float32)
    y_out = (x_f32 + attn_part + mlp_part).astype(jnp.bfloat16)
    return (y_out, k_out, v_out)
```

```python
import functools

import jax
import jax.numpy as jnp
import numpy as np
from jax import lax
from jax.experimental import pallas as pl
from jax.experimental.pallas import tpu as pltpu
from jax.sharding import PartitionSpec as P

EPSILON = 1e-6
ROPE_BASE = 10000.0
MESH = pl.DeviceIdType.MESH
F32 = jnp.float32
BF16 = jnp.bfloat16
VMEM = pltpu.VMEM
DMA = pltpu.SemaphoreType.DMA
SUBS = 4


def place(nx):
    row = lax.axis_index("ty")
    col = lax.axis_index("tx")
    chip = lax.div(col, 2)
    core = lax.rem(col, 2)
    step = 1 - 2 * core
    return row, col, chip, core, step


def remote(src, dst, send_sem, recv_sem, tx=None, ty=None):
    device = {}
    if tx is not None:
        device["tx"] = tx
    if ty is not None:
        device["ty"] = ty
    return pltpu.make_async_remote_copy(src_ref=src, dst_ref=dst, send_sem=send_sem, recv_sem=recv_sem, device_id=device, device_id_type=MESH)


def greet(tx_peers, ty_peers):
    barrier = pltpu.get_barrier_semaphore()
    for peer in tx_peers:
        pl.semaphore_signal(barrier, inc=1, device_id={"tx": peer}, device_id_type=MESH)
    for peer in ty_peers:
        pl.semaphore_signal(barrier, inc=1, device_id={"ty": peer}, device_id_type=MESH)
    pl.semaphore_wait(barrier, len(tx_peers) + len(ty_peers))


def proj_kernel(ny, nx, d_model, x_ref, gamma_ref, perm_ref, wq_h, wk_h, wv_h, wg_h, wu_h,
                q_out, kv_out, act_out,
                wq_v, wb_v, h_v, stat_s, stat_r, qp, qd_s, qd_r, qx_s, qx_r, qsum, qy_s, qy_r, d_s, d_r, own, r_s, r_r,
                wq_sem, wb_sem, stat_ss, stat_rs, qd_ss, qd_rs, qx_ss, qx_rs, qy_ss, qy_rs, d_ss, d_rs, r_ss, r_rs):
    row, col, chip, core, step = place(nx)
    ntx = 2 * nx
    rows = x_ref.shape[0]
    rb = rows // ntx
    sb = rb // ny
    qn = wq_h.shape[1]
    hd = wk_h.shape[1]
    fb = wb_v.shape[2] // 2
    sub = rows // SUBS

    def block_of(s, mine):
        sign = step if mine else -step
        at = lax.rem(chip - (s + 1) * sign + 2 * nx, nx)
        return 2 * at + (core if mine else 1 - core)

    def q_loads():
        return [
            pltpu.make_async_copy(wq_h, wq_v.at[:, pl.ds(0, qn)], wq_sem.at[0]),
            pltpu.make_async_copy(wk_h, wq_v.at[:, pl.ds(qn, hd)], wq_sem.at[1]),
            pltpu.make_async_copy(wv_h, wq_v.at[:, pl.ds(qn + hd, hd)], wq_sem.at[2]),
        ]

    def block_loads(n, b):
        at = pl.ds(pl.multiple_of(b * fb, fb), fb)
        return [
            pltpu.make_async_copy(wg_h.at[:, at], wb_v.at[n, :, pl.ds(0, fb)], wb_sem.at[n, 0]),
            pltpu.make_async_copy(wu_h.at[:, at], wb_v.at[n, :, pl.ds(fb, fb)], wb_sem.at[n, 1]),
        ]

    for c in q_loads():
        c.start()
    for n in range(ntx):
        for c in block_loads(n, block_of(n // 2, n % 2 == 1)):
            c.start()

    xp = jnp.dot(perm_ref[...], x_ref[...], preferred_element_type=F32)
    s1 = jnp.sum(xp, axis=1, keepdims=True)
    s2 = jnp.sum(xp * xp, axis=1, keepdims=True)
    lane = lax.broadcasted_iota(jnp.int32, (rows, rows), 1)
    both = jnp.where(lane == 0, s1, jnp.where(lane == 1, s2, 0.0))
    stat_s[...] = jnp.transpose(both)[:8]

    tx_peers = [lax.rem(col + k, ntx) for k in range(1, ntx)]
    ty_peers = [lax.rem(row + k, ny) for k in range(1, ny)]
    greet(tx_peers, ty_peers)

    stat_cp = [remote(stat_s, stat_r.at[k], stat_ss.at[k], stat_rs.at[k], tx=tx_peers[k - 1]) for k in range(1, ntx)]
    for c in stat_cp:
        c.start()
    total = stat_s[...]
    for k, c in enumerate(stat_cp):
        c.wait_recv()
        total = total + stat_r[k + 1]
    square = jnp.transpose(jnp.concatenate([total, jnp.zeros((rows - 8, rows), F32)], axis=0))
    mean = square[:, 0:1] / d_model
    var = square[:, 1:2] / d_model - mean * mean
    h_v[...] = ((xp - mean) * lax.rsqrt(var + EPSILON) * gamma_ref[...]).astype(BF16)

    for c in q_loads():
        c.wait()
    qw = qn + 2 * hd
    qp[...] = jnp.dot(h_v[...], wq_v[...], preferred_element_type=F32).reshape(ntx, rb, qw)
    for n in range(nx):
        qd_s[n] = qp[2 * n + 1 - core].astype(BF16)
    partner = lax.rem(col + 1, 2) + 2 * chip
    qd_cp = remote(qd_s, qd_r, qd_ss, qd_rs, tx=partner)
    qd_cp.start()

    qx_cp = [remote(qx_s.at[k], qx_r.at[k], qx_ss.at[k], qx_rs.at[k], tx=2 * lax.rem(chip + k, nx) + core) for k in range(1, nx)]
    qy_cp = [remote(qy_s.at[lax.rem(row + k, ny)], qy_r.at[row], qy_ss.at[k], qy_rs.at[k], ty=lax.rem(row + k, ny)) for k in range(1, ny)]
    qy_in = [remote(qy_s.at[lax.rem(row - k + ny, ny)], qy_r.at[lax.rem(row - k + ny, ny)], qy_ss.at[k], qy_rs.at[k], ty=lax.rem(row + k, ny)) for k in range(1, ny)]

    def q_pair():
        qd_cp.wait_recv()
        for k in range(1, nx):
            at = lax.rem(chip + k, nx)
            qx_s[k] = (qp[2 * at + core] + qd_r[at].astype(F32)).astype(BF16)
            qx_cp[k - 1].start()

    def q_rows():
        mine = qp[2 * chip + core] + qd_r[chip].astype(F32)
        for k in range(1, nx):
            qx_cp[k - 1].wait_recv()
            mine = mine + qx_r[k].astype(F32)
        qsum[...] = mine
        for a in range(ny):
            for n in range(qn // hd):
                qy_s[a, n * sb:(n + 1) * sb, :] = qsum[a * sb:(a + 1) * sb, n * hd:(n + 1) * hd]
        kv_out[...] = qsum[:, qn:]
        for c in qy_cp:
            c.start()

    after = 2 * lax.rem(chip + step + nx, nx) + core

    def d_copy(s):
        return remote(d_s.at[s], d_r.at[s], d_ss.at[s], d_rs.at[s], tx=partner)

    def r_copy(s, t):
        at = pl.ds(pl.multiple_of(t * sub, sub), sub)
        return remote(r_s.at[s, at], r_r.at[s, at], r_ss.at[s, t], r_rs.at[s, t], tx=after)

    def ring(s, carry):
        for c in block_loads(2 * s, 0):
            c.wait()
        own[...] = jnp.dot(h_v[...], wb_v[2 * s], preferred_element_type=F32)
        d_s[s] = own[...].astype(BF16)
        d_copy(s).start()

        @pl.when(s == 0)
        def _():
            q_pair()

        for c in block_loads(2 * s + 1, 0):
            c.wait()
        own[...] = jnp.dot(h_v[...], wb_v[2 * s + 1], preferred_element_type=F32)

        @pl.when(s == 2)
        def _():
            q_rows()

        d_copy(s).wait_recv()

        @pl.when(s == 0)
        def _():
            for t in range(SUBS):
                at = pl.ds(t * sub, sub)
                r_s[s, at] = (own[at] + d_r[s, at].astype(F32)).astype(BF16)
                r_copy(s, t).start()

        @pl.when(s > 0)
        def _():
            for t in range(SUBS):
                at = pl.ds(t * sub, sub)
                own[at] = own[at] + d_r[s, at].astype(F32)
                r_copy(s - 1, t).wait_recv()
                own[at] = own[at] + r_r[s - 1, at].astype(F32)

                @pl.when(s < nx - 1)
                def _():
                    r_s[s, at] = own[at].astype(BF16)
                    r_copy(s, t).start()

        return carry

    lax.fori_loop(0, nx, ring, 0)

    gate = own[:, :fb].astype(BF16).astype(F32)
    up = own[:, fb:].astype(BF16).astype(F32)
    act_out[...] = (gate * (1.0 / (1.0 + jnp.exp(-gate))) * up).astype(BF16)

    qy_r[row] = qy_s[row]
    for k in range(1, ny):
        qy_in[k - 1].wait_recv()
    q_out[...] = qy_r[...]

    for c in stat_cp:
        c.wait_send()
    qd_cp.wait_send()
    for c in qx_cp + qy_cp:
        c.wait_send()
    for s in range(nx):
        d_copy(s).wait_send()
    for s in range(nx - 1):
        for t in range(SUBS):
            r_copy(s, t).wait_send()


def attn_kernel(ny, ntx, chunk, lens_ref, q_ref, kv_ref, cs_ref, k_h, v_h, att_out, ko_h, vo_h, kbuf, vbuf, sbuf, qs, o32, in_sem, out_sem):
    row = lax.axis_index("ty")
    col = lax.axis_index("tx")
    sb, ctx, hd = k_h.shape
    heads = q_ref.shape[0] * q_ref.shape[1] // sb
    lh = heads // ny

    def k_in(r):
        return pltpu.make_async_copy(k_h.at[r], kbuf.at[r], in_sem.at[0, r])

    def v_in(r):
        return pltpu.make_async_copy(v_h.at[r], vbuf.at[r], in_sem.at[1, r])

    def k_put(r):
        return pltpu.make_async_copy(kbuf.at[r], ko_h.at[r], out_sem.at[0, r])

    def v_put(r):
        return pltpu.make_async_copy(vbuf.at[r], vo_h.at[r], out_sem.at[1, r])

    for r in range(sb):
        k_in(r).start()
        v_in(r).start()

    def turn(vals, r):
        return vals * cs_ref[r:r + 1, :] + pltpu.roll(vals, hd // 2, 1) * cs_ref[sb + r:sb + r + 1, :]

    def patch(buf, r, length, new):
        base = pl.multiple_of(lax.div(length, 16) * 16, 16)
        at = pl.ds(base, 16)
        old = buf[r, at, :]
        here = lax.broadcasted_iota(jnp.int32, (16, hd), 0) == length - base
        buf[r, at, :] = jnp.where(here, new, old.astype(F32)).astype(BF16)

    for r in range(sb):
        length = lens_ref[(row * ntx + col) * sb + r]
        for a in range(ny):
            part = q_ref[a, pl.ds(r, lh, stride=sb), :]
            qs[a * lh:(a + 1) * lh, :] = turn(part, r)
        q = qs[...].astype(BF16)
        new_rows = kv_ref[pl.ds(row * sb + r, 1), :]
        k_in(r).wait()
        patch(kbuf, r, length, turn(new_rows[:, :hd], r))
        k_put(r).start()
        chunks = lax.div(length, chunk) + 1

        def score(c, top):
            at = pl.ds(pl.multiple_of(c * chunk, chunk), chunk)
            s = lax.dot_general(q, kbuf[r, at, :], (((1,), (1,)), ((), ())), preferred_element_type=F32) * (hd ** -0.5)
            pos = lax.broadcasted_iota(jnp.int32, (heads, chunk), 1) + c * chunk
            s = jnp.where(pos <= length, s, -1e30)
            sbuf[:, at] = s
            return jnp.maximum(top, jnp.max(s, axis=1, keepdims=True))

        top = lax.fori_loop(0, chunks, score, jnp.full((heads, 1), -1e30, F32))

        def weigh(c, low):
            at = pl.ds(pl.multiple_of(c * chunk, chunk), chunk)
            e = jnp.exp(sbuf[:, at] - top)
            sbuf[:, at] = e
            return low + jnp.sum(e, axis=1, keepdims=True)

        low = lax.fori_loop(0, chunks, weigh, jnp.zeros((heads, 1), F32))
        share = 1.0 / low
        v_in(r).wait()
        patch(vbuf, r, length, new_rows[:, hd:])
        v_put(r).start()

        def mix(c, out):
            at = pl.ds(pl.multiple_of(c * chunk, chunk), chunk)
            p = (sbuf[:, at] * share).astype(BF16)
            return out + jnp.dot(p, vbuf[r, at, :], preferred_element_type=F32)

        out = lax.fori_loop(0, chunks, mix, jnp.zeros((heads, hd), F32))
        for a in range(ny):
            o32[a, pl.ds(r, lh, stride=sb), :] = out[a * lh:(a + 1) * lh]
    att_out[...] = o32[...].astype(BF16)
    for r in range(sb):
        k_put(r).wait()
        v_put(r).wait()


def out_kernel(ny, nx, x_ref, perm_ref, att_ref, act_ref, wo_h, wd_h, y_out,
               wo_v, wd_v, ay_r, g32, g_v, b_v, acc, y_s, y_r, yf,
               wo_sem, wd_sem, ay_ss, ay_rs, g_ss, g_rs, gp_ss, gp_rs, b_ss, b_rs, bp_ss, bp_rs, y_ss, y_rs, f_ss, f_rs):
    row, col, chip, core, step = place(nx)
    ntx = 2 * nx
    rows, fb = act_ref.shape
    lh, rb, hd = g32.shape
    sb = rb // ny
    sub = rows // SUBS
    yb = rows // ny
    dl = wo_h.shape[1]
    partner = lax.rem(col + 1, 2) + 2 * chip
    after = 2 * lax.rem(chip + step + nx, nx) + core

    def block_of(s, mine):
        sign = step if mine else -step
        return 2 * lax.rem(chip - s * sign + 2 * nx, nx) + (core if mine else 1 - core)

    def wo_load():
        return pltpu.make_async_copy(wo_h, wo_v, wo_sem)

    def wd_load(n, b):
        at = pl.ds(pl.multiple_of(b * fb, fb), fb)
        return pltpu.make_async_copy(wd_h.at[at, :], wd_v.at[n], wd_sem.at[n])

    for n in range(ntx):
        wd_load(n, block_of(n // 2, n % 2 == 0)).start()
    wo_load().start()

    x_peers = [2 * lax.rem(chip + k, nx) + core for k in range(1, nx)]
    y_peers = [lax.rem(row + k, ny) for k in range(1, ny)]
    greet(x_peers + [partner], y_peers)

    mine = block_of(0, True)
    b_v[mine] = act_ref[...]

    def b_copy(s, t):
        b = block_of(s, True)
        at = pl.ds(pl.multiple_of(t * sub, sub), sub)
        return remote(b_v.at[b, at], b_v.at[b, at], b_ss.at[s, t], b_rs.at[s, t], tx=after)

    def b_in(s, t):
        b = block_of(s + 1, True)
        at = pl.ds(pl.multiple_of(t * sub, sub), sub)
        return remote(b_v.at[b, at], b_v.at[b, at], b_ss.at[s, t], b_rs.at[s, t], tx=after)

    def bp_copy(s):
        b = block_of(s, True)
        return remote(b_v.at[b], b_v.at[b], bp_ss.at[s], bp_rs.at[s], tx=partner)

    def bp_in(s):
        b = block_of(s, False)
        return remote(b_v.at[b], b_v.at[b], bp_ss.at[s], bp_rs.at[s], tx=partner)

    for t in range(SUBS):
        b_copy(0, t).start()
    bp_copy(0).start()

    ay_cp = [remote(att_ref.at[y_peers[k - 1]], ay_r.at[row], ay_ss.at[k], ay_rs.at[k], ty=y_peers[k - 1]) for k in range(1, ny)]
    for c in ay_cp:
        c.start()
    ay_r[row] = att_ref[row]
    for k in range(1, ny):
        src = lax.rem(row - k + ny, ny)
        remote(att_ref.at[src], ay_r.at[src], ay_ss.at[k], ay_rs.at[k], ty=y_peers[k - 1]).wait_recv()
    for a in range(ny):
        part = ay_r[a].astype(F32)
        for n in range(lh):
            g32[n, a * sb:(a + 1) * sb, :] = part[n * sb:(n + 1) * sb, :]
    g_v[col] = g32[...].astype(BF16)

    g_cp = [remote(g_v.at[col], g_v.at[col], g_ss.at[k], g_rs.at[k], tx=x_peers[k - 1]) for k in range(1, nx)]
    for c in g_cp:
        c.start()

    def gp_copy(k):
        at = 2 * lax.rem(chip - k + nx, nx) + core
        return remote(g_v.at[at], g_v.at[at], gp_ss.at[k], gp_rs.at[k], tx=partner)

    def gp_in(k):
        at = 2 * lax.rem(chip - k + nx, nx) + 1 - core
        return remote(g_v.at[at], g_v.at[at], gp_ss.at[k], gp_rs.at[k], tx=partner)

    gp_copy(0).start()
    acc[...] = jnp.zeros_like(acc)

    def blocks(s, carry):
        wd_load(2 * s, 0).wait()
        acc[...] += jnp.dot(b_v[block_of(s, True)], wd_v[2 * s], preferred_element_type=F32)

        @pl.when(s < nx - 1)
        def _():
            for t in range(SUBS):
                b_in(s, t).wait_recv()

                @pl.when(s < nx - 2)
                def _():
                    b_copy(s + 1, t).start()

            bp_copy(s + 1).start()

        @pl.when(s == 0)
        def _():
            for k in range(1, nx):
                at = 2 * lax.rem(chip - k + nx, nx) + core
                remote(g_v.at[at], g_v.at[at], g_ss.at[k], g_rs.at[k], tx=x_peers[k - 1]).wait_recv()
                gp_copy(k).start()

        bp_in(s).wait_recv()
        wd_load(2 * s + 1, 0).wait()
        acc[...] += jnp.dot(b_v[block_of(s, False)], wd_v[2 * s + 1], preferred_element_type=F32)

        @pl.when(s == 1)
        def _():
            wo_load().wait()
            for k in range(nx):
                gp_in(k).wait_recv()
            for n in range(0, lh, 2):
                pair = jnp.concatenate([g_v[:, n].reshape(rows, hd), g_v[:, n + 1].reshape(rows, hd)], axis=1)
                acc[...] += jnp.dot(pair, wo_v[n * hd:(n + 2) * hd, :], preferred_element_type=F32)

        return carry

    lax.fori_loop(0, nx, blocks, 0)

    part = lax.dot_general(perm_ref[...], acc[...].astype(BF16), (((0,), (0,)), ((), ())), preferred_element_type=F32)
    y_s[...] = part.astype(BF16).reshape(ny, yb, dl)
    y_cp = [remote(y_s.at[y_peers[k - 1]], y_r.at[k], y_ss.at[k], y_rs.at[k], ty=y_peers[k - 1]) for k in range(1, ny)]
    for c in y_cp:
        c.start()
    total = x_ref[pl.ds(pl.multiple_of(row * yb, yb), yb), :].astype(F32) + y_s[row].astype(F32)
    for k in range(1, ny):
        y_cp[k - 1].wait_recv()
        total = total + y_r[k].astype(F32)
    yf[row] = total.astype(BF16)
    f_cp = [remote(yf.at[row], yf.at[row], f_ss.at[k], f_rs.at[k], ty=y_peers[k - 1]) for k in range(1, ny)]
    for c in f_cp:
        c.start()
    for k in range(1, ny):
        src = lax.rem(row - k + ny, ny)
        remote(yf.at[src], yf.at[src], f_ss.at[k], f_rs.at[k], ty=y_peers[k - 1]).wait_recv()
    y_out[...] = yf[...].reshape(rows, dl)

    for s in range(nx - 1):
        for t in range(SUBS):
            b_copy(s, t).wait_send()
    for s in range(nx):
        bp_copy(s).wait_send()
        gp_copy(s).wait_send()
    for c in ay_cp + g_cp + y_cp + f_cp:
        c.wait_send()


def solution(mesh):
    ny = mesh.shape["ty"]
    ntx = mesh.shape["tx"]
    nx = ntx // 2
    cache_spec = P(("dp", "ty", "tx"), None, None)
    vspec = pl.BlockSpec(memory_space=VMEM)
    hspec = pl.BlockSpec(memory_space=pltpu.HBM)
    sspec = pl.BlockSpec(memory_space=pltpu.SMEM)

    def layer_shard(x_blk, lens_part, k_blk, v_blk, gamma_blk, w_query, w_key, w_value, w_gate, w_up, w_out, w_down):
        rows, dl = x_blk.shape
        sb, ctx, hd = k_blk.shape
        qn = w_query.shape[1]
        lh = qn // hd
        qw = qn + 2 * hd
        ffl = w_gate.shape[1]
        fb = ffl // ntx
        rb = rows // ntx
        row_idx = lax.axis_index("ty")
        col_idx = lax.axis_index("tx")

        natural = np.arange(rows)
        order = np.reshape(np.transpose(np.reshape(natural, (ny, ntx, sb)), (1, 0, 2)), (rows,))
        perm = jnp.asarray(order[:, None] == natural[None, :], dtype=BF16)

        q_parts, kv_sum, act = pl.pallas_call(
            functools.partial(proj_kernel, ny, nx, dl * ntx),
            out_shape=(
                jax.ShapeDtypeStruct((ny, sb * lh, hd), F32),
                jax.ShapeDtypeStruct((rb, 2 * hd), F32),
                jax.ShapeDtypeStruct((rows, fb), BF16),
            ),
            in_specs=[vspec] * 3 + [hspec] * 5,
            out_specs=(vspec,) * 3,
            scratch_shapes=[
                VMEM((dl, qw), BF16), VMEM((ntx, dl, 2 * fb), BF16), VMEM((rows, dl), BF16),
                VMEM((8, rows), F32), VMEM((ntx, 8, rows), F32),
                VMEM((ntx, rb, qw), F32), VMEM((nx, rb, qw), BF16), VMEM((nx, rb, qw), BF16),
                VMEM((nx, rb, qw), BF16), VMEM((nx, rb, qw), BF16), VMEM((rb, qw), F32),
                VMEM((ny, sb * lh, hd), F32), VMEM((ny, sb * lh, hd), F32),
                VMEM((nx, rows, 2 * fb), BF16), VMEM((nx, rows, 2 * fb), BF16), VMEM((rows, 2 * fb), F32),
                VMEM((nx - 1, rows, 2 * fb), BF16), VMEM((nx - 1, rows, 2 * fb), BF16),
                DMA((3,)), DMA((ntx, 2)), DMA((ntx,)), DMA((ntx,)), DMA, DMA, DMA((nx,)), DMA((nx,)), DMA((ny,)), DMA((ny,)),
                DMA((nx,)), DMA((nx,)), DMA((nx - 1, SUBS)), DMA((nx - 1, SUBS)),
            ],
            compiler_params=pltpu.CompilerParams(collective_id=0, has_side_effects=True, vmem_limit_bytes=60 * 1024 * 1024),
            name="proj",
        )(x_blk, gamma_blk[None, :], perm, w_query, w_key, w_value, w_gate, w_up)

        lens_own = lax.dynamic_slice_in_dim(lens_part, (row_idx * ntx + col_idx) * sb, sb)
        inv_freqs = ROPE_BASE ** (-(jnp.arange(hd // 2, dtype=F32) * 2.0) / hd)
        angles = lens_own.astype(F32)[:, None] * inv_freqs[None, :]
        cosines, sines = jnp.cos(angles), jnp.sin(angles)
        turns = jnp.concatenate([jnp.concatenate([cosines, cosines], axis=1), jnp.concatenate([-sines, sines], axis=1)], axis=0)

        att, k_out, v_out = pl.pallas_call(
            functools.partial(attn_kernel, ny, ntx, 512),
            out_shape=(
                jax.ShapeDtypeStruct((ny, sb * lh, hd), BF16),
                jax.ShapeDtypeStruct(k_blk.shape, BF16),
                jax.ShapeDtypeStruct(v_blk.shape, BF16),
            ),
            in_specs=[sspec, vspec, vspec, vspec, hspec, hspec],
            out_specs=(vspec, hspec, hspec),
            scratch_shapes=[
                VMEM((sb, ctx, hd), BF16), VMEM((sb, ctx, hd), BF16), VMEM((ny * lh, ctx), F32), VMEM((ny * lh, hd), F32),
                VMEM((ny, sb * lh, hd), F32), DMA((2, sb)), DMA((2, sb)),
            ],
            compiler_params=pltpu.CompilerParams(vmem_limit_bytes=40 * 1024 * 1024),
            name="attn",
        )(lens_part, q_parts, kv_sum, turns, k_blk, v_blk)

        y_blk = pl.pallas_call(
            functools.partial(out_kernel, ny, nx),
            out_shape=jax.ShapeDtypeStruct((rows, dl), BF16),
            in_specs=[vspec] * 4 + [hspec] * 2,
            out_specs=vspec,
            scratch_shapes=[
                VMEM((qn, dl), BF16), VMEM((ntx, fb, dl), BF16), VMEM((ny, sb * lh, hd), BF16), VMEM((lh, rb, hd), F32),
                VMEM((ntx, lh, rb, hd), BF16), VMEM((ntx, rows, fb), BF16), VMEM((rows, dl), F32),
                VMEM((ny, rows // ny, dl), BF16), VMEM((ny, rows // ny, dl), BF16), VMEM((ny, rows // ny, dl), BF16),
                DMA, DMA((ntx,)), DMA((ny,)), DMA((ny,)), DMA((nx,)), DMA((nx,)), DMA((nx,)), DMA((nx,)),
                DMA((nx - 1, SUBS)), DMA((nx - 1, SUBS)), DMA((nx,)), DMA((nx,)), DMA((ny,)), DMA((ny,)), DMA((ny,)), DMA((ny,)),
            ],
            compiler_params=pltpu.CompilerParams(collective_id=1, has_side_effects=True, vmem_limit_bytes=60 * 1024 * 1024),
            name="outs",
        )(x_blk, perm, att, act, w_out, w_down)
        return y_blk, k_out, v_out

    in_specs = (P("dp", "tx"), P("dp"), cache_spec, cache_spec, P("tx"), P("tx", "ty"), P("tx", None), P("tx", None), P("tx", "ty"), P("tx", "ty"), P("ty", "tx"), P("ty", "tx"))
    out_specs = (P("dp", "tx"), cache_spec, cache_spec)
    return jax.shard_map(layer_shard, mesh=mesh, in_specs=in_specs, out_specs=out_specs, check_vma=False)
```

```python
import functools

import jax
import jax.numpy as jnp
import numpy as np
from jax import lax
from jax.experimental import pallas as pl
from jax.experimental.pallas import tpu as pltpu
from jax.sharding import PartitionSpec as P

EPSILON = 1e-6
ROPE_BASE = 10000.0
LOG2E = 1.4426950408889634
MESH = pl.DeviceIdType.MESH
F32 = jnp.float32
BF16 = jnp.bfloat16
VMEM = pltpu.VMEM
DMA = pltpu.SemaphoreType.DMA
SUBS = 4
CHUNK = 1024
PIECE = 512
scope = jax.named_scope


def remote(src, dst, send_sem, recv_sem, tx=None, ty=None):
    device = {}
    if tx is not None:
        device["tx"] = tx
    if ty is not None:
        device["ty"] = ty
    return pltpu.make_async_remote_copy(src_ref=src, dst_ref=dst, send_sem=send_sem, recv_sem=recv_sem, device_id=device, device_id_type=MESH)


def step_kernel(ny, nx, d_model, lens_ref, x_h, gamma_h, perm_h, freq_h, wq_h, wk_h, wv_h, wg_h, wu_h, k_h, v_h, wo_h, wd_h,
                y_out, new_out, kbuf, vbuf,
                x_v, gamma_v, perm_v, freq_v, wq_v, wb_v, wo_v, wd_v, h_v, stat_s, stat_r,
                qp, qd_s, qd_r, qx_s, qx_r, qsum, kvs, qy_s, qy_r, own, d_s, d_r, r_s, r_r,
                turns, qs, sbuf, o32, ay_s, ay_r, g32, g_v, b_v, acc, y_s, y_r, yf,
                in_sem, wq_sem, wb_sem, kv_sem, wo_sem, wd_sem, stat_ss, stat_rs, qd_ss, qd_rs, qx_ss, qx_rs, qy_ss, qy_rs,
                d_ss, d_rs, r_ss, r_rs, ay_ss, ay_rs, g_ss, g_rs, gp_ss, gp_rs, b_ss, b_rs, bp_ss, bp_rs, y_ss, y_rs, f_ss, f_rs):
    row = lax.axis_index("ty")
    col = lax.axis_index("tx")
    chip = lax.div(col, 2)
    core = lax.rem(col, 2)
    step = 1 - 2 * core
    ntx = 2 * nx
    rows, dl = x_h.shape
    rb = rows // ntx
    sb = rb // ny
    qn = wq_h.shape[1]
    hd = wk_h.shape[1]
    qw = qn + 2 * hd
    lh = qn // hd
    heads = ny * lh
    ctx = k_h.shape[1]
    fb = wb_v.shape[2] // 2
    sub = rows // SUBS
    yb = rows // ny
    partner = lax.rem(col + 1, 2) + 2 * chip
    after = 2 * lax.rem(chip + step + nx, nx) + core
    tx_peers = [lax.rem(col + k, ntx) for k in range(1, ntx)]
    x_peers = [2 * lax.rem(chip + k, nx) + core for k in range(1, nx)]
    y_peers = [lax.rem(row + k, ny) for k in range(1, ny)]
    y_froms = [lax.rem(row - k + ny, ny) for k in range(1, ny)]

    barrier = pltpu.get_barrier_semaphore()
    for peer in tx_peers:
        pl.semaphore_signal(barrier, inc=1, device_id={"tx": peer}, device_id_type=MESH)
    for peer in y_peers:
        pl.semaphore_signal(barrier, inc=1, device_id={"ty": peer}, device_id_type=MESH)

    def piece(t):
        return pl.ds(pl.multiple_of(t * sub, sub), sub)

    def block_of(s, mine):
        sign = step if mine else -step
        at = lax.rem(chip - (s + 1) * sign + 2 * nx, nx)
        return 2 * at + (core if mine else 1 - core)

    def held(s, mine):
        sign = step if mine else -step
        return 2 * lax.rem(chip - s * sign + 2 * nx, nx) + (core if mine else 1 - core)

    def block_loads(n, b):
        at = pl.ds(pl.multiple_of(b * fb, fb), fb)
        return [
            pltpu.make_async_copy(wg_h.at[:, at], wb_v.at[n, :, pl.ds(0, fb)], wb_sem.at[n, 0]),
            pltpu.make_async_copy(wu_h.at[:, at], wb_v.at[n, :, pl.ds(fb, fb)], wb_sem.at[n, 1]),
        ]

    def wd_load(n, b):
        at = pl.ds(pl.multiple_of(b * fb, fb), fb)
        return pltpu.make_async_copy(wd_h.at[at, :], wd_v.at[n], wd_sem.at[n])

    first_loads = [
        pltpu.make_async_copy(x_h, x_v, in_sem.at[0]),
        pltpu.make_async_copy(perm_h, perm_v, in_sem.at[1]),
        pltpu.make_async_copy(gamma_h, gamma_v, in_sem.at[2]),
        pltpu.make_async_copy(freq_h, freq_v, in_sem.at[3]),
    ]
    q_loads = [
        pltpu.make_async_copy(wq_h, wq_v.at[:, pl.ds(0, qn)], wq_sem.at[0]),
        pltpu.make_async_copy(wk_h, wq_v.at[:, pl.ds(qn, hd)], wq_sem.at[1]),
        pltpu.make_async_copy(wv_h, wq_v.at[:, pl.ds(qn + hd, hd)], wq_sem.at[2]),
    ]
    k_in = [pltpu.make_async_copy(k_h.at[r], kbuf.at[r], kv_sem.at[0, r]) for r in range(sb)]
    v_in = [pltpu.make_async_copy(v_h.at[r], vbuf.at[r], kv_sem.at[1, r]) for r in range(sb)]
    wo_load = pltpu.make_async_copy(wo_h, wo_v, wo_sem)
    for c in first_loads + q_loads:
        c.start()
    for n in range(ntx):
        for c in block_loads(n, block_of(n // 2, n % 2 == 1)):
            c.start()
    for c in k_in + v_in:
        c.start()
    for n in range(ntx):
        wd_load(n, held(n // 2, n % 2 == 0)).start()
    wo_load.start()

    for c in first_loads:
        c.wait()
    xp = jnp.dot(perm_v[...], x_v[...], preferred_element_type=F32)
    s1 = jnp.sum(xp, axis=1, keepdims=True)
    s2 = jnp.sum(xp * xp, axis=1, keepdims=True)
    lane = lax.broadcasted_iota(jnp.int32, (rows, rows), 1)
    both = jnp.where(lane == 0, s1, jnp.where(lane == 1, s2, 0.0))
    stat_s[...] = jnp.transpose(both)[:8]

    at_row = lax.broadcasted_iota(jnp.int32, (8, hd), 0)
    places = jnp.zeros((8, hd), F32)
    for r in range(sb):
        places = jnp.where(at_row == r, lens_ref[(row * ntx + col) * sb + r].astype(F32), places)
    angles = places * freq_v[...]
    turns[0] = jnp.cos(angles)
    low_half = lax.broadcasted_iota(jnp.int32, (8, hd), 1) < hd // 2
    sines = jnp.sin(angles)
    turns[1] = jnp.where(low_half, -sines, sines)

    with scope("greet"):
        pl.semaphore_wait(barrier, ntx - 1 + ny - 1)

    stat_cp = [remote(stat_s, stat_r.at[k], stat_ss.at[k], stat_rs.at[k], tx=tx_peers[k - 1]) for k in range(1, ntx)]
    for c in stat_cp:
        c.start()
    total = stat_s[...]
    with scope("stat"):
        for k, c in enumerate(stat_cp):
            c.wait_recv()
            total = total + stat_r[k + 1]
    square = jnp.transpose(jnp.concatenate([total, jnp.zeros((rows - 8, rows), F32)], axis=0))
    mean = square[:, 0:1] / d_model
    var = square[:, 1:2] / d_model - mean * mean
    h_v[...] = ((xp - mean) * lax.rsqrt(var + EPSILON) * gamma_v[...].reshape(1, dl)).astype(BF16)

    for c in q_loads:
        c.wait()
    qp[...] = jnp.dot(h_v[...], wq_v[...], preferred_element_type=F32).reshape(ntx, rb, qw)
    for n in range(nx):
        qd_s[n] = qp[2 * n + 1 - core].astype(BF16)
    qd_cp = remote(qd_s, qd_r, qd_ss, qd_rs, tx=partner)
    qd_cp.start()
    qx_cp = [remote(qx_s.at[k], qx_r.at[k], qx_ss.at[k], qx_rs.at[k], tx=x_peers[k - 1]) for k in range(1, nx)]
    qy_cp = [remote(qy_s.at[y_peers[k - 1]], qy_r.at[row], qy_ss.at[k], qy_rs.at[k], ty=y_peers[k - 1]) for k in range(1, ny)]
    qy_in = [remote(qy_s.at[y_froms[k - 1]], qy_r.at[y_froms[k - 1]], qy_ss.at[k], qy_rs.at[k], ty=y_peers[k - 1]) for k in range(1, ny)]

    def q_pair():
        with scope("qd"):
            qd_cp.wait_recv()
        for k in range(1, nx):
            at = lax.rem(chip + k, nx)
            qx_s[k] = (qp[2 * at + core] + qd_r[at].astype(F32)).astype(BF16)
            qx_cp[k - 1].start()

    def q_rows():
        mine = qp[2 * chip + core] + qd_r[chip].astype(F32)
        with scope("qx"):
            for k in range(1, nx):
                qx_cp[k - 1].wait_recv()
                mine = mine + qx_r[k].astype(F32)
        qsum[...] = mine
        kvs[0] = mine[:, qn:qn + hd]
        kvs[1] = mine[:, qn + hd:]
        for a in range(ny):
            for n in range(lh):
                qy_s[a, n * sb:(n + 1) * sb, :] = qsum[a * sb:(a + 1) * sb, n * hd:(n + 1) * hd]
        for c in qy_cp:
            c.start()
        qy_r[row] = qy_s[row]

    def d_copy(s):
        return remote(d_s.at[s], d_r.at[s], d_ss.at[s], d_rs.at[s], tx=partner)

    def r_copy(s, t):
        return remote(r_s.at[s, piece(t)], r_r.at[s, piece(t)], r_ss.at[s, t], r_rs.at[s, t], tx=after)

    def product(s, carry):
        for c in block_loads(2 * s, 0):
            c.wait()
        d_s[s] = jnp.dot(h_v[...], wb_v[2 * s], preferred_element_type=F32).astype(BF16)
        d_copy(s).start()

        @pl.when(s == 0)
        def _():
            q_pair()

        for c in block_loads(2 * s + 1, 0):
            c.wait()
        own[s] = jnp.dot(h_v[...], wb_v[2 * s + 1], preferred_element_type=F32)

        @pl.when(s == 0)
        def _():
            with scope("d0"):
                d_copy(0).wait_recv()
            for t in range(SUBS):
                at = piece(t)
                r_s[0, at] = (own[0, at] + d_r[0, at].astype(F32)).astype(BF16)
                r_copy(0, t).start()

        return carry

    with scope("products"):
        lax.fori_loop(0, nx, product, 0)

    def ring(s, t):
        at = piece(t)
        if t == 0:
            with scope("d%d" % s):
                d_copy(s).wait_recv()
        part = own[s, at] + d_r[s, at].astype(F32)
        with scope("r%d%d" % (s, t)):
            r_copy(s - 1, t).wait_recv()
        part = part + r_r[s - 1, at].astype(F32)
        if s < nx - 1:
            r_s[s, at] = part.astype(BF16)
            r_copy(s, t).start()
        else:
            gate = part[:, :fb].astype(BF16).astype(F32)
            up = part[:, fb:].astype(BF16).astype(F32)
            b_v[col, at] = (gate * (1.0 / (1.0 + jnp.exp(-gate))) * up).astype(BF16)

    def turn(vals, r):
        return vals * turns[0, r:r + 1, :] + pltpu.roll(vals, hd // 2, 1) * turns[1, r:r + 1, :]

    def attend(r):
        length = lens_ref[(row * ntx + col) * sb + r]
        for a in range(ny):
            qs[a * lh:(a + 1) * lh, :] = turn(qy_r[a, pl.ds(r, lh, stride=sb), :], r)
        q = qs[...].astype(BF16)
        k_new = turn(kvs[0, pl.ds(row * sb + r, 1), :], r).astype(BF16).astype(F32)
        v_new = kvs[1, pl.ds(row * sb + r, 1), :].astype(BF16).astype(F32)
        new_out[r:r + 1, :] = k_new
        new_out[sb + r:sb + r + 1, :] = v_new
        k_in[r].wait()
        s_new = jnp.sum(q.astype(F32) * k_new, axis=1, keepdims=True)
        top = jnp.full((heads, hd), -1e30, F32)
        for c in range(ctx // CHUNK):
            s = lax.dot_general(q, kbuf[r, c * CHUNK:(c + 1) * CHUNK, :], (((1,), (1,)), ((), ())), preferred_element_type=F32)
            pos = lax.broadcasted_iota(jnp.int32, (1, CHUNK), 1) + c * CHUNK
            s = jnp.where(pos < length, s, -1e30)
            sbuf[:, c * CHUNK:(c + 1) * CHUNK] = s
            for t in range(CHUNK // hd):
                top = jnp.maximum(top, s[:, t * hd:(t + 1) * hd])
        high = jnp.maximum(jnp.max(top, axis=1, keepdims=True), s_new)
        rate = hd ** -0.5 * LOG2E
        e_new = jnp.exp2((s_new - high) * rate)
        low = jnp.zeros((heads, hd), F32)
        out = e_new.astype(BF16).astype(F32) * v_new
        v_in[r].wait()
        for c in range(ctx // CHUNK):
            e = jnp.exp2((sbuf[:, c * CHUNK:(c + 1) * CHUNK] - high) * rate)
            for t in range(CHUNK // hd):
                low = low + e[:, t * hd:(t + 1) * hd]
            out = out + jnp.dot(e.astype(BF16), vbuf[r, c * CHUNK:(c + 1) * CHUNK, :], preferred_element_type=F32)
        out = out / (jnp.sum(low, axis=1, keepdims=True) + e_new)
        for a in range(ny):
            o32[a, pl.ds(r, lh, stride=sb), :] = out[a * lh:(a + 1) * lh]

    def b_copy(s, t):
        b = held(s, True)
        return remote(b_v.at[b, piece(t)], b_v.at[b, piece(t)], b_ss.at[s, t], b_rs.at[s, t], tx=after)

    def b_in(s, t):
        b = held(s + 1, True)
        return remote(b_v.at[b, piece(t)], b_v.at[b, piece(t)], b_ss.at[s, t], b_rs.at[s, t], tx=after)

    def bp_copy(s, t):
        b = held(s, True)
        return remote(b_v.at[b, piece(t)], b_v.at[b, piece(t)], bp_ss.at[s, t], bp_rs.at[s, t], tx=partner)

    def bp_in(s, t):
        b = held(s, False)
        return remote(b_v.at[b, piece(t)], b_v.at[b, piece(t)], bp_ss.at[s, t], bp_rs.at[s, t], tx=partner)

    ay_cp = [remote(ay_s.at[y_peers[k - 1]], ay_r.at[row], ay_ss.at[k], ay_rs.at[k], ty=y_peers[k - 1]) for k in range(1, ny)]
    ay_in = [remote(ay_s.at[y_froms[k - 1]], ay_r.at[y_froms[k - 1]], ay_ss.at[k], ay_rs.at[k], ty=y_peers[k - 1]) for k in range(1, ny)]
    g_cp = [remote(g_v.at[col], g_v.at[col], g_ss.at[k], g_rs.at[k], tx=x_peers[k - 1]) for k in range(1, nx)]

    def g_from(k, mine):
        return 2 * lax.rem(chip - k + nx, nx) + (core if mine else 1 - core)

    def g_in(k):
        at = g_from(k, True)
        return remote(g_v.at[at], g_v.at[at], g_ss.at[k], g_rs.at[k], tx=x_peers[k - 1])

    def gp_copy(k):
        at = g_from(k, True)
        return remote(g_v.at[at], g_v.at[at], gp_ss.at[k], gp_rs.at[k], tx=partner)

    def gp_in(k):
        at = g_from(k, False)
        return remote(g_v.at[at], g_v.at[at], gp_ss.at[k], gp_rs.at[k], tx=partner)

    def att_out():
        ay_s[...] = o32[...].astype(BF16)
        for c in ay_cp:
            c.start()
        ay_r[row] = ay_s[row]

    def att_rows():
        with scope("ay"):
            for c in ay_in:
                c.wait_recv()
        for a in range(ny):
            part = ay_r[a].astype(F32)
            for n in range(lh):
                g32[n, a * sb:(a + 1) * sb, :] = part[n * sb:(n + 1) * sb, :]
        g_v[col] = g32[...].astype(BF16)
        for c in g_cp:
            c.start()
        gp_copy(0).start()

    def forward(s):
        for t in range(SUBS):
            with scope("b%d%d" % (s, t)):
                b_in(s, t).wait_recv()
            if s < nx - 2:
                b_copy(s + 1, t).start()
            bp_copy(s + 1, t).start()

    def down(n, first=False):
        wd_load(n, 0).wait()
        part = jnp.dot(b_v[held(n // 2, n % 2 == 0)], wd_v[n], preferred_element_type=F32)
        acc[...] = part if first else acc[...] + part

    def from_pair(s):
        with scope("bp%d" % s):
            for t in range(SUBS):
                bp_in(s, t).wait_recv()

    ring(1, 0)
    q_rows()
    for t in range(1, SUBS):
        ring(1, t)
    ring(2, 0)
    ring(2, 1)
    with scope("qy"):
        for c in qy_in:
            c.wait_recv()
    with scope("a0"):
        attend(0)
    ring(2, 2)
    ring(2, 3)
    with scope("a1"):
        attend(1)
    ring(3, 0)
    with scope("a2"):
        attend(2)
    ring(3, 1)
    with scope("a3"):
        attend(3)
    att_out()
    for t in range(2, SUBS):
        ring(3, t)
    for t in range(SUBS):
        b_copy(0, t).start()
        bp_copy(0, t).start()
    down(0, True)
    att_rows()
    forward(0)
    from_pair(0)
    down(1)
    down(2)
    forward(1)
    with scope("g"):
        for k in range(1, nx):
            g_in(k).wait_recv()
            gp_copy(k).start()
    from_pair(1)
    down(3)
    down(4)
    with scope("gp"):
        for k in range(nx):
            gp_in(k).wait_recv()
    wo_load.wait()
    for n in range(0, lh, 2):
        pair = jnp.concatenate([g_v[:, n].reshape(rows, hd), g_v[:, n + 1].reshape(rows, hd)], axis=1)
        acc[...] += jnp.dot(pair, wo_v[n * hd:(n + 2) * hd, :], preferred_element_type=F32)
    forward(2)
    from_pair(2)
    down(5)
    down(6)
    from_pair(3)
    down(7)

    part = lax.dot_general(perm_v[...], acc[...].astype(BF16), (((0,), (0,)), ((), ())), preferred_element_type=F32)
    y_s[...] = part.astype(BF16).reshape(ny, yb, dl)
    y_cp = [remote(y_s.at[y_peers[k - 1]], y_r.at[k], y_ss.at[k], y_rs.at[k], ty=y_peers[k - 1]) for k in range(1, ny)]
    for c in y_cp:
        c.start()
    total = x_v[pl.ds(pl.multiple_of(row * yb, yb), yb), :].astype(F32) + y_s[row].astype(F32)
    with scope("y"):
        for k in range(1, ny):
            y_cp[k - 1].wait_recv()
            total = total + y_r[k].astype(F32)
    yf[row] = total.astype(BF16)
    f_cp = [remote(yf.at[row], yf.at[row], f_ss.at[k], f_rs.at[k], ty=y_peers[k - 1]) for k in range(1, ny)]
    for c in f_cp:
        c.start()
    with scope("f"):
        for k in range(1, ny):
            src = y_froms[k - 1]
            remote(yf.at[src], yf.at[src], f_ss.at[k], f_rs.at[k], ty=y_peers[k - 1]).wait_recv()
    y_out[...] = yf[...].reshape(rows, dl)

    with scope("sends"):
        for c in stat_cp + [qd_cp] + qx_cp + qy_cp + ay_cp + g_cp + y_cp + f_cp:
            c.wait_send()
        for s in range(nx):
            d_copy(s).wait_send()
            gp_copy(s).wait_send()
            for t in range(SUBS):
                bp_copy(s, t).wait_send()
        for s in range(nx - 1):
            for t in range(SUBS):
                r_copy(s, t).wait_send()
                b_copy(s, t).wait_send()


def store_kernel(ny, ntx, lens_ref, y_v, new_v, k_v, v_v, y_h, ko_h, vo_h, patch, y_sem, out_sem):
    first = (lax.axis_index("ty") * ntx + lax.axis_index("tx")) * k_v.shape[0]
    sb, ctx, hd = k_v.shape
    pieces = ctx // PIECE
    y_cp = pltpu.make_async_copy(y_v, y_h, y_sem)
    y_cp.start()

    def write(a, buf, out):
        def sequence(r, carry):
            length = lens_ref[first + r]
            spot = lax.div(length, PIECE)
            at = pl.ds(pl.multiple_of(spot * PIECE, PIECE), PIECE)
            here = lax.broadcasted_iota(jnp.int32, (PIECE, hd), 0) == length - spot * PIECE
            patch[a, r] = jnp.where(here, new_v[pl.ds(a * sb + r, 1), :], buf[r, at, :].astype(F32)).astype(BF16)
            pltpu.make_async_copy(patch.at[a, r], out.at[r, at], out_sem.at[a, r, 0]).start()

            def other(c, inner):
                c = c + jnp.where(c >= spot, 1, 0)
                rest = pl.ds(pl.multiple_of(c * PIECE, PIECE), PIECE)
                pltpu.make_async_copy(buf.at[r, rest], out.at[r, rest], out_sem.at[a, r, 1]).start()
                return inner

            lax.fori_loop(0, pieces - 1, other, 0)
            return carry

        lax.fori_loop(0, sb, sequence, 0)

    def finish(a, buf, out):
        for r in range(sb):
            pltpu.make_async_copy(patch.at[a, r], out.at[r, pl.ds(0, PIECE)], out_sem.at[a, r, 0]).wait()
            rest = pl.ds(0, ctx - PIECE)
            pltpu.make_async_copy(buf.at[r, rest], out.at[r, rest], out_sem.at[a, r, 1]).wait()

    write(0, k_v, ko_h)
    write(1, v_v, vo_h)
    y_cp.wait()
    finish(0, k_v, ko_h)
    finish(1, v_v, vo_h)


def solution(mesh):
    ny = mesh.shape["ty"]
    ntx = mesh.shape["tx"]
    nx = ntx // 2
    cache_spec = P(("dp", "ty", "tx"), None, None)
    vspec = pl.BlockSpec(memory_space=VMEM)
    hspec = pl.BlockSpec(memory_space=pltpu.HBM)
    sspec = pl.BlockSpec(memory_space=pltpu.SMEM)

    def layer_shard(x_blk, lens_part, k_blk, v_blk, gamma_blk, w_query, w_key, w_value, w_gate, w_up, w_out, w_down):
        rows, dl = x_blk.shape
        sb, ctx, hd = k_blk.shape
        qn = w_query.shape[1]
        lh = qn // hd
        qw = qn + 2 * hd
        fb = w_gate.shape[1] // ntx
        rb = rows // ntx
        yb = rows // ny

        natural = np.arange(rows)
        order = np.reshape(np.transpose(np.reshape(natural, (ny, ntx, sb)), (1, 0, 2)), (rows,))
        perm = jnp.asarray(order[:, None] == natural[None, :], dtype=BF16)
        freqs = np.power(ROPE_BASE, -(np.arange(hd // 2, dtype=np.float32) * 2.0) / hd).astype(np.float32)
        freqs = jnp.asarray(np.tile(np.concatenate([freqs, freqs])[None, :], (8, 1)))

        y_vm, new_rows, k_vm, v_vm = pl.pallas_call(
            functools.partial(step_kernel, ny, nx, dl * ntx),
            out_shape=(
                pltpu.VMEM((rows, dl), BF16),
                pltpu.VMEM((2 * sb, hd), F32),
                pltpu.VMEM(k_blk.shape, BF16),
                pltpu.VMEM(v_blk.shape, BF16),
            ),
            in_specs=[sspec] + [hspec] * 13,
            out_specs=(vspec,) * 4,
            scratch_shapes=[
                VMEM((rows, dl), BF16), VMEM((dl,), F32), VMEM((rows, rows), BF16), VMEM((8, hd), F32),
                VMEM((dl, qw), BF16), VMEM((ntx, dl, 2 * fb), BF16), VMEM((qn, dl), BF16), VMEM((ntx, fb, dl), BF16),
                VMEM((rows, dl), BF16), VMEM((8, rows), F32), VMEM((ntx, 8, rows), F32),
                VMEM((ntx, rb, qw), F32), VMEM((nx, rb, qw), BF16), VMEM((nx, rb, qw), BF16),
                VMEM((nx, rb, qw), BF16), VMEM((nx, rb, qw), BF16), VMEM((rb, qw), F32), VMEM((2, rb, hd), F32),
                VMEM((ny, sb * lh, hd), F32), VMEM((ny, sb * lh, hd), F32),
                VMEM((nx, rows, 2 * fb), F32), VMEM((nx, rows, 2 * fb), BF16), VMEM((nx, rows, 2 * fb), BF16),
                VMEM((nx - 1, rows, 2 * fb), BF16), VMEM((nx - 1, rows, 2 * fb), BF16),
                VMEM((2, 8, hd), F32), VMEM((ny * lh, hd), F32), VMEM((ny * lh, ctx), F32), VMEM((ny, sb * lh, hd), F32),
                VMEM((ny, sb * lh, hd), BF16), VMEM((ny, sb * lh, hd), BF16), VMEM((lh, rb, hd), F32),
                VMEM((ntx, lh, rb, hd), BF16), VMEM((ntx, rows, fb), BF16), VMEM((rows, dl), F32),
                VMEM((ny, yb, dl), BF16), VMEM((ny, yb, dl), BF16), VMEM((ny, yb, dl), BF16),
                DMA((4,)), DMA((3,)), DMA((ntx, 2)), DMA((2, sb)), DMA, DMA((ntx,)),
                DMA((ntx,)), DMA((ntx,)), DMA, DMA, DMA((nx,)), DMA((nx,)), DMA((ny,)), DMA((ny,)),
                DMA((nx,)), DMA((nx,)), DMA((nx - 1, SUBS)), DMA((nx - 1, SUBS)),
                DMA((ny,)), DMA((ny,)), DMA((nx,)), DMA((nx,)), DMA((nx,)), DMA((nx,)),
                DMA((nx - 1, SUBS)), DMA((nx - 1, SUBS)), DMA((nx, SUBS)), DMA((nx, SUBS)), DMA((ny,)), DMA((ny,)), DMA((ny,)), DMA((ny,)),
            ],
            compiler_params=pltpu.CompilerParams(collective_id=0, has_side_effects=True, vmem_limit_bytes=52 * 1024 * 1024),
            name="step",
        )(lens_part, x_blk, gamma_blk, perm, freqs, w_query, w_key, w_value, w_gate, w_up, k_blk, v_blk, w_out, w_down)

        return pl.pallas_call(
            functools.partial(store_kernel, ny, ntx),
            out_shape=(
                jax.ShapeDtypeStruct((rows, dl), BF16),
                jax.ShapeDtypeStruct(k_blk.shape, BF16),
                jax.ShapeDtypeStruct(v_blk.shape, BF16),
            ),
            in_specs=[sspec] + [vspec] * 4,
            out_specs=(hspec,) * 3,
            scratch_shapes=[VMEM((2, sb, PIECE, hd), BF16), DMA, DMA((2, sb, 2))],
            compiler_params=pltpu.CompilerParams(vmem_limit_bytes=4 * 1024 * 1024),
            name="store",
        )(lens_part, y_vm, new_rows, k_vm, v_vm)

    in_specs = (P("dp", "tx"), P("dp"), cache_spec, cache_spec, P("tx"), P("tx", "ty"), P("tx", None), P("tx", None), P("tx", "ty"), P("tx", "ty"), P("ty", "tx"), P("ty", "tx"))
    out_specs = (P("dp", "tx"), cache_spec, cache_spec)
    return jax.shard_map(layer_shard, mesh=mesh, in_specs=in_specs, out_specs=out_specs, check_vma=False)
```

```python
import functools

import jax
import jax.numpy as jnp
import numpy as np
from jax import lax
from jax.experimental import pallas as pl
from jax.experimental.pallas import tpu as pltpu
from jax.sharding import PartitionSpec as P

EPSILON = 1e-6
ROPE_BASE = 10000.0
LOG2E = 1.4426950408889634
MESH = pl.DeviceIdType.MESH
F32 = jnp.float32
BF16 = jnp.bfloat16
VMEM = pltpu.VMEM
DMA = pltpu.SemaphoreType.DMA
SUBS = 4
CHUNK = 1024
PIECE = 512
scope = jax.named_scope


def remote(src, dst, send_sem, recv_sem, tx=None, ty=None):
    device = {}
    if tx is not None:
        device["tx"] = tx
    if ty is not None:
        device["ty"] = ty
    return pltpu.make_async_remote_copy(src_ref=src, dst_ref=dst, send_sem=send_sem, recv_sem=recv_sem, device_id=device, device_id_type=MESH)


def step_kernel(ny, nx, d_model, lens_ref, x_h, gamma_h, perm_h, freq_h, wq_h, wk_h, wv_h, wg_h, wu_h, k_h, v_h, wo_h, wd_h,
                y_out, new_out, kbuf, vbuf,
                x_v, gamma_v, perm_v, freq_v, wq_v, wb_v, wo_v, wd_v, h_v, stat_s, stat_r,
                qp, qd_s, qd_r, qx_s, qx_r, qsum, kvs, qy_s, qy_r, own, d_s, d_r, r_s, r_r,
                turns, qs, sbuf, o32, ay_s, ay_r, g32, g_v, b_v, acc, y_s, y_r, yf,
                in_sem, wq_sem, wb_sem, kv_sem, wo_sem, wd_sem, stat_ss, stat_rs, qd_ss, qd_rs, qx_ss, qx_rs, qy_ss, qy_rs,
                d_ss, d_rs, r_ss, r_rs, ay_ss, ay_rs, g_ss, g_rs, gp_ss, gp_rs, b_ss, b_rs, bp_ss, bp_rs, y_ss, y_rs, f_ss, f_rs):
    row = lax.axis_index("ty")
    col = lax.axis_index("tx")
    chip = lax.div(col, 2)
    core = lax.rem(col, 2)
    step = 1 - 2 * core
    ntx = 2 * nx
    rows, dl = x_h.shape
    rb = rows // ntx
    sb = rb // ny
    qn = wq_h.shape[1]
    hd = wk_h.shape[1]
    qw = qn + 2 * hd
    lh = qn // hd
    heads = ny * lh
    ctx = k_h.shape[1]
    fb = wb_v.shape[2] // 2
    sub = rows // SUBS
    yb = rows // ny
    partner = lax.rem(col + 1, 2) + 2 * chip
    after = 2 * lax.rem(chip + step + nx, nx) + core
    tx_peers = [lax.rem(col + k, ntx) for k in range(1, ntx)]
    x_peers = [2 * lax.rem(chip + k, nx) + core for k in range(1, nx)]
    y_peers = [lax.rem(row + k, ny) for k in range(1, ny)]
    y_froms = [lax.rem(row - k + ny, ny) for k in range(1, ny)]

    barrier = pltpu.get_barrier_semaphore()
    for peer in tx_peers:
        pl.semaphore_signal(barrier, inc=1, device_id={"tx": peer}, device_id_type=MESH)
    for peer in y_peers:
        pl.semaphore_signal(barrier, inc=1, device_id={"ty": peer}, device_id_type=MESH)

    def piece(t):
        return pl.ds(pl.multiple_of(t * sub, sub), sub)

    def block_of(s, mine):
        sign = step if mine else -step
        at = lax.rem(chip - (s + 1) * sign + 2 * nx, nx)
        return 2 * at + (core if mine else 1 - core)

    def held(s, mine):
        sign = step if mine else -step
        return 2 * lax.rem(chip - s * sign + 2 * nx, nx) + (core if mine else 1 - core)

    def block_loads(n, b):
        at = pl.ds(pl.multiple_of(b * fb, fb), fb)
        return [
            pltpu.make_async_copy(wg_h.at[:, at], wb_v.at[n, :, pl.ds(0, fb)], wb_sem.at[n, 0]),
            pltpu.make_async_copy(wu_h.at[:, at], wb_v.at[n, :, pl.ds(fb, fb)], wb_sem.at[n, 1]),
        ]

    def wd_load(n, b):
        at = pl.ds(pl.multiple_of(b * fb, fb), fb)
        return pltpu.make_async_copy(wd_h.at[at, :], wd_v.at[n], wd_sem.at[n])

    first_loads = [
        pltpu.make_async_copy(x_h, x_v, in_sem.at[0]),
        pltpu.make_async_copy(perm_h, perm_v, in_sem.at[1]),
        pltpu.make_async_copy(gamma_h, gamma_v, in_sem.at[2]),
        pltpu.make_async_copy(freq_h, freq_v, in_sem.at[3]),
    ]
    q_loads = [
        pltpu.make_async_copy(wq_h, wq_v.at[:, pl.ds(0, qn)], wq_sem.at[0]),
        pltpu.make_async_copy(wk_h, wq_v.at[:, pl.ds(qn, hd)], wq_sem.at[1]),
        pltpu.make_async_copy(wv_h, wq_v.at[:, pl.ds(qn + hd, hd)], wq_sem.at[2]),
    ]
    k_in = [pltpu.make_async_copy(k_h.at[r], kbuf.at[r], kv_sem.at[0, r]) for r in range(sb)]
    v_in = [pltpu.make_async_copy(v_h.at[r], vbuf.at[r], kv_sem.at[1, r]) for r in range(sb)]
    wo_load = pltpu.make_async_copy(wo_h, wo_v, wo_sem)
    for c in first_loads:
        c.start()
    for c in first_loads:
        c.wait()
    for c in q_loads:
        c.start()
    for n in range(ntx):
        for c in block_loads(n, block_of(n // 2, n % 2 == 1)):
            c.start()

    xp = jnp.dot(perm_v[...], x_v[...], preferred_element_type=F32)
    s1 = jnp.sum(xp, axis=1, keepdims=True)
    s2 = jnp.sum(xp * xp, axis=1, keepdims=True)
    lane = lax.broadcasted_iota(jnp.int32, (rows, rows), 1)
    both = jnp.where(lane == 0, s1, jnp.where(lane == 1, s2, 0.0))
    stat_s[...] = jnp.transpose(both)[:8]

    at_row = lax.broadcasted_iota(jnp.int32, (8, hd), 0)
    places = jnp.zeros((8, hd), F32)
    for r in range(sb):
        places = jnp.where(at_row == r, lens_ref[(row * ntx + col) * sb + r].astype(F32), places)
    angles = places * freq_v[...]
    turns[0] = jnp.cos(angles)
    low_half = lax.broadcasted_iota(jnp.int32, (8, hd), 1) < hd // 2
    sines = jnp.sin(angles)
    turns[1] = jnp.where(low_half, -sines, sines)

    with scope("greet"):
        pl.semaphore_wait(barrier, ntx - 1 + ny - 1)

    stat_cp = [remote(stat_s, stat_r.at[k], stat_ss.at[k], stat_rs.at[k], tx=tx_peers[k - 1]) for k in range(1, ntx)]
    for c in stat_cp:
        c.start()
    total = stat_s[...]
    with scope("stat"):
        for k, c in enumerate(stat_cp):
            c.wait_recv()
            total = total + stat_r[k + 1]
    square = jnp.transpose(jnp.concatenate([total, jnp.zeros((rows - 8, rows), F32)], axis=0))
    mean = square[:, 0:1] / d_model
    var = square[:, 1:2] / d_model - mean * mean
    h_v[...] = ((xp - mean) * lax.rsqrt(var + EPSILON) * gamma_v[...].reshape(1, dl)).astype(BF16)

    for c in q_loads:
        c.wait()
    qp[...] = jnp.dot(h_v[...], wq_v[...], preferred_element_type=F32).reshape(ntx, rb, qw)
    for n in range(nx):
        qd_s[n] = qp[2 * n + 1 - core].astype(BF16)
    qd_cp = remote(qd_s, qd_r, qd_ss, qd_rs, tx=partner)
    qd_cp.start()
    qx_cp = [remote(qx_s.at[k], qx_r.at[k], qx_ss.at[k], qx_rs.at[k], tx=x_peers[k - 1]) for k in range(1, nx)]
    qy_cp = [remote(qy_s.at[y_peers[k - 1]], qy_r.at[row], qy_ss.at[k], qy_rs.at[k], ty=y_peers[k - 1]) for k in range(1, ny)]
    qy_in = [remote(qy_s.at[y_froms[k - 1]], qy_r.at[y_froms[k - 1]], qy_ss.at[k], qy_rs.at[k], ty=y_peers[k - 1]) for k in range(1, ny)]

    def q_pair():
        with scope("qd"):
            qd_cp.wait_recv()
        for k in range(1, nx):
            at = lax.rem(chip + k, nx)
            qx_s[k] = (qp[2 * at + core] + qd_r[at].astype(F32)).astype(BF16)
            qx_cp[k - 1].start()

    def q_rows():
        mine = qp[2 * chip + core] + qd_r[chip].astype(F32)
        with scope("qx"):
            for k in range(1, nx):
                qx_cp[k - 1].wait_recv()
                mine = mine + qx_r[k].astype(F32)
        qsum[...] = mine
        kvs[0] = mine[:, qn:qn + hd]
        kvs[1] = mine[:, qn + hd:]
        for a in range(ny):
            for n in range(lh):
                qy_s[a, n * sb:(n + 1) * sb, :] = qsum[a * sb:(a + 1) * sb, n * hd:(n + 1) * hd]
        for c in qy_cp:
            c.start()
        qy_r[row] = qy_s[row]

    def d_copy(s):
        return remote(d_s.at[s], d_r.at[s], d_ss.at[s], d_rs.at[s], tx=partner)

    def r_copy(s, t):
        return remote(r_s.at[s, piece(t)], r_r.at[s, piece(t)], r_ss.at[s, t], r_rs.at[s, t], tx=after)

    def product(s, carry):
        for c in block_loads(2 * s, 0):
            c.wait()
        d_s[s] = jnp.dot(h_v[...], wb_v[2 * s], preferred_element_type=F32).astype(BF16)
        d_copy(s).start()

        @pl.when(s == 0)
        def _():
            q_pair()

        for c in block_loads(2 * s + 1, 0):
            c.wait()
        own[s] = jnp.dot(h_v[...], wb_v[2 * s + 1], preferred_element_type=F32)

        @pl.when(s == 0)
        def _():
            with scope("d0"):
                d_copy(0).wait_recv()
            for t in range(SUBS):
                at = piece(t)
                r_s[0, at] = (own[0, at] + d_r[0, at].astype(F32)).astype(BF16)
                r_copy(0, t).start()

        return carry

    for c in k_in + v_in:
        c.start()
    with scope("products"):
        lax.fori_loop(0, nx, product, 0)
    for n in range(ntx):
        wd_load(n, held(n // 2, n % 2 == 0)).start()
    wo_load.start()

    def ring(s, t):
        at = piece(t)
        if t == 0:
            with scope("d%d" % s):
                d_copy(s).wait_recv()
        part = own[s, at] + d_r[s, at].astype(F32)
        with scope("r%d%d" % (s, t)):
            r_copy(s - 1, t).wait_recv()
        part = part + r_r[s - 1, at].astype(F32)
        if s < nx - 1:
            r_s[s, at] = part.astype(BF16)
            r_copy(s, t).start()
        else:
            gate = part[:, :fb].astype(BF16).astype(F32)
            up = part[:, fb:].astype(BF16).astype(F32)
            b_v[col, at] = (gate * (1.0 / (1.0 + jnp.exp(-gate))) * up).astype(BF16)

    def turn(vals, r):
        return vals * turns[0, r:r + 1, :] + pltpu.roll(vals, hd // 2, 1) * turns[1, r:r + 1, :]

    def attend(r):
        length = lens_ref[(row * ntx + col) * sb + r]
        for a in range(ny):
            qs[a * lh:(a + 1) * lh, :] = turn(qy_r[a, pl.ds(r, lh, stride=sb), :], r)
        q = qs[...].astype(BF16)
        k_new = turn(kvs[0, pl.ds(row * sb + r, 1), :], r).astype(BF16).astype(F32)
        v_new = kvs[1, pl.ds(row * sb + r, 1), :].astype(BF16).astype(F32)
        new_out[r:r + 1, :] = k_new
        new_out[sb + r:sb + r + 1, :] = v_new
        k_in[r].wait()
        s_new = jnp.sum(q.astype(F32) * k_new, axis=1, keepdims=True)
        top = jnp.full((heads, hd), -1e30, F32)
        for c in range(ctx // CHUNK):
            s = lax.dot_general(q, kbuf[r, c * CHUNK:(c + 1) * CHUNK, :], (((1,), (1,)), ((), ())), preferred_element_type=F32)
            pos = lax.broadcasted_iota(jnp.int32, (1, CHUNK), 1) + c * CHUNK
            s = jnp.where(pos < length, s, -1e30)
            sbuf[:, c * CHUNK:(c + 1) * CHUNK] = s
            for t in range(CHUNK // hd):
                top = jnp.maximum(top, s[:, t * hd:(t + 1) * hd])
        high = jnp.maximum(jnp.max(top, axis=1, keepdims=True), s_new)
        rate = hd ** -0.5 * LOG2E
        e_new = jnp.exp2((s_new - high) * rate)
        low = jnp.zeros((heads, hd), F32)
        out = e_new.astype(BF16).astype(F32) * v_new
        v_in[r].wait()
        for c in range(ctx // CHUNK):
            e = jnp.exp2((sbuf[:, c * CHUNK:(c + 1) * CHUNK] - high) * rate)
            for t in range(CHUNK // hd):
                low = low + e[:, t * hd:(t + 1) * hd]
            out = out + jnp.dot(e.astype(BF16), vbuf[r, c * CHUNK:(c + 1) * CHUNK, :], preferred_element_type=F32)
        out = out / (jnp.sum(low, axis=1, keepdims=True) + e_new)
        for a in range(ny):
            o32[a, pl.ds(r, lh, stride=sb), :] = out[a * lh:(a + 1) * lh]

    def b_copy(s, t):
        b = held(s, True)
        return remote(b_v.at[b, piece(t)], b_v.at[b, piece(t)], b_ss.at[s, t], b_rs.at[s, t], tx=after)

    def b_in(s, t):
        b = held(s + 1, True)
        return remote(b_v.at[b, piece(t)], b_v.at[b, piece(t)], b_ss.at[s, t], b_rs.at[s, t], tx=after)

    def bp_copy(s, t):
        b = held(s, True)
        return remote(b_v.at[b, piece(t)], b_v.at[b, piece(t)], bp_ss.at[s, t], bp_rs.at[s, t], tx=partner)

    def bp_in(s, t):
        b = held(s, False)
        return remote(b_v.at[b, piece(t)], b_v.at[b, piece(t)], bp_ss.at[s, t], bp_rs.at[s, t], tx=partner)

    ay_cp = [remote(ay_s.at[y_peers[k - 1]], ay_r.at[row], ay_ss.at[k], ay_rs.at[k], ty=y_peers[k - 1]) for k in range(1, ny)]
    ay_in = [remote(ay_s.at[y_froms[k - 1]], ay_r.at[y_froms[k - 1]], ay_ss.at[k], ay_rs.at[k], ty=y_peers[k - 1]) for k in range(1, ny)]
    g_cp = [remote(g_v.at[col], g_v.at[col], g_ss.at[k], g_rs.at[k], tx=x_peers[k - 1]) for k in range(1, nx)]

    def g_from(k, mine):
        return 2 * lax.rem(chip - k + nx, nx) + (core if mine else 1 - core)

    def g_in(k):
        at = g_from(k, True)
        return remote(g_v.at[at], g_v.at[at], g_ss.at[k], g_rs.at[k], tx=x_peers[k - 1])

    def gp_copy(k):
        at = g_from(k, True)
        return remote(g_v.at[at], g_v.at[at], gp_ss.at[k], gp_rs.at[k], tx=partner)

    def gp_in(k):
        at = g_from(k, False)
        return remote(g_v.at[at], g_v.at[at], gp_ss.at[k], gp_rs.at[k], tx=partner)

    def att_out():
        ay_s[...] = o32[...].astype(BF16)
        for c in ay_cp:
            c.start()
        ay_r[row] = ay_s[row]

    def att_rows():
        with scope("ay"):
            for c in ay_in:
                c.wait_recv()
        for a in range(ny):
            part = ay_r[a].astype(F32)
            for n in range(lh):
                g32[n, a * sb:(a + 1) * sb, :] = part[n * sb:(n + 1) * sb, :]
        g_v[col] = g32[...].astype(BF16)
        for c in g_cp:
            c.start()
        gp_copy(0).start()

    def forward(s):
        for t in range(SUBS):
            with scope("b%d%d" % (s, t)):
                b_in(s, t).wait_recv()
            if s < nx - 2:
                b_copy(s + 1, t).start()
            bp_copy(s + 1, t).start()

    def down(n, first=False):
        wd_load(n, 0).wait()
        part = jnp.dot(b_v[held(n // 2, n % 2 == 0)], wd_v[n], preferred_element_type=F32)
        acc[...] = part if first else acc[...] + part

    def from_pair(s):
        with scope("bp%d" % s):
            for t in range(SUBS):
                bp_in(s, t).wait_recv()

    ring(1, 0)
    q_rows()
    for t in range(1, SUBS):
        ring(1, t)
    ring(2, 0)
    ring(2, 1)
    with scope("qy"):
        for c in qy_in:
            c.wait_recv()
    with scope("a0"):
        attend(0)
    ring(2, 2)
    ring(2, 3)
    with scope("a1"):
        attend(1)
    ring(3, 0)
    with scope("a2"):
        attend(2)
    ring(3, 1)
    with scope("a3"):
        attend(3)
    att_out()
    for t in range(2, SUBS):
        ring(3, t)
    for t in range(SUBS):
        b_copy(0, t).start()
        bp_copy(0, t).start()
    down(0, True)
    forward(0)
    att_rows()
    from_pair(0)
    down(1)
    down(2)
    forward(1)
    with scope("g"):
        for k in range(1, nx):
            g_in(k).wait_recv()
            gp_copy(k).start()
    from_pair(1)
    down(3)
    down(4)
    with scope("gp"):
        for k in range(nx):
            gp_in(k).wait_recv()
    wo_load.wait()
    for n in range(0, lh, 2):
        pair = jnp.concatenate([g_v[:, n].reshape(rows, hd), g_v[:, n + 1].reshape(rows, hd)], axis=1)
        acc[...] += jnp.dot(pair, wo_v[n * hd:(n + 2) * hd, :], preferred_element_type=F32)
    forward(2)
    from_pair(2)
    down(5)
    down(6)
    from_pair(3)
    down(7)

    part = lax.dot_general(perm_v[...], acc[...].astype(BF16), (((0,), (0,)), ((), ())), preferred_element_type=F32)
    y_s[...] = part.astype(BF16).reshape(ny, yb, dl)
    y_cp = [remote(y_s.at[y_peers[k - 1]], y_r.at[k], y_ss.at[k], y_rs.at[k], ty=y_peers[k - 1]) for k in range(1, ny)]
    for c in y_cp:
        c.start()
    total = x_v[pl.ds(pl.multiple_of(row * yb, yb), yb), :].astype(F32) + y_s[row].astype(F32)
    with scope("y"):
        for k in range(1, ny):
            y_cp[k - 1].wait_recv()
            total = total + y_r[k].astype(F32)
    yf[row] = total.astype(BF16)
    f_cp = [remote(yf.at[row], yf.at[row], f_ss.at[k], f_rs.at[k], ty=y_peers[k - 1]) for k in range(1, ny)]
    for c in f_cp:
        c.start()
    with scope("f"):
        for k in range(1, ny):
            src = y_froms[k - 1]
            remote(yf.at[src], yf.at[src], f_ss.at[k], f_rs.at[k], ty=y_peers[k - 1]).wait_recv()
    y_out[...] = yf[...].reshape(rows, dl)

    with scope("sends"):
        for c in stat_cp + [qd_cp] + qx_cp + qy_cp + ay_cp + g_cp + y_cp + f_cp:
            c.wait_send()
        for s in range(nx):
            d_copy(s).wait_send()
            gp_copy(s).wait_send()
            for t in range(SUBS):
                bp_copy(s, t).wait_send()
        for s in range(nx - 1):
            for t in range(SUBS):
                r_copy(s, t).wait_send()
                b_copy(s, t).wait_send()


def store_kernel(ny, ntx, lens_ref, y_v, new_v, k_v, v_v, y_h, ko_h, vo_h, patch, y_sem, out_sem):
    first = (lax.axis_index("ty") * ntx + lax.axis_index("tx")) * k_v.shape[0]
    sb, ctx, hd = k_v.shape
    pieces = ctx // PIECE
    y_cp = pltpu.make_async_copy(y_v, y_h, y_sem)
    y_cp.start()

    def write(a, buf, out):
        def sequence(r, carry):
            length = lens_ref[first + r]
            spot = lax.div(length, PIECE)

            def other(c, inner):
                c = c + jnp.where(c >= spot, 1, 0)
                rest = pl.ds(pl.multiple_of(c * PIECE, PIECE), PIECE)
                pltpu.make_async_copy(buf.at[r, rest], out.at[r, rest], out_sem.at[a, r, 1]).start()
                return inner

            lax.fori_loop(0, pieces - 1, other, 0)
            at = pl.ds(pl.multiple_of(spot * PIECE, PIECE), PIECE)
            here = lax.broadcasted_iota(jnp.int32, (PIECE, hd), 0) == length - spot * PIECE
            patch[a, r] = jnp.where(here, new_v[pl.ds(a * sb + r, 1), :], buf[r, at, :].astype(F32)).astype(BF16)
            pltpu.make_async_copy(patch.at[a, r], out.at[r, at], out_sem.at[a, r, 0]).start()
            return carry

        lax.fori_loop(0, sb, sequence, 0)

    def finish(a, buf, out):
        for r in range(sb):
            pltpu.make_async_copy(patch.at[a, r], out.at[r, pl.ds(0, PIECE)], out_sem.at[a, r, 0]).wait()
            rest = pl.ds(0, ctx - PIECE)
            pltpu.make_async_copy(buf.at[r, rest], out.at[r, rest], out_sem.at[a, r, 1]).wait()

    write(0, k_v, ko_h)
    write(1, v_v, vo_h)
    y_cp.wait()
    finish(0, k_v, ko_h)
    finish(1, v_v, vo_h)


def solution(mesh):
    ny = mesh.shape["ty"]
    ntx = mesh.shape["tx"]
    nx = ntx // 2
    cache_spec = P(("dp", "ty", "tx"), None, None)
    vspec = pl.BlockSpec(memory_space=VMEM)
    hspec = pl.BlockSpec(memory_space=pltpu.HBM)
    sspec = pl.BlockSpec(memory_space=pltpu.SMEM)

    def layer_shard(x_blk, lens_part, k_blk, v_blk, gamma_blk, w_query, w_key, w_value, w_gate, w_up, w_out, w_down):
        rows, dl = x_blk.shape
        sb, ctx, hd = k_blk.shape
        qn = w_query.shape[1]
        lh = qn // hd
        qw = qn + 2 * hd
        fb = w_gate.shape[1] // ntx
        rb = rows // ntx
        yb = rows // ny

        natural = np.arange(rows)
        order = np.reshape(np.transpose(np.reshape(natural, (ny, ntx, sb)), (1, 0, 2)), (rows,))
        perm = jnp.asarray(order[:, None] == natural[None, :], dtype=BF16)
        freqs = np.power(ROPE_BASE, -(np.arange(hd // 2, dtype=np.float32) * 2.0) / hd).astype(np.float32)
        freqs = jnp.asarray(np.tile(np.concatenate([freqs, freqs])[None, :], (8, 1)))

        y_vm, new_rows, k_vm, v_vm = pl.pallas_call(
            functools.partial(step_kernel, ny, nx, dl * ntx),
            out_shape=(
                pltpu.VMEM((rows, dl), BF16),
                pltpu.VMEM((2 * sb, hd), F32),
                pltpu.VMEM(k_blk.shape, BF16),
                pltpu.VMEM(v_blk.shape, BF16),
            ),
            in_specs=[sspec] + [hspec] * 13,
            out_specs=(vspec,) * 4,
            scratch_shapes=[
                VMEM((rows, dl), BF16), VMEM((dl,), F32), VMEM((rows, rows), BF16), VMEM((8, hd), F32),
                VMEM((dl, qw), BF16), VMEM((ntx, dl, 2 * fb), BF16), VMEM((qn, dl), BF16), VMEM((ntx, fb, dl), BF16),
                VMEM((rows, dl), BF16), VMEM((8, rows), F32), VMEM((ntx, 8, rows), F32),
                VMEM((ntx, rb, qw), F32), VMEM((nx, rb, qw), BF16), VMEM((nx, rb, qw), BF16),
                VMEM((nx, rb, qw), BF16), VMEM((nx, rb, qw), BF16), VMEM((rb, qw), F32), VMEM((2, rb, hd), F32),
                VMEM((ny, sb * lh, hd), F32), VMEM((ny, sb * lh, hd), F32),
                VMEM((nx, rows, 2 * fb), F32), VMEM((nx, rows, 2 * fb), BF16), VMEM((nx, rows, 2 * fb), BF16),
                VMEM((nx - 1, rows, 2 * fb), BF16), VMEM((nx - 1, rows, 2 * fb), BF16),
                VMEM((2, 8, hd), F32), VMEM((ny * lh, hd), F32), VMEM((ny * lh, ctx), F32), VMEM((ny, sb * lh, hd), F32),
                VMEM((ny, sb * lh, hd), BF16), VMEM((ny, sb * lh, hd), BF16), VMEM((lh, rb, hd), F32),
                VMEM((ntx, lh, rb, hd), BF16), VMEM((ntx, rows, fb), BF16), VMEM((rows, dl), F32),
                VMEM((ny, yb, dl), BF16), VMEM((ny, yb, dl), BF16), VMEM((ny, yb, dl), BF16),
                DMA((4,)), DMA((3,)), DMA((ntx, 2)), DMA((2, sb)), DMA, DMA((ntx,)),
                DMA((ntx,)), DMA((ntx,)), DMA, DMA, DMA((nx,)), DMA((nx,)), DMA((ny,)), DMA((ny,)),
                DMA((nx,)), DMA((nx,)), DMA((nx - 1, SUBS)), DMA((nx - 1, SUBS)),
                DMA((ny,)), DMA((ny,)), DMA((nx,)), DMA((nx,)), DMA((nx,)), DMA((nx,)),
                DMA((nx - 1, SUBS)), DMA((nx - 1, SUBS)), DMA((nx, SUBS)), DMA((nx, SUBS)), DMA((ny,)), DMA((ny,)), DMA((ny,)), DMA((ny,)),
            ],
            compiler_params=pltpu.CompilerParams(collective_id=0, has_side_effects=True, vmem_limit_bytes=52 * 1024 * 1024),
            name="step",
        )(lens_part, x_blk, gamma_blk, perm, freqs, w_query, w_key, w_value, w_gate, w_up, k_blk, v_blk, w_out, w_down)

        return pl.pallas_call(
            functools.partial(store_kernel, ny, ntx),
            out_shape=(
                jax.ShapeDtypeStruct((rows, dl), BF16),
                jax.ShapeDtypeStruct(k_blk.shape, BF16),
                jax.ShapeDtypeStruct(v_blk.shape, BF16),
            ),
            in_specs=[sspec] + [vspec] * 4,
            out_specs=(hspec,) * 3,
            scratch_shapes=[VMEM((2, sb, PIECE, hd), BF16), DMA, DMA((2, sb, 2))],
            compiler_params=pltpu.CompilerParams(vmem_limit_bytes=4 * 1024 * 1024),
            name="store",
        )(lens_part, y_vm, new_rows, k_vm, v_vm)

    in_specs = (P("dp", "tx"), P("dp"), cache_spec, cache_spec, P("tx"), P("tx", "ty"), P("tx", None), P("tx", None), P("tx", "ty"), P("tx", "ty"), P("ty", "tx"), P("ty", "tx"))
    out_specs = (P("dp", "tx"), cache_spec, cache_spec)
    return jax.shard_map(layer_shard, mesh=mesh, in_specs=in_specs, out_specs=out_specs, check_vma=False)
```

```python
import functools

import jax
import jax.numpy as jnp
import numpy as np
from jax import lax
from jax.experimental import pallas as pl
from jax.experimental.pallas import tpu as pltpu
from jax.sharding import PartitionSpec as P

EPSILON = 1e-6
ROPE_BASE = 10000.0
LOG2E = 1.4426950408889634
MESH = pl.DeviceIdType.MESH
F32 = jnp.float32
BF16 = jnp.bfloat16
VMEM = pltpu.VMEM
DMA = pltpu.SemaphoreType.DMA
SUBS = 4
CHUNK = 1024
PIECE = 512
scope = jax.named_scope


def remote(src, dst, send_sem, recv_sem, tx=None, ty=None):
    device = {}
    if tx is not None:
        device["tx"] = tx
    if ty is not None:
        device["ty"] = ty
    return pltpu.make_async_remote_copy(src_ref=src, dst_ref=dst, send_sem=send_sem, recv_sem=recv_sem, device_id=device, device_id_type=MESH)


def step_kernel(ny, nx, d_model, lens_ref, x_h, gamma_h, perm_h, freq_h, wq_h, wk_h, wv_h, wg_h, wu_h, k_h, v_h, wo_h, wd_h,
                y_out, new_out, kbuf, vbuf,
                x_v, gamma_v, perm_v, freq_v, wq_v, wb_v, wo_v, wd_v, h_v, stat_s, stat_r, gq_s, gq_r, gb_s, gb_r, norm,
                qp, qd_s, qd_r, qx_s, qx_r, qsum, kvs, qy_s, qy_r, own, d_s, d_r, r_s, r_r,
                turns, qs, sbuf, o32, ay_s, ay_r, g32, g_v, b_v, acc, y_s, y_r, yf,
                in_sem, wq_sem, wb_sem, kv_sem, wo_sem, wd_sem, stat_ss, stat_rs, gq_ss, gq_rs, gb_ss, gb_rs, qd_ss, qd_rs, qx_ss, qx_rs, qy_ss, qy_rs,
                d_ss, d_rs, r_ss, r_rs, ay_ss, ay_rs, g_ss, g_rs, gp_ss, gp_rs, b_ss, b_rs, bp_ss, bp_rs, y_ss, y_rs, f_ss, f_rs):
    row = lax.axis_index("ty")
    col = lax.axis_index("tx")
    chip = lax.div(col, 2)
    core = lax.rem(col, 2)
    step = 1 - 2 * core
    ntx = 2 * nx
    rows, dl = x_h.shape
    rb = rows // ntx
    sb = rb // ny
    qn = wq_h.shape[1]
    hd = wk_h.shape[1]
    qw = qn + 2 * hd
    lh = qn // hd
    heads = ny * lh
    ctx = k_h.shape[1]
    fb = wb_v.shape[2] // 2
    sub = rows // SUBS
    yb = rows // ny
    partner = lax.rem(col + 1, 2) + 2 * chip
    after = 2 * lax.rem(chip + step + nx, nx) + core
    tx_peers = [lax.rem(col + k, ntx) for k in range(1, ntx)]
    x_peers = [2 * lax.rem(chip + k, nx) + core for k in range(1, nx)]
    y_peers = [lax.rem(row + k, ny) for k in range(1, ny)]
    y_froms = [lax.rem(row - k + ny, ny) for k in range(1, ny)]

    barrier = pltpu.get_barrier_semaphore()
    for peer in tx_peers:
        pl.semaphore_signal(barrier, inc=1, device_id={"tx": peer}, device_id_type=MESH)
    for peer in y_peers:
        pl.semaphore_signal(barrier, inc=1, device_id={"ty": peer}, device_id_type=MESH)

    def piece(t):
        return pl.ds(pl.multiple_of(t * sub, sub), sub)

    def block_of(s, mine):
        sign = step if mine else -step
        at = lax.rem(chip - (s + 1) * sign + 2 * nx, nx)
        return 2 * at + (core if mine else 1 - core)

    def held(s, mine):
        sign = step if mine else -step
        return 2 * lax.rem(chip - s * sign + 2 * nx, nx) + (core if mine else 1 - core)

    def block_loads(n, b):
        at = pl.ds(pl.multiple_of(b * fb, fb), fb)
        return [
            pltpu.make_async_copy(wg_h.at[:, at], wb_v.at[n, :, pl.ds(0, fb)], wb_sem.at[n]),
            pltpu.make_async_copy(wu_h.at[:, at], wb_v.at[n, :, pl.ds(fb, fb)], wb_sem.at[n]),
        ]

    def wd_load(n, b):
        at = pl.ds(pl.multiple_of(b * fb, fb), fb)
        return pltpu.make_async_copy(wd_h.at[at, :], wd_v.at[n], wd_sem.at[n])

    first_loads = [
        pltpu.make_async_copy(x_h, x_v, in_sem.at[0]),
        pltpu.make_async_copy(perm_h, perm_v, in_sem.at[1]),
        pltpu.make_async_copy(gamma_h, gamma_v, in_sem.at[2]),
        pltpu.make_async_copy(freq_h, freq_v, in_sem.at[3]),
    ]
    q_loads = [
        pltpu.make_async_copy(wq_h, wq_v.at[:, pl.ds(0, qn)], wq_sem),
        pltpu.make_async_copy(wk_h, wq_v.at[:, pl.ds(qn, hd)], wq_sem),
        pltpu.make_async_copy(wv_h, wq_v.at[:, pl.ds(qn + hd, hd)], wq_sem),
    ]
    k_in = [pltpu.make_async_copy(k_h.at[r], kbuf.at[r], kv_sem.at[0, r]) for r in range(sb)]
    v_in = [pltpu.make_async_copy(v_h.at[r], vbuf.at[r], kv_sem.at[1, r]) for r in range(sb)]
    wo_load = pltpu.make_async_copy(wo_h, wo_v, wo_sem)
    for c in first_loads:
        c.start()
    for c in first_loads:
        c.wait()
    for c in q_loads:
        c.start()
    for n in range(ntx):
        for c in block_loads(n, block_of(n // 2, n % 2 == 1)):
            c.start()

    xp = jnp.dot(perm_v[...], x_v[...], preferred_element_type=F32)
    own_mean = jnp.sum(xp, axis=1, keepdims=True) / dl
    xc = xp - own_mean
    gamma = gamma_v[...].reshape(1, dl)
    h_v[:rows] = (xc * gamma).astype(BF16)
    extra = lax.broadcasted_iota(jnp.int32, (16, dl), 0)
    h_v[rows:] = jnp.where(extra == 0, gamma, jnp.where(extra == 1, gamma - gamma.astype(BF16).astype(F32), 0.0)).astype(BF16)
    lane = lax.broadcasted_iota(jnp.int32, (rows, rows), 1)
    both = jnp.where(lane == 0, own_mean, jnp.where(lane == 1, jnp.sum(xc * xc, axis=1, keepdims=True), 0.0))
    stat_s[...] = jnp.transpose(both)[:8]

    def gamma_row(vals, tiles):
        row_sum = vals[0:1, :] + vals[1:2, :]
        parts = [row_sum[:, n * hd:(n + 1) * hd] for n in range(tiles)]
        return jnp.concatenate(parts + [jnp.zeros((16 - tiles, hd), F32)], axis=0).astype(BF16)

    pltpu.make_async_copy(wq_v, wq_v, wq_sem).wait()
    part = jnp.dot(h_v[...], wq_v[...], preferred_element_type=F32)
    qp[...] = part[:rows].reshape(ntx, rb, qw)
    gq_s[...] = gamma_row(part[rows:], qw // hd)
    for n in range(nx):
        qd_s[n] = qp[2 * n + 1 - core].astype(BF16)
    qd_cp = remote(qd_s, qd_r, qd_ss, qd_rs, tx=partner)
    stat_cp = [remote(stat_s, stat_r.at[k], stat_ss, stat_rs, tx=tx_peers[k - 1]) for k in range(1, ntx)]
    gq_cp = [remote(gq_s, gq_r.at[k], gq_ss, gq_rs, tx=tx_peers[k - 1]) for k in range(1, ntx)]
    gb_cp = [remote(gb_s.at[tx_peers[k - 1]], gb_r.at[k], gb_ss, gb_rs, tx=tx_peers[k - 1]) for k in range(1, ntx)]
    with scope("greet"):
        pl.semaphore_wait(barrier, ntx - 1 + ny - 1)
    qd_cp.start()
    for c in stat_cp + gq_cp:
        c.start()
    stat_r[0] = stat_s[...]
    gq_r[0] = gq_s[...]

    def rest_of_norm():
        with scope("stat"):
            remote(stat_r.at[pl.ds(1, ntx - 1)], stat_r.at[pl.ds(1, ntx - 1)], stat_ss, stat_rs, tx=partner).wait_recv()
            remote(gq_r.at[pl.ds(1, ntx - 1)], gq_r.at[pl.ds(1, ntx - 1)], gq_ss, gq_rs, tx=partner).wait_recv()
        means = jnp.concatenate([stat_r[k, 0:1, :] for k in range(ntx)], axis=0)
        squares = jnp.concatenate([stat_r[k, 1:2, :] for k in range(ntx)], axis=0)
        off = means - jnp.sum(means, axis=0, keepdims=True) / ntx
        var = jnp.sum(squares, axis=0, keepdims=True) / d_model + jnp.sum(off * off, axis=0, keepdims=True) / ntx
        scale = lax.rsqrt(var + EPSILON)
        norm[...] = jnp.transpose(jnp.concatenate([off, scale, jnp.zeros((rows - ntx - 1, rows), F32)], axis=0))

    def normed(vals, at, g_ref):
        cols = norm[at, :]
        tiles = []
        for n in range(vals.shape[1] // hd):
            tile = vals[:, n * hd:(n + 1) * hd]
            for k in range(ntx):
                tile = tile + cols[:, k:k + 1] * g_ref[k, n:n + 1, :].astype(F32)
            tiles.append(tile * cols[:, ntx:ntx + 1])
        return jnp.concatenate(tiles, axis=1)

    qx_cp = [remote(qx_s.at[k], qx_r.at[k], qx_ss, qx_rs, tx=x_peers[k - 1]) for k in range(1, nx)]
    qy_cp = [remote(qy_s.at[y_peers[k - 1]], qy_r.at[row], qy_ss, qy_rs, ty=y_peers[k - 1]) for k in range(1, ny)]

    def q_pair():
        with scope("qd"):
            qd_cp.wait_recv()
        for k in range(1, nx):
            at = lax.rem(chip + k, nx)
            qx_s[k] = (qp[2 * at + core] + qd_r[at].astype(F32)).astype(BF16)
            qx_cp[k - 1].start()

    def q_rows():
        mine = qp[2 * chip + core] + qd_r[chip].astype(F32)
        rest_of_norm()
        with scope("qx"):
            remote(qx_r.at[pl.ds(1, nx - 1)], qx_r.at[pl.ds(1, nx - 1)], qx_ss, qx_rs, tx=partner).wait_recv()
        for k in range(1, nx):
            mine = mine + qx_r[k].astype(F32)
        mine = normed(mine, pl.ds(pl.multiple_of(col * rb, rb), rb), gq_r)
        qsum[...] = mine
        kvs[0] = mine[:, qn:qn + hd]
        kvs[1] = mine[:, qn + hd:]
        for a in range(ny):
            for n in range(lh):
                qy_s[a, n * sb:(n + 1) * sb, :] = qsum[a * sb:(a + 1) * sb, n * hd:(n + 1) * hd]
        for c in qy_cp:
            c.start()
        qy_r[row] = qy_s[row]

    def tables():
        at_row = lax.broadcasted_iota(jnp.int32, (8, hd), 0)
        places = jnp.zeros((8, hd), F32)
        for r in range(sb):
            places = jnp.where(at_row == r, lens_ref[(row * ntx + col) * sb + r].astype(F32), places)
        angles = places * freq_v[...]
        turns[0] = jnp.cos(angles)
        low_half = lax.broadcasted_iota(jnp.int32, (8, hd), 1) < hd // 2
        sines = jnp.sin(angles)
        turns[1] = jnp.where(low_half, -sines, sines)

    def d_copy(s):
        return remote(d_s.at[s], d_r.at[s], d_ss, d_rs.at[s], tx=partner)

    def r_copy(s, t):
        return remote(r_s.at[s, piece(t)], r_r.at[s, piece(t)], r_ss, r_rs.at[s, t], tx=after)

    def product(s, carry):
        pltpu.make_async_copy(wb_v.at[2 * s], wb_v.at[2 * s], wb_sem.at[2 * s]).wait()
        part = jnp.dot(h_v[...], wb_v[2 * s], preferred_element_type=F32)
        d_s[s] = part[:rows].astype(BF16)
        d_copy(s).start()
        gb_s[block_of(s, False)] = gamma_row(part[rows:], 2 * fb // hd)

        @pl.when(s == 0)
        def _():
            q_pair()

        pltpu.make_async_copy(wb_v.at[2 * s + 1], wb_v.at[2 * s + 1], wb_sem.at[2 * s + 1]).wait()
        part = jnp.dot(h_v[...], wb_v[2 * s + 1], preferred_element_type=F32)
        own[s] = part[:rows]
        gb_s[block_of(s, True)] = gamma_row(part[rows:], 2 * fb // hd)

        @pl.when(s == 0)
        def _():
            with scope("d0"):
                d_copy(0).wait_recv()
            for t in range(SUBS):
                at = piece(t)
                r_s[0, at] = (own[0, at] + d_r[0, at].astype(F32)).astype(BF16)
                r_copy(0, t).start()

        return carry

    with scope("products"):
        lax.fori_loop(0, nx, product, 0)
    for c in gb_cp + k_in + v_in:
        c.start()
    gb_r[0] = gb_s[col]
    tables()

    def ring(s, t):
        at = piece(t)
        if t == 0:
            with scope("d%d" % s):
                d_copy(s).wait_recv()
        part = own[s, at] + d_r[s, at].astype(F32)
        with scope("r%d%d" % (s, t)):
            r_copy(s - 1, t).wait_recv()
        part = part + r_r[s - 1, at].astype(F32)
        if s < nx - 1:
            r_s[s, at] = part.astype(BF16)
            r_copy(s, t).start()
        else:
            if t == 0:
                with scope("gb"):
                    remote(gb_r.at[pl.ds(1, ntx - 1)], gb_r.at[pl.ds(1, ntx - 1)], gb_ss, gb_rs, tx=partner).wait_recv()
            part = normed(part, at, gb_r)
            gate = part[:, :fb].astype(BF16).astype(F32)
            up = part[:, fb:].astype(BF16).astype(F32)
            b_v[col, at] = (gate * (1.0 / (1.0 + jnp.exp(-gate))) * up).astype(BF16)

    def turn(vals, r):
        return vals * turns[0, r:r + 1, :] + pltpu.roll(vals, hd // 2, 1) * turns[1, r:r + 1, :]

    def attend(r):
        length = lens_ref[(row * ntx + col) * sb + r]
        for a in range(ny):
            qs[a * lh:(a + 1) * lh, :] = turn(qy_r[a, pl.ds(r, lh, stride=sb), :], r)
        q = qs[...].astype(BF16)
        k_new = turn(kvs[0, pl.ds(row * sb + r, 1), :], r).astype(BF16).astype(F32)
        v_new = kvs[1, pl.ds(row * sb + r, 1), :].astype(BF16).astype(F32)
        new_out[r:r + 1, :] = k_new
        new_out[sb + r:sb + r + 1, :] = v_new
        k_in[r].wait()
        s_new = jnp.sum(q.astype(F32) * k_new, axis=1, keepdims=True)
        top = jnp.full((heads, hd), -1e30, F32)
        for c in range(ctx // CHUNK):
            s = lax.dot_general(q, kbuf[r, c * CHUNK:(c + 1) * CHUNK, :], (((1,), (1,)), ((), ())), preferred_element_type=F32)
            pos = lax.broadcasted_iota(jnp.int32, (1, CHUNK), 1) + c * CHUNK
            s = jnp.where(pos < length, s, -1e30)
            sbuf[:, c * CHUNK:(c + 1) * CHUNK] = s
            for t in range(CHUNK // hd):
                top = jnp.maximum(top, s[:, t * hd:(t + 1) * hd])
        high = jnp.maximum(jnp.max(top, axis=1, keepdims=True), s_new)
        rate = hd ** -0.5 * LOG2E
        e_new = jnp.exp2((s_new - high) * rate)
        low = jnp.zeros((heads, hd), F32)
        out = e_new.astype(BF16).astype(F32) * v_new
        v_in[r].wait()
        for c in range(ctx // CHUNK):
            e = jnp.exp2((sbuf[:, c * CHUNK:(c + 1) * CHUNK] - high) * rate)
            for t in range(CHUNK // hd):
                low = low + e[:, t * hd:(t + 1) * hd]
            out = out + jnp.dot(e.astype(BF16), vbuf[r, c * CHUNK:(c + 1) * CHUNK, :], preferred_element_type=F32)
        out = out / (jnp.sum(low, axis=1, keepdims=True) + e_new)
        for a in range(ny):
            o32[a, pl.ds(r, lh, stride=sb), :] = out[a * lh:(a + 1) * lh]

    def b_copy(s, t):
        b = held(s, True)
        return remote(b_v.at[b, piece(t)], b_v.at[b, piece(t)], b_ss, b_rs.at[s, t], tx=after)

    def b_in(s, t):
        b = held(s + 1, True)
        return remote(b_v.at[b, piece(t)], b_v.at[b, piece(t)], b_ss, b_rs.at[s, t], tx=after)

    def bp_copy(s, t):
        b = held(s, True)
        return remote(b_v.at[b, piece(t)], b_v.at[b, piece(t)], bp_ss, bp_rs.at[s], tx=partner)

    ay_cp = [remote(ay_s.at[y_peers[k - 1]], ay_r.at[row], ay_ss, ay_rs, ty=y_peers[k - 1]) for k in range(1, ny)]
    g_cp = [remote(g_v.at[col], g_v.at[col], g_ss, g_rs.at[k], tx=x_peers[k - 1]) for k in range(1, nx)]

    def g_from(k, mine):
        return 2 * lax.rem(chip - k + nx, nx) + (core if mine else 1 - core)

    def g_in(k):
        at = g_from(k, True)
        return remote(g_v.at[at], g_v.at[at], g_ss, g_rs.at[k], tx=x_peers[k - 1])

    def gp_copy(k):
        at = g_from(k, True)
        return remote(g_v.at[at], g_v.at[at], gp_ss, gp_rs, tx=partner)

    def att_out():
        ay_s[...] = o32[...].astype(BF16)
        for c in ay_cp:
            c.start()
        ay_r[row] = ay_s[row]

    def att_rows():
        with scope("ay"):
            remote(ay_r.at[pl.ds(0, ny - 1)], ay_r.at[pl.ds(0, ny - 1)], ay_ss, ay_rs, ty=y_peers[0]).wait_recv()
        for a in range(ny):
            part = ay_r[a].astype(F32)
            for n in range(lh):
                g32[n, a * sb:(a + 1) * sb, :] = part[n * sb:(n + 1) * sb, :]
        g_v[col] = g32[...].astype(BF16)
        for c in g_cp:
            c.start()
        gp_copy(0).start()

    def forward(s):
        for t in range(SUBS):
            with scope("b%d%d" % (s, t)):
                b_in(s, t).wait_recv()
            if s < nx - 2:
                b_copy(s + 1, t).start()
            bp_copy(s + 1, t).start()

    def down(n, first=False):
        wd_load(n, 0).wait()
        part = jnp.dot(b_v[held(n // 2, n % 2 == 0)], wd_v[n], preferred_element_type=F32)
        acc[...] = part if first else acc[...] + part

    def from_pair(s):
        with scope("bp%d" % s):
            b = held(s, False)
            remote(b_v.at[b], b_v.at[b], bp_ss, bp_rs.at[s], tx=partner).wait_recv()

    ring(1, 0)
    q_rows()
    for t in range(1, SUBS):
        ring(1, t)
    for n in range(ntx):
        wd_load(n, held(n // 2, n % 2 == 0)).start()
    wo_load.start()
    ring(2, 0)
    ring(2, 1)
    with scope("qy"):
        remote(qy_r.at[pl.ds(0, ny - 1)], qy_r.at[pl.ds(0, ny - 1)], qy_ss, qy_rs, ty=y_peers[0]).wait_recv()
    with scope("a0"):
        attend(0)
    ring(2, 2)
    ring(2, 3)
    with scope("a1"):
        attend(1)
    ring(3, 0)
    with scope("a2"):
        attend(2)
    ring(3, 1)
    with scope("a3"):
        attend(3)
    att_out()
    for t in range(2, SUBS):
        ring(3, t)
    for t in range(SUBS):
        b_copy(0, t).start()
        bp_copy(0, t).start()
    down(0, True)
    forward(0)
    att_rows()
    from_pair(0)
    down(1)
    down(2)
    forward(1)
    with scope("g"):
        for k in range(1, nx):
            g_in(k).wait_recv()
            gp_copy(k).start()
    from_pair(1)
    down(3)
    down(4)
    with scope("gp"):
        remote(g_v.at[pl.ds(0, nx)], g_v.at[pl.ds(0, nx)], gp_ss, gp_rs, tx=partner).wait_recv()
    wo_load.wait()
    for n in range(0, lh, 2):
        pair = jnp.concatenate([g_v[:, n].reshape(rows, hd), g_v[:, n + 1].reshape(rows, hd)], axis=1)
        acc[...] += jnp.dot(pair, wo_v[n * hd:(n + 2) * hd, :], preferred_element_type=F32)
    forward(2)
    from_pair(2)
    down(5)
    down(6)
    from_pair(3)
    down(7)

    part = lax.dot_general(perm_v[...], acc[...].astype(BF16), (((0,), (0,)), ((), ())), preferred_element_type=F32)
    y_s[...] = part.astype(BF16).reshape(ny, yb, dl)
    y_cp = [remote(y_s.at[y_peers[k - 1]], y_r.at[k], y_ss, y_rs, ty=y_peers[k - 1]) for k in range(1, ny)]
    for c in y_cp:
        c.start()
    total = x_v[pl.ds(pl.multiple_of(row * yb, yb), yb), :].astype(F32) + y_s[row].astype(F32)
    with scope("y"):
        remote(y_r.at[pl.ds(1, ny - 1)], y_r.at[pl.ds(1, ny - 1)], y_ss, y_rs, ty=y_peers[0]).wait_recv()
    for k in range(1, ny):
        total = total + y_r[k].astype(F32)
    yf[row] = total.astype(BF16)
    f_cp = [remote(yf.at[row], yf.at[row], f_ss, f_rs, ty=y_peers[k - 1]) for k in range(1, ny)]
    for c in f_cp:
        c.start()
    with scope("f"):
        remote(yf.at[pl.ds(0, ny - 1)], yf.at[pl.ds(0, ny - 1)], f_ss, f_rs, ty=y_peers[0]).wait_recv()
    y_out[...] = yf[...].reshape(rows, dl)

    with scope("sends"):
        qd_cp.wait_send()
        for ref, send, recv in (
            (stat_r.at[pl.ds(1, ntx - 1)], stat_ss, stat_rs), (gq_r.at[pl.ds(1, ntx - 1)], gq_ss, gq_rs), (gb_r.at[pl.ds(1, ntx - 1)], gb_ss, gb_rs),
            (qx_s.at[pl.ds(1, nx - 1)], qx_ss, qx_rs), (qy_s.at[pl.ds(1, ny - 1)], qy_ss, qy_rs), (ay_s.at[pl.ds(1, ny - 1)], ay_ss, ay_rs),
            (y_s.at[pl.ds(1, ny - 1)], y_ss, y_rs), (yf.at[pl.ds(1, ny - 1)], f_ss, f_rs),
            (d_s, d_ss, d_rs.at[0]), (r_s, r_ss, r_rs.at[0, 0]), (g_v.at[pl.ds(1, nx - 1)], g_ss, g_rs.at[0]), (g_v.at[pl.ds(0, nx)], gp_ss, gp_rs),
            (b_v.at[pl.ds(1, nx - 1)], b_ss, b_rs.at[0, 0]), (b_v.at[pl.ds(0, nx)], bp_ss, bp_rs.at[0]),
        ):
            remote(ref, ref, send, recv, tx=partner).wait_send()


def store_kernel(ny, ntx, lens_ref, y_v, new_v, k_v, v_v, y_h, ko_h, vo_h, patch, y_sem, out_sem):
    first = (lax.axis_index("ty") * ntx + lax.axis_index("tx")) * k_v.shape[0]
    sb, ctx, hd = k_v.shape
    pieces = ctx // PIECE
    y_cp = pltpu.make_async_copy(y_v, y_h, y_sem)
    y_cp.start()

    def write(a, buf, out):
        def sequence(r, carry):
            length = lens_ref[first + r]
            spot = lax.div(length, PIECE)

            def other(c, inner):
                c = c + jnp.where(c >= spot, 1, 0)
                rest = pl.ds(pl.multiple_of(c * PIECE, PIECE), PIECE)
                pltpu.make_async_copy(buf.at[r, rest], out.at[r, rest], out_sem.at[a, r, 1]).start()
                return inner

            lax.fori_loop(0, pieces - 1, other, 0)
            at = pl.ds(pl.multiple_of(spot * PIECE, PIECE), PIECE)
            here = lax.broadcasted_iota(jnp.int32, (PIECE, hd), 0) == length - spot * PIECE
            patch[a, r] = jnp.where(here, new_v[pl.ds(a * sb + r, 1), :], buf[r, at, :].astype(F32)).astype(BF16)
            pltpu.make_async_copy(patch.at[a, r], out.at[r, at], out_sem.at[a, r, 0]).start()
            return carry

        lax.fori_loop(0, sb, sequence, 0)

    def finish(a, buf, out):
        for r in range(sb):
            pltpu.make_async_copy(patch.at[a, r], out.at[r, pl.ds(0, PIECE)], out_sem.at[a, r, 0]).wait()
            rest = pl.ds(0, ctx - PIECE)
            pltpu.make_async_copy(buf.at[r, rest], out.at[r, rest], out_sem.at[a, r, 1]).wait()

    write(0, k_v, ko_h)
    write(1, v_v, vo_h)
    y_cp.wait()
    finish(0, k_v, ko_h)
    finish(1, v_v, vo_h)


def solution(mesh):
    ny = mesh.shape["ty"]
    ntx = mesh.shape["tx"]
    nx = ntx // 2
    cache_spec = P(("dp", "ty", "tx"), None, None)
    vspec = pl.BlockSpec(memory_space=VMEM)
    hspec = pl.BlockSpec(memory_space=pltpu.HBM)
    sspec = pl.BlockSpec(memory_space=pltpu.SMEM)

    def layer_shard(x_blk, lens_part, k_blk, v_blk, gamma_blk, w_query, w_key, w_value, w_gate, w_up, w_out, w_down):
        rows, dl = x_blk.shape
        sb, ctx, hd = k_blk.shape
        qn = w_query.shape[1]
        lh = qn // hd
        qw = qn + 2 * hd
        fb = w_gate.shape[1] // ntx
        rb = rows // ntx
        yb = rows // ny

        natural = np.arange(rows)
        order = np.reshape(np.transpose(np.reshape(natural, (ny, ntx, sb)), (1, 0, 2)), (rows,))
        perm = jnp.asarray(order[:, None] == natural[None, :], dtype=BF16)
        freqs = np.power(ROPE_BASE, -(np.arange(hd // 2, dtype=np.float32) * 2.0) / hd).astype(np.float32)
        freqs = jnp.asarray(np.tile(np.concatenate([freqs, freqs])[None, :], (8, 1)))

        y_vm, new_rows, k_vm, v_vm = pl.pallas_call(
            functools.partial(step_kernel, ny, nx, dl * ntx),
            out_shape=(
                pltpu.VMEM((rows, dl), BF16),
                pltpu.VMEM((2 * sb, hd), F32),
                pltpu.VMEM(k_blk.shape, BF16),
                pltpu.VMEM(v_blk.shape, BF16),
            ),
            in_specs=[sspec] + [hspec] * 13,
            out_specs=(vspec,) * 4,
            scratch_shapes=[
                VMEM((rows, dl), BF16), VMEM((dl,), F32), VMEM((rows, rows), BF16), VMEM((8, hd), F32),
                VMEM((dl, qw), BF16), VMEM((ntx, dl, 2 * fb), BF16), VMEM((qn, dl), BF16), VMEM((ntx, fb, dl), BF16),
                VMEM((rows + 16, dl), BF16), VMEM((8, rows), F32), VMEM((ntx, 8, rows), F32),
                VMEM((16, hd), BF16), VMEM((ntx, 16, hd), BF16), VMEM((ntx, 16, hd), BF16), VMEM((ntx, 16, hd), BF16), VMEM((rows, rows), F32),
                VMEM((ntx, rb, qw), F32), VMEM((nx, rb, qw), BF16), VMEM((nx, rb, qw), BF16),
                VMEM((nx, rb, qw), BF16), VMEM((nx, rb, qw), BF16), VMEM((rb, qw), F32), VMEM((2, rb, hd), F32),
                VMEM((ny, sb * lh, hd), F32), VMEM((ny, sb * lh, hd), F32),
                VMEM((nx, rows, 2 * fb), F32), VMEM((nx, rows, 2 * fb), BF16), VMEM((nx, rows, 2 * fb), BF16),
                VMEM((nx - 1, rows, 2 * fb), BF16), VMEM((nx - 1, rows, 2 * fb), BF16),
                VMEM((2, 8, hd), F32), VMEM((ny * lh, hd), F32), VMEM((ny * lh, ctx), F32), VMEM((ny, sb * lh, hd), F32),
                VMEM((ny, sb * lh, hd), BF16), VMEM((ny, sb * lh, hd), BF16), VMEM((lh, rb, hd), F32),
                VMEM((ntx, lh, rb, hd), BF16), VMEM((ntx, rows, fb), BF16), VMEM((rows, dl), F32),
                VMEM((ny, yb, dl), BF16), VMEM((ny, yb, dl), BF16), VMEM((ny, yb, dl), BF16),
                DMA((4,)), DMA, DMA((ntx,)), DMA((2, sb)), DMA, DMA((ntx,)),
                DMA, DMA, DMA, DMA, DMA, DMA, DMA, DMA, DMA, DMA, DMA, DMA,
                DMA, DMA((nx,)), DMA, DMA((nx - 1, SUBS)),
                DMA, DMA, DMA, DMA((nx,)), DMA, DMA,
                DMA, DMA((nx - 1, SUBS)), DMA, DMA((nx,)), DMA, DMA, DMA, DMA,
            ],
            compiler_params=pltpu.CompilerParams(collective_id=0, has_side_effects=True, vmem_limit_bytes=52 * 1024 * 1024),
            name="step",
        )(lens_part, x_blk, gamma_blk, perm, freqs, w_query, w_key, w_value, w_gate, w_up, k_blk, v_blk, w_out, w_down)

        return pl.pallas_call(
            functools.partial(store_kernel, ny, ntx),
            out_shape=(
                jax.ShapeDtypeStruct((rows, dl), BF16),
                jax.ShapeDtypeStruct(k_blk.shape, BF16),
                jax.ShapeDtypeStruct(v_blk.shape, BF16),
            ),
            in_specs=[sspec] + [vspec] * 4,
            out_specs=(hspec,) * 3,
            scratch_shapes=[VMEM((2, sb, PIECE, hd), BF16), DMA, DMA((2, sb, 2))],
            compiler_params=pltpu.CompilerParams(vmem_limit_bytes=4 * 1024 * 1024),
            name="store",
        )(lens_part, y_vm, new_rows, k_vm, v_vm)

    in_specs = (P("dp", "tx"), P("dp"), cache_spec, cache_spec, P("tx"), P("tx", "ty"), P("tx", None), P("tx", None), P("tx", "ty"), P("tx", "ty"), P("ty", "tx"), P("ty", "tx"))
    out_specs = (P("dp", "tx"), cache_spec, cache_spec)
    return jax.shard_map(layer_shard, mesh=mesh, in_specs=in_specs, out_specs=out_specs, check_vma=False)
```

```python
import functools

import jax
import jax.numpy as jnp
import numpy as np
from jax import lax
from jax.experimental import pallas as pl
from jax.experimental.pallas import tpu as pltpu
from jax.sharding import PartitionSpec as P

EPSILON = 1e-6
ROPE_BASE = 10000.0
LOG2E = 1.4426950408889634
MESH = pl.DeviceIdType.MESH
F32 = jnp.float32
BF16 = jnp.bfloat16
VMEM = pltpu.VMEM
DMA = pltpu.SemaphoreType.DMA
SUBS = 4
CHUNK = 1024
PIECE = 512
scope = jax.named_scope


def remote(src, dst, send_sem, recv_sem, tx=None, ty=None):
    device = {}
    if tx is not None:
        device["tx"] = tx
    if ty is not None:
        device["ty"] = ty
    return pltpu.make_async_remote_copy(src_ref=src, dst_ref=dst, send_sem=send_sem, recv_sem=recv_sem, device_id=device, device_id_type=MESH)


def step_kernel(ny, nx, d_model, lens_ref, x_h, gamma_h, perm_h, freq_h, wq_h, wk_h, wv_h, wg_h, wu_h, k_h, v_h, wo_h, wd_h,
                y_out, new_out, kbuf, vbuf,
                x_v, gamma_v, perm_v, freq_v, wq_v, wb_v, wo_v, wd_v, h_v, stat_s, stat_r, gq_s, gq_r, gb_s, gb_r, norm,
                qp, qd_s, qd_r, qx_s, qx_r, qsum, kvs, qy_s, qy_r, own, d_s, d_r, r_s, r_r,
                turns, qs, sbuf, o32, ay_s, ay_r, g32, g_v, b_v, acc, y_s, y_r, yf,
                in_sem, wq_sem, wb_sem, kv_sem, wo_sem, wd_sem, stat_ss, stat_rs, gq_ss, gq_rs, gb_ss, gb_rs, qd_ss, qd_rs, qx_ss, qx_rs, qy_ss, qy_rs,
                d_ss, d_rs, r_ss, r_rs, ay_ss, ay_rs, g_ss, g_rs, gp_ss, gp_rs, b_ss, b_rs, bp_ss, bp_rs, y_ss, y_rs, f_ss, f_rs):
    row = lax.axis_index("ty")
    col = lax.axis_index("tx")
    chip = lax.div(col, 2)
    core = lax.rem(col, 2)
    step = 1 - 2 * core
    ntx = 2 * nx
    rows, dl = x_h.shape
    rb = rows // ntx
    sb = rb // ny
    qn = wq_h.shape[1]
    hd = wk_h.shape[1]
    qw = qn + 2 * hd
    lh = qn // hd
    heads = ny * lh
    ctx = k_h.shape[1]
    fb = wb_v.shape[2] // 2
    sub = rows // SUBS
    yb = rows // ny
    partner = lax.rem(col + 1, 2) + 2 * chip
    after = 2 * lax.rem(chip + step + nx, nx) + core
    tx_peers = [lax.rem(col + k, ntx) for k in range(1, ntx)]
    x_peers = [2 * lax.rem(chip + k, nx) + core for k in range(1, nx)]
    y_peers = [lax.rem(row + k, ny) for k in range(1, ny)]
    y_froms = [lax.rem(row - k + ny, ny) for k in range(1, ny)]

    barrier = pltpu.get_barrier_semaphore()
    for peer in tx_peers:
        pl.semaphore_signal(barrier, inc=1, device_id={"tx": peer}, device_id_type=MESH)
    for peer in y_peers:
        pl.semaphore_signal(barrier, inc=1, device_id={"ty": peer}, device_id_type=MESH)

    def piece(t):
        return pl.ds(pl.multiple_of(t * sub, sub), sub)

    def block_of(s, mine):
        sign = step if mine else -step
        at = lax.rem(chip - (s + 1) * sign + 2 * nx, nx)
        return 2 * at + (core if mine else 1 - core)

    def held(s, mine):
        sign = step if mine else -step
        return 2 * lax.rem(chip - s * sign + 2 * nx, nx) + (core if mine else 1 - core)

    def block_loads(n, b):
        at = pl.ds(pl.multiple_of(b * fb, fb), fb)
        return [
            pltpu.make_async_copy(wg_h.at[:, at], wb_v.at[n, :, pl.ds(0, fb)], wb_sem.at[n]),
            pltpu.make_async_copy(wu_h.at[:, at], wb_v.at[n, :, pl.ds(fb, fb)], wb_sem.at[n]),
        ]

    def wd_load(n, b):
        at = pl.ds(pl.multiple_of(b * fb, fb), fb)
        return pltpu.make_async_copy(wd_h.at[at, :], wd_v.at[n], wd_sem.at[n])

    first_loads = [
        pltpu.make_async_copy(x_h, x_v, in_sem.at[0]),
        pltpu.make_async_copy(perm_h, perm_v, in_sem.at[1]),
        pltpu.make_async_copy(gamma_h, gamma_v, in_sem.at[2]),
        pltpu.make_async_copy(freq_h, freq_v, in_sem.at[3]),
    ]
    q_loads = [
        pltpu.make_async_copy(wq_h, wq_v.at[:, pl.ds(0, qn)], wq_sem),
        pltpu.make_async_copy(wk_h, wq_v.at[:, pl.ds(qn, hd)], wq_sem),
        pltpu.make_async_copy(wv_h, wq_v.at[:, pl.ds(qn + hd, hd)], wq_sem),
    ]
    k_in = [pltpu.make_async_copy(k_h.at[r], kbuf.at[r], kv_sem.at[0, r]) for r in range(sb)]
    v_in = [pltpu.make_async_copy(v_h.at[r], vbuf.at[r], kv_sem.at[1, r]) for r in range(sb)]
    wo_load = pltpu.make_async_copy(wo_h, wo_v, wo_sem)
    def start_block(s, mine):
        for c in block_loads(2 * s + int(mine), block_of(s, mine)):
            c.start()

    for c in first_loads + q_loads:
        c.start()
    for c in first_loads:
        c.wait()
    start_block(0, False)
    start_block(0, True)

    xp = jnp.dot(perm_v[...], x_v[...], preferred_element_type=F32)
    own_mean = jnp.sum(xp, axis=1, keepdims=True) / dl
    xc = xp - own_mean
    gamma = gamma_v[...].reshape(1, dl)
    h_v[:rows] = (xc * gamma).astype(BF16)
    extra = lax.broadcasted_iota(jnp.int32, (16, dl), 0)
    h_v[rows:] = jnp.where(extra == 0, gamma, jnp.where(extra == 1, gamma - gamma.astype(BF16).astype(F32), 0.0)).astype(BF16)
    lane = lax.broadcasted_iota(jnp.int32, (rows, rows), 1)
    both = jnp.where(lane == 0, own_mean, jnp.where(lane == 1, jnp.sum(xc * xc, axis=1, keepdims=True), 0.0))
    stat_s[...] = jnp.transpose(both)[:8]

    def gamma_row(vals, tiles):
        row_sum = vals[0:1, :] + vals[1:2, :]
        parts = [row_sum[:, n * hd:(n + 1) * hd] for n in range(tiles)]
        return jnp.concatenate(parts + [jnp.zeros((16 - tiles, hd), F32)], axis=0).astype(BF16)

    pltpu.make_async_copy(wq_v, wq_v, wq_sem).wait()
    start_block(1, False)
    part = jnp.dot(h_v[...], wq_v[...], preferred_element_type=F32)
    qp[...] = part[:rows].reshape(ntx, rb, qw)
    gq_s[...] = gamma_row(part[rows:], qw // hd)
    for n in range(nx):
        qd_s[n] = qp[2 * n + 1 - core].astype(BF16)
    qd_cp = remote(qd_s, qd_r, qd_ss, qd_rs, tx=partner)
    stat_cp = [remote(stat_s, stat_r.at[k], stat_ss, stat_rs, tx=tx_peers[k - 1]) for k in range(1, ntx)]
    gq_cp = [remote(gq_s, gq_r.at[k], gq_ss, gq_rs, tx=tx_peers[k - 1]) for k in range(1, ntx)]
    gb_cp = [remote(gb_s.at[tx_peers[k - 1]], gb_r.at[k], gb_ss, gb_rs, tx=tx_peers[k - 1]) for k in range(1, ntx)]
    with scope("greet"):
        pl.semaphore_wait(barrier, ntx - 1 + ny - 1)
    qd_cp.start()
    for c in stat_cp + gq_cp:
        c.start()
    stat_r[0] = stat_s[...]
    gq_r[0] = gq_s[...]

    def rest_of_norm():
        with scope("stat"):
            remote(stat_r.at[pl.ds(1, ntx - 1)], stat_r.at[pl.ds(1, ntx - 1)], stat_ss, stat_rs, tx=partner).wait_recv()
            remote(gq_r.at[pl.ds(1, ntx - 1)], gq_r.at[pl.ds(1, ntx - 1)], gq_ss, gq_rs, tx=partner).wait_recv()
        means = jnp.concatenate([stat_r[k, 0:1, :] for k in range(ntx)], axis=0)
        squares = jnp.concatenate([stat_r[k, 1:2, :] for k in range(ntx)], axis=0)
        off = means - jnp.sum(means, axis=0, keepdims=True) / ntx
        var = jnp.sum(squares, axis=0, keepdims=True) / d_model + jnp.sum(off * off, axis=0, keepdims=True) / ntx
        scale = lax.rsqrt(var + EPSILON)
        norm[...] = jnp.transpose(jnp.concatenate([off, scale, jnp.zeros((rows - ntx - 1, rows), F32)], axis=0))

    def normed(vals, at, g_ref):
        cols = norm[at, :]
        tiles = []
        for n in range(vals.shape[1] // hd):
            tile = vals[:, n * hd:(n + 1) * hd]
            for k in range(ntx):
                tile = tile + cols[:, k:k + 1] * g_ref[k, n:n + 1, :].astype(F32)
            tiles.append(tile * cols[:, ntx:ntx + 1])
        return jnp.concatenate(tiles, axis=1)

    qx_cp = [remote(qx_s.at[k], qx_r.at[k], qx_ss, qx_rs, tx=x_peers[k - 1]) for k in range(1, nx)]
    qy_cp = [remote(qy_s.at[y_peers[k - 1]], qy_r.at[row], qy_ss, qy_rs, ty=y_peers[k - 1]) for k in range(1, ny)]

    def q_pair():
        with scope("qd"):
            qd_cp.wait_recv()
        for k in range(1, nx):
            at = lax.rem(chip + k, nx)
            qx_s[k] = (qp[2 * at + core] + qd_r[at].astype(F32)).astype(BF16)
            qx_cp[k - 1].start()

    def q_rows():
        mine = qp[2 * chip + core] + qd_r[chip].astype(F32)
        rest_of_norm()
        with scope("qx"):
            remote(qx_r.at[pl.ds(1, nx - 1)], qx_r.at[pl.ds(1, nx - 1)], qx_ss, qx_rs, tx=partner).wait_recv()
        for k in range(1, nx):
            mine = mine + qx_r[k].astype(F32)
        mine = normed(mine, pl.ds(pl.multiple_of(col * rb, rb), rb), gq_r)
        qsum[...] = mine
        kvs[0] = mine[:, qn:qn + hd]
        kvs[1] = mine[:, qn + hd:]
        for a in range(ny):
            for n in range(lh):
                qy_s[a, n * sb:(n + 1) * sb, :] = qsum[a * sb:(a + 1) * sb, n * hd:(n + 1) * hd]
        for c in qy_cp:
            c.start()
        qy_r[row] = qy_s[row]

    def tables():
        at_row = lax.broadcasted_iota(jnp.int32, (8, hd), 0)
        places = jnp.zeros((8, hd), F32)
        for r in range(sb):
            places = jnp.where(at_row == r, lens_ref[(row * ntx + col) * sb + r].astype(F32), places)
        angles = places * freq_v[...]
        turns[0] = jnp.cos(angles)
        low_half = lax.broadcasted_iota(jnp.int32, (8, hd), 1) < hd // 2
        sines = jnp.sin(angles)
        turns[1] = jnp.where(low_half, -sines, sines)

    def d_copy(s):
        return remote(d_s.at[s], d_r.at[s], d_ss, d_rs.at[s], tx=partner)

    def r_copy(s, t):
        return remote(r_s.at[s, piece(t)], r_r.at[s, piece(t)], r_ss, r_rs.at[s, t], tx=after)

    def product(s, carry):
        pltpu.make_async_copy(wb_v.at[2 * s], wb_v.at[2 * s], wb_sem.at[2 * s]).wait()

        @pl.when(s < nx - 1)
        def _():
            start_block(s + 1, True)

        part = jnp.dot(h_v[...], wb_v[2 * s], preferred_element_type=F32)
        d_s[s] = part[:rows].astype(BF16)
        d_copy(s).start()
        gb_s[block_of(s, False)] = gamma_row(part[rows:], 2 * fb // hd)

        @pl.when(s == 0)
        def _():
            q_pair()

        pltpu.make_async_copy(wb_v.at[2 * s + 1], wb_v.at[2 * s + 1], wb_sem.at[2 * s + 1]).wait()

        @pl.when(s < nx - 2)
        def _():
            start_block(s + 2, False)

        part = jnp.dot(h_v[...], wb_v[2 * s + 1], preferred_element_type=F32)
        own[s] = part[:rows]
        gb_s[block_of(s, True)] = gamma_row(part[rows:], 2 * fb // hd)

        @pl.when(s == 0)
        def _():
            with scope("d0"):
                d_copy(0).wait_recv()
            for t in range(SUBS):
                at = piece(t)
                r_s[0, at] = (own[0, at] + d_r[0, at].astype(F32)).astype(BF16)
                r_copy(0, t).start()

        return carry

    with scope("products"):
        lax.fori_loop(0, nx, product, 0)
    for c in gb_cp + k_in + v_in:
        c.start()
    gb_r[0] = gb_s[col]
    tables()

    def ring(s, t):
        at = piece(t)
        if t == 0:
            with scope("d%d" % s):
                d_copy(s).wait_recv()
        part = own[s, at] + d_r[s, at].astype(F32)
        with scope("r%d%d" % (s, t)):
            r_copy(s - 1, t).wait_recv()
        part = part + r_r[s - 1, at].astype(F32)
        if s < nx - 1:
            r_s[s, at] = part.astype(BF16)
            r_copy(s, t).start()
        else:
            if t == 0:
                with scope("gb"):
                    remote(gb_r.at[pl.ds(1, ntx - 1)], gb_r.at[pl.ds(1, ntx - 1)], gb_ss, gb_rs, tx=partner).wait_recv()
            part = normed(part, at, gb_r)
            gate = part[:, :fb].astype(BF16).astype(F32)
            up = part[:, fb:].astype(BF16).astype(F32)
            b_v[col, at] = (gate * (1.0 / (1.0 + jnp.exp(-gate))) * up).astype(BF16)

    def turn(vals, r):
        return vals * turns[0, r:r + 1, :] + pltpu.roll(vals, hd // 2, 1) * turns[1, r:r + 1, :]

    def attend(r):
        length = lens_ref[(row * ntx + col) * sb + r]
        for a in range(ny):
            qs[a * lh:(a + 1) * lh, :] = turn(qy_r[a, pl.ds(r, lh, stride=sb), :], r)
        q = qs[...].astype(BF16)
        k_new = turn(kvs[0, pl.ds(row * sb + r, 1), :], r).astype(BF16).astype(F32)
        v_new = kvs[1, pl.ds(row * sb + r, 1), :].astype(BF16).astype(F32)
        new_out[r:r + 1, :] = k_new
        new_out[sb + r:sb + r + 1, :] = v_new
        k_in[r].wait()
        s_new = jnp.sum(q.astype(F32) * k_new, axis=1, keepdims=True)
        top = jnp.full((heads, hd), -1e30, F32)
        for c in range(ctx // CHUNK):
            s = lax.dot_general(q, kbuf[r, c * CHUNK:(c + 1) * CHUNK, :], (((1,), (1,)), ((), ())), preferred_element_type=F32)
            pos = lax.broadcasted_iota(jnp.int32, (1, CHUNK), 1) + c * CHUNK
            s = jnp.where(pos < length, s, -1e30)
            sbuf[:, c * CHUNK:(c + 1) * CHUNK] = s
            for t in range(CHUNK // hd):
                top = jnp.maximum(top, s[:, t * hd:(t + 1) * hd])
        high = jnp.maximum(jnp.max(top, axis=1, keepdims=True), s_new)
        rate = hd ** -0.5 * LOG2E
        e_new = jnp.exp2((s_new - high) * rate)
        low = jnp.zeros((heads, hd), F32)
        out = e_new.astype(BF16).astype(F32) * v_new
        v_in[r].wait()
        for c in range(ctx // CHUNK):
            e = jnp.exp2((sbuf[:, c * CHUNK:(c + 1) * CHUNK] - high) * rate)
            for t in range(CHUNK // hd):
                low = low + e[:, t * hd:(t + 1) * hd]
            out = out + jnp.dot(e.astype(BF16), vbuf[r, c * CHUNK:(c + 1) * CHUNK, :], preferred_element_type=F32)
        out = out / (jnp.sum(low, axis=1, keepdims=True) + e_new)
        for a in range(ny):
            o32[a, pl.ds(r, lh, stride=sb), :] = out[a * lh:(a + 1) * lh]

    def b_copy(s, t):
        b = held(s, True)
        return remote(b_v.at[b, piece(t)], b_v.at[b, piece(t)], b_ss, b_rs.at[s, t], tx=after)

    def b_in(s, t):
        b = held(s + 1, True)
        return remote(b_v.at[b, piece(t)], b_v.at[b, piece(t)], b_ss, b_rs.at[s, t], tx=after)

    def bp_copy(s, t):
        b = held(s, True)
        return remote(b_v.at[b, piece(t)], b_v.at[b, piece(t)], bp_ss, bp_rs.at[s], tx=partner)

    ay_cp = [remote(ay_s.at[y_peers[k - 1]], ay_r.at[row], ay_ss, ay_rs, ty=y_peers[k - 1]) for k in range(1, ny)]
    g_cp = [remote(g_v.at[col], g_v.at[col], g_ss, g_rs.at[k], tx=x_peers[k - 1]) for k in range(1, nx)]

    def g_from(k, mine):
        return 2 * lax.rem(chip - k + nx, nx) + (core if mine else 1 - core)

    def g_in(k):
        at = g_from(k, True)
        return remote(g_v.at[at], g_v.at[at], g_ss, g_rs.at[k], tx=x_peers[k - 1])

    def gp_copy(k):
        at = g_from(k, True)
        return remote(g_v.at[at], g_v.at[at], gp_ss, gp_rs, tx=partner)

    def att_out():
        ay_s[...] = o32[...].astype(BF16)
        for c in ay_cp:
            c.start()
        ay_r[row] = ay_s[row]

    def att_rows():
        with scope("ay"):
            remote(ay_r.at[pl.ds(0, ny - 1)], ay_r.at[pl.ds(0, ny - 1)], ay_ss, ay_rs, ty=y_peers[0]).wait_recv()
        for a in range(ny):
            part = ay_r[a].astype(F32)
            for n in range(lh):
                g32[n, a * sb:(a + 1) * sb, :] = part[n * sb:(n + 1) * sb, :]
        g_v[col] = g32[...].astype(BF16)
        for c in g_cp:
            c.start()
        gp_copy(0).start()

    def forward(s):
        for t in range(SUBS):
            with scope("b%d%d" % (s, t)):
                b_in(s, t).wait_recv()
            if s < nx - 2:
                b_copy(s + 1, t).start()
            bp_copy(s + 1, t).start()

    def down(n, first=False):
        wd_load(n, 0).wait()
        part = jnp.dot(b_v[held(n // 2, n % 2 == 0)], wd_v[n], preferred_element_type=F32)
        acc[...] = part if first else acc[...] + part

    def from_pair(s):
        with scope("bp%d" % s):
            b = held(s, False)
            remote(b_v.at[b], b_v.at[b], bp_ss, bp_rs.at[s], tx=partner).wait_recv()

    q_rows()
    for t in range(SUBS):
        ring(1, t)
    for n in range(ntx):
        wd_load(n, held(n // 2, n % 2 == 0)).start()
    wo_load.start()
    ring(2, 0)
    ring(2, 1)
    with scope("qy"):
        remote(qy_r.at[pl.ds(0, ny - 1)], qy_r.at[pl.ds(0, ny - 1)], qy_ss, qy_rs, ty=y_peers[0]).wait_recv()
    with scope("a0"):
        attend(0)
    ring(2, 2)
    ring(2, 3)
    with scope("a1"):
        attend(1)
    ring(3, 0)
    with scope("a2"):
        attend(2)
    ring(3, 1)
    with scope("a3"):
        attend(3)
    att_out()
    for t in range(2, SUBS):
        ring(3, t)
    for t in range(SUBS):
        b_copy(0, t).start()
        bp_copy(0, t).start()
    down(0, True)
    forward(0)
    att_rows()
    from_pair(0)
    down(1)
    down(2)
    forward(1)
    with scope("g"):
        for k in range(1, nx):
            g_in(k).wait_recv()
            gp_copy(k).start()
    from_pair(1)
    down(3)
    down(4)
    with scope("gp"):
        remote(g_v.at[pl.ds(0, nx)], g_v.at[pl.ds(0, nx)], gp_ss, gp_rs, tx=partner).wait_recv()
    wo_load.wait()
    for n in range(0, lh, 2):
        pair = jnp.concatenate([g_v[:, n].reshape(rows, hd), g_v[:, n + 1].reshape(rows, hd)], axis=1)
        acc[...] += jnp.dot(pair, wo_v[n * hd:(n + 2) * hd, :], preferred_element_type=F32)
    forward(2)
    from_pair(2)
    down(5)
    down(6)
    from_pair(3)
    down(7)

    part = lax.dot_general(perm_v[...], acc[...].astype(BF16), (((0,), (0,)), ((), ())), preferred_element_type=F32)
    y_s[...] = part.astype(BF16).reshape(ny, yb, dl)
    y_cp = [remote(y_s.at[y_peers[k - 1]], y_r.at[k], y_ss, y_rs, ty=y_peers[k - 1]) for k in range(1, ny)]
    for c in y_cp:
        c.start()
    total = x_v[pl.ds(pl.multiple_of(row * yb, yb), yb), :].astype(F32) + y_s[row].astype(F32)
    with scope("y"):
        remote(y_r.at[pl.ds(1, ny - 1)], y_r.at[pl.ds(1, ny - 1)], y_ss, y_rs, ty=y_peers[0]).wait_recv()
    for k in range(1, ny):
        total = total + y_r[k].astype(F32)
    yf[row] = total.astype(BF16)
    f_cp = [remote(yf.at[row], yf.at[row], f_ss, f_rs, ty=y_peers[k - 1]) for k in range(1, ny)]
    for c in f_cp:
        c.start()
    with scope("f"):
        remote(yf.at[pl.ds(0, ny - 1)], yf.at[pl.ds(0, ny - 1)], f_ss, f_rs, ty=y_peers[0]).wait_recv()
    y_out[...] = yf[...].reshape(rows, dl)

    with scope("sends"):
        qd_cp.wait_send()
        for ref, send, recv in (
            (stat_r.at[pl.ds(1, ntx - 1)], stat_ss, stat_rs), (gq_r.at[pl.ds(1, ntx - 1)], gq_ss, gq_rs), (gb_r.at[pl.ds(1, ntx - 1)], gb_ss, gb_rs),
            (qx_s.at[pl.ds(1, nx - 1)], qx_ss, qx_rs), (qy_s.at[pl.ds(1, ny - 1)], qy_ss, qy_rs), (ay_s.at[pl.ds(1, ny - 1)], ay_ss, ay_rs),
            (y_s.at[pl.ds(1, ny - 1)], y_ss, y_rs), (yf.at[pl.ds(1, ny - 1)], f_ss, f_rs),
            (d_s, d_ss, d_rs.at[0]), (r_s, r_ss, r_rs.at[0, 0]), (g_v.at[pl.ds(1, nx - 1)], g_ss, g_rs.at[0]), (g_v.at[pl.ds(0, nx)], gp_ss, gp_rs),
            (b_v.at[pl.ds(1, nx - 1)], b_ss, b_rs.at[0, 0]), (b_v.at[pl.ds(0, nx)], bp_ss, bp_rs.at[0]),
        ):
            remote(ref, ref, send, recv, tx=partner).wait_send()


def store_kernel(ny, ntx, lens_ref, y_v, new_v, k_v, v_v, y_h, ko_h, vo_h, patch, y_sem, out_sem):
    first = (lax.axis_index("ty") * ntx + lax.axis_index("tx")) * k_v.shape[0]
    sb, ctx, hd = k_v.shape
    pieces = ctx // PIECE
    y_cp = pltpu.make_async_copy(y_v, y_h, y_sem)
    y_cp.start()

    def write(a, buf, out):
        def sequence(r, carry):
            length = lens_ref[first + r]
            spot = lax.div(length, PIECE)

            def other(c, inner):
                c = c + jnp.where(c >= spot, 1, 0)
                rest = pl.ds(pl.multiple_of(c * PIECE, PIECE), PIECE)
                pltpu.make_async_copy(buf.at[r, rest], out.at[r, rest], out_sem.at[a, r, 1]).start()
                return inner

            lax.fori_loop(0, pieces - 1, other, 0)
            at = pl.ds(pl.multiple_of(spot * PIECE, PIECE), PIECE)
            here = lax.broadcasted_iota(jnp.int32, (PIECE, hd), 0) == length - spot * PIECE
            patch[a, r] = jnp.where(here, new_v[pl.ds(a * sb + r, 1), :], buf[r, at, :].astype(F32)).astype(BF16)
            pltpu.make_async_copy(patch.at[a, r], out.at[r, at], out_sem.at[a, r, 0]).start()
            return carry

        lax.fori_loop(0, sb, sequence, 0)

    def finish(a, buf, out):
        for r in range(sb):
            pltpu.make_async_copy(patch.at[a, r], out.at[r, pl.ds(0, PIECE)], out_sem.at[a, r, 0]).wait()
            rest = pl.ds(0, ctx - PIECE)
            pltpu.make_async_copy(buf.at[r, rest], out.at[r, rest], out_sem.at[a, r, 1]).wait()

    write(0, k_v, ko_h)
    write(1, v_v, vo_h)
    y_cp.wait()
    finish(0, k_v, ko_h)
    finish(1, v_v, vo_h)


def solution(mesh):
    ny = mesh.shape["ty"]
    ntx = mesh.shape["tx"]
    nx = ntx // 2
    cache_spec = P(("dp", "ty", "tx"), None, None)
    vspec = pl.BlockSpec(memory_space=VMEM)
    hspec = pl.BlockSpec(memory_space=pltpu.HBM)
    sspec = pl.BlockSpec(memory_space=pltpu.SMEM)

    def layer_shard(x_blk, lens_part, k_blk, v_blk, gamma_blk, w_query, w_key, w_value, w_gate, w_up, w_out, w_down):
        rows, dl = x_blk.shape
        sb, ctx, hd = k_blk.shape
        qn = w_query.shape[1]
        lh = qn // hd
        qw = qn + 2 * hd
        fb = w_gate.shape[1] // ntx
        rb = rows // ntx
        yb = rows // ny

        natural = np.arange(rows)
        order = np.reshape(np.transpose(np.reshape(natural, (ny, ntx, sb)), (1, 0, 2)), (rows,))
        perm = jnp.asarray(order[:, None] == natural[None, :], dtype=BF16)
        freqs = np.power(ROPE_BASE, -(np.arange(hd // 2, dtype=np.float32) * 2.0) / hd).astype(np.float32)
        freqs = jnp.asarray(np.tile(np.concatenate([freqs, freqs])[None, :], (8, 1)))

        y_vm, new_rows, k_vm, v_vm = pl.pallas_call(
            functools.partial(step_kernel, ny, nx, dl * ntx),
            out_shape=(
                pltpu.VMEM((rows, dl), BF16),
                pltpu.VMEM((2 * sb, hd), F32),
                pltpu.VMEM(k_blk.shape, BF16),
                pltpu.VMEM(v_blk.shape, BF16),
            ),
            in_specs=[sspec] + [hspec] * 13,
            out_specs=(vspec,) * 4,
            scratch_shapes=[
                VMEM((rows, dl), BF16), VMEM((dl,), F32), VMEM((rows, rows), BF16), VMEM((8, hd), F32),
                VMEM((dl, qw), BF16), VMEM((ntx, dl, 2 * fb), BF16), VMEM((qn, dl), BF16), VMEM((ntx, fb, dl), BF16),
                VMEM((rows + 16, dl), BF16), VMEM((8, rows), F32), VMEM((ntx, 8, rows), F32),
                VMEM((16, hd), BF16), VMEM((ntx, 16, hd), BF16), VMEM((ntx, 16, hd), BF16), VMEM((ntx, 16, hd), BF16), VMEM((rows, rows), F32),
                VMEM((ntx, rb, qw), F32), VMEM((nx, rb, qw), BF16), VMEM((nx, rb, qw), BF16),
                VMEM((nx, rb, qw), BF16), VMEM((nx, rb, qw), BF16), VMEM((rb, qw), F32), VMEM((2, rb, hd), F32),
                VMEM((ny, sb * lh, hd), F32), VMEM((ny, sb * lh, hd), F32),
                VMEM((nx, rows, 2 * fb), F32), VMEM((nx, rows, 2 * fb), BF16), VMEM((nx, rows, 2 * fb), BF16),
                VMEM((nx - 1, rows, 2 * fb), BF16), VMEM((nx - 1, rows, 2 * fb), BF16),
                VMEM((2, 8, hd), F32), VMEM((ny * lh, hd), F32), VMEM((ny * lh, ctx), F32), VMEM((ny, sb * lh, hd), F32),
                VMEM((ny, sb * lh, hd), BF16), VMEM((ny, sb * lh, hd), BF16), VMEM((lh, rb, hd), F32),
                VMEM((ntx, lh, rb, hd), BF16), VMEM((ntx, rows, fb), BF16), VMEM((rows, dl), F32),
                VMEM((ny, yb, dl), BF16), VMEM((ny, yb, dl), BF16), VMEM((ny, yb, dl), BF16),
                DMA((4,)), DMA, DMA((ntx,)), DMA((2, sb)), DMA, DMA((ntx,)),
                DMA, DMA, DMA, DMA, DMA, DMA, DMA, DMA, DMA, DMA, DMA, DMA,
                DMA, DMA((nx,)), DMA, DMA((nx - 1, SUBS)),
                DMA, DMA, DMA, DMA((nx,)), DMA, DMA,
                DMA, DMA((nx - 1, SUBS)), DMA, DMA((nx,)), DMA, DMA, DMA, DMA,
            ],
            compiler_params=pltpu.CompilerParams(collective_id=0, has_side_effects=True, vmem_limit_bytes=52 * 1024 * 1024),
            name="step",
        )(lens_part, x_blk, gamma_blk, perm, freqs, w_query, w_key, w_value, w_gate, w_up, k_blk, v_blk, w_out, w_down)

        return pl.pallas_call(
            functools.partial(store_kernel, ny, ntx),
            out_shape=(
                jax.ShapeDtypeStruct((rows, dl), BF16),
                jax.ShapeDtypeStruct(k_blk.shape, BF16),
                jax.ShapeDtypeStruct(v_blk.shape, BF16),
            ),
            in_specs=[sspec] + [vspec] * 4,
            out_specs=(hspec,) * 3,
            scratch_shapes=[VMEM((2, sb, PIECE, hd), BF16), DMA, DMA((2, sb, 2))],
            compiler_params=pltpu.CompilerParams(vmem_limit_bytes=4 * 1024 * 1024),
            name="store",
        )(lens_part, y_vm, new_rows, k_vm, v_vm)

    in_specs = (P("dp", "tx"), P("dp"), cache_spec, cache_spec, P("tx"), P("tx", "ty"), P("tx", None), P("tx", None), P("tx", "ty"), P("tx", "ty"), P("ty", "tx"), P("ty", "tx"))
    out_specs = (P("dp", "tx"), cache_spec, cache_spec)
    return jax.shard_map(layer_shard, mesh=mesh, in_specs=in_specs, out_specs=out_specs, check_vma=False)
```

```python
import functools

import jax
import jax.numpy as jnp
import numpy as np
from jax import lax
from jax.experimental import pallas as pl
from jax.experimental.pallas import tpu as pltpu
from jax.sharding import PartitionSpec as P

EPSILON = 1e-6
ROPE_BASE = 10000.0
LOG2E = 1.4426950408889634
MESH = pl.DeviceIdType.MESH
F32 = jnp.float32
BF16 = jnp.bfloat16
VMEM = pltpu.VMEM
DMA = pltpu.SemaphoreType.DMA
SUBS = 4
CHUNK = 1024
PIECE = 512
scope = jax.named_scope


def remote(src, dst, send_sem, recv_sem, tx=None, ty=None):
    device = {}
    if tx is not None:
        device["tx"] = tx
    if ty is not None:
        device["ty"] = ty
    return pltpu.make_async_remote_copy(src_ref=src, dst_ref=dst, send_sem=send_sem, recv_sem=recv_sem, device_id=device, device_id_type=MESH)


def step_kernel(ny, nx, d_model, lens_ref, x_h, gamma_h, perm_h, freq_h, wq_h, wk_h, wv_h, wg_h, wu_h, k_h, v_h, wo_h, wd_h,
                y_out, new_out, kbuf, vbuf,
                x_v, gamma_v, perm_v, freq_v, wq_v, wb_v, wo_v, wd_v, h_v, stat_s, stat_r, gq_s, gq_r, gb_s, gb_r, norm,
                qp, qd_s, qd_r, qx_s, qx_r, qsum, kvs, qy_s, qy_r, own, d_s, d_r, r_s, r_r,
                turns, qs, sbuf, o32, ay_s, ay_r, g32, g_v, b_v, acc, y_s, y_r, yf,
                in_sem, wq_sem, wb_sem, kv_sem, wo_sem, wd_sem, stat_ss, stat_rs, gq_ss, gq_rs, gb_ss, gb_rs, qd_ss, qd_rs, qx_ss, qx_rs, qy_ss, qy_rs,
                d_ss, d_rs, r_ss, r_rs, ay_ss, ay_rs, g_ss, g_rs, gp_ss, gp_rs, b_ss, b_rs, bp_ss, bp_rs, y_ss, y_rs, f_ss, f_rs):
    row = lax.axis_index("ty")
    col = lax.axis_index("tx")
    chip = lax.div(col, 2)
    core = lax.rem(col, 2)
    step = 1 - 2 * core
    ntx = 2 * nx
    rows, dl = x_h.shape
    rb = rows // ntx
    sb = rb // ny
    qn = wq_h.shape[1]
    hd = wk_h.shape[1]
    qw = qn + 2 * hd
    lh = qn // hd
    heads = ny * lh
    ctx = k_h.shape[1]
    fb = wb_v.shape[2] // 2
    sub = rows // SUBS
    yb = rows // ny
    partner = lax.rem(col + 1, 2) + 2 * chip
    after = 2 * lax.rem(chip + step + nx, nx) + core
    before = 2 * lax.rem(chip - step + nx, nx) + core
    tx_peers = [lax.rem(col + k, ntx) for k in range(1, ntx)]
    x_peers = [2 * lax.rem(chip + k, nx) + core for k in range(1, nx)]
    y_peers = [lax.rem(row + k, ny) for k in range(1, ny)]
    y_froms = [lax.rem(row - k + ny, ny) for k in range(1, ny)]

    barrier = pltpu.get_barrier_semaphore()
    for peer in tx_peers:
        pl.semaphore_signal(barrier, inc=1, device_id={"tx": peer}, device_id_type=MESH)
    for peer in y_peers:
        pl.semaphore_signal(barrier, inc=1, device_id={"ty": peer}, device_id_type=MESH)

    def piece(t):
        return pl.ds(pl.multiple_of(t * sub, sub), sub)

    def block_of(s, mine):
        sign = step if mine else -step
        at = lax.rem(chip - (s + 1) * sign + 2 * nx, nx)
        return 2 * at + (core if mine else 1 - core)

    def held(kind, mine):
        away = (0, -1, 1, -2)[kind] * (step if mine else -step)
        return 2 * lax.rem(chip + away + 2 * nx, nx) + (core if mine else 1 - core)

    def block_loads(n, b):
        at = pl.ds(pl.multiple_of(b * fb, fb), fb)
        return [
            pltpu.make_async_copy(wg_h.at[:, at], wb_v.at[n, :, pl.ds(0, fb)], wb_sem.at[n]),
            pltpu.make_async_copy(wu_h.at[:, at], wb_v.at[n, :, pl.ds(fb, fb)], wb_sem.at[n]),
        ]

    def wd_load(n, b):
        at = pl.ds(pl.multiple_of(b * fb, fb), fb)
        return pltpu.make_async_copy(wd_h.at[at, :], wd_v.at[n], wd_sem.at[n])

    first_loads = [
        pltpu.make_async_copy(x_h, x_v, in_sem.at[0]),
        pltpu.make_async_copy(perm_h, perm_v, in_sem.at[1]),
        pltpu.make_async_copy(gamma_h, gamma_v, in_sem.at[2]),
        pltpu.make_async_copy(freq_h, freq_v, in_sem.at[3]),
    ]
    q_loads = [
        pltpu.make_async_copy(wq_h, wq_v.at[:, pl.ds(0, qn)], wq_sem),
        pltpu.make_async_copy(wk_h, wq_v.at[:, pl.ds(qn, hd)], wq_sem),
        pltpu.make_async_copy(wv_h, wq_v.at[:, pl.ds(qn + hd, hd)], wq_sem),
    ]
    k_in = [pltpu.make_async_copy(k_h.at[r], kbuf.at[r], kv_sem.at[0, r]) for r in range(sb)]
    v_in = [pltpu.make_async_copy(v_h.at[r], vbuf.at[r], kv_sem.at[1, r]) for r in range(sb)]
    wo_load = pltpu.make_async_copy(wo_h, wo_v, wo_sem)
    def start_block(s, mine):
        for c in block_loads(2 * s + int(mine), block_of(s, mine)):
            c.start()

    for c in first_loads + q_loads:
        c.start()
    for c in first_loads:
        c.wait()
    start_block(0, False)
    start_block(0, True)

    xp = jnp.dot(perm_v[...], x_v[...], preferred_element_type=F32)
    own_mean = jnp.sum(xp, axis=1, keepdims=True) / dl
    xc = xp - own_mean
    gamma = gamma_v[...].reshape(1, dl)
    h_v[:rows] = (xc * gamma).astype(BF16)
    extra = lax.broadcasted_iota(jnp.int32, (16, dl), 0)
    h_v[rows:] = jnp.where(extra == 0, gamma, jnp.where(extra == 1, gamma - gamma.astype(BF16).astype(F32), 0.0)).astype(BF16)
    lane = lax.broadcasted_iota(jnp.int32, (rows, rows), 1)
    both = jnp.where(lane == 0, own_mean, jnp.where(lane == 1, jnp.sum(xc * xc, axis=1, keepdims=True), 0.0))
    stat_s[...] = jnp.transpose(both)[:8]

    def gamma_row(vals, tiles):
        row_sum = vals[0:1, :] + vals[1:2, :]
        parts = [row_sum[:, n * hd:(n + 1) * hd] for n in range(tiles)]
        return jnp.concatenate(parts + [jnp.zeros((16 - tiles, hd), F32)], axis=0).astype(BF16)

    pltpu.make_async_copy(wq_v, wq_v, wq_sem).wait()
    start_block(1, False)
    part = jnp.dot(h_v[...], wq_v[...], preferred_element_type=F32)
    qp[...] = part[:rows].reshape(ntx, rb, qw)
    gq_s[...] = gamma_row(part[rows:], qw // hd)
    for n in range(nx):
        qd_s[n] = qp[2 * n + 1 - core].astype(BF16)
    qd_cp = remote(qd_s, qd_r, qd_ss, qd_rs, tx=partner)
    stat_cp = [remote(stat_s, stat_r.at[k], stat_ss, stat_rs, tx=tx_peers[k - 1]) for k in range(1, ntx)]
    gq_cp = [remote(gq_s, gq_r.at[k], gq_ss, gq_rs, tx=tx_peers[k - 1]) for k in range(1, ntx)]
    gb_cp = [remote(gb_s.at[tx_peers[k - 1]], gb_r.at[k], gb_ss, gb_rs, tx=tx_peers[k - 1]) for k in range(1, ntx)]
    with scope("greet"):
        pl.semaphore_wait(barrier, ntx - 1 + ny - 1)
    qd_cp.start()
    for c in stat_cp + gq_cp:
        c.start()
    stat_r[0] = stat_s[...]
    gq_r[0] = gq_s[...]

    def rest_of_norm():
        with scope("stat"):
            remote(stat_r.at[pl.ds(1, ntx - 1)], stat_r.at[pl.ds(1, ntx - 1)], stat_ss, stat_rs, tx=partner).wait_recv()
            remote(gq_r.at[pl.ds(1, ntx - 1)], gq_r.at[pl.ds(1, ntx - 1)], gq_ss, gq_rs, tx=partner).wait_recv()
        means = jnp.concatenate([stat_r[k, 0:1, :] for k in range(ntx)], axis=0)
        squares = jnp.concatenate([stat_r[k, 1:2, :] for k in range(ntx)], axis=0)
        off = means - jnp.sum(means, axis=0, keepdims=True) / ntx
        var = jnp.sum(squares, axis=0, keepdims=True) / d_model + jnp.sum(off * off, axis=0, keepdims=True) / ntx
        scale = lax.rsqrt(var + EPSILON)
        norm[...] = jnp.transpose(jnp.concatenate([off, scale, jnp.zeros((rows - ntx - 1, rows), F32)], axis=0))

    def normed(vals, at, g_ref):
        cols = norm[at, :]
        tiles = []
        for n in range(vals.shape[1] // hd):
            tile = vals[:, n * hd:(n + 1) * hd]
            for k in range(ntx):
                tile = tile + cols[:, k:k + 1] * g_ref[k, n:n + 1, :].astype(F32)
            tiles.append(tile * cols[:, ntx:ntx + 1])
        return jnp.concatenate(tiles, axis=1)

    qx_cp = [remote(qx_s.at[k], qx_r.at[k], qx_ss, qx_rs, tx=x_peers[k - 1]) for k in range(1, nx)]
    qy_cp = [remote(qy_s.at[y_peers[k - 1]], qy_r.at[row], qy_ss, qy_rs, ty=y_peers[k - 1]) for k in range(1, ny)]

    def q_pair():
        with scope("qd"):
            qd_cp.wait_recv()
        for k in range(1, nx):
            at = lax.rem(chip + k, nx)
            qx_s[k] = (qp[2 * at + core] + qd_r[at].astype(F32)).astype(BF16)
            qx_cp[k - 1].start()

    def q_rows():
        mine = qp[2 * chip + core] + qd_r[chip].astype(F32)
        rest_of_norm()
        with scope("qx"):
            remote(qx_r.at[pl.ds(1, nx - 1)], qx_r.at[pl.ds(1, nx - 1)], qx_ss, qx_rs, tx=partner).wait_recv()
        for k in range(1, nx):
            mine = mine + qx_r[k].astype(F32)
        mine = normed(mine, pl.ds(pl.multiple_of(col * rb, rb), rb), gq_r)
        qsum[...] = mine
        kvs[0] = mine[:, qn:qn + hd]
        kvs[1] = mine[:, qn + hd:]
        for a in range(ny):
            for n in range(lh):
                qy_s[a, n * sb:(n + 1) * sb, :] = qsum[a * sb:(a + 1) * sb, n * hd:(n + 1) * hd]
        for c in qy_cp:
            c.start()
        qy_r[row] = qy_s[row]

    def tables():
        at_row = lax.broadcasted_iota(jnp.int32, (8, hd), 0)
        places = jnp.zeros((8, hd), F32)
        for r in range(sb):
            places = jnp.where(at_row == r, lens_ref[(row * ntx + col) * sb + r].astype(F32), places)
        angles = places * freq_v[...]
        turns[0] = jnp.cos(angles)
        low_half = lax.broadcasted_iota(jnp.int32, (8, hd), 1) < hd // 2
        sines = jnp.sin(angles)
        turns[1] = jnp.where(low_half, -sines, sines)

    def d_copy(s):
        return remote(d_s.at[s], d_r.at[s], d_ss, d_rs.at[s], tx=partner)

    def r_copy(s, t):
        return remote(r_s.at[s, piece(t)], r_r.at[s, piece(t)], r_ss, r_rs.at[s, t], tx=after)

    def product(s, carry):
        pltpu.make_async_copy(wb_v.at[2 * s], wb_v.at[2 * s], wb_sem.at[2 * s]).wait()

        @pl.when(s < nx - 1)
        def _():
            start_block(s + 1, True)

        part = jnp.dot(h_v[...], wb_v[2 * s], preferred_element_type=F32)
        d_s[s] = part[:rows].astype(BF16)
        d_copy(s).start()
        gb_s[block_of(s, False)] = gamma_row(part[rows:], 2 * fb // hd)

        @pl.when(s == 0)
        def _():
            q_pair()

        pltpu.make_async_copy(wb_v.at[2 * s + 1], wb_v.at[2 * s + 1], wb_sem.at[2 * s + 1]).wait()

        @pl.when(s < nx - 2)
        def _():
            start_block(s + 2, False)

        part = jnp.dot(h_v[...], wb_v[2 * s + 1], preferred_element_type=F32)
        own[s] = part[:rows]
        gb_s[block_of(s, True)] = gamma_row(part[rows:], 2 * fb // hd)

        @pl.when(s == 0)
        def _():
            with scope("d0"):
                d_copy(0).wait_recv()
            for t in range(SUBS):
                at = piece(t)
                r_s[0, at] = (own[0, at] + d_r[0, at].astype(F32)).astype(BF16)
                r_copy(0, t).start()

        return carry

    with scope("products"):
        lax.fori_loop(0, nx, product, 0)
    for c in gb_cp + k_in + v_in:
        c.start()
    gb_r[0] = gb_s[col]
    tables()

    def ring(s, t):
        at = piece(t)
        if t == 0:
            with scope("d%d" % s):
                d_copy(s).wait_recv()
        part = own[s, at] + d_r[s, at].astype(F32)
        with scope("r%d%d" % (s, t)):
            r_copy(s - 1, t).wait_recv()
        part = part + r_r[s - 1, at].astype(F32)
        if s < nx - 1:
            r_s[s, at] = part.astype(BF16)
            r_copy(s, t).start()
        else:
            if t == 0:
                with scope("gb"):
                    remote(gb_r.at[pl.ds(1, ntx - 1)], gb_r.at[pl.ds(1, ntx - 1)], gb_ss, gb_rs, tx=partner).wait_recv()
            part = normed(part, at, gb_r)
            gate = part[:, :fb].astype(BF16).astype(F32)
            up = part[:, fb:].astype(BF16).astype(F32)
            b_v[col, at] = (gate * (1.0 / (1.0 + jnp.exp(-gate))) * up).astype(BF16)
            act_out(t)

    def turn(vals, r):
        return vals * turns[0, r:r + 1, :] + pltpu.roll(vals, hd // 2, 1) * turns[1, r:r + 1, :]

    def attend(r):
        length = lens_ref[(row * ntx + col) * sb + r]
        for a in range(ny):
            qs[a * lh:(a + 1) * lh, :] = turn(qy_r[a, pl.ds(r, lh, stride=sb), :], r)
        q = qs[...].astype(BF16)
        k_new = turn(kvs[0, pl.ds(row * sb + r, 1), :], r).astype(BF16).astype(F32)
        v_new = kvs[1, pl.ds(row * sb + r, 1), :].astype(BF16).astype(F32)
        new_out[r:r + 1, :] = k_new
        new_out[sb + r:sb + r + 1, :] = v_new
        k_in[r].wait()
        s_new = jnp.sum(q.astype(F32) * k_new, axis=1, keepdims=True)
        top = jnp.full((heads, hd), -1e30, F32)
        for c in range(ctx // CHUNK):
            s = lax.dot_general(q, kbuf[r, c * CHUNK:(c + 1) * CHUNK, :], (((1,), (1,)), ((), ())), preferred_element_type=F32)
            pos = lax.broadcasted_iota(jnp.int32, (1, CHUNK), 1) + c * CHUNK
            s = jnp.where(pos < length, s, -1e30)
            sbuf[:, c * CHUNK:(c + 1) * CHUNK] = s
            for t in range(CHUNK // hd):
                top = jnp.maximum(top, s[:, t * hd:(t + 1) * hd])
        high = jnp.maximum(jnp.max(top, axis=1, keepdims=True), s_new)
        rate = hd ** -0.5 * LOG2E
        e_new = jnp.exp2((s_new - high) * rate)
        low = jnp.zeros((heads, hd), F32)
        out = e_new.astype(BF16).astype(F32) * v_new
        v_in[r].wait()
        for c in range(ctx // CHUNK):
            e = jnp.exp2((sbuf[:, c * CHUNK:(c + 1) * CHUNK] - high) * rate)
            for t in range(CHUNK // hd):
                low = low + e[:, t * hd:(t + 1) * hd]
            out = out + jnp.dot(e.astype(BF16), vbuf[r, c * CHUNK:(c + 1) * CHUNK, :], preferred_element_type=F32)
        out = out / (jnp.sum(low, axis=1, keepdims=True) + e_new)
        for a in range(ny):
            o32[a, pl.ds(r, lh, stride=sb), :] = out[a * lh:(a + 1) * lh]

    def b_send(kind, t, slot, to):
        b = held(kind, True)
        return remote(b_v.at[b, piece(t)], b_v.at[b, piece(t)], b_ss, b_rs.at[slot - 1, t], tx=to)

    def b_in(kind, t):
        b = held(kind, True)
        return remote(b_v.at[b, piece(t)], b_v.at[b, piece(t)], b_ss, b_rs.at[kind - 1, t], tx=after)

    def b_pair(kind, t):
        b = held(kind, True)
        return remote(b_v.at[b, piece(t)], b_v.at[b, piece(t)], bp_ss, bp_rs.at[kind], tx=partner)

    def act_out(t):
        b_send(0, t, 1, after).start()
        b_send(0, t, 2, before).start()
        b_pair(0, t).start()

    def act_in(kind):
        for t in range(SUBS):
            with scope("b%d%d" % (kind, t)):
                b_in(kind, t).wait_recv()
            if kind == 1:
                b_send(1, t, 3, after).start()
            b_pair(kind, t).start()

    ay_cp = [remote(ay_s.at[y_peers[k - 1]], ay_r.at[row], ay_ss, ay_rs, ty=y_peers[k - 1]) for k in range(1, ny)]

    def g_send(kind, slot, to):
        at = held(kind, True)
        return remote(g_v.at[at], g_v.at[at], g_ss, g_rs.at[slot - 1], tx=to)

    def g_pair(kind):
        at = held(kind, True)
        return remote(g_v.at[at], g_v.at[at], gp_ss, gp_rs, tx=partner)

    def g_in(kind):
        at = held(kind, True)
        with scope("g%d" % kind):
            remote(g_v.at[at], g_v.at[at], g_ss, g_rs.at[kind - 1], tx=after).wait_recv()
        if kind == 1:
            g_send(1, 3, after).start()
        g_pair(kind).start()

    def att_out():
        ay_s[...] = o32[...].astype(BF16)
        for c in ay_cp:
            c.start()
        ay_r[row] = ay_s[row]

    def att_rows():
        with scope("ay"):
            remote(ay_r.at[pl.ds(0, ny - 1)], ay_r.at[pl.ds(0, ny - 1)], ay_ss, ay_rs, ty=y_peers[0]).wait_recv()
        for a in range(ny):
            part = ay_r[a].astype(F32)
            for n in range(lh):
                g32[n, a * sb:(a + 1) * sb, :] = part[n * sb:(n + 1) * sb, :]
        g_v[col] = g32[...].astype(BF16)
        g_send(0, 1, after).start()
        g_send(0, 2, before).start()
        g_pair(0).start()

    def down(n, first=False):
        wd_load(n, 0).wait()
        part = jnp.dot(b_v[held(n // 2, n % 2 == 0)], wd_v[n], preferred_element_type=F32)
        acc[...] = part if first else acc[...] + part

    def from_pair(s):
        with scope("bp%d" % s):
            b = held(s, False)
            remote(b_v.at[b], b_v.at[b], bp_ss, bp_rs.at[s], tx=partner).wait_recv()

    q_rows()
    for t in range(SUBS):
        ring(1, t)
    for n in range(ntx):
        wd_load(n, held(n // 2, n % 2 == 0)).start()
    wo_load.start()
    with scope("qy"):
        remote(qy_r.at[pl.ds(0, ny - 1)], qy_r.at[pl.ds(0, ny - 1)], qy_ss, qy_rs, ty=y_peers[0]).wait_recv()
    for t in range(SUBS):
        with scope("a%d" % t):
            attend(t)
        if t == SUBS - 1:
            att_out()
        ring(2, t)
    for t in range(SUBS):
        ring(3, t)
    down(0, True)
    att_rows()
    act_in(1)
    act_in(2)
    from_pair(0)
    down(1)
    down(2)
    g_in(1)
    g_in(2)
    down(4)
    from_pair(1)
    down(3)
    act_in(3)
    from_pair(2)
    down(5)
    down(6)
    g_in(3)
    from_pair(3)
    down(7)
    with scope("gp"):
        remote(g_v.at[pl.ds(0, nx)], g_v.at[pl.ds(0, nx)], gp_ss, gp_rs, tx=partner).wait_recv()
    wo_load.wait()
    for n in range(0, lh, 2):
        pair = jnp.concatenate([g_v[:, n].reshape(rows, hd), g_v[:, n + 1].reshape(rows, hd)], axis=1)
        acc[...] += jnp.dot(pair, wo_v[n * hd:(n + 2) * hd, :], preferred_element_type=F32)

    part = lax.dot_general(perm_v[...], acc[...].astype(BF16), (((0,), (0,)), ((), ())), preferred_element_type=F32)
    y_s[...] = part.astype(BF16).reshape(ny, yb, dl)
    y_cp = [remote(y_s.at[y_peers[k - 1]], y_r.at[k], y_ss, y_rs, ty=y_peers[k - 1]) for k in range(1, ny)]
    for c in y_cp:
        c.start()
    total = x_v[pl.ds(pl.multiple_of(row * yb, yb), yb), :].astype(F32) + y_s[row].astype(F32)
    with scope("y"):
        remote(y_r.at[pl.ds(1, ny - 1)], y_r.at[pl.ds(1, ny - 1)], y_ss, y_rs, ty=y_peers[0]).wait_recv()
    for k in range(1, ny):
        total = total + y_r[k].astype(F32)
    yf[row] = total.astype(BF16)
    f_cp = [remote(yf.at[row], yf.at[row], f_ss, f_rs, ty=y_peers[k - 1]) for k in range(1, ny)]
    for c in f_cp:
        c.start()
    with scope("f"):
        remote(yf.at[pl.ds(0, ny - 1)], yf.at[pl.ds(0, ny - 1)], f_ss, f_rs, ty=y_peers[0]).wait_recv()
    y_out[...] = yf[...].reshape(rows, dl)

    with scope("sends"):
        qd_cp.wait_send()
        for ref, send, recv in (
            (stat_r.at[pl.ds(1, ntx - 1)], stat_ss, stat_rs), (gq_r.at[pl.ds(1, ntx - 1)], gq_ss, gq_rs), (gb_r.at[pl.ds(1, ntx - 1)], gb_ss, gb_rs),
            (qx_s.at[pl.ds(1, nx - 1)], qx_ss, qx_rs), (qy_s.at[pl.ds(1, ny - 1)], qy_ss, qy_rs), (ay_s.at[pl.ds(1, ny - 1)], ay_ss, ay_rs),
            (y_s.at[pl.ds(1, ny - 1)], y_ss, y_rs), (yf.at[pl.ds(1, ny - 1)], f_ss, f_rs),
            (d_s, d_ss, d_rs.at[0]), (r_s, r_ss, r_rs.at[0, 0]), (g_v.at[pl.ds(1, nx - 1)], g_ss, g_rs.at[0]), (g_v.at[pl.ds(0, nx)], gp_ss, gp_rs),
            (b_v.at[pl.ds(1, nx - 1)], b_ss, b_rs.at[0, 0]), (b_v.at[pl.ds(0, nx)], bp_ss, bp_rs.at[0]),
        ):
            remote(ref, ref, send, recv, tx=partner).wait_send()


def store_kernel(ny, ntx, lens_ref, y_v, new_v, k_v, v_v, y_h, ko_h, vo_h, patch, y_sem, out_sem):
    first = (lax.axis_index("ty") * ntx + lax.axis_index("tx")) * k_v.shape[0]
    sb, ctx, hd = k_v.shape
    pieces = ctx // PIECE
    y_cp = pltpu.make_async_copy(y_v, y_h, y_sem)
    y_cp.start()

    def write(a, buf, out):
        def sequence(r, carry):
            length = lens_ref[first + r]
            spot = lax.div(length, PIECE)

            def other(c, inner):
                c = c + jnp.where(c >= spot, 1, 0)
                rest = pl.ds(pl.multiple_of(c * PIECE, PIECE), PIECE)
                pltpu.make_async_copy(buf.at[r, rest], out.at[r, rest], out_sem.at[a, r, 1]).start()
                return inner

            lax.fori_loop(0, pieces - 1, other, 0)
            at = pl.ds(pl.multiple_of(spot * PIECE, PIECE), PIECE)
            here = lax.broadcasted_iota(jnp.int32, (PIECE, hd), 0) == length - spot * PIECE
            patch[a, r] = jnp.where(here, new_v[pl.ds(a * sb + r, 1), :], buf[r, at, :].astype(F32)).astype(BF16)
            pltpu.make_async_copy(patch.at[a, r], out.at[r, at], out_sem.at[a, r, 0]).start()
            return carry

        lax.fori_loop(0, sb, sequence, 0)

    def finish(a, buf, out):
        for r in range(sb):
            pltpu.make_async_copy(patch.at[a, r], out.at[r, pl.ds(0, PIECE)], out_sem.at[a, r, 0]).wait()
            rest = pl.ds(0, ctx - PIECE)
            pltpu.make_async_copy(buf.at[r, rest], out.at[r, rest], out_sem.at[a, r, 1]).wait()

    write(0, k_v, ko_h)
    write(1, v_v, vo_h)
    y_cp.wait()
    finish(0, k_v, ko_h)
    finish(1, v_v, vo_h)


def solution(mesh):
    ny = mesh.shape["ty"]
    ntx = mesh.shape["tx"]
    nx = ntx // 2
    cache_spec = P(("dp", "ty", "tx"), None, None)
    vspec = pl.BlockSpec(memory_space=VMEM)
    hspec = pl.BlockSpec(memory_space=pltpu.HBM)
    sspec = pl.BlockSpec(memory_space=pltpu.SMEM)

    def layer_shard(x_blk, lens_part, k_blk, v_blk, gamma_blk, w_query, w_key, w_value, w_gate, w_up, w_out, w_down):
        rows, dl = x_blk.shape
        sb, ctx, hd = k_blk.shape
        qn = w_query.shape[1]
        lh = qn // hd
        qw = qn + 2 * hd
        fb = w_gate.shape[1] // ntx
        rb = rows // ntx
        yb = rows // ny

        natural = np.arange(rows)
        order = np.reshape(np.transpose(np.reshape(natural, (ny, ntx, sb)), (1, 0, 2)), (rows,))
        perm = jnp.asarray(order[:, None] == natural[None, :], dtype=BF16)
        freqs = np.power(ROPE_BASE, -(np.arange(hd // 2, dtype=np.float32) * 2.0) / hd).astype(np.float32)
        freqs = jnp.asarray(np.tile(np.concatenate([freqs, freqs])[None, :], (8, 1)))

        y_vm, new_rows, k_vm, v_vm = pl.pallas_call(
            functools.partial(step_kernel, ny, nx, dl * ntx),
            out_shape=(
                pltpu.VMEM((rows, dl), BF16),
                pltpu.VMEM((2 * sb, hd), F32),
                pltpu.VMEM(k_blk.shape, BF16),
                pltpu.VMEM(v_blk.shape, BF16),
            ),
            in_specs=[sspec] + [hspec] * 13,
            out_specs=(vspec,) * 4,
            scratch_shapes=[
                VMEM((rows, dl), BF16), VMEM((dl,), F32), VMEM((rows, rows), BF16), VMEM((8, hd), F32),
                VMEM((dl, qw), BF16), VMEM((ntx, dl, 2 * fb), BF16), VMEM((qn, dl), BF16), VMEM((ntx, fb, dl), BF16),
                VMEM((rows + 16, dl), BF16), VMEM((8, rows), F32), VMEM((ntx, 8, rows), F32),
                VMEM((16, hd), BF16), VMEM((ntx, 16, hd), BF16), VMEM((ntx, 16, hd), BF16), VMEM((ntx, 16, hd), BF16), VMEM((rows, rows), F32),
                VMEM((ntx, rb, qw), F32), VMEM((nx, rb, qw), BF16), VMEM((nx, rb, qw), BF16),
                VMEM((nx, rb, qw), BF16), VMEM((nx, rb, qw), BF16), VMEM((rb, qw), F32), VMEM((2, rb, hd), F32),
                VMEM((ny, sb * lh, hd), F32), VMEM((ny, sb * lh, hd), F32),
                VMEM((nx, rows, 2 * fb), F32), VMEM((nx, rows, 2 * fb), BF16), VMEM((nx, rows, 2 * fb), BF16),
                VMEM((nx - 1, rows, 2 * fb), BF16), VMEM((nx - 1, rows, 2 * fb), BF16),
                VMEM((2, 8, hd), F32), VMEM((ny * lh, hd), F32), VMEM((ny * lh, ctx), F32), VMEM((ny, sb * lh, hd), F32),
                VMEM((ny, sb * lh, hd), BF16), VMEM((ny, sb * lh, hd), BF16), VMEM((lh, rb, hd), F32),
                VMEM((ntx, lh, rb, hd), BF16), VMEM((ntx, rows, fb), BF16), VMEM((rows, dl), F32),
                VMEM((ny, yb, dl), BF16), VMEM((ny, yb, dl), BF16), VMEM((ny, yb, dl), BF16),
                DMA((4,)), DMA, DMA((ntx,)), DMA((2, sb)), DMA, DMA((ntx,)),
                DMA, DMA, DMA, DMA, DMA, DMA, DMA, DMA, DMA, DMA, DMA, DMA,
                DMA, DMA((nx,)), DMA, DMA((nx - 1, SUBS)),
                DMA, DMA, DMA, DMA((nx - 1,)), DMA, DMA,
                DMA, DMA((nx - 1, SUBS)), DMA, DMA((nx,)), DMA, DMA, DMA, DMA,
            ],
            compiler_params=pltpu.CompilerParams(collective_id=0, has_side_effects=True, vmem_limit_bytes=52 * 1024 * 1024),
            name="step",
        )(lens_part, x_blk, gamma_blk, perm, freqs, w_query, w_key, w_value, w_gate, w_up, k_blk, v_blk, w_out, w_down)

        return pl.pallas_call(
            functools.partial(store_kernel, ny, ntx),
            out_shape=(
                jax.ShapeDtypeStruct((rows, dl), BF16),
                jax.ShapeDtypeStruct(k_blk.shape, BF16),
                jax.ShapeDtypeStruct(v_blk.shape, BF16),
            ),
            in_specs=[sspec] + [vspec] * 4,
            out_specs=(hspec,) * 3,
            scratch_shapes=[VMEM((2, sb, PIECE, hd), BF16), DMA, DMA((2, sb, 2))],
            compiler_params=pltpu.CompilerParams(vmem_limit_bytes=4 * 1024 * 1024),
            name="store",
        )(lens_part, y_vm, new_rows, k_vm, v_vm)

    in_specs = (P("dp", "tx"), P("dp"), cache_spec, cache_spec, P("tx"), P("tx", "ty"), P("tx", None), P("tx", None), P("tx", "ty"), P("tx", "ty"), P("ty", "tx"), P("ty", "tx"))
    out_specs = (P("dp", "tx"), cache_spec, cache_spec)
    return jax.shard_map(layer_shard, mesh=mesh, in_specs=in_specs, out_specs=out_specs, check_vma=False)
```

```python
import functools

import jax
import jax.numpy as jnp
import numpy as np
from jax import lax
from jax.experimental import pallas as pl
from jax.experimental.pallas import tpu as pltpu
from jax.sharding import PartitionSpec as P

EPSILON = 1e-6
ROPE_BASE = 10000.0
LOG2E = 1.4426950408889634
MESH = pl.DeviceIdType.MESH
F32 = jnp.float32
BF16 = jnp.bfloat16
VMEM = pltpu.VMEM
DMA = pltpu.SemaphoreType.DMA
SUBS = 4
CHUNK = 1024
PIECE = 1024
scope = jax.named_scope


def remote(src, dst, send_sem, recv_sem, tx=None, ty=None):
    device = {}
    if tx is not None:
        device["tx"] = tx
    if ty is not None:
        device["ty"] = ty
    return pltpu.make_async_remote_copy(src_ref=src, dst_ref=dst, send_sem=send_sem, recv_sem=recv_sem, device_id=device, device_id_type=MESH)


def step_kernel(ny, nx, d_model, lens_ref, x_h, gamma_h, perm_h, back_h, freq_h, wq_h, wk_h, wv_h, wg_h, wu_h, k_h, v_h, wo_h, wd_h,
                y_out, new_out, kbuf, vbuf,
                x_v, gamma_v, perm_v, back_v, freq_v, wq_v, wb_v, wo_v, wd_v, h_v, stat_s, stat_r, gq_s, gq_r, gb_s, gb_r, norm,
                qp, qd_s, qd_r, qx_s, qx_r, qsum, kvs, qy_s, qy_r, own, d_s, d_r, r_s, r_r,
                turns, qs, sbuf, o32, ay_s, ay_r, g32, g_v, b_v, acc, y_s, y_r, yf,
                in_sem, wq_sem, wb_sem, kv_sem, wo_sem, wd_sem, stat_ss, stat_rs, gq_ss, gq_rs, gb_ss, gb_rs, qd_ss, qd_rs, qx_ss, qx_rs, qy_ss, qy_rs,
                d_ss, d_rs, r_ss, r_rs, ay_ss, ay_rs, g_ss, g_rs, gp_ss, gp_rs, b_ss, b_rs, bp_ss, bp_rs, y_ss, y_rs, f_ss, f_rs):
    row = lax.axis_index("ty")
    col = lax.axis_index("tx")
    chip = lax.div(col, 2)
    core = lax.rem(col, 2)
    step = 1 - 2 * core
    ntx = 2 * nx
    rows, dl = x_h.shape
    rb = rows // ntx
    sb = rb // ny
    qn = wq_h.shape[1]
    hd = wk_h.shape[1]
    qw = qn + 2 * hd
    lh = qn // hd
    heads = ny * lh
    ctx = k_h.shape[1]
    fb = wb_v.shape[2] // 2
    sub = rows // SUBS
    yb = rows // ny
    partner = lax.rem(col + 1, 2) + 2 * chip
    after = 2 * lax.rem(chip + step + nx, nx) + core
    before = 2 * lax.rem(chip - step + nx, nx) + core
    tx_peers = [lax.rem(col + k, ntx) for k in range(1, ntx)]
    x_peers = [2 * lax.rem(chip + k, nx) + core for k in range(1, nx)]
    y_peers = [lax.rem(row + k, ny) for k in range(1, ny)]
    y_froms = [lax.rem(row - k + ny, ny) for k in range(1, ny)]

    barrier = pltpu.get_barrier_semaphore()
    for peer in tx_peers:
        pl.semaphore_signal(barrier, inc=1, device_id={"tx": peer}, device_id_type=MESH)
    for peer in y_peers:
        pl.semaphore_signal(barrier, inc=1, device_id={"ty": peer}, device_id_type=MESH)

    def piece(t):
        return pl.ds(pl.multiple_of(t * sub, sub), sub)

    def block_of(s, mine):
        sign = step if mine else -step
        at = lax.rem(chip - (s + 1) * sign + 2 * nx, nx)
        return 2 * at + (core if mine else 1 - core)

    def held(kind, mine):
        away = (0, -1, 1, -2)[kind] * (step if mine else -step)
        return 2 * lax.rem(chip + away + 2 * nx, nx) + (core if mine else 1 - core)

    def block_loads(n, b):
        at = pl.ds(pl.multiple_of(b * fb, fb), fb)
        return [
            pltpu.make_async_copy(wg_h.at[:, at], wb_v.at[n, :, pl.ds(0, fb)], wb_sem.at[n]),
            pltpu.make_async_copy(wu_h.at[:, at], wb_v.at[n, :, pl.ds(fb, fb)], wb_sem.at[n]),
        ]

    def wd_load(n, b):
        at = pl.ds(pl.multiple_of(b * fb, fb), fb)
        return pltpu.make_async_copy(wd_h.at[at, :], wd_v.at[n], wd_sem.at[n])

    first_loads = [
        pltpu.make_async_copy(x_h, x_v, in_sem.at[0]),
        pltpu.make_async_copy(perm_h, perm_v, in_sem.at[1]),
        pltpu.make_async_copy(gamma_h, gamma_v, in_sem.at[2]),
        pltpu.make_async_copy(freq_h, freq_v, in_sem.at[3]),
        pltpu.make_async_copy(back_h, back_v, in_sem.at[4]),
    ]
    q_loads = [
        pltpu.make_async_copy(wq_h, wq_v.at[:, pl.ds(0, qn)], wq_sem),
        pltpu.make_async_copy(wk_h, wq_v.at[:, pl.ds(qn, hd)], wq_sem),
        pltpu.make_async_copy(wv_h, wq_v.at[:, pl.ds(qn + hd, hd)], wq_sem),
    ]
    k_in = [pltpu.make_async_copy(k_h.at[r], kbuf.at[r], kv_sem.at[0, r]) for r in range(sb)]
    v_in = [pltpu.make_async_copy(v_h.at[r], vbuf.at[r], kv_sem.at[1, r]) for r in range(sb)]
    wo_load = pltpu.make_async_copy(wo_h, wo_v, wo_sem)
    def start_block(s, mine):
        for c in block_loads(2 * s + int(mine), block_of(s, mine)):
            c.start()

    for c in first_loads + q_loads:
        c.start()
    for c in first_loads:
        c.wait()
    start_block(0, False)
    start_block(0, True)

    xp = jnp.dot(perm_v[...], x_v[...], preferred_element_type=F32)
    own_mean = jnp.sum(xp, axis=1, keepdims=True) / dl
    xc = xp - own_mean
    gamma = gamma_v[...].reshape(1, dl)
    h_v[:rows] = (xc * gamma).astype(BF16)
    extra = lax.broadcasted_iota(jnp.int32, (16, dl), 0)
    h_v[rows:] = jnp.where(extra == 0, gamma, jnp.where(extra == 1, gamma - gamma.astype(BF16).astype(F32), 0.0)).astype(BF16)
    lane = lax.broadcasted_iota(jnp.int32, (rows, rows), 1)
    both = jnp.where(lane == 0, own_mean, jnp.where(lane == 1, jnp.sum(xc * xc, axis=1, keepdims=True), 0.0))
    stat_s[...] = jnp.transpose(both)[:8]

    def gamma_row(vals, tiles):
        row_sum = vals[0:1, :] + vals[1:2, :]
        parts = [row_sum[:, n * hd:(n + 1) * hd] for n in range(tiles)]
        return jnp.concatenate(parts + [jnp.zeros((16 - tiles, hd), F32)], axis=0).astype(BF16)

    pltpu.make_async_copy(wq_v, wq_v, wq_sem).wait()
    start_block(1, False)
    part = jnp.dot(h_v[...], wq_v[...], preferred_element_type=F32)
    qp[...] = part[:rows].reshape(ntx, rb, qw)
    gq_s[...] = gamma_row(part[rows:], qw // hd)
    for n in range(nx):
        qd_s[n] = qp[2 * n + 1 - core].astype(BF16)
    qd_cp = remote(qd_s, qd_r, qd_ss, qd_rs, tx=partner)
    stat_cp = [remote(stat_s, stat_r.at[k], stat_ss, stat_rs, tx=tx_peers[k - 1]) for k in range(1, ntx)]
    gq_cp = [remote(gq_s, gq_r.at[k], gq_ss, gq_rs, tx=tx_peers[k - 1]) for k in range(1, ntx)]
    gb_cp = [remote(gb_s.at[tx_peers[k - 1]], gb_r.at[k], gb_ss, gb_rs, tx=tx_peers[k - 1]) for k in range(1, ntx)]
    with scope("greet"):
        pl.semaphore_wait(barrier, ntx - 1 + ny - 1)
    qd_cp.start()
    for c in stat_cp + gq_cp:
        c.start()
    stat_r[0] = stat_s[...]
    gq_r[0] = gq_s[...]

    def rest_of_norm():
        with scope("stat"):
            remote(stat_r.at[pl.ds(1, ntx - 1)], stat_r.at[pl.ds(1, ntx - 1)], stat_ss, stat_rs, tx=partner).wait_recv()
            remote(gq_r.at[pl.ds(1, ntx - 1)], gq_r.at[pl.ds(1, ntx - 1)], gq_ss, gq_rs, tx=partner).wait_recv()
        means = jnp.concatenate([stat_r[k, 0:1, :] for k in range(ntx)], axis=0)
        squares = jnp.concatenate([stat_r[k, 1:2, :] for k in range(ntx)], axis=0)
        off = means - jnp.sum(means, axis=0, keepdims=True) / ntx
        var = jnp.sum(squares, axis=0, keepdims=True) / d_model + jnp.sum(off * off, axis=0, keepdims=True) / ntx
        scale = lax.rsqrt(var + EPSILON)
        norm[...] = jnp.transpose(jnp.concatenate([off, scale, jnp.zeros((rows - ntx - 1, rows), F32)], axis=0))

    def normed(vals, at, g_ref):
        cols = norm[at, :]
        tiles = []
        for n in range(vals.shape[1] // hd):
            tile = vals[:, n * hd:(n + 1) * hd]
            for k in range(ntx):
                tile = tile + cols[:, k:k + 1] * g_ref[k, n:n + 1, :].astype(F32)
            tiles.append(tile * cols[:, ntx:ntx + 1])
        return jnp.concatenate(tiles, axis=1)


    def q_of(away):
        at = lax.rem(chip + away * step + 2 * nx, nx)
        return qp[2 * at + core] + qd_r[at].astype(F32)

    def qx_copy(slot, to):
        return remote(qx_s.at[slot], qx_r.at[slot], qx_ss, qx_rs.at[slot], tx=to)

    qy_cp = [remote(qy_s.at[y_peers[k - 1]], qy_r.at[row], qy_ss, qy_rs, ty=y_peers[k - 1]) for k in range(1, ny)]

    def q_pair():
        with scope("qd"):
            qd_cp.wait_recv()
        qx_s[0] = q_of(2).astype(BF16)
        qx_copy(0, after).start()
        qx_s[1] = q_of(-1).astype(BF16)
        qx_copy(1, before).start()

    def q_relay():
        with scope("qa"):
            qx_copy(0, after).wait_recv()
        qx_s[2] = (q_of(1) + qx_r[0].astype(F32)).astype(BF16)
        qx_copy(2, after).start()

    def q_rows():
        mine = q_of(0)
        rest_of_norm()
        with scope("qx"):
            qx_copy(1, before).wait_recv()
            qx_copy(2, after).wait_recv()
        mine = mine + qx_r[1].astype(F32) + qx_r[2].astype(F32)
        mine = normed(mine, pl.ds(pl.multiple_of(col * rb, rb), rb), gq_r)
        qsum[...] = mine
        kvs[0] = mine[:, qn:qn + hd]
        kvs[1] = mine[:, qn + hd:]
        for a in range(ny):
            for n in range(lh):
                qy_s[a, n * sb:(n + 1) * sb, :] = qsum[a * sb:(a + 1) * sb, n * hd:(n + 1) * hd]
        for c in qy_cp:
            c.start()
        qy_r[row] = qy_s[row]

    def tables():
        at_row = lax.broadcasted_iota(jnp.int32, (8, hd), 0)
        places = jnp.zeros((8, hd), F32)
        for r in range(sb):
            places = jnp.where(at_row == r, lens_ref[(row * ntx + col) * sb + r].astype(F32), places)
        angles = places * freq_v[...]
        turns[0] = jnp.cos(angles)
        low_half = lax.broadcasted_iota(jnp.int32, (8, hd), 1) < hd // 2
        sines = jnp.sin(angles)
        turns[1] = jnp.where(low_half, -sines, sines)

    def d_copy(s):
        return remote(d_s.at[s], d_r.at[s], d_ss, d_rs.at[s], tx=partner)

    def r_copy(s, t):
        return remote(r_s.at[s, piece(t)], r_r.at[s, piece(t)], r_ss, r_rs.at[s, t], tx=after)

    def product(s, carry):
        @pl.when(s == 2)
        def _():
            q_relay()

        pltpu.make_async_copy(wb_v.at[2 * s], wb_v.at[2 * s], wb_sem.at[2 * s]).wait()

        @pl.when(s < nx - 1)
        def _():
            start_block(s + 1, True)

        part = jnp.dot(h_v[...], wb_v[2 * s], preferred_element_type=F32)
        d_s[s] = part[:rows].astype(BF16)
        d_copy(s).start()
        gb_s[block_of(s, False)] = gamma_row(part[rows:], 2 * fb // hd)

        @pl.when(s == 0)
        def _():
            q_pair()

        pltpu.make_async_copy(wb_v.at[2 * s + 1], wb_v.at[2 * s + 1], wb_sem.at[2 * s + 1]).wait()

        @pl.when(s < nx - 2)
        def _():
            start_block(s + 2, False)

        part = jnp.dot(h_v[...], wb_v[2 * s + 1], preferred_element_type=F32)
        own[s] = part[:rows]
        gb_s[block_of(s, True)] = gamma_row(part[rows:], 2 * fb // hd)

        @pl.when(s == 0)
        def _():
            with scope("d0"):
                d_copy(0).wait_recv()
            for t in range(SUBS):
                at = piece(t)
                r_s[0, at] = (own[0, at] + d_r[0, at].astype(F32)).astype(BF16)
                r_copy(0, t).start()

        return carry

    with scope("products"):
        lax.fori_loop(0, nx, product, 0)
    for c in gb_cp + k_in + v_in:
        c.start()
    gb_r[0] = gb_s[col]
    tables()

    def ring(s, t):
        at = piece(t)
        if t == 0:
            with scope("d%d" % s):
                d_copy(s).wait_recv()
        part = own[s, at] + d_r[s, at].astype(F32)
        with scope("r%d%d" % (s, t)):
            r_copy(s - 1, t).wait_recv()
        part = part + r_r[s - 1, at].astype(F32)
        if s < nx - 1:
            r_s[s, at] = part.astype(BF16)
            r_copy(s, t).start()
        else:
            if t == 0:
                with scope("gb"):
                    remote(gb_r.at[pl.ds(1, ntx - 1)], gb_r.at[pl.ds(1, ntx - 1)], gb_ss, gb_rs, tx=partner).wait_recv()
            part = normed(part, at, gb_r)
            gate = part[:, :fb].astype(BF16).astype(F32)
            up = part[:, fb:].astype(BF16).astype(F32)
            b_v[col, at] = (gate * (1.0 / (1.0 + jnp.exp(-gate))) * up).astype(BF16)
            act_out(t)

    def turn(vals, r):
        return vals * turns[0, r:r + 1, :] + pltpu.roll(vals, hd // 2, 1) * turns[1, r:r + 1, :]

    def attend(r):
        length = lens_ref[(row * ntx + col) * sb + r]
        for a in range(ny):
            qs[a * lh:(a + 1) * lh, :] = turn(qy_r[a, pl.ds(r, lh, stride=sb), :], r)
        q = qs[...].astype(BF16)
        k_new = turn(kvs[0, pl.ds(row * sb + r, 1), :], r).astype(BF16).astype(F32)
        v_new = kvs[1, pl.ds(row * sb + r, 1), :].astype(BF16).astype(F32)
        new_out[r:r + 1, :] = k_new
        new_out[sb + r:sb + r + 1, :] = v_new
        k_in[r].wait()
        s_new = jnp.sum(q.astype(F32) * k_new, axis=1, keepdims=True)
        top = jnp.full((heads, hd), -1e30, F32)
        for c in range(ctx // CHUNK):
            s = lax.dot_general(q, kbuf[r, c * CHUNK:(c + 1) * CHUNK, :], (((1,), (1,)), ((), ())), preferred_element_type=F32)
            pos = lax.broadcasted_iota(jnp.int32, (1, CHUNK), 1) + c * CHUNK
            s = jnp.where(pos < length, s, -1e30)
            sbuf[:, c * CHUNK:(c + 1) * CHUNK] = s
            for t in range(CHUNK // hd):
                top = jnp.maximum(top, s[:, t * hd:(t + 1) * hd])
        high = jnp.maximum(jnp.max(top, axis=1, keepdims=True), s_new)
        rate = hd ** -0.5 * LOG2E
        e_new = jnp.exp2((s_new - high) * rate)
        low = jnp.zeros((heads, hd), F32)
        out = e_new.astype(BF16).astype(F32) * v_new
        v_in[r].wait()
        for c in range(ctx // CHUNK):
            e = jnp.exp2((sbuf[:, c * CHUNK:(c + 1) * CHUNK] - high) * rate)
            for t in range(CHUNK // hd):
                low = low + e[:, t * hd:(t + 1) * hd]
            out = out + jnp.dot(e.astype(BF16), vbuf[r, c * CHUNK:(c + 1) * CHUNK, :], preferred_element_type=F32)
        out = out / (jnp.sum(low, axis=1, keepdims=True) + e_new)
        for a in range(ny):
            o32[a, pl.ds(r, lh, stride=sb), :] = out[a * lh:(a + 1) * lh]

    def b_send(kind, t, slot, to):
        b = held(kind, True)
        return remote(b_v.at[b, piece(t)], b_v.at[b, piece(t)], b_ss, b_rs.at[slot - 1, t], tx=to)

    def b_in(kind, t):
        b = held(kind, True)
        return remote(b_v.at[b, piece(t)], b_v.at[b, piece(t)], b_ss, b_rs.at[kind - 1, t], tx=after)

    def b_pair(kind, t):
        b = held(kind, True)
        return remote(b_v.at[b, piece(t)], b_v.at[b, piece(t)], bp_ss, bp_rs.at[kind, t * 2 // SUBS], tx=partner)

    def act_out(t):
        b_send(0, t, 1, after).start()
        b_send(0, t, 2, before).start()
        b_pair(0, t).start()

    def act_in(kind, half):
        for t in range(half * SUBS // 2, (half + 1) * SUBS // 2):
            with scope("b%d%d" % (kind, t)):
                b_in(kind, t).wait_recv()
            if kind == 1:
                b_send(1, t, 3, after).start()
            b_pair(kind, t).start()

    ay_cp = [remote(ay_s.at[y_peers[k - 1]], ay_r.at[row], ay_ss, ay_rs, ty=y_peers[k - 1]) for k in range(1, ny)]

    def g_send(kind, slot, to):
        at = held(kind, True)
        return remote(g_v.at[at], g_v.at[at], g_ss, g_rs.at[slot - 1], tx=to)

    def g_pair(kind):
        at = held(kind, True)
        return remote(g_v.at[at], g_v.at[at], gp_ss, gp_rs, tx=partner)

    def g_in(kind):
        at = held(kind, True)
        with scope("g%d" % kind):
            remote(g_v.at[at], g_v.at[at], g_ss, g_rs.at[kind - 1], tx=after).wait_recv()
        if kind == 1:
            g_send(1, 3, after).start()
        g_pair(kind).start()

    def att_out():
        ay_s[...] = o32[...].astype(BF16)
        for c in ay_cp:
            c.start()
        ay_r[row] = ay_s[row]

    def att_rows():
        with scope("ay"):
            remote(ay_r.at[pl.ds(0, ny - 1)], ay_r.at[pl.ds(0, ny - 1)], ay_ss, ay_rs, ty=y_peers[0]).wait_recv()
        for a in range(ny):
            part = ay_r[a].astype(F32)
            for n in range(lh):
                g32[n, a * sb:(a + 1) * sb, :] = part[n * sb:(n + 1) * sb, :]
        g_v[col] = g32[...].astype(BF16)
        g_send(0, 1, after).start()
        g_send(0, 2, before).start()
        g_pair(0).start()

    mid = rows // 2

    def half_rows(half):
        return pl.ds(half * mid, mid)

    def down(n, half):
        if half == 0:
            wd_load(n, 0).wait()
        part = jnp.dot(b_v[held(n // 2, n % 2 == 0), half_rows(half)], wd_v[n], preferred_element_type=F32)
        acc[half_rows(half)] = part if n == 0 else acc[half_rows(half)] + part

    def from_pair(kind, half):
        b = held(kind, False)
        with scope("bp%d%d" % (kind, half)):
            remote(b_v.at[b, half_rows(half)], b_v.at[b, half_rows(half)], bp_ss, bp_rs.at[kind, half], tx=partner).wait_recv()

    def att_down(half):
        at = pl.ds(half * nx, nx)
        for n in range(0, lh, 2):
            pair = jnp.concatenate([g_v[at, n].reshape(mid, hd), g_v[at, n + 1].reshape(mid, hd)], axis=1)
            acc[half_rows(half)] += jnp.dot(pair, wo_v[n * hd:(n + 2) * hd, :], preferred_element_type=F32)

    def y_out_half(half):
        part = jnp.dot(back_v[...], acc[half_rows(half)].astype(BF16), preferred_element_type=F32)
        y_s[half] = part.astype(BF16).reshape(ny, yb // 2, dl)
        for k in range(1, ny):
            remote(y_s.at[half, y_peers[k - 1]], y_r.at[half, k], y_ss.at[half], y_rs.at[half], ty=y_peers[k - 1]).start()

    def y_sum_half(half):
        at = pl.ds(pl.multiple_of(row * yb + half * (yb // 2), yb // 2), yb // 2)
        total = x_v[at, :].astype(F32) + y_s[half, row].astype(F32)
        rest = y_r.at[half, pl.ds(1, ny - 1)]
        with scope("y%d" % half):
            remote(rest, rest, y_ss.at[half], y_rs.at[half], ty=y_peers[0]).wait_recv()
        for k in range(1, ny):
            total = total + y_r[half, k].astype(F32)
        yf[half, row] = total.astype(BF16)
        for k in range(1, ny):
            remote(yf.at[half, row], yf.at[half, row], f_ss.at[half], f_rs.at[half], ty=y_peers[k - 1]).start()

    def y_all_half(half):
        rest = yf.at[half, pl.ds(0, ny - 1)]
        with scope("f%d" % half):
            remote(rest, rest, f_ss.at[half], f_rs.at[half], ty=y_peers[0]).wait_recv()
        for a in range(ny):
            y_out[a * yb + half * (yb // 2):a * yb + (half + 1) * (yb // 2), :] = yf[half, a]

    q_rows()
    for t in range(SUBS):
        ring(1, t)
    for n in range(ntx):
        wd_load(n, held(n // 2, n % 2 == 0)).start()
    wo_load.start()
    with scope("qy"):
        remote(qy_r.at[pl.ds(0, ny - 1)], qy_r.at[pl.ds(0, ny - 1)], qy_ss, qy_rs, ty=y_peers[0]).wait_recv()
    for t in range(SUBS):
        with scope("a%d" % t):
            attend(t)
        if t == SUBS - 1:
            att_out()
        ring(2, t)
    for t in range(SUBS - 1):
        ring(3, t)
    att_rows()
    ring(3, SUBS - 1)
    down(0, 0)
    act_in(1, 0)
    g_in(1)
    act_in(2, 0)
    down(0, 1)
    act_in(1, 1)
    g_in(2)
    act_in(2, 1)
    from_pair(0, 0)
    down(1, 0)
    down(2, 0)
    down(4, 0)
    act_in(3, 0)
    g_in(3)
    from_pair(1, 0)
    down(3, 0)
    from_pair(2, 0)
    down(5, 0)
    down(6, 0)
    act_in(3, 1)
    from_pair(3, 0)
    down(7, 0)
    with scope("gp"):
        remote(g_v.at[pl.ds(0, nx)], g_v.at[pl.ds(0, nx)], gp_ss, gp_rs, tx=partner).wait_recv()
    wo_load.wait()
    att_down(0)
    y_out_half(0)
    for kind in range(nx):
        from_pair(kind, 1)
        if kind > 0:
            down(2 * kind, 1)
        down(2 * kind + 1, 1)
    att_down(1)
    y_out_half(1)
    y_sum_half(0)
    y_sum_half(1)
    y_all_half(0)
    y_all_half(1)

    with scope("sends"):
        qd_cp.wait_send()
        for ref, send, recv in (
            (stat_r.at[pl.ds(1, ntx - 1)], stat_ss, stat_rs), (gq_r.at[pl.ds(1, ntx - 1)], gq_ss, gq_rs), (gb_r.at[pl.ds(1, ntx - 1)], gb_ss, gb_rs),
            (qx_s, qx_ss, qx_rs.at[0]), (qy_s.at[pl.ds(1, ny - 1)], qy_ss, qy_rs), (ay_s.at[pl.ds(1, ny - 1)], ay_ss, ay_rs),
            *((y_s.at[half, pl.ds(1, ny - 1)], y_ss.at[half], y_rs.at[half]) for half in range(2)),
            *((yf.at[half, pl.ds(1, ny - 1)], f_ss.at[half], f_rs.at[half]) for half in range(2)),
            (d_s, d_ss, d_rs.at[0]), (r_s, r_ss, r_rs.at[0, 0]), (g_v.at[pl.ds(1, nx - 1)], g_ss, g_rs.at[0]), (g_v.at[pl.ds(0, nx)], gp_ss, gp_rs),
            (b_v.at[pl.ds(1, nx - 1)], b_ss, b_rs.at[0, 0]), (b_v.at[pl.ds(0, nx)], bp_ss, bp_rs.at[0, 0]),
        ):
            remote(ref, ref, send, recv, tx=partner).wait_send()


def store_kernel(ny, ntx, lens_ref, y_v, new_v, k_v, v_v, y_h, ko_h, vo_h, patch, y_sem, out_sem):
    first = (lax.axis_index("ty") * ntx + lax.axis_index("tx")) * k_v.shape[0]
    sb, ctx, hd = k_v.shape
    pieces = ctx // PIECE
    y_cp = pltpu.make_async_copy(y_v, y_h, y_sem)
    y_cp.start()

    def write(a, buf, out):
        def sequence(r, carry):
            length = lens_ref[first + r]
            spot = lax.div(length, PIECE)

            def other(c, inner):
                c = c + jnp.where(c >= spot, 1, 0)
                rest = pl.ds(pl.multiple_of(c * PIECE, PIECE), PIECE)
                pltpu.make_async_copy(buf.at[r, rest], out.at[r, rest], out_sem.at[a, r, 1]).start()
                return inner

            lax.fori_loop(0, pieces - 1, other, 0)
            at = pl.ds(pl.multiple_of(spot * PIECE, PIECE), PIECE)
            here = lax.broadcasted_iota(jnp.int32, (PIECE, hd), 0) == length - spot * PIECE
            patch[a, r] = jnp.where(here, new_v[pl.ds(a * sb + r, 1), :], buf[r, at, :].astype(F32)).astype(BF16)
            pltpu.make_async_copy(patch.at[a, r], out.at[r, at], out_sem.at[a, r, 0]).start()
            return carry

        lax.fori_loop(0, sb, sequence, 0)

    def finish(a, buf, out):
        for r in range(sb):
            pltpu.make_async_copy(patch.at[a, r], out.at[r, pl.ds(0, PIECE)], out_sem.at[a, r, 0]).wait()
            rest = pl.ds(0, ctx - PIECE)
            pltpu.make_async_copy(buf.at[r, rest], out.at[r, rest], out_sem.at[a, r, 1]).wait()

    write(0, k_v, ko_h)
    write(1, v_v, vo_h)
    y_cp.wait()
    finish(0, k_v, ko_h)
    finish(1, v_v, vo_h)


def solution(mesh):
    ny = mesh.shape["ty"]
    ntx = mesh.shape["tx"]
    nx = ntx // 2
    cache_spec = P(("dp", "ty", "tx"), None, None)
    vspec = pl.BlockSpec(memory_space=VMEM)
    hspec = pl.BlockSpec(memory_space=pltpu.HBM)
    sspec = pl.BlockSpec(memory_space=pltpu.SMEM)

    def layer_shard(x_blk, lens_part, k_blk, v_blk, gamma_blk, w_query, w_key, w_value, w_gate, w_up, w_out, w_down):
        rows, dl = x_blk.shape
        sb, ctx, hd = k_blk.shape
        qn = w_query.shape[1]
        lh = qn // hd
        qw = qn + 2 * hd
        fb = w_gate.shape[1] // ntx
        rb = rows // ntx
        yb = rows // ny

        natural = np.arange(rows)
        order = np.reshape(np.transpose(np.reshape(natural, (ny, ntx, sb)), (1, 0, 2)), (rows,))
        perm = jnp.asarray(order[:, None] == natural[None, :], dtype=BF16)
        part = np.arange(rows // 2)
        order = np.reshape(np.transpose(np.reshape(part, (nx, ny, sb)), (1, 0, 2)), (rows // 2,))
        back = jnp.asarray(order[:, None] == part[None, :], dtype=BF16)
        freqs = np.power(ROPE_BASE, -(np.arange(hd // 2, dtype=np.float32) * 2.0) / hd).astype(np.float32)
        freqs = jnp.asarray(np.tile(np.concatenate([freqs, freqs])[None, :], (8, 1)))

        y_vm, new_rows, k_vm, v_vm = pl.pallas_call(
            functools.partial(step_kernel, ny, nx, dl * ntx),
            out_shape=(
                pltpu.VMEM((rows, dl), BF16),
                pltpu.VMEM((2 * sb, hd), F32),
                pltpu.VMEM(k_blk.shape, BF16),
                pltpu.VMEM(v_blk.shape, BF16),
            ),
            in_specs=[sspec] + [hspec] * 14,
            out_specs=(vspec,) * 4,
            scratch_shapes=[
                VMEM((rows, dl), BF16), VMEM((dl,), F32), VMEM((rows, rows), BF16), VMEM((rows // 2, rows // 2), BF16), VMEM((8, hd), F32),
                VMEM((dl, qw), BF16), VMEM((ntx, dl, 2 * fb), BF16), VMEM((qn, dl), BF16), VMEM((ntx, fb, dl), BF16),
                VMEM((rows + 16, dl), BF16), VMEM((8, rows), F32), VMEM((ntx, 8, rows), F32),
                VMEM((16, hd), BF16), VMEM((ntx, 16, hd), BF16), VMEM((ntx, 16, hd), BF16), VMEM((ntx, 16, hd), BF16), VMEM((rows, rows), F32),
                VMEM((ntx, rb, qw), F32), VMEM((nx, rb, qw), BF16), VMEM((nx, rb, qw), BF16),
                VMEM((3, rb, qw), BF16), VMEM((3, rb, qw), BF16), VMEM((rb, qw), F32), VMEM((2, rb, hd), F32),
                VMEM((ny, sb * lh, hd), F32), VMEM((ny, sb * lh, hd), F32),
                VMEM((nx, rows, 2 * fb), F32), VMEM((nx, rows, 2 * fb), BF16), VMEM((nx, rows, 2 * fb), BF16),
                VMEM((nx - 1, rows, 2 * fb), BF16), VMEM((nx - 1, rows, 2 * fb), BF16),
                VMEM((2, 8, hd), F32), VMEM((ny * lh, hd), F32), VMEM((ny * lh, ctx), F32), VMEM((ny, sb * lh, hd), F32),
                VMEM((ny, sb * lh, hd), BF16), VMEM((ny, sb * lh, hd), BF16), VMEM((lh, rb, hd), F32),
                VMEM((ntx, lh, rb, hd), BF16), VMEM((ntx, rows, fb), BF16), VMEM((rows, dl), F32),
                VMEM((2, ny, yb // 2, dl), BF16), VMEM((2, ny, yb // 2, dl), BF16), VMEM((2, ny, yb // 2, dl), BF16),
                DMA((5,)), DMA, DMA((ntx,)), DMA((2, sb)), DMA, DMA((ntx,)),
                DMA, DMA, DMA, DMA, DMA, DMA, DMA, DMA, DMA, DMA((3,)), DMA, DMA,
                DMA, DMA((nx,)), DMA, DMA((nx - 1, SUBS)),
                DMA, DMA, DMA, DMA((nx - 1,)), DMA, DMA,
                DMA, DMA((nx - 1, SUBS)), DMA, DMA((nx, 2)), DMA((2,)), DMA((2,)), DMA((2,)), DMA((2,)),
            ],
            compiler_params=pltpu.CompilerParams(collective_id=0, has_side_effects=True, vmem_limit_bytes=52 * 1024 * 1024),
            name="step",
        )(lens_part, x_blk, gamma_blk, perm, back, freqs, w_query, w_key, w_value, w_gate, w_up, k_blk, v_blk, w_out, w_down)

        return pl.pallas_call(
            functools.partial(store_kernel, ny, ntx),
            out_shape=(
                jax.ShapeDtypeStruct((rows, dl), BF16),
                jax.ShapeDtypeStruct(k_blk.shape, BF16),
                jax.ShapeDtypeStruct(v_blk.shape, BF16),
            ),
            in_specs=[sspec] + [vspec] * 4,
            out_specs=(hspec,) * 3,
            scratch_shapes=[VMEM((2, sb, PIECE, hd), BF16), DMA, DMA((2, sb, 2))],
            compiler_params=pltpu.CompilerParams(vmem_limit_bytes=6 * 1024 * 1024),
            name="store",
        )(lens_part, y_vm, new_rows, k_vm, v_vm)

    in_specs = (P("dp", "tx"), P("dp"), cache_spec, cache_spec, P("tx"), P("tx", "ty"), P("tx", None), P("tx", None), P("tx", "ty"), P("tx", "ty"), P("ty", "tx"), P("ty", "tx"))
    out_specs = (P("dp", "tx"), cache_spec, cache_spec)
    return jax.shard_map(layer_shard, mesh=mesh, in_specs=in_specs, out_specs=out_specs, check_vma=False)
```

```python
import functools

import jax
import jax.numpy as jnp
import numpy as np
from jax import lax
from jax.experimental import pallas as pl
from jax.experimental.pallas import tpu as pltpu
from jax.sharding import PartitionSpec as P

EPSILON = 1e-6
ROPE_BASE = 10000.0
LOG2E = 1.4426950408889634
MESH = pl.DeviceIdType.MESH
F32 = jnp.float32
BF16 = jnp.bfloat16
VMEM = pltpu.VMEM
DMA = pltpu.SemaphoreType.DMA
SUBS = 4
CHUNK = 1024
PIECE = 512
scope = jax.named_scope


def remote(src, dst, send_sem, recv_sem, tx=None, ty=None):
    device = {}
    if tx is not None:
        device["tx"] = tx
    if ty is not None:
        device["ty"] = ty
    return pltpu.make_async_remote_copy(src_ref=src, dst_ref=dst, send_sem=send_sem, recv_sem=recv_sem, device_id=device, device_id_type=MESH)


def step_kernel(ny, nx, d_model, lens_ref, x_h, gamma_h, perm_h, back_h, freq_h, wq_h, wk_h, wv_h, wg_h, wu_h, k_h, v_h, wo_h, wd_h,
                y_out, new_out, kbuf, vbuf,
                x_v, gamma_v, perm_v, back_v, freq_v, wq_v, wb_v, wo_v, wd_v, h_v, stat_s, stat_r, gq_s, gq_r, gb_s, gb_r, norm,
                qp, qd_s, qd_r, qx_s, qx_r, qsum, kvs, qy_s, qy_r, own, d_s, d_r, r_s, r_r,
                turns, qs, sbuf, o32, ay_s, ay_r, g32, g_v, b_v, acc, y_s, y_r, yf,
                in_sem, wq_sem, wb_sem, kv_sem, wo_sem, wd_sem, stat_ss, stat_rs, gq_ss, gq_rs, gb_ss, gb_rs, qd_ss, qd_rs, qx_ss, qx_rs, qy_ss, qy_rs,
                d_ss, d_rs, r_ss, r_rs, ay_ss, ay_rs, g_ss, g_rs, gp_ss, gp_rs, b_ss, b_rs, bp_ss, bp_rs, y_ss, y_rs, f_ss, f_rs):
    row = lax.axis_index("ty")
    col = lax.axis_index("tx")
    chip = lax.div(col, 2)
    core = lax.rem(col, 2)
    step = 1 - 2 * core
    ntx = 2 * nx
    rows, dl = x_h.shape
    rb = rows // ntx
    sb = rb // ny
    qn = wq_h.shape[1]
    hd = wk_h.shape[1]
    qw = qn + 2 * hd
    lh = qn // hd
    heads = ny * lh
    ctx = k_h.shape[1]
    fb = wb_v.shape[2] // 2
    sub = rows // SUBS
    yb = rows // ny
    partner = lax.rem(col + 1, 2) + 2 * chip
    after = 2 * lax.rem(chip + step + nx, nx) + core
    left = 2 * lax.rem(chip + nx - 1, nx) + core
    right = 2 * lax.rem(chip + 1, nx) + core
    tx_peers = [lax.rem(col + k, ntx) for k in range(1, ntx)]
    x_peers = [2 * lax.rem(chip + k, nx) + core for k in range(1, nx)]
    y_peers = [lax.rem(row + k, ny) for k in range(1, ny)]
    y_froms = [lax.rem(row - k + ny, ny) for k in range(1, ny)]

    barrier = pltpu.get_barrier_semaphore()
    for peer in tx_peers:
        pl.semaphore_signal(barrier, inc=1, device_id={"tx": peer}, device_id_type=MESH)
    for peer in y_peers:
        pl.semaphore_signal(barrier, inc=1, device_id={"ty": peer}, device_id_type=MESH)

    def piece(t):
        return pl.ds(pl.multiple_of(t * sub, sub), sub)

    def block_of(s, mine):
        sign = step if mine else -step
        at = lax.rem(chip - (s + 1) * sign + 2 * nx, nx)
        return 2 * at + (core if mine else 1 - core)

    def held(kind, mine):
        return 2 * lax.rem(chip + (0, 1, nx - 1, 2)[kind], nx) + (core if mine else 1 - core)

    def block_loads(n, b):
        at = pl.ds(pl.multiple_of(b * fb, fb), fb)
        return [
            pltpu.make_async_copy(wg_h.at[:, at], wb_v.at[n, :, pl.ds(0, fb)], wb_sem.at[n]),
            pltpu.make_async_copy(wu_h.at[:, at], wb_v.at[n, :, pl.ds(fb, fb)], wb_sem.at[n]),
        ]

    def wd_load(n, b):
        at = pl.ds(pl.multiple_of(b * fb, fb), fb)
        return pltpu.make_async_copy(wd_h.at[at, :], wd_v.at[n], wd_sem.at[n])

    first_loads = [
        pltpu.make_async_copy(x_h, x_v, in_sem.at[0]),
        pltpu.make_async_copy(perm_h, perm_v, in_sem.at[1]),
        pltpu.make_async_copy(gamma_h, gamma_v, in_sem.at[2]),
        pltpu.make_async_copy(freq_h, freq_v, in_sem.at[3]),
        pltpu.make_async_copy(back_h, back_v, in_sem.at[4]),
    ]
    q_loads = [
        pltpu.make_async_copy(wq_h, wq_v.at[:, pl.ds(0, qn)], wq_sem),
        pltpu.make_async_copy(wk_h, wq_v.at[:, pl.ds(qn, hd)], wq_sem),
        pltpu.make_async_copy(wv_h, wq_v.at[:, pl.ds(qn + hd, hd)], wq_sem),
    ]
    k_in = [pltpu.make_async_copy(k_h.at[r], kbuf.at[r], kv_sem.at[0, r]) for r in range(sb)]
    v_in = [pltpu.make_async_copy(v_h.at[r], vbuf.at[r], kv_sem.at[1, r]) for r in range(sb)]
    wo_load = pltpu.make_async_copy(wo_h, wo_v, wo_sem)
    def start_block(s, mine):
        for c in block_loads(2 * s + int(mine), block_of(s, mine)):
            c.start()

    for c in first_loads + q_loads:
        c.start()
    for c in first_loads:
        c.wait()
    start_block(0, False)
    start_block(0, True)

    xp = jnp.dot(perm_v[...], x_v[...], preferred_element_type=F32)
    own_mean = jnp.sum(xp, axis=1, keepdims=True) / dl
    xc = xp - own_mean
    gamma = gamma_v[...].reshape(1, dl)
    h_v[:rows] = (xc * gamma).astype(BF16)
    extra = lax.broadcasted_iota(jnp.int32, (16, dl), 0)
    h_v[rows:] = jnp.where(extra == 0, gamma, jnp.where(extra == 1, gamma - gamma.astype(BF16).astype(F32), 0.0)).astype(BF16)
    lane = lax.broadcasted_iota(jnp.int32, (rows, rows), 1)
    both = jnp.where(lane == 0, own_mean, jnp.where(lane == 1, jnp.sum(xc * xc, axis=1, keepdims=True), 0.0))
    stat_s[...] = jnp.transpose(both)[:8]

    def gamma_row(vals, tiles):
        row_sum = vals[0:1, :] + vals[1:2, :]
        parts = [row_sum[:, n * hd:(n + 1) * hd] for n in range(tiles)]
        return jnp.concatenate(parts + [jnp.zeros((16 - tiles, hd), F32)], axis=0).astype(BF16)

    pltpu.make_async_copy(wq_v, wq_v, wq_sem).wait()
    start_block(1, False)
    part = jnp.dot(h_v[...], wq_v[...], preferred_element_type=F32)
    qp[...] = part[:rows].reshape(ntx, rb, qw)
    gq_s[...] = gamma_row(part[rows:], qw // hd)
    for n in range(nx):
        qd_s[n] = qp[2 * n + 1 - core].astype(BF16)
    qd_cp = remote(qd_s, qd_r, qd_ss, qd_rs, tx=partner)
    stat_cp = [remote(stat_s, stat_r.at[k], stat_ss, stat_rs, tx=tx_peers[k - 1]) for k in range(1, ntx)]
    gq_cp = [remote(gq_s, gq_r.at[k], gq_ss, gq_rs, tx=tx_peers[k - 1]) for k in range(1, ntx)]
    gb_cp = [remote(gb_s.at[tx_peers[k - 1]], gb_r.at[k], gb_ss, gb_rs, tx=tx_peers[k - 1]) for k in range(1, ntx)]
    with scope("greet"):
        pl.semaphore_wait(barrier, ntx - 1 + ny - 1)
    qd_cp.start()
    for c in stat_cp + gq_cp:
        c.start()
    stat_r[0] = stat_s[...]
    gq_r[0] = gq_s[...]

    def rest_of_norm():
        with scope("stat"):
            remote(stat_r.at[pl.ds(1, ntx - 1)], stat_r.at[pl.ds(1, ntx - 1)], stat_ss, stat_rs, tx=partner).wait_recv()
            remote(gq_r.at[pl.ds(1, ntx - 1)], gq_r.at[pl.ds(1, ntx - 1)], gq_ss, gq_rs, tx=partner).wait_recv()
        means = jnp.concatenate([stat_r[k, 0:1, :] for k in range(ntx)], axis=0)
        squares = jnp.concatenate([stat_r[k, 1:2, :] for k in range(ntx)], axis=0)
        off = means - jnp.sum(means, axis=0, keepdims=True) / ntx
        var = jnp.sum(squares, axis=0, keepdims=True) / d_model + jnp.sum(off * off, axis=0, keepdims=True) / ntx
        scale = lax.rsqrt(var + EPSILON)
        norm[...] = jnp.transpose(jnp.concatenate([off, scale, jnp.zeros((rows - ntx - 1, rows), F32)], axis=0))

    def normed(vals, at, g_ref):
        cols = norm[at, :]
        tiles = []
        for n in range(vals.shape[1] // hd):
            tile = vals[:, n * hd:(n + 1) * hd]
            for k in range(ntx):
                tile = tile + cols[:, k:k + 1] * g_ref[k, n:n + 1, :].astype(F32)
            tiles.append(tile * cols[:, ntx:ntx + 1])
        return jnp.concatenate(tiles, axis=1)


    def q_of(away):
        at = lax.rem(chip + away + nx, nx)
        return qp[2 * at + core] + qd_r[at].astype(F32)

    qx_in = qx_r.at[pl.ds(1, nx - 1)]

    qy_cp = [remote(qy_s.at[y_peers[k - 1]], qy_r.at[row], qy_ss, qy_rs, ty=y_peers[k - 1]) for k in range(1, ny)]

    def q_pair():
        with scope("qd"):
            qd_cp.wait_recv()
        for k in (2, 1, 3):
            qx_s[k] = q_of(k).astype(BF16)
            remote(qx_s.at[k], qx_r.at[k], qx_ss, qx_rs, tx=x_peers[k - 1]).start()

    def q_rows():
        mine = q_of(0)
        rest_of_norm()
        with scope("qx"):
            remote(qx_in, qx_in, qx_ss, qx_rs, tx=partner).wait_recv()
        for k in range(1, nx):
            mine = mine + qx_r[k].astype(F32)
        mine = normed(mine, pl.ds(pl.multiple_of(col * rb, rb), rb), gq_r)
        qsum[...] = mine
        kvs[0] = mine[:, qn:qn + hd]
        kvs[1] = mine[:, qn + hd:]
        for a in range(ny):
            for n in range(lh):
                qy_s[a, n * sb:(n + 1) * sb, :] = qsum[a * sb:(a + 1) * sb, n * hd:(n + 1) * hd]
        for c in qy_cp:
            c.start()
        qy_r[row] = qy_s[row]

    def tables():
        at_row = lax.broadcasted_iota(jnp.int32, (8, hd), 0)
        places = jnp.zeros((8, hd), F32)
        for r in range(sb):
            places = jnp.where(at_row == r, lens_ref[(row * ntx + col) * sb + r].astype(F32), places)
        angles = places * freq_v[...]
        turns[0] = jnp.cos(angles)
        low_half = lax.broadcasted_iota(jnp.int32, (8, hd), 1) < hd // 2
        sines = jnp.sin(angles)
        turns[1] = jnp.where(low_half, -sines, sines)

    def d_copy(s):
        return remote(d_s.at[s], d_r.at[s], d_ss, d_rs.at[s], tx=partner)

    def r_copy(s, t):
        return remote(r_s.at[s, piece(t)], r_r.at[s, piece(t)], r_ss, r_rs.at[s, t], tx=after)

    def product(s, carry):
        pltpu.make_async_copy(wb_v.at[2 * s], wb_v.at[2 * s], wb_sem.at[2 * s]).wait()

        @pl.when(s < nx - 1)
        def _():
            start_block(s + 1, True)

        part = jnp.dot(h_v[...], wb_v[2 * s], preferred_element_type=F32)
        d_s[s] = part[:rows].astype(BF16)
        d_copy(s).start()
        gb_s[block_of(s, False)] = gamma_row(part[rows:], 2 * fb // hd)

        @pl.when(s == 0)
        def _():
            q_pair()

        pltpu.make_async_copy(wb_v.at[2 * s + 1], wb_v.at[2 * s + 1], wb_sem.at[2 * s + 1]).wait()

        @pl.when(s < nx - 2)
        def _():
            start_block(s + 2, False)

        part = jnp.dot(h_v[...], wb_v[2 * s + 1], preferred_element_type=F32)
        own[s] = part[:rows]
        gb_s[block_of(s, True)] = gamma_row(part[rows:], 2 * fb // hd)

        @pl.when(s == 0)
        def _():
            with scope("d0"):
                d_copy(0).wait_recv()
            for t in range(SUBS):
                at = piece(t)
                r_s[0, at] = (own[0, at] + d_r[0, at].astype(F32)).astype(BF16)
                r_copy(0, t).start()

        return carry

    with scope("products"):
        lax.fori_loop(0, nx, product, 0)
    for c in gb_cp + k_in + v_in:
        c.start()
    gb_r[0] = gb_s[col]
    tables()

    def ring(s, t):
        at = piece(t)
        if t == 0:
            with scope("d%d" % s):
                d_copy(s).wait_recv()
        part = own[s, at] + d_r[s, at].astype(F32)
        with scope("r%d%d" % (s, t)):
            r_copy(s - 1, t).wait_recv()
        part = part + r_r[s - 1, at].astype(F32)
        if s < nx - 1:
            r_s[s, at] = part.astype(BF16)
            r_copy(s, t).start()
        else:
            if t == 0:
                with scope("gb"):
                    remote(gb_r.at[pl.ds(1, ntx - 1)], gb_r.at[pl.ds(1, ntx - 1)], gb_ss, gb_rs, tx=partner).wait_recv()
            part = normed(part, at, gb_r)
            gate = part[:, :fb].astype(BF16).astype(F32)
            up = part[:, fb:].astype(BF16).astype(F32)
            b_v[col, at] = (gate * (1.0 / (1.0 + jnp.exp(-gate))) * up).astype(BF16)
            act_out(t)

    def turn(vals, r):
        return vals * turns[0, r:r + 1, :] + pltpu.roll(vals, hd // 2, 1) * turns[1, r:r + 1, :]

    def attend(r):
        length = lens_ref[(row * ntx + col) * sb + r]
        for a in range(ny):
            qs[a * lh:(a + 1) * lh, :] = turn(qy_r[a, pl.ds(r, lh, stride=sb), :], r)
        q = qs[...].astype(BF16)
        k_new = turn(kvs[0, pl.ds(row * sb + r, 1), :], r).astype(BF16).astype(F32)
        v_new = kvs[1, pl.ds(row * sb + r, 1), :].astype(BF16).astype(F32)
        new_out[r:r + 1, :] = k_new
        new_out[sb + r:sb + r + 1, :] = v_new
        k_in[r].wait()
        s_new = jnp.sum(q.astype(F32) * k_new, axis=1, keepdims=True)
        top = jnp.full((heads, hd), -1e30, F32)
        for c in range(ctx // CHUNK):
            s = lax.dot_general(q, kbuf[r, c * CHUNK:(c + 1) * CHUNK, :], (((1,), (1,)), ((), ())), preferred_element_type=F32)
            pos = lax.broadcasted_iota(jnp.int32, (1, CHUNK), 1) + c * CHUNK
            s = jnp.where(pos < length, s, -1e30)
            sbuf[:, c * CHUNK:(c + 1) * CHUNK] = s
            for t in range(CHUNK // hd):
                top = jnp.maximum(top, s[:, t * hd:(t + 1) * hd])
        high = jnp.maximum(jnp.max(top, axis=1, keepdims=True), s_new)
        rate = hd ** -0.5 * LOG2E
        e_new = jnp.exp2((s_new - high) * rate)
        low = jnp.zeros((heads, hd), F32)
        out = e_new.astype(BF16).astype(F32) * v_new
        v_in[r].wait()
        for c in range(ctx // CHUNK):
            e = jnp.exp2((sbuf[:, c * CHUNK:(c + 1) * CHUNK] - high) * rate)
            for t in range(CHUNK // hd):
                low = low + e[:, t * hd:(t + 1) * hd]
            out = out + jnp.dot(e.astype(BF16), vbuf[r, c * CHUNK:(c + 1) * CHUNK, :], preferred_element_type=F32)
        out = out / (jnp.sum(low, axis=1, keepdims=True) + e_new)
        for a in range(ny):
            o32[a, pl.ds(r, lh, stride=sb), :] = out[a * lh:(a + 1) * lh]

    def b_send(kind, t, slot, to):
        b = held(kind, True)
        return remote(b_v.at[b, piece(t)], b_v.at[b, piece(t)], b_ss, b_rs.at[slot - 1, t], tx=to)

    def b_in(kind, t):
        b = held(kind, True)
        return remote(b_v.at[b, piece(t)], b_v.at[b, piece(t)], b_ss, b_rs.at[kind - 1, t], tx=left)

    def b_pair(kind, t):
        b = held(kind, True)
        return remote(b_v.at[b, piece(t)], b_v.at[b, piece(t)], bp_ss, bp_rs.at[kind], tx=partner)

    def act_out(t):
        b_send(0, t, 1, left).start()
        b_send(0, t, 2, right).start()
        b_pair(0, t).start()

    def act_in(kind, t):
        with scope("b%d%d" % (kind, t)):
            b_in(kind, t).wait_recv()
        if kind == 1:
            b_send(1, t, 3, left).start()
        b_pair(kind, t).start()

    ay_cp = [remote(ay_s.at[y_peers[k - 1]], ay_r.at[row], ay_ss, ay_rs, ty=y_peers[k - 1]) for k in range(1, ny)]

    def g_send(kind, slot, to):
        at = held(kind, True)
        return remote(g_v.at[at], g_v.at[at], g_ss, g_rs.at[slot - 1], tx=to)

    def g_pair(kind):
        at = held(kind, True)
        return remote(g_v.at[at], g_v.at[at], gp_ss, gp_rs, tx=partner)

    def g_in(kind):
        at = held(kind, True)
        with scope("g%d" % kind):
            remote(g_v.at[at], g_v.at[at], g_ss, g_rs.at[kind - 1], tx=left).wait_recv()
        if kind == 1:
            g_send(1, 3, left).start()
        g_pair(kind).start()

    def att_out():
        ay_s[...] = o32[...].astype(BF16)
        for c in ay_cp:
            c.start()
        ay_r[row] = ay_s[row]

    def att_rows():
        with scope("ay"):
            remote(ay_r.at[pl.ds(0, ny - 1)], ay_r.at[pl.ds(0, ny - 1)], ay_ss, ay_rs, ty=y_peers[0]).wait_recv()
        for a in range(ny):
            part = ay_r[a].astype(F32)
            for n in range(lh):
                g32[n, a * sb:(a + 1) * sb, :] = part[n * sb:(n + 1) * sb, :]
        g_v[col] = g32[...].astype(BF16)
        g_send(0, 1, left).start()
        g_send(0, 2, right).start()
        g_pair(0).start()

    mid = rows // 2

    def half_rows(half):
        return pl.ds(half * mid, mid)

    def down(n):
        wd_load(n, 0).wait()
        if n % 2:
            b = held(n // 2, False)
            with scope("bp%d" % (n // 2)):
                remote(b_v.at[b], b_v.at[b], bp_ss, bp_rs.at[n // 2], tx=partner).wait_recv()
        part = jnp.dot(b_v[held(n // 2, n % 2 == 0)], wd_v[n], preferred_element_type=F32)
        acc[...] = part if n == 0 else acc[...] + part

    def att_down(half):
        at = pl.ds(half * nx, nx)
        for n in range(0, lh, 2):
            pair = jnp.concatenate([g_v[at, n].reshape(mid, hd), g_v[at, n + 1].reshape(mid, hd)], axis=1)
            acc[half_rows(half)] += jnp.dot(pair, wo_v[n * hd:(n + 2) * hd, :], preferred_element_type=F32)

    def y_out_half(half):
        part = jnp.dot(back_v[...], acc[half_rows(half)].astype(BF16), preferred_element_type=F32)
        y_s[half] = part.astype(BF16).reshape(ny, yb // 2, dl)
        for k in range(1, ny):
            remote(y_s.at[half, y_peers[k - 1]], y_r.at[half, k], y_ss.at[half], y_rs.at[half], ty=y_peers[k - 1]).start()

    def y_sum_half(half):
        at = pl.ds(pl.multiple_of(row * yb + half * (yb // 2), yb // 2), yb // 2)
        total = x_v[at, :].astype(F32) + y_s[half, row].astype(F32)
        rest = y_r.at[half, pl.ds(1, ny - 1)]
        with scope("y%d" % half):
            remote(rest, rest, y_ss.at[half], y_rs.at[half], ty=y_peers[0]).wait_recv()
        for k in range(1, ny):
            total = total + y_r[half, k].astype(F32)
        yf[half, row] = total.astype(BF16)
        for k in range(1, ny):
            remote(yf.at[half, row], yf.at[half, row], f_ss.at[half], f_rs.at[half], ty=y_peers[k - 1]).start()

    def y_all_half(half):
        rest = yf.at[half, pl.ds(0, ny - 1)]
        with scope("f%d" % half):
            remote(rest, rest, f_ss.at[half], f_rs.at[half], ty=y_peers[0]).wait_recv()
        for a in range(ny):
            y_out[a * yb + half * (yb // 2):a * yb + (half + 1) * (yb // 2), :] = yf[half, a]

    q_rows()
    for t in range(SUBS):
        ring(1, t)
    for n in range(ntx):
        wd_load(n, held(n // 2, n % 2 == 0)).start()
    wo_load.start()
    with scope("qy"):
        remote(qy_r.at[pl.ds(0, ny - 1)], qy_r.at[pl.ds(0, ny - 1)], qy_ss, qy_rs, ty=y_peers[0]).wait_recv()
    for t in range(SUBS):
        ring(2, t)
        with scope("a%d" % t):
            attend(t)
    att_out()
    for t in range(SUBS - 1):
        ring(3, t)
    att_rows()
    ring(3, SUBS - 1)
    down(0)
    for t in range(SUBS):
        act_in(1, t)
        act_in(2, t)
        if t == 2:
            g_in(1)
    g_in(2)
    for n in (1, 2, 4, 3, 5):
        down(n)
    for t in range(SUBS):
        act_in(3, t)
    down(6)
    g_in(3)
    down(7)
    with scope("gp"):
        remote(g_v.at[pl.ds(0, nx)], g_v.at[pl.ds(0, nx)], gp_ss, gp_rs, tx=partner).wait_recv()
    wo_load.wait()
    att_down(0)
    y_out_half(0)
    att_down(1)
    y_out_half(1)
    y_sum_half(0)
    y_sum_half(1)
    y_all_half(0)
    y_all_half(1)

    with scope("sends"):
        qd_cp.wait_send()
        for ref, send, recv in (
            (stat_r.at[pl.ds(1, ntx - 1)], stat_ss, stat_rs), (gq_r.at[pl.ds(1, ntx - 1)], gq_ss, gq_rs), (gb_r.at[pl.ds(1, ntx - 1)], gb_ss, gb_rs),
            (qx_in, qx_ss, qx_rs), (qy_s.at[pl.ds(1, ny - 1)], qy_ss, qy_rs), (ay_s.at[pl.ds(1, ny - 1)], ay_ss, ay_rs),
            *((y_s.at[half, pl.ds(1, ny - 1)], y_ss.at[half], y_rs.at[half]) for half in range(2)),
            *((yf.at[half, pl.ds(1, ny - 1)], f_ss.at[half], f_rs.at[half]) for half in range(2)),
            (d_s, d_ss, d_rs.at[0]), (r_s, r_ss, r_rs.at[0, 0]), (g_v.at[pl.ds(1, nx - 1)], g_ss, g_rs.at[0]), (g_v.at[pl.ds(0, nx)], gp_ss, gp_rs),
            (b_v.at[pl.ds(1, nx - 1)], b_ss, b_rs.at[0, 0]), (b_v.at[pl.ds(0, nx)], bp_ss, bp_rs.at[0]),
        ):
            remote(ref, ref, send, recv, tx=partner).wait_send()


def store_kernel(ny, ntx, lens_ref, y_v, new_v, k_v, v_v, y_h, ko_h, vo_h, patch, y_sem, out_sem):
    first = (lax.axis_index("ty") * ntx + lax.axis_index("tx")) * k_v.shape[0]
    sb, ctx, hd = k_v.shape
    pieces = ctx // PIECE
    y_cp = pltpu.make_async_copy(y_v, y_h, y_sem)
    y_cp.start()

    def write(a, buf, out):
        def sequence(r, carry):
            length = lens_ref[first + r]
            spot = lax.div(length, PIECE)

            def other(c, inner):
                c = c + jnp.where(c >= spot, 1, 0)
                rest = pl.ds(pl.multiple_of(c * PIECE, PIECE), PIECE)
                pltpu.make_async_copy(buf.at[r, rest], out.at[r, rest], out_sem.at[a, r, 1]).start()
                return inner

            lax.fori_loop(0, pieces - 1, other, 0)
            at = pl.ds(pl.multiple_of(spot * PIECE, PIECE), PIECE)
            here = lax.broadcasted_iota(jnp.int32, (PIECE, hd), 0) == length - spot * PIECE
            patch[a, r] = jnp.where(here, new_v[pl.ds(a * sb + r, 1), :], buf[r, at, :].astype(F32)).astype(BF16)
            pltpu.make_async_copy(patch.at[a, r], out.at[r, at], out_sem.at[a, r, 0]).start()
            return carry

        lax.fori_loop(0, sb, sequence, 0)

    def finish(a, buf, out):
        for r in range(sb):
            pltpu.make_async_copy(patch.at[a, r], out.at[r, pl.ds(0, PIECE)], out_sem.at[a, r, 0]).wait()
            rest = pl.ds(0, ctx - PIECE)
            pltpu.make_async_copy(buf.at[r, rest], out.at[r, rest], out_sem.at[a, r, 1]).wait()

    write(0, k_v, ko_h)
    write(1, v_v, vo_h)
    y_cp.wait()
    finish(0, k_v, ko_h)
    finish(1, v_v, vo_h)


def solution(mesh):
    ny = mesh.shape["ty"]
    ntx = mesh.shape["tx"]
    nx = ntx // 2
    cache_spec = P(("dp", "ty", "tx"), None, None)
    vspec = pl.BlockSpec(memory_space=VMEM)
    hspec = pl.BlockSpec(memory_space=pltpu.HBM)
    sspec = pl.BlockSpec(memory_space=pltpu.SMEM)

    def layer_shard(x_blk, lens_part, k_blk, v_blk, gamma_blk, w_query, w_key, w_value, w_gate, w_up, w_out, w_down):
        rows, dl = x_blk.shape
        sb, ctx, hd = k_blk.shape
        qn = w_query.shape[1]
        lh = qn // hd
        qw = qn + 2 * hd
        fb = w_gate.shape[1] // ntx
        rb = rows // ntx
        yb = rows // ny

        natural = np.arange(rows)
        order = np.reshape(np.transpose(np.reshape(natural, (ny, ntx, sb)), (1, 0, 2)), (rows,))
        perm = jnp.asarray(order[:, None] == natural[None, :], dtype=BF16)
        part = np.arange(rows // 2)
        order = np.reshape(np.transpose(np.reshape(part, (nx, ny, sb)), (1, 0, 2)), (rows // 2,))
        back = jnp.asarray(order[:, None] == part[None, :], dtype=BF16)
        freqs = np.power(ROPE_BASE, -(np.arange(hd // 2, dtype=np.float32) * 2.0) / hd).astype(np.float32)
        freqs = jnp.asarray(np.tile(np.concatenate([freqs, freqs])[None, :], (8, 1)))

        y_vm, new_rows, k_vm, v_vm = pl.pallas_call(
            functools.partial(step_kernel, ny, nx, dl * ntx),
            out_shape=(
                pltpu.VMEM((rows, dl), BF16),
                pltpu.VMEM((2 * sb, hd), F32),
                pltpu.VMEM(k_blk.shape, BF16),
                pltpu.VMEM(v_blk.shape, BF16),
            ),
            in_specs=[sspec] + [hspec] * 14,
            out_specs=(vspec,) * 4,
            scratch_shapes=[
                VMEM((rows, dl), BF16), VMEM((dl,), F32), VMEM((rows, rows), BF16), VMEM((rows // 2, rows // 2), BF16), VMEM((8, hd), F32),
                VMEM((dl, qw), BF16), VMEM((ntx, dl, 2 * fb), BF16), VMEM((qn, dl), BF16), VMEM((ntx, fb, dl), BF16),
                VMEM((rows + 16, dl), BF16), VMEM((8, rows), F32), VMEM((ntx, 8, rows), F32),
                VMEM((16, hd), BF16), VMEM((ntx, 16, hd), BF16), VMEM((ntx, 16, hd), BF16), VMEM((ntx, 16, hd), BF16), VMEM((rows, rows), F32),
                VMEM((ntx, rb, qw), F32), VMEM((nx, rb, qw), BF16), VMEM((nx, rb, qw), BF16),
                VMEM((nx, rb, qw), BF16), VMEM((nx, rb, qw), BF16), VMEM((rb, qw), F32), VMEM((2, rb, hd), F32),
                VMEM((ny, sb * lh, hd), F32), VMEM((ny, sb * lh, hd), F32),
                VMEM((nx, rows, 2 * fb), F32), VMEM((nx, rows, 2 * fb), BF16), VMEM((nx, rows, 2 * fb), BF16),
                VMEM((nx - 1, rows, 2 * fb), BF16), VMEM((nx - 1, rows, 2 * fb), BF16),
                VMEM((2, 8, hd), F32), VMEM((ny * lh, hd), F32), VMEM((ny * lh, ctx), F32), VMEM((ny, sb * lh, hd), F32),
                VMEM((ny, sb * lh, hd), BF16), VMEM((ny, sb * lh, hd), BF16), VMEM((lh, rb, hd), F32),
                VMEM((ntx, lh, rb, hd), BF16), VMEM((ntx, rows, fb), BF16), VMEM((rows, dl), F32),
                VMEM((2, ny, yb // 2, dl), BF16), VMEM((2, ny, yb // 2, dl), BF16), VMEM((2, ny, yb // 2, dl), BF16),
                DMA((5,)), DMA, DMA((ntx,)), DMA((2, sb)), DMA, DMA((ntx,)),
                DMA, DMA, DMA, DMA, DMA, DMA, DMA, DMA, DMA, DMA, DMA, DMA,
                DMA, DMA((nx,)), DMA, DMA((nx - 1, SUBS)),
                DMA, DMA, DMA, DMA((nx - 1,)), DMA, DMA,
                DMA, DMA((nx - 1, SUBS)), DMA, DMA((nx,)), DMA((2,)), DMA((2,)), DMA((2,)), DMA((2,)),
            ],
            compiler_params=pltpu.CompilerParams(collective_id=0, has_side_effects=True, vmem_limit_bytes=52 * 1024 * 1024),
            name="step",
        )(lens_part, x_blk, gamma_blk, perm, back, freqs, w_query, w_key, w_value, w_gate, w_up, k_blk, v_blk, w_out, w_down)

        return pl.pallas_call(
            functools.partial(store_kernel, ny, ntx),
            out_shape=(
                jax.ShapeDtypeStruct((rows, dl), BF16),
                jax.ShapeDtypeStruct(k_blk.shape, BF16),
                jax.ShapeDtypeStruct(v_blk.shape, BF16),
            ),
            in_specs=[sspec] + [vspec] * 4,
            out_specs=(hspec,) * 3,
            scratch_shapes=[VMEM((2, sb, PIECE, hd), BF16), DMA, DMA((2, sb, 2))],
            compiler_params=pltpu.CompilerParams(vmem_limit_bytes=4 * 1024 * 1024),
            name="store",
        )(lens_part, y_vm, new_rows, k_vm, v_vm)

    in_specs = (P("dp", "tx"), P("dp"), cache_spec, cache_spec, P("tx"), P("tx", "ty"), P("tx", None), P("tx", None), P("tx", "ty"), P("tx", "ty"), P("ty", "tx"), P("ty", "tx"))
    out_specs = (P("dp", "tx"), cache_spec, cache_spec)
    return jax.shard_map(layer_shard, mesh=mesh, in_specs=in_specs, out_specs=out_specs, check_vma=False)
```

```python
import functools

import jax
import jax.numpy as jnp
import numpy as np
from jax import lax
from jax.experimental import pallas as pl
from jax.experimental.pallas import tpu as pltpu
from jax.sharding import PartitionSpec as P

EPSILON = 1e-6
ROPE_BASE = 10000.0
LOG2E = 1.4426950408889634
MESH = pl.DeviceIdType.MESH
F32 = jnp.float32
BF16 = jnp.bfloat16
VMEM = pltpu.VMEM
DMA = pltpu.SemaphoreType.DMA
SUBS = 4
CHUNK = 1024
PIECE = 512
scope = jax.named_scope


def remote(src, dst, send_sem, recv_sem, tx=None, ty=None):
    device = {}
    if tx is not None:
        device["tx"] = tx
    if ty is not None:
        device["ty"] = ty
    return pltpu.make_async_remote_copy(src_ref=src, dst_ref=dst, send_sem=send_sem, recv_sem=recv_sem, device_id=device, device_id_type=MESH)


def step_kernel(ny, nx, d_model, lens_ref, x_h, gamma_h, perm_h, back_h, freq_h, wq_h, wk_h, wv_h, wg_h, wu_h, k_h, v_h, wo_h, wd_h,
                y_out, new_out, kbuf, vbuf,
                x_v, gamma_v, perm_v, back_v, freq_v, wq_v, wb_v, wo_v, wd_v, h_v, stat_s, stat_r, gq_s, gq_r, gb_s, gb_r, norm,
                qp, qd_s, qd_r, qx_s, qx_r, qsum, kvs, qy_s, qy_r, own, d_s, d_r, r_s, r_r,
                turns, qs, sbuf, o32, ay_s, ay_r, g32, g_v, b_v, acc, y_s, y_r, yf,
                in_sem, wq_sem, wb_sem, kv_sem, wo_sem, wd_sem, stat_ss, stat_rs, gq_ss, gq_rs, gb_ss, gb_rs, qd_ss, qd_rs, qx_ss, qx_rs, qy_ss, qy_rs,
                d_ss, d_rs, r_ss, r_rs, ay_ss, ay_rs, g_ss, g_rs, gp_ss, gp_rs, b_ss, b_rs, bp_ss, bp_rs, y_ss, y_rs, f_ss, f_rs):
    row = lax.axis_index("ty")
    col = lax.axis_index("tx")
    chip = lax.div(col, 2)
    core = lax.rem(col, 2)
    step = 1 - 2 * core
    ntx = 2 * nx
    rows, dl = x_h.shape
    rb = rows // ntx
    sb = rb // ny
    qn = wq_h.shape[1]
    hd = wk_h.shape[1]
    qw = qn + 2 * hd
    lh = qn // hd
    heads = ny * lh
    ctx = k_h.shape[1]
    fb = wb_v.shape[2] // 2
    sub = rows // SUBS
    yb = rows // ny
    partner = lax.rem(col + 1, 2) + 2 * chip
    after = 2 * lax.rem(chip + step + nx, nx) + core
    before = 2 * lax.rem(chip - step + nx, nx) + core
    tx_peers = [lax.rem(col + k, ntx) for k in range(1, ntx)]
    x_peers = [2 * lax.rem(chip + k, nx) + core for k in range(1, nx)]
    y_peers = [lax.rem(row + k, ny) for k in range(1, ny)]
    y_froms = [lax.rem(row - k + ny, ny) for k in range(1, ny)]

    barrier = pltpu.get_barrier_semaphore()
    for peer in tx_peers:
        pl.semaphore_signal(barrier, inc=1, device_id={"tx": peer}, device_id_type=MESH)
    for peer in y_peers:
        pl.semaphore_signal(barrier, inc=1, device_id={"ty": peer}, device_id_type=MESH)

    def piece(t):
        return pl.ds(pl.multiple_of(t * sub, sub), sub)

    def block_of(s, mine):
        sign = step if mine else -step
        at = lax.rem(chip - (s + 1) * sign + 2 * nx, nx)
        return 2 * at + (core if mine else 1 - core)

    def held(kind, mine):
        away = (0, -1, 1, 2)[kind] * (step if mine else -step)
        return 2 * lax.rem(chip + away + 2 * nx, nx) + (core if mine else 1 - core)

    def block_loads(n, b):
        at = pl.ds(pl.multiple_of(b * fb, fb), fb)
        return [
            pltpu.make_async_copy(wg_h.at[:, at], wb_v.at[n, :, pl.ds(0, fb)], wb_sem.at[n]),
            pltpu.make_async_copy(wu_h.at[:, at], wb_v.at[n, :, pl.ds(fb, fb)], wb_sem.at[n]),
        ]

    def wd_load(n, b):
        at = pl.ds(pl.multiple_of(b * fb, fb), fb)
        return pltpu.make_async_copy(wd_h.at[at, :], wd_v.at[n], wd_sem)

    first_loads = [
        pltpu.make_async_copy(x_h, x_v, in_sem.at[0]),
        pltpu.make_async_copy(perm_h, perm_v, in_sem.at[1]),
        pltpu.make_async_copy(gamma_h, gamma_v, in_sem.at[2]),
        pltpu.make_async_copy(freq_h, freq_v, in_sem.at[3]),
        pltpu.make_async_copy(back_h, back_v, in_sem.at[4]),
    ]
    q_loads = [
        pltpu.make_async_copy(wq_h, wq_v.at[:, pl.ds(0, qn)], wq_sem),
        pltpu.make_async_copy(wk_h, wq_v.at[:, pl.ds(qn, hd)], wq_sem),
        pltpu.make_async_copy(wv_h, wq_v.at[:, pl.ds(qn + hd, hd)], wq_sem),
    ]
    k_in = [pltpu.make_async_copy(k_h.at[r], kbuf.at[r], kv_sem.at[0]) for r in range(sb)]
    v_in = [pltpu.make_async_copy(v_h.at[r], vbuf.at[r], kv_sem.at[1]) for r in range(sb)]
    wo_load = pltpu.make_async_copy(wo_h, wo_v, wo_sem)
    def start_block(s, mine):
        for c in block_loads(2 * s + int(mine), block_of(s, mine)):
            c.start()

    for c in first_loads + q_loads:
        c.start()
    for c in first_loads:
        c.wait()
    start_block(0, False)
    start_block(0, True)

    xp = jnp.dot(perm_v[...], x_v[...], preferred_element_type=F32)
    own_mean = jnp.sum(xp, axis=1, keepdims=True) / dl
    xc = xp - own_mean
    gamma = gamma_v[...].reshape(1, dl)
    h_v[:rows] = (xc * gamma).astype(BF16)
    extra = lax.broadcasted_iota(jnp.int32, (16, dl), 0)
    h_v[rows:] = jnp.where(extra == 0, gamma, jnp.where(extra == 1, gamma - gamma.astype(BF16).astype(F32), 0.0)).astype(BF16)
    lane = lax.broadcasted_iota(jnp.int32, (rows, rows), 1)
    both = jnp.where(lane == 0, own_mean, jnp.where(lane == 1, jnp.sum(xc * xc, axis=1, keepdims=True), 0.0))
    stat_s[...] = jnp.transpose(both)[:8]

    def gamma_row(vals, tiles):
        row_sum = vals[0:1, :] + vals[1:2, :]
        parts = [row_sum[:, n * hd:(n + 1) * hd] for n in range(tiles)]
        return jnp.concatenate(parts + [jnp.zeros((16 - tiles, hd), F32)], axis=0).astype(BF16)

    pltpu.make_async_copy(wq_v, wq_v, wq_sem).wait()
    start_block(1, False)
    part = jnp.dot(h_v[...], wq_v[...], preferred_element_type=F32)
    qp[...] = part[:rows].reshape(ntx, rb, qw)
    gq_s[...] = gamma_row(part[rows:], qw // hd)
    for n in range(nx):
        qd_s[n] = qp[2 * n + 1 - core].astype(BF16)
    qd_cp = remote(qd_s, qd_r, qd_ss, qd_rs, tx=partner)
    stat_cp = [remote(stat_s, stat_r.at[k], stat_ss, stat_rs, tx=tx_peers[k - 1]) for k in range(1, ntx)]
    gq_cp = [remote(gq_s, gq_r.at[k], gq_ss, gq_rs, tx=tx_peers[k - 1]) for k in range(1, ntx)]
    gb_cp = [remote(gb_s.at[tx_peers[k - 1]], gb_r.at[k], gb_ss, gb_rs, tx=tx_peers[k - 1]) for k in range(1, ntx)]
    with scope("greet"):
        pl.semaphore_wait(barrier, ntx - 1 + ny - 1)
    qd_cp.start()
    for c in stat_cp + gq_cp:
        c.start()
    stat_r[0] = stat_s[...]
    gq_r[0] = gq_s[...]

    def rest_of_norm():
        with scope("stat"):
            remote(stat_r.at[pl.ds(1, ntx - 1)], stat_r.at[pl.ds(1, ntx - 1)], stat_ss, stat_rs, tx=partner).wait_recv()
            remote(gq_r.at[pl.ds(1, ntx - 1)], gq_r.at[pl.ds(1, ntx - 1)], gq_ss, gq_rs, tx=partner).wait_recv()
        means = jnp.concatenate([stat_r[k, 0:1, :] for k in range(ntx)], axis=0)
        squares = jnp.concatenate([stat_r[k, 1:2, :] for k in range(ntx)], axis=0)
        off = means - jnp.sum(means, axis=0, keepdims=True) / ntx
        var = jnp.sum(squares, axis=0, keepdims=True) / d_model + jnp.sum(off * off, axis=0, keepdims=True) / ntx
        scale = lax.rsqrt(var + EPSILON)
        norm[...] = jnp.transpose(jnp.concatenate([off, scale, jnp.zeros((rows - ntx - 1, rows), F32)], axis=0))

    def normed(vals, at, g_ref):
        cols = norm[at, :]
        tiles = []
        for n in range(vals.shape[1] // hd):
            tile = vals[:, n * hd:(n + 1) * hd]
            for k in range(ntx):
                tile = tile + cols[:, k:k + 1] * g_ref[k, n:n + 1, :].astype(F32)
            tiles.append(tile * cols[:, ntx:ntx + 1])
        return jnp.concatenate(tiles, axis=1)


    def q_of(away):
        at = lax.rem(chip + away + nx, nx)
        return qp[2 * at + core] + qd_r[at].astype(F32)

    qx_in = qx_r.at[pl.ds(1, nx - 1)]

    qy_cp = [remote(qy_s.at[y_peers[k - 1]], qy_r.at[row], qy_ss, qy_rs, ty=y_peers[k - 1]) for k in range(1, ny)]

    def q_pair():
        with scope("qd"):
            qd_cp.wait_recv()
        for k in (2, 1, 3):
            qx_s[k] = q_of(k).astype(BF16)
            remote(qx_s.at[k], qx_r.at[k], qx_ss, qx_rs, tx=x_peers[k - 1]).start()

    def q_rows():
        mine = q_of(0)
        rest_of_norm()
        with scope("qx"):
            remote(qx_in, qx_in, qx_ss, qx_rs, tx=partner).wait_recv()
        for k in range(1, nx):
            mine = mine + qx_r[k].astype(F32)
        mine = normed(mine, pl.ds(pl.multiple_of(col * rb, rb), rb), gq_r)
        qsum[...] = mine
        kvs[0] = mine[:, qn:qn + hd]
        kvs[1] = mine[:, qn + hd:]
        for a in range(ny):
            for n in range(lh):
                qy_s[a, n * sb:(n + 1) * sb, :] = qsum[a * sb:(a + 1) * sb, n * hd:(n + 1) * hd]
        for c in qy_cp:
            c.start()
        qy_r[row] = qy_s[row]

    def tables():
        at_row = lax.broadcasted_iota(jnp.int32, (8, hd), 0)
        places = jnp.zeros((8, hd), F32)
        for r in range(sb):
            places = jnp.where(at_row == r, lens_ref[(row * ntx + col) * sb + r].astype(F32), places)
        angles = places * freq_v[...]
        turns[0] = jnp.cos(angles)
        low_half = lax.broadcasted_iota(jnp.int32, (8, hd), 1) < hd // 2
        sines = jnp.sin(angles)
        turns[1] = jnp.where(low_half, -sines, sines)

    def d_copy(s):
        return remote(d_s.at[s], d_r.at[s], d_ss, d_rs.at[s], tx=partner)

    def r_copy(s, t):
        return remote(r_s.at[s, piece(t)], r_r.at[s, piece(t)], r_ss, r_rs.at[s, t], tx=after)

    def product(s, carry):
        pltpu.make_async_copy(wb_v.at[2 * s], wb_v.at[2 * s], wb_sem.at[2 * s]).wait()

        @pl.when(s < nx - 1)
        def _():
            start_block(s + 1, True)

        part = jnp.dot(h_v[...], wb_v[2 * s], preferred_element_type=F32)
        d_s[s] = part[:rows].astype(BF16)
        d_copy(s).start()
        gb_s[block_of(s, False)] = gamma_row(part[rows:], 2 * fb // hd)

        @pl.when(s == 0)
        def _():
            q_pair()

        pltpu.make_async_copy(wb_v.at[2 * s + 1], wb_v.at[2 * s + 1], wb_sem.at[2 * s + 1]).wait()

        @pl.when(s < nx - 2)
        def _():
            start_block(s + 2, False)

        part = jnp.dot(h_v[...], wb_v[2 * s + 1], preferred_element_type=F32)
        own[s] = part[:rows]
        gb_s[block_of(s, True)] = gamma_row(part[rows:], 2 * fb // hd)

        @pl.when(s == 0)
        def _():
            with scope("d0"):
                d_copy(0).wait_recv()
            for t in range(SUBS):
                at = piece(t)
                r_s[0, at] = (own[0, at] + d_r[0, at].astype(F32)).astype(BF16)
                r_copy(0, t).start()

        return carry

    with scope("products"):
        lax.fori_loop(0, nx, product, 0)
    for c in gb_cp + k_in + v_in:
        c.start()
    gb_r[0] = gb_s[col]
    tables()

    def ring(s, t):
        at = piece(t)
        if t == 0:
            with scope("d%d" % s):
                d_copy(s).wait_recv()
        part = own[s, at] + d_r[s, at].astype(F32)
        with scope("r%d%d" % (s, t)):
            r_copy(s - 1, t).wait_recv()
        part = part + r_r[s - 1, at].astype(F32)
        if s < nx - 1:
            r_s[s, at] = part.astype(BF16)
            r_copy(s, t).start()
        else:
            if t == 0:
                with scope("gb"):
                    remote(gb_r.at[pl.ds(1, ntx - 1)], gb_r.at[pl.ds(1, ntx - 1)], gb_ss, gb_rs, tx=partner).wait_recv()
            part = normed(part, at, gb_r)
            gate = part[:, :fb].astype(BF16).astype(F32)
            up = part[:, fb:].astype(BF16).astype(F32)
            b_v[col, at] = (gate * (1.0 / (1.0 + jnp.exp(-gate))) * up).astype(BF16)
            act_out(t)

    def turn(vals, r):
        return vals * turns[0, r:r + 1, :] + pltpu.roll(vals, hd // 2, 1) * turns[1, r:r + 1, :]

    def attend(r):
        length = lens_ref[(row * ntx + col) * sb + r]
        for a in range(ny):
            qs[a * lh:(a + 1) * lh, :] = turn(qy_r[a, pl.ds(r, lh, stride=sb), :], r)
        q = qs[...].astype(BF16)
        k_new = turn(kvs[0, pl.ds(row * sb + r, 1), :], r).astype(BF16).astype(F32)
        v_new = kvs[1, pl.ds(row * sb + r, 1), :].astype(BF16).astype(F32)
        new_out[r:r + 1, :] = k_new
        new_out[sb + r:sb + r + 1, :] = v_new
        s_new = jnp.sum(q.astype(F32) * k_new, axis=1, keepdims=True)
        top = jnp.full((heads, hd), -1e30, F32)
        for c in range(ctx // CHUNK):
            s = lax.dot_general(q, kbuf[r, c * CHUNK:(c + 1) * CHUNK, :], (((1,), (1,)), ((), ())), preferred_element_type=F32)
            pos = lax.broadcasted_iota(jnp.int32, (1, CHUNK), 1) + c * CHUNK
            s = jnp.where(pos < length, s, -1e30)
            sbuf[:, c * CHUNK:(c + 1) * CHUNK] = s
            for t in range(CHUNK // hd):
                top = jnp.maximum(top, s[:, t * hd:(t + 1) * hd])
        high = jnp.maximum(jnp.max(top, axis=1, keepdims=True), s_new)
        rate = hd ** -0.5 * LOG2E
        e_new = jnp.exp2((s_new - high) * rate)
        low = jnp.zeros((heads, hd), F32)
        out = e_new.astype(BF16).astype(F32) * v_new
        for c in range(ctx // CHUNK):
            e = jnp.exp2((sbuf[:, c * CHUNK:(c + 1) * CHUNK] - high) * rate)
            for t in range(CHUNK // hd):
                low = low + e[:, t * hd:(t + 1) * hd]
            out = out + jnp.dot(e.astype(BF16), vbuf[r, c * CHUNK:(c + 1) * CHUNK, :], preferred_element_type=F32)
        out = out / (jnp.sum(low, axis=1, keepdims=True) + e_new)
        for a in range(ny):
            o32[a, pl.ds(r, lh, stride=sb), :] = out[a * lh:(a + 1) * lh]

    def b_send(kind, t, slot, to):
        b = held(kind, True)
        return remote(b_v.at[b, piece(t)], b_v.at[b, piece(t)], b_ss, b_rs.at[slot - 1, t], tx=to)

    def b_in(kind, t):
        b = held(kind, True)
        return remote(b_v.at[b, piece(t)], b_v.at[b, piece(t)], b_ss, b_rs.at[kind - 1, t], tx=after)

    def b_pair(kind, t):
        b = held(kind, True)
        return remote(b_v.at[b, piece(t)], b_v.at[b, piece(t)], bp_ss, bp_rs.at[kind], tx=partner)

    def act_out(t):
        b_send(0, t, 1, after).start()
        b_send(0, t, 2, before).start()
        b_pair(0, t).start()

    def act_in(kind, t):
        with scope("b%d%d" % (kind, t)):
            b_in(kind, t).wait_recv()
        if kind == 1:
            b_send(1, t, 3, after).start()
        b_pair(kind, t).start()

    ay_cp = [remote(ay_s.at[y_peers[k - 1]], ay_r.at[row], ay_ss, ay_rs, ty=y_peers[k - 1]) for k in range(1, ny)]

    def g_send(kind, slot, to):
        at = held(kind, True)
        return remote(g_v.at[at], g_v.at[at], g_ss, g_rs.at[slot - 1], tx=to)

    def g_pair(kind):
        at = held(kind, True)
        return remote(g_v.at[at], g_v.at[at], gp_ss, gp_rs, tx=partner)

    def g_in(kind):
        at = held(kind, True)
        with scope("g%d" % kind):
            remote(g_v.at[at], g_v.at[at], g_ss, g_rs.at[kind - 1], tx=after).wait_recv()
        if kind == 1:
            g_send(1, 3, after).start()
        g_pair(kind).start()

    def att_out():
        ay_s[...] = o32[...].astype(BF16)
        for c in ay_cp:
            c.start()
        ay_r[row] = ay_s[row]

    def att_rows():
        with scope("ay"):
            remote(ay_r.at[pl.ds(0, ny - 1)], ay_r.at[pl.ds(0, ny - 1)], ay_ss, ay_rs, ty=y_peers[0]).wait_recv()
        for a in range(ny):
            part = ay_r[a].astype(F32)
            for n in range(lh):
                g32[n, a * sb:(a + 1) * sb, :] = part[n * sb:(n + 1) * sb, :]
        g_v[col] = g32[...].astype(BF16)
        g_send(0, 1, after).start()
        g_send(0, 2, before).start()
        g_pair(0).start()

    mid = rows // 2

    def half_rows(half):
        return pl.ds(half * mid, mid)

    def down(n, half=None):
        if n % 2 and half != 1:
            b = held(n // 2, False)
            with scope("bp%d" % (n // 2)):
                remote(b_v.at[b], b_v.at[b], bp_ss, bp_rs.at[n // 2], tx=partner).wait_recv()
        at = pl.ds(0, rows) if half is None else half_rows(half)
        part = jnp.dot(b_v[held(n // 2, n % 2 == 0), at], wd_v[n], preferred_element_type=F32)
        acc[at] = part if n == 0 else acc[at] + part

    def att_down():
        with scope("gp"):
            remote(g_v.at[pl.ds(0, nx)], g_v.at[pl.ds(0, nx)], gp_ss, gp_rs, tx=partner).wait_recv()
        wo_load.wait()
        part = acc[...]
        for n in range(0, lh, 2):
            pair = jnp.concatenate([g_v[:, n].reshape(rows, hd), g_v[:, n + 1].reshape(rows, hd)], axis=1)
            part = part + jnp.dot(pair, wo_v[n * hd:(n + 2) * hd, :], preferred_element_type=F32)
        acc[...] = part

    def y_out_half(half):
        part = jnp.dot(back_v[...], acc[half_rows(half)].astype(BF16), preferred_element_type=F32)
        y_s[half] = part.astype(BF16).reshape(ny, yb // 2, dl)
        for k in range(1, ny):
            remote(y_s.at[half, y_peers[k - 1]], y_r.at[half, k], y_ss.at[half], y_rs.at[half], ty=y_peers[k - 1]).start()

    def y_sum_half(half):
        at = pl.ds(pl.multiple_of(row * yb + half * (yb // 2), yb // 2), yb // 2)
        total = x_v[at, :].astype(F32) + y_s[half, row].astype(F32)
        rest = y_r.at[half, pl.ds(1, ny - 1)]
        with scope("y%d" % half):
            remote(rest, rest, y_ss.at[half], y_rs.at[half], ty=y_peers[0]).wait_recv()
        for k in range(1, ny):
            total = total + y_r[half, k].astype(F32)
        yf[half, row] = total.astype(BF16)
        for k in range(1, ny):
            remote(yf.at[half, row], yf.at[half, row], f_ss.at[half], f_rs.at[half], ty=y_peers[k - 1]).start()

    def y_all_half(half):
        rest = yf.at[half, pl.ds(0, ny - 1)]
        with scope("f%d" % half):
            remote(rest, rest, f_ss.at[half], f_rs.at[half], ty=y_peers[0]).wait_recv()
        for a in range(ny):
            y_out[a * yb + half * (yb // 2):a * yb + (half + 1) * (yb // 2), :] = yf[half, a]

    q_rows()
    for t in range(SUBS):
        ring(1, t)
    for n in range(ntx):
        wd_load(n, held(n // 2, n % 2 == 0)).start()
    wo_load.start()
    for t in range(SUBS):
        ring(2, t)
        if t == 0:
            with scope("qy"):
                remote(qy_r.at[pl.ds(0, ny - 1)], qy_r.at[pl.ds(0, ny - 1)], qy_ss, qy_rs, ty=y_peers[0]).wait_recv()
            pltpu.make_async_copy(kbuf, kbuf, kv_sem.at[0]).wait()
            pltpu.make_async_copy(vbuf, vbuf, kv_sem.at[1]).wait()
        with scope("a%d" % t):
            attend(t)
    att_out()
    for t in range(SUBS):
        ring(3, t)
    att_rows()
    pltpu.make_async_copy(wd_v, wd_v, wd_sem).wait()
    down(0)
    for t in range(SUBS):
        act_in(1, t)
        act_in(2, t)
        if t == 2:
            g_in(1)
    g_in(2)
    for n in (1, 2, 4, 3, 5):
        down(n)
    for t in range(SUBS):
        act_in(3, t)
    g_in(3)
    down(6)
    att_down()
    for half in range(2):
        down(7, half)
        y_out_half(half)
    y_sum_half(0)
    y_sum_half(1)
    y_all_half(0)
    y_all_half(1)

    with scope("sends"):
        qd_cp.wait_send()
        for ref, send, recv in (
            (stat_r.at[pl.ds(1, ntx - 1)], stat_ss, stat_rs), (gq_r.at[pl.ds(1, ntx - 1)], gq_ss, gq_rs), (gb_r.at[pl.ds(1, ntx - 1)], gb_ss, gb_rs),
            (qx_in, qx_ss, qx_rs), (qy_s.at[pl.ds(1, ny - 1)], qy_ss, qy_rs), (ay_s.at[pl.ds(1, ny - 1)], ay_ss, ay_rs),
            *((y_s.at[half, pl.ds(1, ny - 1)], y_ss.at[half], y_rs.at[half]) for half in range(2)),
            *((yf.at[half, pl.ds(1, ny - 1)], f_ss.at[half], f_rs.at[half]) for half in range(2)),
            (d_s, d_ss, d_rs.at[0]), (r_s, r_ss, r_rs.at[0, 0]), (g_v.at[pl.ds(1, nx - 1)], g_ss, g_rs.at[0]), (g_v.at[pl.ds(0, nx)], gp_ss, gp_rs),
            (b_v.at[pl.ds(1, nx - 1)], b_ss, b_rs.at[0, 0]), (b_v.at[pl.ds(0, nx)], bp_ss, bp_rs.at[0]),
        ):
            remote(ref, ref, send, recv, tx=partner).wait_send()


def store_kernel(ny, ntx, lens_ref, y_v, new_v, k_v, v_v, y_h, ko_h, vo_h, patch, y_sem, out_sem):
    first = (lax.axis_index("ty") * ntx + lax.axis_index("tx")) * k_v.shape[0]
    sb, ctx, hd = k_v.shape
    pieces = ctx // PIECE
    y_cp = pltpu.make_async_copy(y_v, y_h, y_sem)
    y_cp.start()

    def write(a, buf, out):
        def sequence(r, carry):
            length = lens_ref[first + r]
            spot = lax.div(length, PIECE)

            def other(c, inner):
                c = c + jnp.where(c >= spot, 1, 0)
                rest = pl.ds(pl.multiple_of(c * PIECE, PIECE), PIECE)
                pltpu.make_async_copy(buf.at[r, rest], out.at[r, rest], out_sem.at[a, r, 1]).start()
                return inner

            lax.fori_loop(0, pieces - 1, other, 0)
            at = pl.ds(pl.multiple_of(spot * PIECE, PIECE), PIECE)
            here = lax.broadcasted_iota(jnp.int32, (PIECE, hd), 0) == length - spot * PIECE
            patch[a, r] = jnp.where(here, new_v[pl.ds(a * sb + r, 1), :], buf[r, at, :].astype(F32)).astype(BF16)
            pltpu.make_async_copy(patch.at[a, r], out.at[r, at], out_sem.at[a, r, 0]).start()
            return carry

        lax.fori_loop(0, sb, sequence, 0)

    def finish(a, buf, out):
        for r in range(sb):
            pltpu.make_async_copy(patch.at[a, r], out.at[r, pl.ds(0, PIECE)], out_sem.at[a, r, 0]).wait()
            rest = pl.ds(0, ctx - PIECE)
            pltpu.make_async_copy(buf.at[r, rest], out.at[r, rest], out_sem.at[a, r, 1]).wait()

    write(0, k_v, ko_h)
    write(1, v_v, vo_h)
    y_cp.wait()
    finish(0, k_v, ko_h)
    finish(1, v_v, vo_h)


def solution(mesh):
    ny = mesh.shape["ty"]
    ntx = mesh.shape["tx"]
    nx = ntx // 2
    cache_spec = P(("dp", "ty", "tx"), None, None)
    vspec = pl.BlockSpec(memory_space=VMEM)
    hspec = pl.BlockSpec(memory_space=pltpu.HBM)
    sspec = pl.BlockSpec(memory_space=pltpu.SMEM)

    def layer_shard(x_blk, lens_part, k_blk, v_blk, gamma_blk, w_query, w_key, w_value, w_gate, w_up, w_out, w_down):
        rows, dl = x_blk.shape
        sb, ctx, hd = k_blk.shape
        qn = w_query.shape[1]
        lh = qn // hd
        qw = qn + 2 * hd
        fb = w_gate.shape[1] // ntx
        rb = rows // ntx
        yb = rows // ny

        natural = np.arange(rows)
        order = np.reshape(np.transpose(np.reshape(natural, (ny, ntx, sb)), (1, 0, 2)), (rows,))
        perm = jnp.asarray(order[:, None] == natural[None, :], dtype=BF16)
        part = np.arange(rows // 2)
        order = np.reshape(np.transpose(np.reshape(part, (nx, ny, sb)), (1, 0, 2)), (rows // 2,))
        back = jnp.asarray(order[:, None] == part[None, :], dtype=BF16)
        freqs = np.power(ROPE_BASE, -(np.arange(hd // 2, dtype=np.float32) * 2.0) / hd).astype(np.float32)
        freqs = jnp.asarray(np.tile(np.concatenate([freqs, freqs])[None, :], (8, 1)))

        y_vm, new_rows, k_vm, v_vm = pl.pallas_call(
            functools.partial(step_kernel, ny, nx, dl * ntx),
            out_shape=(
                pltpu.VMEM((rows, dl), BF16),
                pltpu.VMEM((2 * sb, hd), F32),
                pltpu.VMEM(k_blk.shape, BF16),
                pltpu.VMEM(v_blk.shape, BF16),
            ),
            in_specs=[sspec] + [hspec] * 14,
            out_specs=(vspec,) * 4,
            scratch_shapes=[
                VMEM((rows, dl), BF16), VMEM((dl,), F32), VMEM((rows, rows), BF16), VMEM((rows // 2, rows // 2), BF16), VMEM((8, hd), F32),
                VMEM((dl, qw), BF16), VMEM((ntx, dl, 2 * fb), BF16), VMEM((qn, dl), BF16), VMEM((ntx, fb, dl), BF16),
                VMEM((rows + 16, dl), BF16), VMEM((8, rows), F32), VMEM((ntx, 8, rows), F32),
                VMEM((16, hd), BF16), VMEM((ntx, 16, hd), BF16), VMEM((ntx, 16, hd), BF16), VMEM((ntx, 16, hd), BF16), VMEM((rows, rows), F32),
                VMEM((ntx, rb, qw), F32), VMEM((nx, rb, qw), BF16), VMEM((nx, rb, qw), BF16),
                VMEM((nx, rb, qw), BF16), VMEM((nx, rb, qw), BF16), VMEM((rb, qw), F32), VMEM((2, rb, hd), F32),
                VMEM((ny, sb * lh, hd), F32), VMEM((ny, sb * lh, hd), F32),
                VMEM((nx, rows, 2 * fb), F32), VMEM((nx, rows, 2 * fb), BF16), VMEM((nx, rows, 2 * fb), BF16),
                VMEM((nx - 1, rows, 2 * fb), BF16), VMEM((nx - 1, rows, 2 * fb), BF16),
                VMEM((2, 8, hd), F32), VMEM((ny * lh, hd), F32), VMEM((ny * lh, ctx), F32), VMEM((ny, sb * lh, hd), F32),
                VMEM((ny, sb * lh, hd), BF16), VMEM((ny, sb * lh, hd), BF16), VMEM((lh, rb, hd), F32),
                VMEM((ntx, lh, rb, hd), BF16), VMEM((ntx, rows, fb), BF16), VMEM((rows, dl), F32),
                VMEM((2, ny, yb // 2, dl), BF16), VMEM((2, ny, yb // 2, dl), BF16), VMEM((2, ny, yb // 2, dl), BF16),
                DMA((5,)), DMA, DMA((ntx,)), DMA((2,)), DMA, DMA,
                DMA, DMA, DMA, DMA, DMA, DMA, DMA, DMA, DMA, DMA, DMA, DMA,
                DMA, DMA((nx,)), DMA, DMA((nx - 1, SUBS)),
                DMA, DMA, DMA, DMA((nx - 1,)), DMA, DMA,
                DMA, DMA((nx - 1, SUBS)), DMA, DMA((nx,)), DMA((2,)), DMA((2,)), DMA((2,)), DMA((2,)),
            ],
            compiler_params=pltpu.CompilerParams(collective_id=0, has_side_effects=True, vmem_limit_bytes=52 * 1024 * 1024),
            name="step",
        )(lens_part, x_blk, gamma_blk, perm, back, freqs, w_query, w_key, w_value, w_gate, w_up, k_blk, v_blk, w_out, w_down)

        return pl.pallas_call(
            functools.partial(store_kernel, ny, ntx),
            out_shape=(
                jax.ShapeDtypeStruct((rows, dl), BF16),
                jax.ShapeDtypeStruct(k_blk.shape, BF16),
                jax.ShapeDtypeStruct(v_blk.shape, BF16),
            ),
            in_specs=[sspec] + [vspec] * 4,
            out_specs=(hspec,) * 3,
            scratch_shapes=[VMEM((2, sb, PIECE, hd), BF16), DMA, DMA((2, sb, 2))],
            compiler_params=pltpu.CompilerParams(vmem_limit_bytes=4 * 1024 * 1024),
            name="store",
        )(lens_part, y_vm, new_rows, k_vm, v_vm)

    in_specs = (P("dp", "tx"), P("dp"), cache_spec, cache_spec, P("tx"), P("tx", "ty"), P("tx", None), P("tx", None), P("tx", "ty"), P("tx", "ty"), P("ty", "tx"), P("ty", "tx"))
    out_specs = (P("dp", "tx"), cache_spec, cache_spec)
    return jax.shard_map(layer_shard, mesh=mesh, in_specs=in_specs, out_specs=out_specs, check_vma=False)
```

```python
import functools

import jax
import jax.numpy as jnp
import numpy as np
from jax import lax
from jax.experimental import pallas as pl
from jax.experimental.pallas import tpu as pltpu
from jax.sharding import PartitionSpec as P

EPSILON = 1e-6
ROPE_BASE = 10000.0
LOG2E = 1.4426950408889634
MESH = pl.DeviceIdType.MESH
F32 = jnp.float32
BF16 = jnp.bfloat16
VMEM = pltpu.VMEM
DMA = pltpu.SemaphoreType.DMA
SUBS = 8
CHUNK = 1024
PIECE = 512
scope = jax.named_scope


def remote(src, dst, send_sem, recv_sem, tx=None, ty=None):
    device = {}
    if tx is not None:
        device["tx"] = tx
    if ty is not None:
        device["ty"] = ty
    return pltpu.make_async_remote_copy(src_ref=src, dst_ref=dst, send_sem=send_sem, recv_sem=recv_sem, device_id=device, device_id_type=MESH)


def step_kernel(ny, nx, d_model, lens_ref, x_h, gamma_h, perm_h, back_h, freq_h, wq_h, wk_h, wv_h, wg_h, wu_h, k_h, v_h, wo_h, wd_h,
                y_out, new_out, kbuf, vbuf,
                x_v, gamma_v, perm_v, back_v, freq_v, wq_v, wb_v, wo_v, wd_v, h_v, stat_s, stat_r, gq_s, gq_r, gb_s, gb_r, norm,
                qp, qd_s, qd_r, qx_s, qx_r, qsum, kvs, qy_s, qy_r, own, d_s, d_r, r_s, r_r,
                turns, qs, sbuf, o32, ay_s, ay_r, g32, g_v, b_v, acc, y_s, y_r, yf,
                in_sem, wq_sem, wb_sem, kv_sem, wo_sem, wd_sem, stat_ss, stat_rs, gq_ss, gq_rs, gb_ss, gb_rs, qd_ss, qd_rs, qx_ss, qx_rs, qy_ss, qy_rs,
                d_ss, d_rs, r_ss, r_rs, ay_ss, ay_rs, g_ss, g_rs, gp_ss, gp_rs, b_ss, b_rs, bp_ss, bp_rs, y_ss, y_rs, f_ss, f_rs):
    row = lax.axis_index("ty")
    col = lax.axis_index("tx")
    chip = lax.div(col, 2)
    core = lax.rem(col, 2)
    step = 1 - 2 * core
    ntx = 2 * nx
    rows, dl = x_h.shape
    rb = rows // ntx
    sb = rb // ny
    qn = wq_h.shape[1]
    hd = wk_h.shape[1]
    qw = qn + 2 * hd
    lh = qn // hd
    heads = ny * lh
    ctx = k_h.shape[1]
    fb = wb_v.shape[2] // 2
    sub = rows // SUBS
    yb = rows // ny
    partner = lax.rem(col + 1, 2) + 2 * chip
    after = 2 * lax.rem(chip + step + nx, nx) + core
    before = 2 * lax.rem(chip - step + nx, nx) + core
    tx_peers = [lax.rem(col + k, ntx) for k in range(1, ntx)]
    x_peers = [2 * lax.rem(chip + k, nx) + core for k in range(1, nx)]
    y_peers = [lax.rem(row + k, ny) for k in range(1, ny)]
    y_froms = [lax.rem(row - k + ny, ny) for k in range(1, ny)]

    barrier = pltpu.get_barrier_semaphore()
    for peer in tx_peers:
        pl.semaphore_signal(barrier, inc=1, device_id={"tx": peer}, device_id_type=MESH)
    for peer in y_peers:
        pl.semaphore_signal(barrier, inc=1, device_id={"ty": peer}, device_id_type=MESH)

    def piece(t):
        return pl.ds(pl.multiple_of(t * sub, sub), sub)

    def block_of(s, mine):
        sign = step if mine else -step
        at = lax.rem(chip - (s + 1) * sign + 2 * nx, nx)
        return 2 * at + (core if mine else 1 - core)

    def held(kind, mine):
        away = (0, -1, 1, 2)[kind] * (step if mine else -step)
        return 2 * lax.rem(chip + away + 2 * nx, nx) + (core if mine else 1 - core)

    def block_loads(n, b):
        at = pl.ds(pl.multiple_of(b * fb, fb), fb)
        return [
            pltpu.make_async_copy(wg_h.at[:, at], wb_v.at[n, :, pl.ds(0, fb)], wb_sem.at[n]),
            pltpu.make_async_copy(wu_h.at[:, at], wb_v.at[n, :, pl.ds(fb, fb)], wb_sem.at[n]),
        ]

    def wd_load(n, b):
        at = pl.ds(pl.multiple_of(b * fb, fb), fb)
        return pltpu.make_async_copy(wd_h.at[at, :], wd_v.at[n], wd_sem)

    first_loads = [
        pltpu.make_async_copy(x_h, x_v, in_sem.at[0]),
        pltpu.make_async_copy(perm_h, perm_v, in_sem.at[1]),
        pltpu.make_async_copy(gamma_h, gamma_v, in_sem.at[2]),
        pltpu.make_async_copy(freq_h, freq_v, in_sem.at[3]),
        pltpu.make_async_copy(back_h, back_v, in_sem.at[4]),
    ]
    q_loads = [
        pltpu.make_async_copy(wq_h, wq_v.at[:, pl.ds(0, qn)], wq_sem),
        pltpu.make_async_copy(wk_h, wq_v.at[:, pl.ds(qn, hd)], wq_sem),
        pltpu.make_async_copy(wv_h, wq_v.at[:, pl.ds(qn + hd, hd)], wq_sem),
    ]
    k_in = [pltpu.make_async_copy(k_h.at[r], kbuf.at[r], kv_sem.at[0]) for r in range(sb)]
    v_in = [pltpu.make_async_copy(v_h.at[r], vbuf.at[r], kv_sem.at[1]) for r in range(sb)]
    wo_load = pltpu.make_async_copy(wo_h, wo_v, wo_sem)
    def start_block(s, mine):
        for c in block_loads(2 * s + int(mine), block_of(s, mine)):
            c.start()

    for c in first_loads + q_loads:
        c.start()
    for c in first_loads:
        c.wait()
    start_block(0, False)
    start_block(0, True)

    xp = jnp.dot(perm_v[...], x_v[...], preferred_element_type=F32)
    own_mean = jnp.sum(xp, axis=1, keepdims=True) / dl
    xc = xp - own_mean
    gamma = gamma_v[...].reshape(1, dl)
    h_v[:rows] = (xc * gamma).astype(BF16)
    extra = lax.broadcasted_iota(jnp.int32, (16, dl), 0)
    h_v[rows:] = jnp.where(extra == 0, gamma, jnp.where(extra == 1, gamma - gamma.astype(BF16).astype(F32), 0.0)).astype(BF16)
    lane = lax.broadcasted_iota(jnp.int32, (rows, rows), 1)
    both = jnp.where(lane == 0, own_mean, jnp.where(lane == 1, jnp.sum(xc * xc, axis=1, keepdims=True), 0.0))
    stat_s[...] = jnp.transpose(both)[:8]

    def gamma_row(vals, tiles):
        row_sum = vals[0:1, :] + vals[1:2, :]
        parts = [row_sum[:, n * hd:(n + 1) * hd] for n in range(tiles)]
        return jnp.concatenate(parts + [jnp.zeros((16 - tiles, hd), F32)], axis=0).astype(BF16)

    pltpu.make_async_copy(wq_v, wq_v, wq_sem).wait()
    start_block(1, False)
    part = jnp.dot(h_v[...], wq_v[...], preferred_element_type=F32)
    qp[...] = part[:rows].reshape(ntx, rb, qw)
    gq_s[...] = gamma_row(part[rows:], qw // hd)
    for n in range(nx):
        qd_s[n] = qp[2 * n + 1 - core].astype(BF16)
    qd_cp = remote(qd_s, qd_r, qd_ss, qd_rs, tx=partner)
    stat_cp = [remote(stat_s, stat_r.at[k], stat_ss, stat_rs, tx=tx_peers[k - 1]) for k in range(1, ntx)]
    gq_cp = [remote(gq_s, gq_r.at[k], gq_ss, gq_rs, tx=tx_peers[k - 1]) for k in range(1, ntx)]
    gb_cp = [remote(gb_s.at[tx_peers[k - 1]], gb_r.at[k], gb_ss, gb_rs, tx=tx_peers[k - 1]) for k in range(1, ntx)]
    with scope("greet"):
        pl.semaphore_wait(barrier, ntx - 1 + ny - 1)
    qd_cp.start()
    for c in stat_cp + gq_cp:
        c.start()
    stat_r[0] = stat_s[...]
    gq_r[0] = gq_s[...]

    def rest_of_norm():
        with scope("stat"):
            remote(stat_r.at[pl.ds(1, ntx - 1)], stat_r.at[pl.ds(1, ntx - 1)], stat_ss, stat_rs, tx=partner).wait_recv()
            remote(gq_r.at[pl.ds(1, ntx - 1)], gq_r.at[pl.ds(1, ntx - 1)], gq_ss, gq_rs, tx=partner).wait_recv()
        means = jnp.concatenate([stat_r[k, 0:1, :] for k in range(ntx)], axis=0)
        squares = jnp.concatenate([stat_r[k, 1:2, :] for k in range(ntx)], axis=0)
        off = means - jnp.sum(means, axis=0, keepdims=True) / ntx
        var = jnp.sum(squares, axis=0, keepdims=True) / d_model + jnp.sum(off * off, axis=0, keepdims=True) / ntx
        scale = lax.rsqrt(var + EPSILON)
        norm[...] = jnp.transpose(jnp.concatenate([off, scale, jnp.zeros((rows - ntx - 1, rows), F32)], axis=0))

    def normed(vals, at, g_ref):
        cols = norm[at, :]
        tiles = []
        for n in range(vals.shape[1] // hd):
            tile = vals[:, n * hd:(n + 1) * hd]
            for k in range(ntx):
                tile = tile + cols[:, k:k + 1] * g_ref[k, n:n + 1, :].astype(F32)
            tiles.append(tile * cols[:, ntx:ntx + 1])
        return jnp.concatenate(tiles, axis=1)


    def q_of(away):
        at = lax.rem(chip + away + nx, nx)
        return qp[2 * at + core] + qd_r[at].astype(F32)

    qx_in = qx_r.at[pl.ds(1, nx - 1)]

    qy_cp = [remote(qy_s.at[y_peers[k - 1]], qy_r.at[row], qy_ss, qy_rs, ty=y_peers[k - 1]) for k in range(1, ny)]

    def q_pair():
        with scope("qd"):
            qd_cp.wait_recv()
        for k in (2, 1, 3):
            qx_s[k] = q_of(k).astype(BF16)
            remote(qx_s.at[k], qx_r.at[k], qx_ss, qx_rs, tx=x_peers[k - 1]).start()

    def q_rows():
        mine = q_of(0)
        rest_of_norm()
        with scope("qx"):
            remote(qx_in, qx_in, qx_ss, qx_rs, tx=partner).wait_recv()
        for k in range(1, nx):
            mine = mine + qx_r[k].astype(F32)
        mine = normed(mine, pl.ds(pl.multiple_of(col * rb, rb), rb), gq_r)
        qsum[...] = mine
        kvs[0] = mine[:, qn:qn + hd]
        kvs[1] = mine[:, qn + hd:]
        for a in range(ny):
            for n in range(lh):
                qy_s[a, n * sb:(n + 1) * sb, :] = qsum[a * sb:(a + 1) * sb, n * hd:(n + 1) * hd]
        for c in qy_cp:
            c.start()
        qy_r[row] = qy_s[row]

    def tables():
        at_row = lax.broadcasted_iota(jnp.int32, (8, hd), 0)
        places = jnp.zeros((8, hd), F32)
        for r in range(sb):
            places = jnp.where(at_row == r, lens_ref[(row * ntx + col) * sb + r].astype(F32), places)
        angles = places * freq_v[...]
        turns[0] = jnp.cos(angles)
        low_half = lax.broadcasted_iota(jnp.int32, (8, hd), 1) < hd // 2
        sines = jnp.sin(angles)
        turns[1] = jnp.where(low_half, -sines, sines)

    def d_copy(s):
        return remote(d_s.at[s], d_r.at[s], d_ss, d_rs.at[s], tx=partner)

    def r_copy(s, t):
        return remote(r_s.at[s, piece(t)], r_r.at[s, piece(t)], r_ss, r_rs.at[s, t], tx=after)

    def product(s, carry):
        pltpu.make_async_copy(wb_v.at[2 * s], wb_v.at[2 * s], wb_sem.at[2 * s]).wait()

        @pl.when(s < nx - 1)
        def _():
            start_block(s + 1, True)

        part = jnp.dot(h_v[...], wb_v[2 * s], preferred_element_type=F32)
        d_s[s] = part[:rows].astype(BF16)
        d_copy(s).start()
        gb_s[block_of(s, False)] = gamma_row(part[rows:], 2 * fb // hd)

        @pl.when(s == 0)
        def _():
            q_pair()

        pltpu.make_async_copy(wb_v.at[2 * s + 1], wb_v.at[2 * s + 1], wb_sem.at[2 * s + 1]).wait()

        @pl.when(s < nx - 2)
        def _():
            start_block(s + 2, False)

        part = jnp.dot(h_v[...], wb_v[2 * s + 1], preferred_element_type=F32)
        own[s] = part[:rows]
        gb_s[block_of(s, True)] = gamma_row(part[rows:], 2 * fb // hd)

        @pl.when(s == 0)
        def _():
            with scope("d0"):
                d_copy(0).wait_recv()
            for t in range(SUBS):
                at = piece(t)
                r_s[0, at] = (own[0, at] + d_r[0, at].astype(F32)).astype(BF16)
                r_copy(0, t).start()

        return carry

    with scope("products"):
        lax.fori_loop(0, nx, product, 0)
    for c in gb_cp + k_in + v_in:
        c.start()
    gb_r[0] = gb_s[col]
    tables()

    def ring(s, t):
        at = piece(t)
        if t == 0:
            with scope("d%d" % s):
                d_copy(s).wait_recv()
        part = own[s, at] + d_r[s, at].astype(F32)
        with scope("r%d%d" % (s, t)):
            r_copy(s - 1, t).wait_recv()
        part = part + r_r[s - 1, at].astype(F32)
        if s < nx - 1:
            r_s[s, at] = part.astype(BF16)
            r_copy(s, t).start()
        else:
            if t == 0:
                with scope("gb"):
                    remote(gb_r.at[pl.ds(1, ntx - 1)], gb_r.at[pl.ds(1, ntx - 1)], gb_ss, gb_rs, tx=partner).wait_recv()
            part = normed(part, at, gb_r)
            gate = part[:, :fb].astype(BF16).astype(F32)
            up = part[:, fb:].astype(BF16).astype(F32)
            b_v[col, at] = (gate * (1.0 / (1.0 + jnp.exp(-gate))) * up).astype(BF16)
            act_out(t)

    def turn(vals, r):
        return vals * turns[0, r:r + 1, :] + pltpu.roll(vals, hd // 2, 1) * turns[1, r:r + 1, :]

    def attend(r):
        length = lens_ref[(row * ntx + col) * sb + r]
        for a in range(ny):
            qs[a * lh:(a + 1) * lh, :] = turn(qy_r[a, pl.ds(r, lh, stride=sb), :], r)
        q = qs[...].astype(BF16)
        k_new = turn(kvs[0, pl.ds(row * sb + r, 1), :], r).astype(BF16).astype(F32)
        v_new = kvs[1, pl.ds(row * sb + r, 1), :].astype(BF16).astype(F32)
        new_out[r:r + 1, :] = k_new
        new_out[sb + r:sb + r + 1, :] = v_new
        s_new = jnp.sum(q.astype(F32) * k_new, axis=1, keepdims=True)
        top = jnp.full((heads, hd), -1e30, F32)
        for c in range(ctx // CHUNK):
            s = lax.dot_general(q, kbuf[r, c * CHUNK:(c + 1) * CHUNK, :], (((1,), (1,)), ((), ())), preferred_element_type=F32)
            pos = lax.broadcasted_iota(jnp.int32, (1, CHUNK), 1) + c * CHUNK
            s = jnp.where(pos < length, s, -1e30)
            sbuf[:, c * CHUNK:(c + 1) * CHUNK] = s
            for t in range(CHUNK // hd):
                top = jnp.maximum(top, s[:, t * hd:(t + 1) * hd])
        high = jnp.maximum(jnp.max(top, axis=1, keepdims=True), s_new)
        rate = hd ** -0.5 * LOG2E
        e_new = jnp.exp2((s_new - high) * rate)
        low = jnp.zeros((heads, hd), F32)
        out = e_new.astype(BF16).astype(F32) * v_new
        for c in range(ctx // CHUNK):
            e = jnp.exp2((sbuf[:, c * CHUNK:(c + 1) * CHUNK] - high) * rate)
            for t in range(CHUNK // hd):
                low = low + e[:, t * hd:(t + 1) * hd]
            out = out + jnp.dot(e.astype(BF16), vbuf[r, c * CHUNK:(c + 1) * CHUNK, :], preferred_element_type=F32)
        out = out / (jnp.sum(low, axis=1, keepdims=True) + e_new)
        for a in range(ny):
            o32[a, pl.ds(r, lh, stride=sb), :] = out[a * lh:(a + 1) * lh]

    def b_send(kind, t, slot, to):
        b = held(kind, True)
        return remote(b_v.at[b, piece(t)], b_v.at[b, piece(t)], b_ss, b_rs.at[slot - 1, t], tx=to)

    def b_in(kind, t):
        b = held(kind, True)
        return remote(b_v.at[b, piece(t)], b_v.at[b, piece(t)], b_ss, b_rs.at[kind - 1, t], tx=after)

    def b_pair(kind, t):
        b = held(kind, True)
        return remote(b_v.at[b, piece(t)], b_v.at[b, piece(t)], bp_ss, bp_rs.at[kind], tx=partner)

    def act_out(t):
        b_send(0, t, 1, after).start()
        b_send(0, t, 2, before).start()
        b_pair(0, t).start()

    def act_in(kind, t):
        with scope("b%d%d" % (kind, t)):
            b_in(kind, t).wait_recv()
        if kind == 1:
            b_send(1, t, 3, after).start()
        b_pair(kind, t).start()

    ay_cp = [remote(ay_s.at[y_peers[k - 1]], ay_r.at[row], ay_ss, ay_rs, ty=y_peers[k - 1]) for k in range(1, ny)]

    def g_send(kind, slot, to):
        at = held(kind, True)
        return remote(g_v.at[at], g_v.at[at], g_ss, g_rs.at[slot - 1], tx=to)

    def g_pair(kind):
        at = held(kind, True)
        return remote(g_v.at[at], g_v.at[at], gp_ss, gp_rs, tx=partner)

    def g_in(kind):
        at = held(kind, True)
        with scope("g%d" % kind):
            remote(g_v.at[at], g_v.at[at], g_ss, g_rs.at[kind - 1], tx=after).wait_recv()
        if kind == 1:
            g_send(1, 3, after).start()
        g_pair(kind).start()

    def att_out():
        ay_s[...] = o32[...].astype(BF16)
        for c in ay_cp:
            c.start()
        ay_r[row] = ay_s[row]

    def att_rows():
        with scope("ay"):
            remote(ay_r.at[pl.ds(0, ny - 1)], ay_r.at[pl.ds(0, ny - 1)], ay_ss, ay_rs, ty=y_peers[0]).wait_recv()
        for a in range(ny):
            part = ay_r[a].astype(F32)
            for n in range(lh):
                g32[n, a * sb:(a + 1) * sb, :] = part[n * sb:(n + 1) * sb, :]
        g_v[col] = g32[...].astype(BF16)
        g_send(0, 1, after).start()
        g_send(0, 2, before).start()
        g_pair(0).start()

    mid = rows // 2

    def half_rows(half):
        return pl.ds(half * mid, mid)

    def down(n):
        if n % 2:
            b = held(n // 2, False)
            with scope("bp%d" % (n // 2)):
                remote(b_v.at[b], b_v.at[b], bp_ss, bp_rs.at[n // 2], tx=partner).wait_recv()
        part = jnp.dot(b_v[held(n // 2, n % 2 == 0)], wd_v[n], preferred_element_type=F32)
        acc[...] = part if n == 0 else acc[...] + part

    def att_down(half):
        at = pl.ds(half * nx, nx)
        part = acc[half_rows(half)]
        for n in range(0, lh, 2):
            pair = jnp.concatenate([g_v[at, n].reshape(mid, hd), g_v[at, n + 1].reshape(mid, hd)], axis=1)
            part = part + jnp.dot(pair, wo_v[n * hd:(n + 2) * hd, :], preferred_element_type=F32)
        acc[half_rows(half)] = part

    def y_out_half(half):
        part = jnp.dot(back_v[...], acc[half_rows(half)].astype(BF16), preferred_element_type=F32)
        y_s[half] = part.astype(BF16).reshape(ny, yb // 2, dl)
        for k in range(1, ny):
            remote(y_s.at[half, y_peers[k - 1]], y_r.at[half, k], y_ss.at[half], y_rs.at[half], ty=y_peers[k - 1]).start()

    def y_sum_half(half):
        at = pl.ds(pl.multiple_of(row * yb + half * (yb // 2), yb // 2), yb // 2)
        total = x_v[at, :].astype(F32) + y_s[half, row].astype(F32)
        rest = y_r.at[half, pl.ds(1, ny - 1)]
        with scope("y%d" % half):
            remote(rest, rest, y_ss.at[half], y_rs.at[half], ty=y_peers[0]).wait_recv()
        for k in range(1, ny):
            total = total + y_r[half, k].astype(F32)
        yf[half, row] = total.astype(BF16)
        for k in range(1, ny):
            remote(yf.at[half, row], yf.at[half, row], f_ss.at[half], f_rs.at[half], ty=y_peers[k - 1]).start()

    def y_all_half(half):
        rest = yf.at[half, pl.ds(0, ny - 1)]
        with scope("f%d" % half):
            remote(rest, rest, f_ss.at[half], f_rs.at[half], ty=y_peers[0]).wait_recv()
        for a in range(ny):
            y_out[a * yb + half * (yb // 2):a * yb + (half + 1) * (yb // 2), :] = yf[half, a]

    q_rows()
    for t in range(SUBS):
        ring(1, t)
    for n in range(ntx):
        wd_load(n, held(n // 2, n % 2 == 0)).start()
    wo_load.start()
    for t in range(SUBS):
        ring(2, t)
        if t == 0:
            with scope("qy"):
                remote(qy_r.at[pl.ds(0, ny - 1)], qy_r.at[pl.ds(0, ny - 1)], qy_ss, qy_rs, ty=y_peers[0]).wait_recv()
            pltpu.make_async_copy(kbuf, kbuf, kv_sem.at[0]).wait()
            pltpu.make_async_copy(vbuf, vbuf, kv_sem.at[1]).wait()
        if t % (SUBS // sb) == 0:
            with scope("a%d" % (t * sb // SUBS)):
                attend(t * sb // SUBS)
    att_out()
    for t in range(SUBS):
        ring(3, t)
    att_rows()
    pltpu.make_async_copy(wd_v, wd_v, wd_sem).wait()
    down(0)
    for t in range(SUBS):
        act_in(1, t)
        act_in(2, t)
    g_in(1)
    g_in(2)
    for n in (1, 2, 4, 3, 5):
        down(n)
    for t in range(SUBS):
        act_in(3, t)
    g_in(3)
    down(6)
    down(7)
    with scope("gp"):
        remote(g_v.at[pl.ds(0, nx)], g_v.at[pl.ds(0, nx)], gp_ss, gp_rs, tx=partner).wait_recv()
    wo_load.wait()
    for half in range(2):
        att_down(half)
        y_out_half(half)
    y_sum_half(0)
    y_sum_half(1)
    y_all_half(0)
    y_all_half(1)

    with scope("sends"):
        qd_cp.wait_send()
        for ref, send, recv in (
            (stat_r.at[pl.ds(1, ntx - 1)], stat_ss, stat_rs), (gq_r.at[pl.ds(1, ntx - 1)], gq_ss, gq_rs), (gb_r.at[pl.ds(1, ntx - 1)], gb_ss, gb_rs),
            (qx_in, qx_ss, qx_rs), (qy_s.at[pl.ds(1, ny - 1)], qy_ss, qy_rs), (ay_s.at[pl.ds(1, ny - 1)], ay_ss, ay_rs),
            *((y_s.at[half, pl.ds(1, ny - 1)], y_ss.at[half], y_rs.at[half]) for half in range(2)),
            *((yf.at[half, pl.ds(1, ny - 1)], f_ss.at[half], f_rs.at[half]) for half in range(2)),
            (d_s, d_ss, d_rs.at[0]), (r_s, r_ss, r_rs.at[0, 0]), (g_v.at[pl.ds(1, nx - 1)], g_ss, g_rs.at[0]), (g_v.at[pl.ds(0, nx)], gp_ss, gp_rs),
            (b_v.at[pl.ds(1, nx - 1)], b_ss, b_rs.at[0, 0]), (b_v.at[pl.ds(0, nx)], bp_ss, bp_rs.at[0]),
        ):
            remote(ref, ref, send, recv, tx=partner).wait_send()


def store_kernel(ny, ntx, lens_ref, y_v, new_v, k_v, v_v, y_h, ko_h, vo_h, patch, y_sem, out_sem):
    first = (lax.axis_index("ty") * ntx + lax.axis_index("tx")) * k_v.shape[0]
    sb, ctx, hd = k_v.shape
    pieces = ctx // PIECE
    y_cp = pltpu.make_async_copy(y_v, y_h, y_sem)
    y_cp.start()

    def write(a, buf, out):
        def sequence(r, carry):
            length = lens_ref[first + r]
            spot = lax.div(length, PIECE)

            def other(c, inner):
                c = c + jnp.where(c >= spot, 1, 0)
                rest = pl.ds(pl.multiple_of(c * PIECE, PIECE), PIECE)
                pltpu.make_async_copy(buf.at[r, rest], out.at[r, rest], out_sem.at[a, r, 1]).start()
                return inner

            lax.fori_loop(0, pieces - 1, other, 0)
            at = pl.ds(pl.multiple_of(spot * PIECE, PIECE), PIECE)
            here = lax.broadcasted_iota(jnp.int32, (PIECE, hd), 0) == length - spot * PIECE
            patch[a, r] = jnp.where(here, new_v[pl.ds(a * sb + r, 1), :], buf[r, at, :].astype(F32)).astype(BF16)
            pltpu.make_async_copy(patch.at[a, r], out.at[r, at], out_sem.at[a, r, 0]).start()
            return carry

        lax.fori_loop(0, sb, sequence, 0)

    def finish(a, buf, out):
        for r in range(sb):
            pltpu.make_async_copy(patch.at[a, r], out.at[r, pl.ds(0, PIECE)], out_sem.at[a, r, 0]).wait()
            rest = pl.ds(0, ctx - PIECE)
            pltpu.make_async_copy(buf.at[r, rest], out.at[r, rest], out_sem.at[a, r, 1]).wait()

    write(0, k_v, ko_h)
    write(1, v_v, vo_h)
    y_cp.wait()
    finish(0, k_v, ko_h)
    finish(1, v_v, vo_h)


def solution(mesh):
    ny = mesh.shape["ty"]
    ntx = mesh.shape["tx"]
    nx = ntx // 2
    cache_spec = P(("dp", "ty", "tx"), None, None)
    vspec = pl.BlockSpec(memory_space=VMEM)
    hspec = pl.BlockSpec(memory_space=pltpu.HBM)
    sspec = pl.BlockSpec(memory_space=pltpu.SMEM)

    def layer_shard(x_blk, lens_part, k_blk, v_blk, gamma_blk, w_query, w_key, w_value, w_gate, w_up, w_out, w_down):
        rows, dl = x_blk.shape
        sb, ctx, hd = k_blk.shape
        qn = w_query.shape[1]
        lh = qn // hd
        qw = qn + 2 * hd
        fb = w_gate.shape[1] // ntx
        rb = rows // ntx
        yb = rows // ny

        natural = np.arange(rows)
        order = np.reshape(np.transpose(np.reshape(natural, (ny, ntx, sb)), (1, 0, 2)), (rows,))
        perm = jnp.asarray(order[:, None] == natural[None, :], dtype=BF16)
        part = np.arange(rows // 2)
        order = np.reshape(np.transpose(np.reshape(part, (nx, ny, sb)), (1, 0, 2)), (rows // 2,))
        back = jnp.asarray(order[:, None] == part[None, :], dtype=BF16)
        freqs = np.power(ROPE_BASE, -(np.arange(hd // 2, dtype=np.float32) * 2.0) / hd).astype(np.float32)
        freqs = jnp.asarray(np.tile(np.concatenate([freqs, freqs])[None, :], (8, 1)))

        y_vm, new_rows, k_vm, v_vm = pl.pallas_call(
            functools.partial(step_kernel, ny, nx, dl * ntx),
            out_shape=(
                pltpu.VMEM((rows, dl), BF16),
                pltpu.VMEM((2 * sb, hd), F32),
                pltpu.VMEM(k_blk.shape, BF16),
                pltpu.VMEM(v_blk.shape, BF16),
            ),
            in_specs=[sspec] + [hspec] * 14,
            out_specs=(vspec,) * 4,
            scratch_shapes=[
                VMEM((rows, dl), BF16), VMEM((dl,), F32), VMEM((rows, rows), BF16), VMEM((rows // 2, rows // 2), BF16), VMEM((8, hd), F32),
                VMEM((dl, qw), BF16), VMEM((ntx, dl, 2 * fb), BF16), VMEM((qn, dl), BF16), VMEM((ntx, fb, dl), BF16),
                VMEM((rows + 16, dl), BF16), VMEM((8, rows), F32), VMEM((ntx, 8, rows), F32),
                VMEM((16, hd), BF16), VMEM((ntx, 16, hd), BF16), VMEM((ntx, 16, hd), BF16), VMEM((ntx, 16, hd), BF16), VMEM((rows, rows), F32),
                VMEM((ntx, rb, qw), F32), VMEM((nx, rb, qw), BF16), VMEM((nx, rb, qw), BF16),
                VMEM((nx, rb, qw), BF16), VMEM((nx, rb, qw), BF16), VMEM((rb, qw), F32), VMEM((2, rb, hd), F32),
                VMEM((ny, sb * lh, hd), F32), VMEM((ny, sb * lh, hd), F32),
                VMEM((nx, rows, 2 * fb), F32), VMEM((nx, rows, 2 * fb), BF16), VMEM((nx, rows, 2 * fb), BF16),
                VMEM((nx - 1, rows, 2 * fb), BF16), VMEM((nx - 1, rows, 2 * fb), BF16),
                VMEM((2, 8, hd), F32), VMEM((ny * lh, hd), F32), VMEM((ny * lh, ctx), F32), VMEM((ny, sb * lh, hd), F32),
                VMEM((ny, sb * lh, hd), BF16), VMEM((ny, sb * lh, hd), BF16), VMEM((lh, rb, hd), F32),
                VMEM((ntx, lh, rb, hd), BF16), VMEM((ntx, rows, fb), BF16), VMEM((rows, dl), F32),
                VMEM((2, ny, yb // 2, dl), BF16), VMEM((2, ny, yb // 2, dl), BF16), VMEM((2, ny, yb // 2, dl), BF16),
                DMA((5,)), DMA, DMA((ntx,)), DMA((2,)), DMA, DMA,
                DMA, DMA, DMA, DMA, DMA, DMA, DMA, DMA, DMA, DMA, DMA, DMA,
                DMA, DMA((nx,)), DMA, DMA((nx - 1, SUBS)),
                DMA, DMA, DMA, DMA((nx - 1,)), DMA, DMA,
                DMA, DMA((nx - 1, SUBS)), DMA, DMA((nx,)), DMA((2,)), DMA((2,)), DMA((2,)), DMA((2,)),
            ],
            compiler_params=pltpu.CompilerParams(collective_id=0, has_side_effects=True, vmem_limit_bytes=52 * 1024 * 1024),
            name="step",
        )(lens_part, x_blk, gamma_blk, perm, back, freqs, w_query, w_key, w_value, w_gate, w_up, k_blk, v_blk, w_out, w_down)

        return pl.pallas_call(
            functools.partial(store_kernel, ny, ntx),
            out_shape=(
                jax.ShapeDtypeStruct((rows, dl), BF16),
                jax.ShapeDtypeStruct(k_blk.shape, BF16),
                jax.ShapeDtypeStruct(v_blk.shape, BF16),
            ),
            in_specs=[sspec] + [vspec] * 4,
            out_specs=(hspec,) * 3,
            scratch_shapes=[VMEM((2, sb, PIECE, hd), BF16), DMA, DMA((2, sb, 2))],
            compiler_params=pltpu.CompilerParams(vmem_limit_bytes=4 * 1024 * 1024),
            name="store",
        )(lens_part, y_vm, new_rows, k_vm, v_vm)

    in_specs = (P("dp", "tx"), P("dp"), cache_spec, cache_spec, P("tx"), P("tx", "ty"), P("tx", None), P("tx", None), P("tx", "ty"), P("tx", "ty"), P("ty", "tx"), P("ty", "tx"))
    out_specs = (P("dp", "tx"), cache_spec, cache_spec)
    return jax.shard_map(layer_shard, mesh=mesh, in_specs=in_specs, out_specs=out_specs, check_vma=False)
```

```python
import functools

import jax
import jax.numpy as jnp
import numpy as np
from jax import lax
from jax.experimental import pallas as pl
from jax.experimental.pallas import tpu as pltpu
from jax.sharding import PartitionSpec as P

EPSILON = 1e-6
ROPE_BASE = 10000.0
LOG2E = 1.4426950408889634
MESH = pl.DeviceIdType.MESH
F32 = jnp.float32
BF16 = jnp.bfloat16
VMEM = pltpu.VMEM
DMA = pltpu.SemaphoreType.DMA
SUBS = 8
CHUNK = 1024
EVEN = 6
scope = jax.named_scope


def remote(src, dst, send_sem, recv_sem, tx=None, ty=None):
    device = {}
    if tx is not None:
        device["tx"] = tx
    if ty is not None:
        device["ty"] = ty
    return pltpu.make_async_remote_copy(src_ref=src, dst_ref=dst, send_sem=send_sem, recv_sem=recv_sem, device_id=device, device_id_type=MESH)


def step_kernel(ny, nx, d_model, lens_ref, x_h, gamma_h, perm_h, back_h, freq_h, wq_h, wk_h, wv_h, wg_h, wu_h, k_h, v_h, wo_h, wd_h,
                y_out, kbuf, vbuf,
                x_v, gamma_v, perm_v, back_v, freq_v, wq_v, wb_v, wo_v, wd_v, h_v, stat_s, stat_r, gq_s, gq_r, gb_s, gb_r, norm,
                qp, qd_s, qd_r, new_rows, qx_s, qx_r, qsum, kvs, qy_s, qy_r, own, d_s, d_r, r_s, r_r,
                turns, qs, sbuf, o32, ay_s, ay_r, g32, g_v, b_v, acc, y_s, y_r, yf,
                in_sem, wq_sem, wb_sem, kv_sem, wo_sem, wd_sem, stat_ss, stat_rs, gq_ss, gq_rs, gb_ss, gb_rs, qd_ss, qd_rs, qx_ss, qx_rs, qy_ss, qy_rs,
                d_ss, d_rs, r_ss, r_rs, ay_ss, ay_rs, g_ss, g_rs, gp_ss, gp_rs, b_ss, b_rs, bp_ss, bp_rs, y_ss, y_rs, f_ss, f_rs):
    row = lax.axis_index("ty")
    col = lax.axis_index("tx")
    chip = lax.div(col, 2)
    core = lax.rem(col, 2)
    step = 1 - 2 * core
    ntx = 2 * nx
    rows, dl = x_h.shape
    rb = rows // ntx
    sb = rb // ny
    qn = wq_h.shape[1]
    hd = wk_h.shape[1]
    qw = qn + 2 * hd
    lh = qn // hd
    heads = ny * lh
    ctx = k_h.shape[1]
    fb = wb_v.shape[2] // 2
    sub = rows // SUBS
    yb = rows // ny
    partner = lax.rem(col + 1, 2) + 2 * chip
    after = 2 * lax.rem(chip + step + nx, nx) + core
    before = 2 * lax.rem(chip - step + nx, nx) + core
    right = 2 * lax.rem(chip + 1, nx) + core
    left = 2 * lax.rem(chip + nx - 1, nx) + core
    tx_peers = [lax.rem(col + k, ntx) for k in range(1, ntx)]
    x_peers = [2 * lax.rem(chip + k, nx) + core for k in range(1, nx)]
    y_peers = [lax.rem(row + k, ny) for k in range(1, ny)]
    y_froms = [lax.rem(row - k + ny, ny) for k in range(1, ny)]

    barrier = pltpu.get_barrier_semaphore()
    for peer in tx_peers:
        pl.semaphore_signal(barrier, inc=1, device_id={"tx": peer}, device_id_type=MESH)
    for peer in y_peers:
        pl.semaphore_signal(barrier, inc=1, device_id={"ty": peer}, device_id_type=MESH)

    def piece(t):
        return pl.ds(pl.multiple_of(t * sub, sub), sub)

    def block_of(s, mine):
        sign = step if mine else -step
        at = lax.rem(chip - (s + 1) * sign + 2 * nx, nx)
        return 2 * at + (core if mine else 1 - core)

    def held(kind, mine):
        away = (0, -1, 1, 2)[kind] * (step if mine else -step)
        return 2 * lax.rem(chip + away + 2 * nx, nx) + (core if mine else 1 - core)

    def block_loads(n, b):
        at = pl.ds(pl.multiple_of(b * fb, fb), fb)
        return [
            pltpu.make_async_copy(wg_h.at[:, at], wb_v.at[n, :, pl.ds(0, fb)], wb_sem.at[n]),
            pltpu.make_async_copy(wu_h.at[:, at], wb_v.at[n, :, pl.ds(fb, fb)], wb_sem.at[n]),
        ]

    def wd_load(n, b):
        at = pl.ds(pl.multiple_of(b * fb, fb), fb)
        return pltpu.make_async_copy(wd_h.at[at, :], wd_v.at[n], wd_sem)

    first_loads = [
        pltpu.make_async_copy(x_h, x_v, in_sem.at[0]),
        pltpu.make_async_copy(perm_h, perm_v, in_sem.at[1]),
        pltpu.make_async_copy(gamma_h, gamma_v, in_sem.at[2]),
        pltpu.make_async_copy(freq_h, freq_v, in_sem.at[3]),
        pltpu.make_async_copy(back_h, back_v, in_sem.at[4]),
    ]
    q_loads = [
        pltpu.make_async_copy(wq_h, wq_v.at[:, pl.ds(0, qn)], wq_sem),
        pltpu.make_async_copy(wk_h, wq_v.at[:, pl.ds(qn, hd)], wq_sem),
        pltpu.make_async_copy(wv_h, wq_v.at[:, pl.ds(qn + hd, hd)], wq_sem),
    ]
    k_in = [pltpu.make_async_copy(k_h.at[r], kbuf.at[r], kv_sem.at[0]) for r in range(sb)]
    v_in = [pltpu.make_async_copy(v_h.at[r], vbuf.at[r], kv_sem.at[1]) for r in range(sb)]
    wo_load = pltpu.make_async_copy(wo_h, wo_v, wo_sem)
    def start_block(s, mine):
        for c in block_loads(2 * s + int(mine), block_of(s, mine)):
            c.start()

    for c in first_loads + q_loads:
        c.start()
    for c in first_loads:
        c.wait()
    start_block(0, False)
    start_block(0, True)

    xp = jnp.dot(perm_v[...], x_v[...], preferred_element_type=F32)
    own_mean = jnp.sum(xp, axis=1, keepdims=True) / dl
    xc = xp - own_mean
    gamma = gamma_v[...].reshape(1, dl)
    h_v[:rows] = (xc * gamma).astype(BF16)
    extra = lax.broadcasted_iota(jnp.int32, (16, dl), 0)
    h_v[rows:] = jnp.where(extra == 0, gamma, jnp.where(extra == 1, gamma - gamma.astype(BF16).astype(F32), 0.0)).astype(BF16)
    lane = lax.broadcasted_iota(jnp.int32, (rows, rows), 1)
    both = jnp.where(lane == 0, own_mean, jnp.where(lane == 1, jnp.sum(xc * xc, axis=1, keepdims=True), 0.0))
    stat_s[...] = jnp.transpose(both)[:8]

    def gamma_row(vals, tiles):
        row_sum = vals[0:1, :] + vals[1:2, :]
        parts = [row_sum[:, n * hd:(n + 1) * hd] for n in range(tiles)]
        return jnp.concatenate(parts + [jnp.zeros((16 - tiles, hd), F32)], axis=0).astype(BF16)

    pltpu.make_async_copy(wq_v, wq_v, wq_sem).wait()
    start_block(1, False)
    part = jnp.dot(h_v[...], wq_v[...], preferred_element_type=F32)
    qp[...] = part[:rows].reshape(ntx, rb, qw)
    gq_s[...] = gamma_row(part[rows:], qw // hd)
    for n in range(nx):
        qd_s[n] = qp[2 * n + 1 - core].astype(BF16)
    qd_cp = remote(qd_s, qd_r, qd_ss, qd_rs, tx=partner)
    stat_cp = [remote(stat_s, stat_r.at[k], stat_ss, stat_rs, tx=tx_peers[k - 1]) for k in range(1, ntx)]
    gq_cp = [remote(gq_s, gq_r.at[k], gq_ss, gq_rs, tx=tx_peers[k - 1]) for k in range(1, ntx)]
    gb_cp = [remote(gb_s.at[tx_peers[k - 1]], gb_r.at[k], gb_ss, gb_rs, tx=tx_peers[k - 1]) for k in range(1, ntx)]
    with scope("greet"):
        pl.semaphore_wait(barrier, ntx - 1 + ny - 1)
    qd_cp.start()
    for c in stat_cp + gq_cp:
        c.start()
    stat_r[0] = stat_s[...]
    gq_r[0] = gq_s[...]

    def rest_of_norm():
        with scope("stat"):
            remote(stat_r.at[pl.ds(1, ntx - 1)], stat_r.at[pl.ds(1, ntx - 1)], stat_ss, stat_rs, tx=partner).wait_recv()
            remote(gq_r.at[pl.ds(1, ntx - 1)], gq_r.at[pl.ds(1, ntx - 1)], gq_ss, gq_rs, tx=partner).wait_recv()
        means = jnp.concatenate([stat_r[k, 0:1, :] for k in range(ntx)], axis=0)
        squares = jnp.concatenate([stat_r[k, 1:2, :] for k in range(ntx)], axis=0)
        off = means - jnp.sum(means, axis=0, keepdims=True) / ntx
        var = jnp.sum(squares, axis=0, keepdims=True) / d_model + jnp.sum(off * off, axis=0, keepdims=True) / ntx
        scale = lax.rsqrt(var + EPSILON)
        norm[...] = jnp.transpose(jnp.concatenate([off, scale, jnp.zeros((rows - ntx - 1, rows), F32)], axis=0))

    def normed(vals, at, g_ref):
        cols = norm[at, :]
        tiles = []
        for n in range(vals.shape[1] // hd):
            tile = vals[:, n * hd:(n + 1) * hd]
            for k in range(ntx):
                tile = tile + cols[:, k:k + 1] * g_ref[k, n:n + 1, :].astype(F32)
            tiles.append(tile * cols[:, ntx:ntx + 1])
        return jnp.concatenate(tiles, axis=1)


    def q_of(away):
        at = lax.rem(chip + away + nx, nx)
        return qp[2 * at + core] + qd_r[at].astype(F32)

    qx_in = qx_r.at[pl.ds(1, nx - 1)]

    qy_cp = [remote(qy_s.at[y_peers[k - 1]], qy_r.at[row], qy_ss, qy_rs, ty=y_peers[k - 1]) for k in range(1, ny)]

    def q_pair():
        with scope("qd"):
            qd_cp.wait_recv()
        for k in (2, 1, 3):
            qx_s[k] = q_of(k).astype(BF16)
            remote(qx_s.at[k], qx_r.at[k], qx_ss, qx_rs, tx=x_peers[k - 1]).start()

    def q_rows():
        mine = q_of(0)
        rest_of_norm()
        with scope("qx"):
            remote(qx_in, qx_in, qx_ss, qx_rs, tx=partner).wait_recv()
        for k in range(1, nx):
            mine = mine + qx_r[k].astype(F32)
        mine = normed(mine, pl.ds(pl.multiple_of(col * rb, rb), rb), gq_r)
        qsum[...] = mine
        kvs[0] = mine[:, qn:qn + hd]
        kvs[1] = mine[:, qn + hd:]
        for a in range(ny):
            for n in range(lh):
                qy_s[a, n * sb:(n + 1) * sb, :] = qsum[a * sb:(a + 1) * sb, n * hd:(n + 1) * hd]
        for c in qy_cp:
            c.start()
        qy_r[row] = qy_s[row]

    def tables():
        at_row = lax.broadcasted_iota(jnp.int32, (8, hd), 0)
        places = jnp.zeros((8, hd), F32)
        for r in range(sb):
            places = jnp.where(at_row == r, lens_ref[(row * ntx + col) * sb + r].astype(F32), places)
        angles = places * freq_v[...]
        turns[0] = jnp.cos(angles)
        low_half = lax.broadcasted_iota(jnp.int32, (8, hd), 1) < hd // 2
        sines = jnp.sin(angles)
        turns[1] = jnp.where(low_half, -sines, sines)

    def d_copy(s):
        return remote(d_s.at[s], d_r.at[s], d_ss, d_rs.at[s], tx=partner)

    def r_copy(s, t):
        return remote(r_s.at[s, piece(t)], r_r.at[s, piece(t)], r_ss, r_rs.at[s, t], tx=after)

    def product(s, carry):
        pltpu.make_async_copy(wb_v.at[2 * s], wb_v.at[2 * s], wb_sem.at[2 * s]).wait()

        @pl.when(s < nx - 1)
        def _():
            start_block(s + 1, True)

        part = jnp.dot(h_v[...], wb_v[2 * s], preferred_element_type=F32)
        d_s[s] = part[:rows].astype(BF16)
        d_copy(s).start()
        gb_s[block_of(s, False)] = gamma_row(part[rows:], 2 * fb // hd)

        @pl.when(s == 0)
        def _():
            q_pair()

        pltpu.make_async_copy(wb_v.at[2 * s + 1], wb_v.at[2 * s + 1], wb_sem.at[2 * s + 1]).wait()

        @pl.when(s < nx - 2)
        def _():
            start_block(s + 2, False)

        part = jnp.dot(h_v[...], wb_v[2 * s + 1], preferred_element_type=F32)
        own[s] = part[:rows]
        gb_s[block_of(s, True)] = gamma_row(part[rows:], 2 * fb // hd)

        @pl.when(s == 0)
        def _():
            with scope("d0"):
                d_copy(0).wait_recv()
            for t in range(SUBS):
                at = piece(t)
                r_s[0, at] = (own[0, at] + d_r[0, at].astype(F32)).astype(BF16)
                r_copy(0, t).start()

        return carry

    with scope("products"):
        lax.fori_loop(0, nx, product, 0)
    for c in gb_cp + k_in + v_in:
        c.start()
    gb_r[0] = gb_s[col]
    tables()

    def ring(s, t):
        at = piece(t)
        if t == 0:
            with scope("d%d" % s):
                d_copy(s).wait_recv()
        part = own[s, at] + d_r[s, at].astype(F32)
        with scope("r%d%d" % (s, t)):
            r_copy(s - 1, t).wait_recv()
        part = part + r_r[s - 1, at].astype(F32)
        if s < nx - 1:
            r_s[s, at] = part.astype(BF16)
            r_copy(s, t).start()
        else:
            if t == 0:
                with scope("gb"):
                    remote(gb_r.at[pl.ds(1, ntx - 1)], gb_r.at[pl.ds(1, ntx - 1)], gb_ss, gb_rs, tx=partner).wait_recv()
            part = normed(part, at, gb_r)
            gate = part[:, :fb].astype(BF16).astype(F32)
            up = part[:, fb:].astype(BF16).astype(F32)
            b_v[col, at] = (gate * (1.0 / (1.0 + jnp.exp(-gate))) * up).astype(BF16)
            act_out(t)

    def turn(vals, r):
        return vals * turns[0, r:r + 1, :] + pltpu.roll(vals, hd // 2, 1) * turns[1, r:r + 1, :]

    def attend(r):
        length = lens_ref[(row * ntx + col) * sb + r]
        for a in range(ny):
            qs[a * lh:(a + 1) * lh, :] = turn(qy_r[a, pl.ds(r, lh, stride=sb), :], r)
        q = qs[...].astype(BF16)
        k_new = turn(kvs[0, pl.ds(row * sb + r, 1), :], r).astype(BF16).astype(F32)
        v_new = kvs[1, pl.ds(row * sb + r, 1), :].astype(BF16).astype(F32)
        new_rows[r:r + 1, :] = k_new
        new_rows[sb + r:sb + r + 1, :] = v_new
        s_new = jnp.sum(q.astype(F32) * k_new, axis=1, keepdims=True)
        top = jnp.full((heads, hd), -1e30, F32)
        for c in range(ctx // CHUNK):
            s = lax.dot_general(q, kbuf[r, c * CHUNK:(c + 1) * CHUNK, :], (((1,), (1,)), ((), ())), preferred_element_type=F32)
            pos = lax.broadcasted_iota(jnp.int32, (1, CHUNK), 1) + c * CHUNK
            s = jnp.where(pos < length, s, -1e30)
            sbuf[:, c * CHUNK:(c + 1) * CHUNK] = s
            for t in range(CHUNK // hd):
                top = jnp.maximum(top, s[:, t * hd:(t + 1) * hd])
        high = jnp.maximum(jnp.max(top, axis=1, keepdims=True), s_new)
        rate = hd ** -0.5 * LOG2E
        e_new = jnp.exp2((s_new - high) * rate)
        low = jnp.zeros((heads, hd), F32)
        out = e_new.astype(BF16).astype(F32) * v_new
        for c in range(ctx // CHUNK):
            e = jnp.exp2((sbuf[:, c * CHUNK:(c + 1) * CHUNK] - high) * rate)
            for t in range(CHUNK // hd):
                low = low + e[:, t * hd:(t + 1) * hd]
            out = out + jnp.dot(e.astype(BF16), vbuf[r, c * CHUNK:(c + 1) * CHUNK, :], preferred_element_type=F32)
        out = out / (jnp.sum(low, axis=1, keepdims=True) + e_new)
        for a in range(ny):
            o32[a, pl.ds(r, lh, stride=sb), :] = out[a * lh:(a + 1) * lh]

    def b_send(b, t, slot, to):
        return remote(b_v.at[b, piece(t)], b_v.at[b, piece(t)], b_ss, b_rs.at[slot - 1, t], tx=to)

    def b_in(kind, t):
        b = held(kind, True)
        return remote(b_v.at[b, piece(t)], b_v.at[b, piece(t)], b_ss, b_rs.at[kind - 1, t], tx=after)

    def b_pair(kind, t):
        b = held(kind, True)
        return remote(b_v.at[b, piece(t)], b_v.at[b, piece(t)], bp_ss, bp_rs.at[kind], tx=partner)

    def act_out(t):
        b_send(col, t, 1, after).start()
        b_send(col, t, 2, before).start()
        b_pair(0, t).start()

    def act_in(kind, t):
        with scope("b%d%d" % (kind, t)):
            b_in(kind, t).wait_recv()
        if kind == 1 and t < EVEN:
            b_send(before, t, 3, after).start()
        if kind == 2 and t >= EVEN:
            b_send(right, t, 3, left).start()
        b_pair(kind, t).start()

    ay_cp = [remote(ay_s.at[y_peers[k - 1]], ay_r.at[row], ay_ss, ay_rs, ty=y_peers[k - 1]) for k in range(1, ny)]

    def g_send(at, slot, to):
        return remote(g_v.at[at], g_v.at[at], g_ss, g_rs.at[slot - 1], tx=to)

    def g_pair(at):
        return remote(g_v.at[at], g_v.at[at], gp_ss, gp_rs, tx=partner)

    def g_in(kind):
        at = (right, left, held(3, True))[kind - 1]
        with scope("g%d" % kind):
            g_send(at, kind, left).wait_recv()
        if kind == 1:
            g_send(right, 3, left).start()
        g_pair(at).start()

    def att_out():
        ay_s[...] = o32[...].astype(BF16)
        for c in ay_cp:
            c.start()
        ay_r[row] = ay_s[row]

    def att_rows():
        with scope("ay"):
            remote(ay_r.at[pl.ds(0, ny - 1)], ay_r.at[pl.ds(0, ny - 1)], ay_ss, ay_rs, ty=y_peers[0]).wait_recv()
        for a in range(ny):
            part = ay_r[a].astype(F32)
            for n in range(lh):
                g32[n, a * sb:(a + 1) * sb, :] = part[n * sb:(n + 1) * sb, :]
        g_v[col] = g32[...].astype(BF16)
        g_send(col, 1, left).start()
        g_send(col, 2, right).start()
        g_pair(col).start()

    mid = rows // 2

    def half_rows(half):
        return pl.ds(half * mid, mid)

    def down(n):
        if n % 2:
            b = held(n // 2, False)
            with scope("bp%d" % (n // 2)):
                remote(b_v.at[b], b_v.at[b], bp_ss, bp_rs.at[n // 2], tx=partner).wait_recv()
        part = jnp.dot(b_v[held(n // 2, n % 2 == 0)], wd_v[n], preferred_element_type=F32)
        acc[...] = part if n == 0 else acc[...] + part

    def att_down(half):
        at = pl.ds(half * nx, nx)
        part = acc[half_rows(half)]
        for n in range(0, lh, 2):
            pair = jnp.concatenate([g_v[at, n].reshape(mid, hd), g_v[at, n + 1].reshape(mid, hd)], axis=1)
            part = part + jnp.dot(pair, wo_v[n * hd:(n + 2) * hd, :], preferred_element_type=F32)
        acc[half_rows(half)] = part

    def y_out_half(half):
        part = jnp.dot(back_v[...], acc[half_rows(half)].astype(BF16), preferred_element_type=F32)
        y_s[half] = part.astype(BF16).reshape(ny, yb // 2, dl)
        for k in range(1, ny):
            remote(y_s.at[half, y_peers[k - 1]], y_r.at[half, k], y_ss.at[half], y_rs.at[half], ty=y_peers[k - 1]).start()

    def y_sum_half(half):
        at = pl.ds(pl.multiple_of(row * yb + half * (yb // 2), yb // 2), yb // 2)
        total = x_v[at, :].astype(F32) + y_s[half, row].astype(F32)
        rest = y_r.at[half, pl.ds(1, ny - 1)]
        with scope("y%d" % half):
            remote(rest, rest, y_ss.at[half], y_rs.at[half], ty=y_peers[0]).wait_recv()
        for k in range(1, ny):
            total = total + y_r[half, k].astype(F32)
        yf[half, row] = total.astype(BF16)
        for k in range(1, ny):
            remote(yf.at[half, row], yf.at[half, row], f_ss.at[half], f_rs.at[half], ty=y_peers[k - 1]).start()

    def y_all_half(half):
        rest = yf.at[half, pl.ds(0, ny - 1)]
        with scope("f%d" % half):
            remote(rest, rest, f_ss.at[half], f_rs.at[half], ty=y_peers[0]).wait_recv()
        for a in range(ny):
            y_out[a * yb + half * (yb // 2):a * yb + (half + 1) * (yb // 2), :] = yf[half, a]

    q_rows()
    for t in range(SUBS):
        ring(1, t)
    for n in range(ntx):
        wd_load(n, held(n // 2, n % 2 == 0)).start()
    wo_load.start()
    for t in range(SUBS):
        ring(2, t)
        if t == 0:
            with scope("qy"):
                remote(qy_r.at[pl.ds(0, ny - 1)], qy_r.at[pl.ds(0, ny - 1)], qy_ss, qy_rs, ty=y_peers[0]).wait_recv()
            pltpu.make_async_copy(kbuf, kbuf, kv_sem.at[0]).wait()
            pltpu.make_async_copy(vbuf, vbuf, kv_sem.at[1]).wait()
        if t % (SUBS // sb) == 0:
            with scope("a%d" % (t * sb // SUBS)):
                attend(t * sb // SUBS)
    att_out()
    for t in range(SUBS):
        ring(3, t)
    att_rows()
    pltpu.make_async_copy(wd_v, wd_v, wd_sem).wait()
    down(0)
    for t in range(SUBS):
        act_in(1, t)
        act_in(2, t)
    g_in(1)
    g_in(2)
    for n in (1, 2, 4, 3, 5):
        down(n)
    for t in range(SUBS):
        act_in(3, t)
    g_in(3)
    down(6)
    down(7)
    with scope("gp"):
        remote(g_v.at[pl.ds(0, nx)], g_v.at[pl.ds(0, nx)], gp_ss, gp_rs, tx=partner).wait_recv()
    wo_load.wait()
    for half in range(2):
        att_down(half)
        y_out_half(half)
    def put_rows(buf, base):
        for r in range(sb):
            length = lens_ref[(row * ntx + col) * sb + r]

            def some(c, carry):
                at = pl.ds(pl.multiple_of(c * CHUNK, CHUNK), CHUNK)
                here = lax.broadcasted_iota(jnp.int32, (CHUNK, hd), 0) + c * CHUNK == length
                buf[r, at, :] = jnp.where(here, new_rows[base + r:base + r + 1, :], buf[r, at, :].astype(F32)).astype(BF16)
                return carry

            lax.fori_loop(0, ctx // CHUNK, some, 0)

    with scope("putk"):
        put_rows(kbuf, 0)
    y_sum_half(0)
    y_sum_half(1)
    with scope("putv"):
        put_rows(vbuf, sb)
    y_all_half(0)
    y_all_half(1)

    with scope("sends"):
        qd_cp.wait_send()
        for ref, send, recv in (
            (stat_r.at[pl.ds(1, ntx - 1)], stat_ss, stat_rs), (gq_r.at[pl.ds(1, ntx - 1)], gq_ss, gq_rs), (gb_r.at[pl.ds(1, ntx - 1)], gb_ss, gb_rs),
            (qx_in, qx_ss, qx_rs), (qy_s.at[pl.ds(1, ny - 1)], qy_ss, qy_rs), (ay_s.at[pl.ds(1, ny - 1)], ay_ss, ay_rs),
            *((y_s.at[half, pl.ds(1, ny - 1)], y_ss.at[half], y_rs.at[half]) for half in range(2)),
            *((yf.at[half, pl.ds(1, ny - 1)], f_ss.at[half], f_rs.at[half]) for half in range(2)),
            (d_s, d_ss, d_rs.at[0]), (r_s, r_ss, r_rs.at[0, 0]), (g_v.at[pl.ds(1, nx - 1)], g_ss, g_rs.at[0]), (g_v.at[pl.ds(0, nx)], gp_ss, gp_rs),
            (b_v.at[pl.ds(1, nx - 1)], b_ss, b_rs.at[0, 0]), (b_v.at[pl.ds(0, nx)], bp_ss, bp_rs.at[0]),
        ):
            remote(ref, ref, send, recv, tx=partner).wait_send()


def store_kernel(y_v, k_v, v_v, y_h, ko_h, vo_h, y_sem, out_sem):
    copies = [pltpu.make_async_copy(k_v.at[r], ko_h.at[r], out_sem.at[0, r]) for r in range(k_v.shape[0])]
    copies += [pltpu.make_async_copy(v_v.at[r], vo_h.at[r], out_sem.at[1, r]) for r in range(v_v.shape[0])]
    copies += [pltpu.make_async_copy(y_v, y_h, y_sem)]
    for c in copies:
        c.start()
    for c in copies:
        c.wait()


def solution(mesh):
    ny = mesh.shape["ty"]
    ntx = mesh.shape["tx"]
    nx = ntx // 2
    cache_spec = P(("dp", "ty", "tx"), None, None)
    vspec = pl.BlockSpec(memory_space=VMEM)
    hspec = pl.BlockSpec(memory_space=pltpu.HBM)
    sspec = pl.BlockSpec(memory_space=pltpu.SMEM)

    def layer_shard(x_blk, lens_part, k_blk, v_blk, gamma_blk, w_query, w_key, w_value, w_gate, w_up, w_out, w_down):
        rows, dl = x_blk.shape
        sb, ctx, hd = k_blk.shape
        qn = w_query.shape[1]
        lh = qn // hd
        qw = qn + 2 * hd
        fb = w_gate.shape[1] // ntx
        rb = rows // ntx
        yb = rows // ny

        natural = np.arange(rows)
        order = np.reshape(np.transpose(np.reshape(natural, (ny, ntx, sb)), (1, 0, 2)), (rows,))
        perm = jnp.asarray(order[:, None] == natural[None, :], dtype=BF16)
        part = np.arange(rows // 2)
        order = np.reshape(np.transpose(np.reshape(part, (nx, ny, sb)), (1, 0, 2)), (rows // 2,))
        back = jnp.asarray(order[:, None] == part[None, :], dtype=BF16)
        freqs = np.power(ROPE_BASE, -(np.arange(hd // 2, dtype=np.float32) * 2.0) / hd).astype(np.float32)
        freqs = jnp.asarray(np.tile(np.concatenate([freqs, freqs])[None, :], (8, 1)))

        y_vm, k_vm, v_vm = pl.pallas_call(
            functools.partial(step_kernel, ny, nx, dl * ntx),
            out_shape=(
                pltpu.VMEM((rows, dl), BF16),
                pltpu.VMEM(k_blk.shape, BF16),
                pltpu.VMEM(v_blk.shape, BF16),
            ),
            in_specs=[sspec] + [hspec] * 14,
            out_specs=(vspec,) * 3,
            scratch_shapes=[
                VMEM((rows, dl), BF16), VMEM((dl,), F32), VMEM((rows, rows), BF16), VMEM((rows // 2, rows // 2), BF16), VMEM((8, hd), F32),
                VMEM((dl, qw), BF16), VMEM((ntx, dl, 2 * fb), BF16), VMEM((qn, dl), BF16), VMEM((ntx, fb, dl), BF16),
                VMEM((rows + 16, dl), BF16), VMEM((8, rows), F32), VMEM((ntx, 8, rows), F32),
                VMEM((16, hd), BF16), VMEM((ntx, 16, hd), BF16), VMEM((ntx, 16, hd), BF16), VMEM((ntx, 16, hd), BF16), VMEM((rows, rows), F32),
                VMEM((ntx, rb, qw), F32), VMEM((nx, rb, qw), BF16), VMEM((nx, rb, qw), BF16),
                VMEM((2 * sb, hd), F32), VMEM((nx, rb, qw), BF16), VMEM((nx, rb, qw), BF16), VMEM((rb, qw), F32), VMEM((2, rb, hd), F32),
                VMEM((ny, sb * lh, hd), F32), VMEM((ny, sb * lh, hd), F32),
                VMEM((nx, rows, 2 * fb), F32), VMEM((nx, rows, 2 * fb), BF16), VMEM((nx, rows, 2 * fb), BF16),
                VMEM((nx - 1, rows, 2 * fb), BF16), VMEM((nx - 1, rows, 2 * fb), BF16),
                VMEM((2, 8, hd), F32), VMEM((ny * lh, hd), F32), VMEM((ny * lh, ctx), F32), VMEM((ny, sb * lh, hd), F32),
                VMEM((ny, sb * lh, hd), BF16), VMEM((ny, sb * lh, hd), BF16), VMEM((lh, rb, hd), F32),
                VMEM((ntx, lh, rb, hd), BF16), VMEM((ntx, rows, fb), BF16), VMEM((rows, dl), F32),
                VMEM((2, ny, yb // 2, dl), BF16), VMEM((2, ny, yb // 2, dl), BF16), VMEM((2, ny, yb // 2, dl), BF16),
                DMA((5,)), DMA, DMA((ntx,)), DMA((2,)), DMA, DMA,
                DMA, DMA, DMA, DMA, DMA, DMA, DMA, DMA, DMA, DMA, DMA, DMA,
                DMA, DMA((nx,)), DMA, DMA((nx - 1, SUBS)),
                DMA, DMA, DMA, DMA((nx - 1,)), DMA, DMA,
                DMA, DMA((nx - 1, SUBS)), DMA, DMA((nx,)), DMA((2,)), DMA((2,)), DMA((2,)), DMA((2,)),
            ],
            compiler_params=pltpu.CompilerParams(collective_id=0, has_side_effects=True, vmem_limit_bytes=52 * 1024 * 1024),
            name="step",
        )(lens_part, x_blk, gamma_blk, perm, back, freqs, w_query, w_key, w_value, w_gate, w_up, k_blk, v_blk, w_out, w_down)

        return pl.pallas_call(
            store_kernel,
            out_shape=(
                jax.ShapeDtypeStruct((rows, dl), BF16),
                jax.ShapeDtypeStruct(k_blk.shape, BF16),
                jax.ShapeDtypeStruct(v_blk.shape, BF16),
            ),
            in_specs=[vspec] * 3,
            out_specs=(hspec,) * 3,
            scratch_shapes=[DMA, DMA((2, sb))],
            compiler_params=pltpu.CompilerParams(vmem_limit_bytes=4 * 1024 * 1024),
            name="store",
        )(y_vm, k_vm, v_vm)

    in_specs = (P("dp", "tx"), P("dp"), cache_spec, cache_spec, P("tx"), P("tx", "ty"), P("tx", None), P("tx", None), P("tx", "ty"), P("tx", "ty"), P("ty", "tx"), P("ty", "tx"))
    out_specs = (P("dp", "tx"), cache_spec, cache_spec)
    return jax.shard_map(layer_shard, mesh=mesh, in_specs=in_specs, out_specs=out_specs, check_vma=False)
```

```python
import functools

import jax
import jax.numpy as jnp
import numpy as np
from jax import lax
from jax.experimental import pallas as pl
from jax.experimental.pallas import tpu as pltpu
from jax.sharding import PartitionSpec as P

EPSILON = 1e-6
ROPE_BASE = 10000.0
LOG2E = 1.4426950408889634
MESH = pl.DeviceIdType.MESH
F32 = jnp.float32
BF16 = jnp.bfloat16
VMEM = pltpu.VMEM
DMA = pltpu.SemaphoreType.DMA
SUBS = 8
CHUNK = 1024
EVEN = 4
scope = jax.named_scope


def remote(src, dst, send_sem, recv_sem, tx=None, ty=None):
    device = {}
    if tx is not None:
        device["tx"] = tx
    if ty is not None:
        device["ty"] = ty
    return pltpu.make_async_remote_copy(src_ref=src, dst_ref=dst, send_sem=send_sem, recv_sem=recv_sem, device_id=device, device_id_type=MESH)


def step_kernel(ny, nx, d_model, lens_ref, x_h, gamma_h, perm_h, back_h, freq_h, wq_h, wk_h, wv_h, wg_h, wu_h, k_h, v_h, wo_h, wd_h,
                y_out, kbuf, vbuf,
                x_v, gamma_v, perm_v, back_v, freq_v, wq_v, wb_v, wo_v, wd_v, h_v, stat_s, stat_r, gq_s, gq_r, gb_s, gb_r, norm,
                qp, qd_s, qd_r, new_rows, qx_s, qx_r, qsum, kvs, qy_s, qy_r, own, d_s, d_r, r_s, r_r,
                turns, qs, sbuf, o32, ay_s, ay_r, g32, g_v, b_v, acc, y_s, y_r, yf,
                in_sem, wq_sem, wb_sem, kv_sem, wo_sem, wd_sem, stat_ss, stat_rs, gq_ss, gq_rs, gb_ss, gb_rs, qd_ss, qd_rs, qx_ss, qx_rs, qy_ss, qy_rs,
                d_ss, d_rs, r_ss, r_rs, ay_ss, ay_rs, g_ss, g_rs, gp_ss, gp_rs, b_ss, b_rs, bp_ss, bp_rs, y_ss, y_rs, f_ss, f_rs):
    row = lax.axis_index("ty")
    col = lax.axis_index("tx")
    chip = lax.div(col, 2)
    core = lax.rem(col, 2)
    step = 1 - 2 * core
    ntx = 2 * nx
    rows, dl = x_h.shape
    rb = rows // ntx
    sb = rb // ny
    qn = wq_h.shape[1]
    hd = wk_h.shape[1]
    qw = qn + 2 * hd
    lh = qn // hd
    heads = ny * lh
    ctx = k_h.shape[1]
    fb = wb_v.shape[2] // 2
    sub = rows // SUBS
    yb = rows // ny
    partner = lax.rem(col + 1, 2) + 2 * chip
    after = 2 * lax.rem(chip + step + nx, nx) + core
    before = 2 * lax.rem(chip - step + nx, nx) + core
    right = 2 * lax.rem(chip + 1, nx) + core
    left = 2 * lax.rem(chip + nx - 1, nx) + core
    tx_peers = [lax.rem(col + k, ntx) for k in range(1, ntx)]
    x_peers = [2 * lax.rem(chip + k, nx) + core for k in range(1, nx)]
    y_peers = [lax.rem(row + k, ny) for k in range(1, ny)]
    y_froms = [lax.rem(row - k + ny, ny) for k in range(1, ny)]

    barrier = pltpu.get_barrier_semaphore()
    for peer in tx_peers:
        pl.semaphore_signal(barrier, inc=1, device_id={"tx": peer}, device_id_type=MESH)
    for peer in y_peers:
        pl.semaphore_signal(barrier, inc=1, device_id={"ty": peer}, device_id_type=MESH)

    def piece(t):
        return pl.ds(pl.multiple_of(t * sub, sub), sub)

    def block_of(s, mine):
        sign = step if mine else -step
        at = lax.rem(chip - (s + 1) * sign + 2 * nx, nx)
        return 2 * at + (core if mine else 1 - core)

    def held(kind, mine):
        away = (0, -1, 1, 2)[kind] * (step if mine else -step)
        return 2 * lax.rem(chip + away + 2 * nx, nx) + (core if mine else 1 - core)

    def block_loads(n, b):
        at = pl.ds(pl.multiple_of(b * fb, fb), fb)
        return [
            pltpu.make_async_copy(wg_h.at[:, at], wb_v.at[n, :, pl.ds(0, fb)], wb_sem.at[n]),
            pltpu.make_async_copy(wu_h.at[:, at], wb_v.at[n, :, pl.ds(fb, fb)], wb_sem.at[n]),
        ]

    def wd_load(n, b):
        at = pl.ds(pl.multiple_of(b * fb, fb), fb)
        return pltpu.make_async_copy(wd_h.at[at, :], wd_v.at[n], wd_sem)

    first_loads = [
        pltpu.make_async_copy(x_h, x_v, in_sem.at[0]),
        pltpu.make_async_copy(perm_h, perm_v, in_sem.at[1]),
        pltpu.make_async_copy(gamma_h, gamma_v, in_sem.at[2]),
        pltpu.make_async_copy(freq_h, freq_v, in_sem.at[3]),
        pltpu.make_async_copy(back_h, back_v, in_sem.at[4]),
    ]
    q_loads = [
        pltpu.make_async_copy(wq_h, wq_v.at[:, pl.ds(0, qn)], wq_sem),
        pltpu.make_async_copy(wk_h, wq_v.at[:, pl.ds(qn, hd)], wq_sem),
        pltpu.make_async_copy(wv_h, wq_v.at[:, pl.ds(qn + hd, hd)], wq_sem),
    ]
    k_in = [pltpu.make_async_copy(k_h.at[r], kbuf.at[r], kv_sem.at[0]) for r in range(sb)]
    v_in = [pltpu.make_async_copy(v_h.at[r], vbuf.at[r], kv_sem.at[1]) for r in range(sb)]
    wo_load = pltpu.make_async_copy(wo_h, wo_v, wo_sem)
    def start_block(s, mine):
        for c in block_loads(2 * s + int(mine), block_of(s, mine)):
            c.start()

    for c in first_loads + q_loads:
        c.start()
    for c in first_loads:
        c.wait()
    start_block(0, False)

    xp = jnp.dot(perm_v[...], x_v[...], preferred_element_type=F32)
    own_mean = jnp.sum(xp, axis=1, keepdims=True) / dl
    xc = xp - own_mean
    gamma = gamma_v[...].reshape(1, dl)
    h_v[:rows] = (xc * gamma).astype(BF16)
    extra = lax.broadcasted_iota(jnp.int32, (16, dl), 0)
    h_v[rows:] = jnp.where(extra == 0, gamma, jnp.where(extra == 1, gamma - gamma.astype(BF16).astype(F32), 0.0)).astype(BF16)
    lane = lax.broadcasted_iota(jnp.int32, (rows, rows), 1)
    both = jnp.where(lane == 0, own_mean, jnp.where(lane == 1, jnp.sum(xc * xc, axis=1, keepdims=True), 0.0))
    stat_s[...] = jnp.transpose(both)[:8]

    def gamma_row(vals, tiles):
        row_sum = vals[0:1, :] + vals[1:2, :]
        parts = [row_sum[:, n * hd:(n + 1) * hd] for n in range(tiles)]
        return jnp.concatenate(parts + [jnp.zeros((16 - tiles, hd), F32)], axis=0).astype(BF16)

    pltpu.make_async_copy(wq_v, wq_v, wq_sem).wait()
    start_block(0, True)
    start_block(1, False)
    part = jnp.dot(h_v[...], wq_v[...], preferred_element_type=F32)
    qp[...] = part[:rows].reshape(ntx, rb, qw)
    gq_s[...] = gamma_row(part[rows:], qw // hd)
    for n in range(nx):
        qd_s[n] = qp[2 * n + 1 - core].astype(BF16)
    qd_cp = remote(qd_s, qd_r, qd_ss, qd_rs, tx=partner)
    stat_cp = [remote(stat_s, stat_r.at[k], stat_ss, stat_rs, tx=tx_peers[k - 1]) for k in range(1, ntx)]
    gq_cp = [remote(gq_s, gq_r.at[k], gq_ss, gq_rs, tx=tx_peers[k - 1]) for k in range(1, ntx)]
    gb_cp = [remote(gb_s.at[tx_peers[k - 1]], gb_r.at[k], gb_ss, gb_rs, tx=tx_peers[k - 1]) for k in range(1, ntx)]
    with scope("greet"):
        pl.semaphore_wait(barrier, ntx - 1 + ny - 1)
    qd_cp.start()
    for c in stat_cp + gq_cp:
        c.start()
    stat_r[0] = stat_s[...]
    gq_r[0] = gq_s[...]

    def rest_of_norm():
        with scope("stat"):
            remote(stat_r.at[pl.ds(1, ntx - 1)], stat_r.at[pl.ds(1, ntx - 1)], stat_ss, stat_rs, tx=partner).wait_recv()
            remote(gq_r.at[pl.ds(1, ntx - 1)], gq_r.at[pl.ds(1, ntx - 1)], gq_ss, gq_rs, tx=partner).wait_recv()
        means = jnp.concatenate([stat_r[k, 0:1, :] for k in range(ntx)], axis=0)
        squares = jnp.concatenate([stat_r[k, 1:2, :] for k in range(ntx)], axis=0)
        off = means - jnp.sum(means, axis=0, keepdims=True) / ntx
        var = jnp.sum(squares, axis=0, keepdims=True) / d_model + jnp.sum(off * off, axis=0, keepdims=True) / ntx
        scale = lax.rsqrt(var + EPSILON)
        norm[...] = jnp.transpose(jnp.concatenate([off, scale, jnp.zeros((rows - ntx - 1, rows), F32)], axis=0))

    def normed(vals, at, g_ref):
        cols = norm[at, :]
        tiles = []
        for n in range(vals.shape[1] // hd):
            tile = vals[:, n * hd:(n + 1) * hd]
            for k in range(ntx):
                tile = tile + cols[:, k:k + 1] * g_ref[k, n:n + 1, :].astype(F32)
            tiles.append(tile * cols[:, ntx:ntx + 1])
        return jnp.concatenate(tiles, axis=1)


    def q_of(away):
        at = lax.rem(chip + away + nx, nx)
        return qp[2 * at + core] + qd_r[at].astype(F32)

    qx_in = qx_r.at[pl.ds(1, nx - 1)]

    qy_cp = [remote(qy_s.at[y_peers[k - 1]], qy_r.at[row], qy_ss, qy_rs, ty=y_peers[k - 1]) for k in range(1, ny)]

    def q_pair():
        with scope("qd"):
            qd_cp.wait_recv()
        for k in (2, 1, 3):
            qx_s[k] = q_of(k).astype(BF16)
            remote(qx_s.at[k], qx_r.at[k], qx_ss, qx_rs, tx=x_peers[k - 1]).start()

    def q_rows():
        mine = q_of(0)
        rest_of_norm()
        with scope("qx"):
            remote(qx_in, qx_in, qx_ss, qx_rs, tx=partner).wait_recv()
        for k in range(1, nx):
            mine = mine + qx_r[k].astype(F32)
        mine = normed(mine, pl.ds(pl.multiple_of(col * rb, rb), rb), gq_r)
        qsum[...] = mine
        kvs[0] = mine[:, qn:qn + hd]
        kvs[1] = mine[:, qn + hd:]
        for a in range(ny):
            for n in range(lh):
                qy_s[a, n * sb:(n + 1) * sb, :] = qsum[a * sb:(a + 1) * sb, n * hd:(n + 1) * hd]
        for c in qy_cp:
            c.start()
        qy_r[row] = qy_s[row]

    def tables():
        at_row = lax.broadcasted_iota(jnp.int32, (8, hd), 0)
        places = jnp.zeros((8, hd), F32)
        for r in range(sb):
            places = jnp.where(at_row == r, lens_ref[(row * ntx + col) * sb + r].astype(F32), places)
        angles = places * freq_v[...]
        turns[0] = jnp.cos(angles)
        low_half = lax.broadcasted_iota(jnp.int32, (8, hd), 1) < hd // 2
        sines = jnp.sin(angles)
        turns[1] = jnp.where(low_half, -sines, sines)

    def d_copy(s):
        return remote(d_s.at[s], d_r.at[s], d_ss, d_rs.at[s], tx=partner)

    def r_copy(s, t):
        return remote(r_s.at[s, piece(t)], r_r.at[s, piece(t)], r_ss, r_rs.at[s, t], tx=after)

    def product(s, carry):
        pltpu.make_async_copy(wb_v.at[2 * s], wb_v.at[2 * s], wb_sem.at[2 * s]).wait()

        @pl.when(s < nx - 1)
        def _():
            start_block(s + 1, True)

        part = jnp.dot(h_v[...], wb_v[2 * s], preferred_element_type=F32)
        d_s[s] = part[:rows].astype(BF16)
        d_copy(s).start()
        gb_s[block_of(s, False)] = gamma_row(part[rows:], 2 * fb // hd)

        @pl.when(s == 0)
        def _():
            q_pair()

        pltpu.make_async_copy(wb_v.at[2 * s + 1], wb_v.at[2 * s + 1], wb_sem.at[2 * s + 1]).wait()

        @pl.when(s < nx - 2)
        def _():
            start_block(s + 2, False)

        part = jnp.dot(h_v[...], wb_v[2 * s + 1], preferred_element_type=F32)
        own[s] = part[:rows]
        gb_s[block_of(s, True)] = gamma_row(part[rows:], 2 * fb // hd)

        @pl.when(s == 0)
        def _():
            with scope("d0"):
                d_copy(0).wait_recv()
            for t in range(SUBS):
                at = piece(t)
                r_s[0, at] = (own[0, at] + d_r[0, at].astype(F32)).astype(BF16)
                r_copy(0, t).start()

        return carry

    with scope("products"):
        lax.fori_loop(0, nx, product, 0)
    for c in gb_cp + k_in + v_in:
        c.start()
    gb_r[0] = gb_s[col]
    tables()

    def ring(s, t):
        at = piece(t)
        if t == 0:
            with scope("d%d" % s):
                d_copy(s).wait_recv()
        part = own[s, at] + d_r[s, at].astype(F32)
        with scope("r%d%d" % (s, t)):
            r_copy(s - 1, t).wait_recv()
        part = part + r_r[s - 1, at].astype(F32)
        if s < nx - 1:
            r_s[s, at] = part.astype(BF16)
            r_copy(s, t).start()
        else:
            if t == 0:
                with scope("gb"):
                    remote(gb_r.at[pl.ds(1, ntx - 1)], gb_r.at[pl.ds(1, ntx - 1)], gb_ss, gb_rs, tx=partner).wait_recv()
            part = normed(part, at, gb_r)
            gate = part[:, :fb].astype(BF16).astype(F32)
            up = part[:, fb:].astype(BF16).astype(F32)
            b_v[col, at] = (gate * (1.0 / (1.0 + jnp.exp(-gate))) * up).astype(BF16)
            act_out(t)

    def turn(vals, r):
        return vals * turns[0, r:r + 1, :] + pltpu.roll(vals, hd // 2, 1) * turns[1, r:r + 1, :]

    def attend(r):
        length = lens_ref[(row * ntx + col) * sb + r]
        for a in range(ny):
            qs[a * lh:(a + 1) * lh, :] = turn(qy_r[a, pl.ds(r, lh, stride=sb), :], r)
        q = qs[...].astype(BF16)
        k_new = turn(kvs[0, pl.ds(row * sb + r, 1), :], r).astype(BF16).astype(F32)
        v_new = kvs[1, pl.ds(row * sb + r, 1), :].astype(BF16).astype(F32)
        new_rows[r:r + 1, :] = k_new
        new_rows[sb + r:sb + r + 1, :] = v_new
        s_new = jnp.sum(q.astype(F32) * k_new, axis=1, keepdims=True)
        top = jnp.full((heads, hd), -1e30, F32)
        for c in range(ctx // CHUNK):
            s = lax.dot_general(q, kbuf[r, c * CHUNK:(c + 1) * CHUNK, :], (((1,), (1,)), ((), ())), preferred_element_type=F32)
            pos = lax.broadcasted_iota(jnp.int32, (1, CHUNK), 1) + c * CHUNK
            s = jnp.where(pos < length, s, -1e30)
            sbuf[:, c * CHUNK:(c + 1) * CHUNK] = s
            for t in range(CHUNK // hd):
                top = jnp.maximum(top, s[:, t * hd:(t + 1) * hd])
        high = jnp.maximum(jnp.max(top, axis=1, keepdims=True), s_new)
        rate = hd ** -0.5 * LOG2E
        e_new = jnp.exp2((s_new - high) * rate)
        low = jnp.zeros((heads, hd), F32)
        out = e_new.astype(BF16).astype(F32) * v_new
        for c in range(ctx // CHUNK):
            e = jnp.exp2((sbuf[:, c * CHUNK:(c + 1) * CHUNK] - high) * rate)
            for t in range(CHUNK // hd):
                low = low + e[:, t * hd:(t + 1) * hd]
            out = out + jnp.dot(e.astype(BF16), vbuf[r, c * CHUNK:(c + 1) * CHUNK, :], preferred_element_type=F32)
        out = out / (jnp.sum(low, axis=1, keepdims=True) + e_new)
        for a in range(ny):
            o32[a, pl.ds(r, lh, stride=sb), :] = out[a * lh:(a + 1) * lh]

    def b_send(b, t, slot, to):
        return remote(b_v.at[b, piece(t)], b_v.at[b, piece(t)], b_ss, b_rs.at[slot - 1, t], tx=to)

    def b_in(kind, t):
        b = held(kind, True)
        return remote(b_v.at[b, piece(t)], b_v.at[b, piece(t)], b_ss, b_rs.at[kind - 1, t], tx=after)

    def b_pair(kind, t):
        b = held(kind, True)
        return remote(b_v.at[b, piece(t)], b_v.at[b, piece(t)], bp_ss, bp_rs.at[kind], tx=partner)

    def act_out(t):
        b_send(col, t, 1, after).start()
        b_send(col, t, 2, before).start()
        b_pair(0, t).start()

    def act_in(kind, t):
        with scope("b%d%d" % (kind, t)):
            b_in(kind, t).wait_recv()
        if kind == 1 and t < EVEN:
            b_send(before, t, 3, after).start()
        if kind == 2 and t >= EVEN:
            b_send(right, t, 3, left).start()
        b_pair(kind, t).start()

    ay_cp = [remote(ay_s.at[y_peers[k - 1]], ay_r.at[row], ay_ss, ay_rs, ty=y_peers[k - 1]) for k in range(1, ny)]

    def g_send(at, slot, to):
        return remote(g_v.at[at], g_v.at[at], g_ss, g_rs.at[slot - 1], tx=to)

    def g_pair(at):
        return remote(g_v.at[at], g_v.at[at], gp_ss, gp_rs, tx=partner)

    def g_in(kind):
        at = (right, left, held(3, True))[kind - 1]
        with scope("g%d" % kind):
            g_send(at, kind, left).wait_recv()
        if kind == 1:
            g_send(right, 3, left).start()
        g_pair(at).start()

    def att_out():
        ay_s[...] = o32[...].astype(BF16)
        for c in ay_cp:
            c.start()
        ay_r[row] = ay_s[row]

    def att_rows():
        with scope("ay"):
            remote(ay_r.at[pl.ds(0, ny - 1)], ay_r.at[pl.ds(0, ny - 1)], ay_ss, ay_rs, ty=y_peers[0]).wait_recv()
        for a in range(ny):
            part = ay_r[a].astype(F32)
            for n in range(lh):
                g32[n, a * sb:(a + 1) * sb, :] = part[n * sb:(n + 1) * sb, :]
        g_v[col] = g32[...].astype(BF16)
        g_send(col, 1, left).start()
        g_send(col, 2, right).start()
        g_pair(col).start()

    mid = rows // 2

    def half_rows(half):
        return pl.ds(half * mid, mid)

    def down(n):
        if n % 2:
            b = held(n // 2, False)
            with scope("bp%d" % (n // 2)):
                remote(b_v.at[b], b_v.at[b], bp_ss, bp_rs.at[n // 2], tx=partner).wait_recv()
        part = jnp.dot(b_v[held(n // 2, n % 2 == 0)], wd_v[n], preferred_element_type=F32)
        acc[...] = part if n == 0 else acc[...] + part

    def att_down(half):
        at = pl.ds(half * nx, nx)
        part = acc[half_rows(half)]
        for n in range(0, lh, 2):
            pair = jnp.concatenate([g_v[at, n].reshape(mid, hd), g_v[at, n + 1].reshape(mid, hd)], axis=1)
            part = part + jnp.dot(pair, wo_v[n * hd:(n + 2) * hd, :], preferred_element_type=F32)
        acc[half_rows(half)] = part

    def y_out_half(half):
        part = jnp.dot(back_v[...], acc[half_rows(half)].astype(BF16), preferred_element_type=F32)
        y_s[half] = part.astype(BF16).reshape(ny, yb // 2, dl)
        for k in range(1, ny):
            remote(y_s.at[half, y_peers[k - 1]], y_r.at[half, k], y_ss.at[half], y_rs.at[half], ty=y_peers[k - 1]).start()

    def y_sum_half(half):
        at = pl.ds(pl.multiple_of(row * yb + half * (yb // 2), yb // 2), yb // 2)
        total = x_v[at, :].astype(F32) + y_s[half, row].astype(F32)
        rest = y_r.at[half, pl.ds(1, ny - 1)]
        with scope("y%d" % half):
            remote(rest, rest, y_ss.at[half], y_rs.at[half], ty=y_peers[0]).wait_recv()
        for k in range(1, ny):
            total = total + y_r[half, k].astype(F32)
        yf[half, row] = total.astype(BF16)
        for k in range(1, ny):
            remote(yf.at[half, row], yf.at[half, row], f_ss.at[half], f_rs.at[half], ty=y_peers[k - 1]).start()

    def y_all_half(half):
        rest = yf.at[half, pl.ds(0, ny - 1)]
        with scope("f%d" % half):
            remote(rest, rest, f_ss.at[half], f_rs.at[half], ty=y_peers[0]).wait_recv()
        for a in range(ny):
            y_out[a * yb + half * (yb // 2):a * yb + (half + 1) * (yb // 2), :] = yf[half, a]

    q_rows()
    for t in range(SUBS):
        ring(1, t)
    for n in range(ntx):
        wd_load(n, held(n // 2, n % 2 == 0)).start()
    wo_load.start()
    for t in range(SUBS):
        ring(2, t)
        if t == 0:
            with scope("qy"):
                remote(qy_r.at[pl.ds(0, ny - 1)], qy_r.at[pl.ds(0, ny - 1)], qy_ss, qy_rs, ty=y_peers[0]).wait_recv()
            pltpu.make_async_copy(kbuf, kbuf, kv_sem.at[0]).wait()
            pltpu.make_async_copy(vbuf, vbuf, kv_sem.at[1]).wait()
        if t % (SUBS // sb) == 0:
            with scope("a%d" % (t * sb // SUBS)):
                attend(t * sb // SUBS)
    att_out()
    for t in range(SUBS):
        ring(3, t)
    att_rows()
    pltpu.make_async_copy(wd_v, wd_v, wd_sem).wait()
    down(0)
    for t in range(SUBS):
        act_in(1, t)
        act_in(2, t)
    g_in(1)
    g_in(2)
    for n in (1, 2, 4, 3, 5):
        down(n)
    for t in range(SUBS):
        act_in(3, t)
    g_in(3)
    down(6)
    down(7)
    with scope("gp"):
        remote(g_v.at[pl.ds(0, nx)], g_v.at[pl.ds(0, nx)], gp_ss, gp_rs, tx=partner).wait_recv()
    wo_load.wait()
    for half in range(2):
        att_down(half)
        y_out_half(half)
    def put_rows(buf, base):
        for r in range(sb):
            length = lens_ref[(row * ntx + col) * sb + r]

            def some(c, carry):
                at = pl.ds(pl.multiple_of(c * CHUNK, CHUNK), CHUNK)
                here = lax.broadcasted_iota(jnp.int32, (CHUNK, hd), 0) + c * CHUNK == length
                buf[r, at, :] = jnp.where(here, new_rows[base + r:base + r + 1, :], buf[r, at, :].astype(F32)).astype(BF16)
                return carry

            lax.fori_loop(0, ctx // CHUNK, some, 0)

    with scope("putk"):
        put_rows(kbuf, 0)
    y_sum_half(0)
    y_sum_half(1)
    with scope("putv"):
        put_rows(vbuf, sb)
    y_all_half(0)
    y_all_half(1)

    with scope("sends"):
        qd_cp.wait_send()
        for ref, send, recv in (
            (stat_r.at[pl.ds(1, ntx - 1)], stat_ss, stat_rs), (gq_r.at[pl.ds(1, ntx - 1)], gq_ss, gq_rs), (gb_r.at[pl.ds(1, ntx - 1)], gb_ss, gb_rs),
            (qx_in, qx_ss, qx_rs), (qy_s.at[pl.ds(1, ny - 1)], qy_ss, qy_rs), (ay_s.at[pl.ds(1, ny - 1)], ay_ss, ay_rs),
            *((y_s.at[half, pl.ds(1, ny - 1)], y_ss.at[half], y_rs.at[half]) for half in range(2)),
            *((yf.at[half, pl.ds(1, ny - 1)], f_ss.at[half], f_rs.at[half]) for half in range(2)),
            (d_s, d_ss, d_rs.at[0]), (r_s, r_ss, r_rs.at[0, 0]), (g_v.at[pl.ds(1, nx - 1)], g_ss, g_rs.at[0]), (g_v.at[pl.ds(0, nx)], gp_ss, gp_rs),
            (b_v.at[pl.ds(1, nx - 1)], b_ss, b_rs.at[0, 0]), (b_v.at[pl.ds(0, nx)], bp_ss, bp_rs.at[0]),
        ):
            remote(ref, ref, send, recv, tx=partner).wait_send()


def store_kernel(y_v, k_v, v_v, y_h, ko_h, vo_h, y_sem, out_sem):
    copies = [pltpu.make_async_copy(k_v.at[r], ko_h.at[r], out_sem.at[0, r]) for r in range(k_v.shape[0])]
    copies += [pltpu.make_async_copy(v_v.at[r], vo_h.at[r], out_sem.at[1, r]) for r in range(v_v.shape[0])]
    copies += [pltpu.make_async_copy(y_v, y_h, y_sem)]
    for c in copies:
        c.start()
    for c in copies:
        c.wait()


def solution(mesh):
    ny = mesh.shape["ty"]
    ntx = mesh.shape["tx"]
    nx = ntx // 2
    cache_spec = P(("dp", "ty", "tx"), None, None)
    vspec = pl.BlockSpec(memory_space=VMEM)
    hspec = pl.BlockSpec(memory_space=pltpu.HBM)
    sspec = pl.BlockSpec(memory_space=pltpu.SMEM)

    def layer_shard(x_blk, lens_part, k_blk, v_blk, gamma_blk, w_query, w_key, w_value, w_gate, w_up, w_out, w_down):
        rows, dl = x_blk.shape
        sb, ctx, hd = k_blk.shape
        qn = w_query.shape[1]
        lh = qn // hd
        qw = qn + 2 * hd
        fb = w_gate.shape[1] // ntx
        rb = rows // ntx
        yb = rows // ny

        natural = np.arange(rows)
        order = np.reshape(np.transpose(np.reshape(natural, (ny, ntx, sb)), (1, 0, 2)), (rows,))
        perm = jnp.asarray(order[:, None] == natural[None, :], dtype=BF16)
        part = np.arange(rows // 2)
        order = np.reshape(np.transpose(np.reshape(part, (nx, ny, sb)), (1, 0, 2)), (rows // 2,))
        back = jnp.asarray(order[:, None] == part[None, :], dtype=BF16)
        freqs = np.power(ROPE_BASE, -(np.arange(hd // 2, dtype=np.float32) * 2.0) / hd).astype(np.float32)
        freqs = jnp.asarray(np.tile(np.concatenate([freqs, freqs])[None, :], (8, 1)))

        y_vm, k_vm, v_vm = pl.pallas_call(
            functools.partial(step_kernel, ny, nx, dl * ntx),
            out_shape=(
                pltpu.VMEM((rows, dl), BF16),
                pltpu.VMEM(k_blk.shape, BF16),
                pltpu.VMEM(v_blk.shape, BF16),
            ),
            in_specs=[sspec] + [hspec] * 14,
            out_specs=(vspec,) * 3,
            scratch_shapes=[
                VMEM((rows, dl), BF16), VMEM((dl,), F32), VMEM((rows, rows), BF16), VMEM((rows // 2, rows // 2), BF16), VMEM((8, hd), F32),
                VMEM((dl, qw), BF16), VMEM((ntx, dl, 2 * fb), BF16), VMEM((qn, dl), BF16), VMEM((ntx, fb, dl), BF16),
                VMEM((rows + 16, dl), BF16), VMEM((8, rows), F32), VMEM((ntx, 8, rows), F32),
                VMEM((16, hd), BF16), VMEM((ntx, 16, hd), BF16), VMEM((ntx, 16, hd), BF16), VMEM((ntx, 16, hd), BF16), VMEM((rows, rows), F32),
                VMEM((ntx, rb, qw), F32), VMEM((nx, rb, qw), BF16), VMEM((nx, rb, qw), BF16),
                VMEM((2 * sb, hd), F32), VMEM((nx, rb, qw), BF16), VMEM((nx, rb, qw), BF16), VMEM((rb, qw), F32), VMEM((2, rb, hd), F32),
                VMEM((ny, sb * lh, hd), F32), VMEM((ny, sb * lh, hd), F32),
                VMEM((nx, rows, 2 * fb), F32), VMEM((nx, rows, 2 * fb), BF16), VMEM((nx, rows, 2 * fb), BF16),
                VMEM((nx - 1, rows, 2 * fb), BF16), VMEM((nx - 1, rows, 2 * fb), BF16),
                VMEM((2, 8, hd), F32), VMEM((ny * lh, hd), F32), VMEM((ny * lh, ctx), F32), VMEM((ny, sb * lh, hd), F32),
                VMEM((ny, sb * lh, hd), BF16), VMEM((ny, sb * lh, hd), BF16), VMEM((lh, rb, hd), F32),
                VMEM((ntx, lh, rb, hd), BF16), VMEM((ntx, rows, fb), BF16), VMEM((rows, dl), F32),
                VMEM((2, ny, yb // 2, dl), BF16), VMEM((2, ny, yb // 2, dl), BF16), VMEM((2, ny, yb // 2, dl), BF16),
                DMA((5,)), DMA, DMA((ntx,)), DMA((2,)), DMA, DMA,
                DMA, DMA, DMA, DMA, DMA, DMA, DMA, DMA, DMA, DMA, DMA, DMA,
                DMA, DMA((nx,)), DMA, DMA((nx - 1, SUBS)),
                DMA, DMA, DMA, DMA((nx - 1,)), DMA, DMA,
                DMA, DMA((nx - 1, SUBS)), DMA, DMA((nx,)), DMA((2,)), DMA((2,)), DMA((2,)), DMA((2,)),
            ],
            compiler_params=pltpu.CompilerParams(collective_id=0, has_side_effects=True, vmem_limit_bytes=52 * 1024 * 1024),
            name="step",
        )(lens_part, x_blk, gamma_blk, perm, back, freqs, w_query, w_key, w_value, w_gate, w_up, k_blk, v_blk, w_out, w_down)

        return pl.pallas_call(
            store_kernel,
            out_shape=(
                jax.ShapeDtypeStruct((rows, dl), BF16),
                jax.ShapeDtypeStruct(k_blk.shape, BF16),
                jax.ShapeDtypeStruct(v_blk.shape, BF16),
            ),
            in_specs=[vspec] * 3,
            out_specs=(hspec,) * 3,
            scratch_shapes=[DMA, DMA((2, sb))],
            compiler_params=pltpu.CompilerParams(vmem_limit_bytes=4 * 1024 * 1024),
            name="store",
        )(y_vm, k_vm, v_vm)

    in_specs = (P("dp", "tx"), P("dp"), cache_spec, cache_spec, P("tx"), P("tx", "ty"), P("tx", None), P("tx", None), P("tx", "ty"), P("tx", "ty"), P("ty", "tx"), P("ty", "tx"))
    out_specs = (P("dp", "tx"), cache_spec, cache_spec)
    return jax.shard_map(layer_shard, mesh=mesh, in_specs=in_specs, out_specs=out_specs, check_vma=False)
```

```python
import functools

import jax
import jax.numpy as jnp
import numpy as np
from jax import lax
from jax.experimental import pallas as pl
from jax.experimental.pallas import tpu as pltpu
from jax.sharding import PartitionSpec as P

EPSILON = 1e-6
ROPE_BASE = 10000.0
LOG2E = 1.4426950408889634
MESH = pl.DeviceIdType.MESH
F32 = jnp.float32
BF16 = jnp.bfloat16
VMEM = pltpu.VMEM
DMA = pltpu.SemaphoreType.DMA
SUBS = 8
CHUNK = 1024
EVEN = 6
scope = jax.named_scope


def remote(src, dst, send_sem, recv_sem, tx=None, ty=None):
    device = {}
    if tx is not None:
        device["tx"] = tx
    if ty is not None:
        device["ty"] = ty
    return pltpu.make_async_remote_copy(src_ref=src, dst_ref=dst, send_sem=send_sem, recv_sem=recv_sem, device_id=device, device_id_type=MESH)


def step_kernel(ny, nx, d_model, lens_ref, x_h, gamma_h, perm_h, back_h, freq_h, wq_h, wk_h, wv_h, wg_h, wu_h, k_h, v_h, wo_h, wd_h,
                y_out, kbuf, vbuf,
                x_v, gamma_v, perm_v, back_v, freq_v, wq_v, wb_v, wo_v, wd_v, h_v, stat_s, stat_r, gq_s, gq_r, gb_s, gb_r, norm,
                qp, qd_s, qd_r, new_rows, qx_s, qx_r, qsum, kvs, qy_s, qy_r, own, d_s, d_r, r_s, r_r,
                turns, qs, sbuf, o32, ay_s, ay_r, g32, g_v, b_v, acc, y_s, y_r, yf,
                in_sem, wq_sem, wb_sem, kv_sem, wo_sem, wd_sem, stat_ss, stat_rs, gq_ss, gq_rs, gb_ss, gb_rs, qd_ss, qd_rs, qx_ss, qx_rs, qy_ss, qy_rs,
                d_ss, d_rs, r_ss, r_rs, ay_ss, ay_rs, g_ss, g_rs, gp_ss, gp_rs, b_ss, b_rs, bp_ss, bp_rs, y_ss, y_rs, f_ss, f_rs):
    row = lax.axis_index("ty")
    col = lax.axis_index("tx")
    chip = lax.div(col, 2)
    core = lax.rem(col, 2)
    step = 1 - 2 * core
    ntx = 2 * nx
    rows, dl = x_h.shape
    rb = rows // ntx
    sb = rb // ny
    qn = wq_h.shape[1]
    hd = wk_h.shape[1]
    qw = qn + 2 * hd
    lh = qn // hd
    heads = ny * lh
    ctx = k_h.shape[1]
    fb = wb_v.shape[2] // 2
    sub = rows // SUBS
    yb = rows // ny
    partner = lax.rem(col + 1, 2) + 2 * chip
    after = 2 * lax.rem(chip + step + nx, nx) + core
    before = 2 * lax.rem(chip - step + nx, nx) + core
    right = 2 * lax.rem(chip + 1, nx) + core
    left = 2 * lax.rem(chip + nx - 1, nx) + core
    tx_peers = [lax.rem(col + k, ntx) for k in range(1, ntx)]
    x_peers = [2 * lax.rem(chip + k, nx) + core for k in range(1, nx)]
    y_peers = [lax.rem(row + k, ny) for k in range(1, ny)]
    y_froms = [lax.rem(row - k + ny, ny) for k in range(1, ny)]

    barrier = pltpu.get_barrier_semaphore()
    for peer in tx_peers:
        pl.semaphore_signal(barrier, inc=1, device_id={"tx": peer}, device_id_type=MESH)
    for peer in y_peers:
        pl.semaphore_signal(barrier, inc=1, device_id={"ty": peer}, device_id_type=MESH)

    def piece(t):
        return pl.ds(pl.multiple_of(t * sub, sub), sub)

    def block_of(s, mine):
        sign = step if mine else -step
        at = lax.rem(chip - (s + 1) * sign + 2 * nx, nx)
        return 2 * at + (core if mine else 1 - core)

    def held(kind, mine):
        away = (0, -1, 1, 2)[kind] * (step if mine else -step)
        return 2 * lax.rem(chip + away + 2 * nx, nx) + (core if mine else 1 - core)

    def block_loads(n, b):
        at = pl.ds(pl.multiple_of(b * fb, fb), fb)
        return [
            pltpu.make_async_copy(wg_h.at[:, at], wb_v.at[n, :, pl.ds(0, fb)], wb_sem.at[n]),
            pltpu.make_async_copy(wu_h.at[:, at], wb_v.at[n, :, pl.ds(fb, fb)], wb_sem.at[n]),
        ]

    def wd_load(n, b):
        at = pl.ds(pl.multiple_of(b * fb, fb), fb)
        return pltpu.make_async_copy(wd_h.at[at, :], wd_v.at[n], wd_sem)

    first_loads = [
        pltpu.make_async_copy(x_h, x_v, in_sem.at[0]),
        pltpu.make_async_copy(perm_h, perm_v, in_sem.at[1]),
        pltpu.make_async_copy(gamma_h, gamma_v, in_sem.at[2]),
        pltpu.make_async_copy(freq_h, freq_v, in_sem.at[3]),
        pltpu.make_async_copy(back_h, back_v, in_sem.at[4]),
    ]
    q_loads = [
        pltpu.make_async_copy(wq_h, wq_v.at[:, pl.ds(0, qn)], wq_sem),
        pltpu.make_async_copy(wk_h, wq_v.at[:, pl.ds(qn, hd)], wq_sem),
        pltpu.make_async_copy(wv_h, wq_v.at[:, pl.ds(qn + hd, hd)], wq_sem),
    ]
    k_in = [pltpu.make_async_copy(k_h.at[r], kbuf.at[r], kv_sem.at[0]) for r in range(sb)]
    v_in = [pltpu.make_async_copy(v_h.at[r], vbuf.at[r], kv_sem.at[1]) for r in range(sb)]
    wo_load = pltpu.make_async_copy(wo_h, wo_v, wo_sem)
    def start_block(s, mine):
        for c in block_loads(2 * s + int(mine), block_of(s, mine)):
            c.start()

    for c in first_loads + q_loads:
        c.start()
    for c in first_loads:
        c.wait()
    start_block(0, False)

    xp = jnp.dot(perm_v[...], x_v[...], preferred_element_type=F32)
    own_mean = jnp.sum(xp, axis=1, keepdims=True) / dl
    xc = xp - own_mean
    gamma = gamma_v[...].reshape(1, dl)
    h_v[:rows] = (xc * gamma).astype(BF16)
    extra = lax.broadcasted_iota(jnp.int32, (16, dl), 0)
    h_v[rows:] = jnp.where(extra == 0, gamma, jnp.where(extra == 1, gamma - gamma.astype(BF16).astype(F32), 0.0)).astype(BF16)
    lane = lax.broadcasted_iota(jnp.int32, (rows, rows), 1)
    both = jnp.where(lane == 0, own_mean, jnp.where(lane == 1, jnp.sum(xc * xc, axis=1, keepdims=True), 0.0))
    stat_s[...] = jnp.transpose(both)[:8]

    def gamma_row(vals, tiles):
        row_sum = vals[0:1, :] + vals[1:2, :]
        parts = [row_sum[:, n * hd:(n + 1) * hd] for n in range(tiles)]
        return jnp.concatenate(parts + [jnp.zeros((16 - tiles, hd), F32)], axis=0).astype(BF16)

    pltpu.make_async_copy(wq_v, wq_v, wq_sem).wait()
    start_block(0, True)
    start_block(1, False)
    part = jnp.dot(h_v[...], wq_v[...], preferred_element_type=F32)
    qp[...] = part[:rows].reshape(ntx, rb, qw)
    gq_s[...] = gamma_row(part[rows:], qw // hd)
    for n in range(nx):
        qd_s[n] = qp[2 * n + 1 - core].astype(BF16)
    qd_cp = remote(qd_s, qd_r, qd_ss, qd_rs, tx=partner)
    stat_cp = [remote(stat_s, stat_r.at[k], stat_ss, stat_rs, tx=tx_peers[k - 1]) for k in range(1, ntx)]
    gq_cp = [remote(gq_s, gq_r.at[k], gq_ss, gq_rs, tx=tx_peers[k - 1]) for k in range(1, ntx)]
    gb_cp = [remote(gb_s.at[tx_peers[k - 1]], gb_r.at[k], gb_ss, gb_rs, tx=tx_peers[k - 1]) for k in range(1, ntx)]
    with scope("greet"):
        pl.semaphore_wait(barrier, ntx - 1 + ny - 1)
    qd_cp.start()
    for c in stat_cp + gq_cp:
        c.start()
    stat_r[0] = stat_s[...]
    gq_r[0] = gq_s[...]

    def rest_of_norm():
        with scope("stat"):
            remote(stat_r.at[pl.ds(1, ntx - 1)], stat_r.at[pl.ds(1, ntx - 1)], stat_ss, stat_rs, tx=partner).wait_recv()
            remote(gq_r.at[pl.ds(1, ntx - 1)], gq_r.at[pl.ds(1, ntx - 1)], gq_ss, gq_rs, tx=partner).wait_recv()
        means = jnp.concatenate([stat_r[k, 0:1, :] for k in range(ntx)], axis=0)
        squares = jnp.concatenate([stat_r[k, 1:2, :] for k in range(ntx)], axis=0)
        off = means - jnp.sum(means, axis=0, keepdims=True) / ntx
        var = jnp.sum(squares, axis=0, keepdims=True) / d_model + jnp.sum(off * off, axis=0, keepdims=True) / ntx
        scale = lax.rsqrt(var + EPSILON)
        norm[...] = jnp.transpose(jnp.concatenate([off, scale, jnp.zeros((rows - ntx - 1, rows), F32)], axis=0))

    def normed(vals, at, g_ref):
        cols = norm[at, :]
        tiles = []
        for n in range(vals.shape[1] // hd):
            tile = vals[:, n * hd:(n + 1) * hd]
            for k in range(ntx):
                tile = tile + cols[:, k:k + 1] * g_ref[k, n:n + 1, :].astype(F32)
            tiles.append(tile * cols[:, ntx:ntx + 1])
        return jnp.concatenate(tiles, axis=1)


    def q_of(away):
        at = lax.rem(chip + away + nx, nx)
        return qp[2 * at + core] + qd_r[at].astype(F32)

    qx_in = qx_r.at[pl.ds(1, nx - 1)]

    qy_cp = [remote(qy_s.at[y_peers[k - 1]], qy_r.at[row], qy_ss, qy_rs, ty=y_peers[k - 1]) for k in range(1, ny)]

    def q_pair():
        with scope("qd"):
            qd_cp.wait_recv()
        for k in (2, 1, 3):
            qx_s[k] = q_of(k).astype(BF16)
            remote(qx_s.at[k], qx_r.at[k], qx_ss, qx_rs, tx=x_peers[k - 1]).start()

    def q_rows():
        mine = q_of(0)
        rest_of_norm()
        with scope("qx"):
            remote(qx_in, qx_in, qx_ss, qx_rs, tx=partner).wait_recv()
        for k in range(1, nx):
            mine = mine + qx_r[k].astype(F32)
        mine = normed(mine, pl.ds(pl.multiple_of(col * rb, rb), rb), gq_r)
        qsum[...] = mine
        kvs[0] = mine[:, qn:qn + hd]
        kvs[1] = mine[:, qn + hd:]
        for a in range(ny):
            for n in range(lh):
                qy_s[a, n * sb:(n + 1) * sb, :] = qsum[a * sb:(a + 1) * sb, n * hd:(n + 1) * hd]
        for c in qy_cp:
            c.start()
        qy_r[row] = qy_s[row]

    def tables():
        at_row = lax.broadcasted_iota(jnp.int32, (8, hd), 0)
        places = jnp.zeros((8, hd), F32)
        for r in range(sb):
            places = jnp.where(at_row == r, lens_ref[(row * ntx + col) * sb + r].astype(F32), places)
        angles = places * freq_v[...]
        turns[0] = jnp.cos(angles)
        low_half = lax.broadcasted_iota(jnp.int32, (8, hd), 1) < hd // 2
        sines = jnp.sin(angles)
        turns[1] = jnp.where(low_half, -sines, sines)

    def d_copy(s):
        return remote(d_s.at[s], d_r.at[s], d_ss, d_rs.at[s], tx=partner)

    def r_copy(s, t):
        return remote(r_s.at[s, piece(t)], r_r.at[s, piece(t)], r_ss, r_rs.at[s, t], tx=after)

    def product(s, carry):
        pltpu.make_async_copy(wb_v.at[2 * s], wb_v.at[2 * s], wb_sem.at[2 * s]).wait()

        @pl.when(s < nx - 1)
        def _():
            start_block(s + 1, True)

        part = jnp.dot(h_v[...], wb_v[2 * s], preferred_element_type=F32)
        d_s[s] = part[:rows].astype(BF16)
        d_copy(s).start()
        gb_s[block_of(s, False)] = gamma_row(part[rows:], 2 * fb // hd)

        @pl.when(s == 0)
        def _():
            q_pair()

        pltpu.make_async_copy(wb_v.at[2 * s + 1], wb_v.at[2 * s + 1], wb_sem.at[2 * s + 1]).wait()

        @pl.when(s < nx - 2)
        def _():
            start_block(s + 2, False)

        part = jnp.dot(h_v[...], wb_v[2 * s + 1], preferred_element_type=F32)
        own[s] = part[:rows]
        gb_s[block_of(s, True)] = gamma_row(part[rows:], 2 * fb // hd)

        @pl.when(s == 0)
        def _():
            with scope("d0"):
                d_copy(0).wait_recv()
            for t in range(SUBS):
                at = piece(t)
                r_s[0, at] = (own[0, at] + d_r[0, at].astype(F32)).astype(BF16)
                r_copy(0, t).start()

        return carry

    with scope("products"):
        lax.fori_loop(0, nx, product, 0)
    for c in gb_cp + k_in + v_in:
        c.start()
    gb_r[0] = gb_s[col]
    tables()

    def ring(s, t):
        at = piece(t)
        if t == 0:
            with scope("d%d" % s):
                d_copy(s).wait_recv()
        part = own[s, at] + d_r[s, at].astype(F32)
        with scope("r%d%d" % (s, t)):
            r_copy(s - 1, t).wait_recv()
        part = part + r_r[s - 1, at].astype(F32)
        if s < nx - 1:
            r_s[s, at] = part.astype(BF16)
            r_copy(s, t).start()
        else:
            if t == 0:
                with scope("gb"):
                    remote(gb_r.at[pl.ds(1, ntx - 1)], gb_r.at[pl.ds(1, ntx - 1)], gb_ss, gb_rs, tx=partner).wait_recv()
            part = normed(part, at, gb_r)
            gate = part[:, :fb].astype(BF16).astype(F32)
            up = part[:, fb:].astype(BF16).astype(F32)
            b_v[col, at] = (gate * (1.0 / (1.0 + jnp.exp(-gate))) * up).astype(BF16)
            act_out(t)

    def turn(vals, r):
        return vals * turns[0, r:r + 1, :] + pltpu.roll(vals, hd // 2, 1) * turns[1, r:r + 1, :]

    def attend(r):
        length = lens_ref[(row * ntx + col) * sb + r]
        for a in range(ny):
            qs[a * lh:(a + 1) * lh, :] = turn(qy_r[a, pl.ds(r, lh, stride=sb), :], r)
        q = qs[...].astype(BF16)
        k_new = turn(kvs[0, pl.ds(row * sb + r, 1), :], r).astype(BF16).astype(F32)
        v_new = kvs[1, pl.ds(row * sb + r, 1), :].astype(BF16).astype(F32)
        new_rows[r:r + 1, :] = k_new
        new_rows[sb + r:sb + r + 1, :] = v_new
        s_new = jnp.sum(q.astype(F32) * k_new, axis=1, keepdims=True)
        top = jnp.full((heads, hd), -1e30, F32)
        for c in range(ctx // CHUNK):
            s = lax.dot_general(q, kbuf[r, c * CHUNK:(c + 1) * CHUNK, :], (((1,), (1,)), ((), ())), preferred_element_type=F32)
            pos = lax.broadcasted_iota(jnp.int32, (1, CHUNK), 1) + c * CHUNK
            s = jnp.where(pos < length, s, -1e30)
            sbuf[:, c * CHUNK:(c + 1) * CHUNK] = s
            for t in range(CHUNK // hd):
                top = jnp.maximum(top, s[:, t * hd:(t + 1) * hd])
        high = jnp.maximum(jnp.max(top, axis=1, keepdims=True), s_new)
        rate = hd ** -0.5 * LOG2E
        e_new = jnp.exp2((s_new - high) * rate)
        low = jnp.zeros((heads, hd), F32)
        out = e_new.astype(BF16).astype(F32) * v_new
        for c in range(ctx // CHUNK):
            e = jnp.exp2((sbuf[:, c * CHUNK:(c + 1) * CHUNK] - high) * rate)
            for t in range(CHUNK // hd):
                low = low + e[:, t * hd:(t + 1) * hd]
            out = out + jnp.dot(e.astype(BF16), vbuf[r, c * CHUNK:(c + 1) * CHUNK, :], preferred_element_type=F32)
        out = out / (jnp.sum(low, axis=1, keepdims=True) + e_new)
        for a in range(ny):
            o32[a, pl.ds(r, lh, stride=sb), :] = out[a * lh:(a + 1) * lh]

    def b_send(b, t, slot, to):
        return remote(b_v.at[b, piece(t)], b_v.at[b, piece(t)], b_ss, b_rs.at[slot - 1, t], tx=to)

    def b_in(kind, t):
        b = held(kind, True)
        return remote(b_v.at[b, piece(t)], b_v.at[b, piece(t)], b_ss, b_rs.at[kind - 1, t], tx=after)

    def b_pair(kind, t):
        b = held(kind, True)
        return remote(b_v.at[b, piece(t)], b_v.at[b, piece(t)], bp_ss, bp_rs.at[kind], tx=partner)

    def act_out(t):
        b_send(col, t, 1, after).start()
        b_send(col, t, 2, before).start()
        b_pair(0, t).start()

    def act_in(kind, t):
        with scope("b%d%d" % (kind, t)):
            b_in(kind, t).wait_recv()
        if kind == 1 and t < EVEN:
            b_send(before, t, 3, after).start()
        if kind == 2 and t >= EVEN:
            b_send(right, t, 3, left).start()
        b_pair(kind, t).start()

    ay_cp = [remote(ay_s.at[y_peers[k - 1]], ay_r.at[row], ay_ss, ay_rs, ty=y_peers[k - 1]) for k in range(1, ny)]

    def g_send(at, slot, to):
        return remote(g_v.at[at], g_v.at[at], g_ss, g_rs.at[slot - 1], tx=to)

    def g_pair(at):
        return remote(g_v.at[at], g_v.at[at], gp_ss, gp_rs, tx=partner)

    def g_in(kind):
        at = (right, left, held(3, True))[kind - 1]
        with scope("g%d" % kind):
            g_send(at, kind, left).wait_recv()
        if kind == 1:
            g_send(right, 3, left).start()
        g_pair(at).start()

    def att_out():
        ay_s[...] = o32[...].astype(BF16)
        for c in ay_cp:
            c.start()
        ay_r[row] = ay_s[row]

    def att_rows():
        with scope("ay"):
            remote(ay_r.at[pl.ds(0, ny - 1)], ay_r.at[pl.ds(0, ny - 1)], ay_ss, ay_rs, ty=y_peers[0]).wait_recv()
        for a in range(ny):
            part = ay_r[a].astype(F32)
            for n in range(lh):
                g32[n, a * sb:(a + 1) * sb, :] = part[n * sb:(n + 1) * sb, :]
        g_v[col] = g32[...].astype(BF16)
        g_send(col, 1, left).start()
        g_send(col, 2, right).start()
        g_pair(col).start()

    mid = rows // 2

    def half_rows(half):
        return pl.ds(half * mid, mid)

    def down(n):
        if n % 2:
            b = held(n // 2, False)
            with scope("bp%d" % (n // 2)):
                remote(b_v.at[b], b_v.at[b], bp_ss, bp_rs.at[n // 2], tx=partner).wait_recv()
        part = jnp.dot(b_v[held(n // 2, n % 2 == 0)], wd_v[n], preferred_element_type=F32)
        acc[...] = part if n == 0 else acc[...] + part

    def att_down(half):
        at = pl.ds(half * nx, nx)
        part = acc[half_rows(half)]
        for n in range(0, lh, 2):
            pair = jnp.concatenate([g_v[at, n].reshape(mid, hd), g_v[at, n + 1].reshape(mid, hd)], axis=1)
            part = part + jnp.dot(pair, wo_v[n * hd:(n + 2) * hd, :], preferred_element_type=F32)
        acc[half_rows(half)] = part

    def y_out_half(half):
        part = jnp.dot(back_v[...], acc[half_rows(half)].astype(BF16), preferred_element_type=F32)
        y_s[half] = part.astype(BF16).reshape(ny, yb // 2, dl)
        for k in range(1, ny):
            remote(y_s.at[half, y_peers[k - 1]], y_r.at[half, k], y_ss.at[half], y_rs.at[half], ty=y_peers[k - 1]).start()

    def y_sum_half(half):
        at = pl.ds(pl.multiple_of(row * yb + half * (yb // 2), yb // 2), yb // 2)
        total = x_v[at, :].astype(F32) + y_s[half, row].astype(F32)
        rest = y_r.at[half, pl.ds(1, ny - 1)]
        with scope("y%d" % half):
            remote(rest, rest, y_ss.at[half], y_rs.at[half], ty=y_peers[0]).wait_recv()
        for k in range(1, ny):
            total = total + y_r[half, k].astype(F32)
        yf[half, row] = total.astype(BF16)
        for k in range(1, ny):
            remote(yf.at[half, row], yf.at[half, row], f_ss.at[half], f_rs.at[half], ty=y_peers[k - 1]).start()

    def y_all_half(half):
        rest = yf.at[half, pl.ds(0, ny - 1)]
        with scope("f%d" % half):
            remote(rest, rest, f_ss.at[half], f_rs.at[half], ty=y_peers[0]).wait_recv()
        for a in range(ny):
            y_out[a * yb + half * (yb // 2):a * yb + (half + 1) * (yb // 2), :] = yf[half, a]

    q_rows()
    for t in range(SUBS):
        ring(1, t)
    for n in range(ntx):
        wd_load(n, held(n // 2, n % 2 == 0)).start()
    wo_load.start()
    for t in range(SUBS):
        ring(2, t)
        if t == 0:
            with scope("qy"):
                remote(qy_r.at[pl.ds(0, ny - 1)], qy_r.at[pl.ds(0, ny - 1)], qy_ss, qy_rs, ty=y_peers[0]).wait_recv()
            pltpu.make_async_copy(kbuf, kbuf, kv_sem.at[0]).wait()
            pltpu.make_async_copy(vbuf, vbuf, kv_sem.at[1]).wait()
        if t % (SUBS // sb) == 0:
            with scope("a%d" % (t * sb // SUBS)):
                attend(t * sb // SUBS)
    att_out()
    for t in range(SUBS):
        ring(3, t)
    att_rows()
    pltpu.make_async_copy(wd_v, wd_v, wd_sem).wait()
    down(0)
    for t in range(SUBS):
        act_in(1, t)
        act_in(2, t)
    g_in(1)
    g_in(2)
    for n in (1, 2, 4, 3, 5):
        down(n)
    for t in range(SUBS):
        act_in(3, t)
    g_in(3)
    down(6)
    down(7)
    with scope("gp"):
        remote(g_v.at[pl.ds(0, nx)], g_v.at[pl.ds(0, nx)], gp_ss, gp_rs, tx=partner).wait_recv()
    wo_load.wait()
    for half in range(2):
        att_down(half)
        y_out_half(half)
    def put_rows(buf, base):
        for r in range(sb):
            length = lens_ref[(row * ntx + col) * sb + r]

            def some(c, carry):
                at = pl.ds(pl.multiple_of(c * CHUNK, CHUNK), CHUNK)
                here = lax.broadcasted_iota(jnp.int32, (CHUNK, hd), 0) + c * CHUNK == length
                buf[r, at, :] = jnp.where(here, new_rows[base + r:base + r + 1, :], buf[r, at, :].astype(F32)).astype(BF16)
                return carry

            lax.fori_loop(0, ctx // CHUNK, some, 0)

    with scope("putk"):
        put_rows(kbuf, 0)
    y_sum_half(0)
    y_sum_half(1)
    with scope("putv"):
        put_rows(vbuf, sb)
    y_all_half(0)
    y_all_half(1)

    with scope("sends"):
        qd_cp.wait_send()
        for ref, send, recv in (
            (stat_r.at[pl.ds(1, ntx - 1)], stat_ss, stat_rs), (gq_r.at[pl.ds(1, ntx - 1)], gq_ss, gq_rs), (gb_r.at[pl.ds(1, ntx - 1)], gb_ss, gb_rs),
            (qx_in, qx_ss, qx_rs), (qy_s.at[pl.ds(1, ny - 1)], qy_ss, qy_rs), (ay_s.at[pl.ds(1, ny - 1)], ay_ss, ay_rs),
            *((y_s.at[half, pl.ds(1, ny - 1)], y_ss.at[half], y_rs.at[half]) for half in range(2)),
            *((yf.at[half, pl.ds(1, ny - 1)], f_ss.at[half], f_rs.at[half]) for half in range(2)),
            (d_s, d_ss, d_rs.at[0]), (r_s, r_ss, r_rs.at[0, 0]), (g_v.at[pl.ds(1, nx - 1)], g_ss, g_rs.at[0]), (g_v.at[pl.ds(0, nx)], gp_ss, gp_rs),
            (b_v.at[pl.ds(1, nx - 1)], b_ss, b_rs.at[0, 0]), (b_v.at[pl.ds(0, nx)], bp_ss, bp_rs.at[0]),
        ):
            remote(ref, ref, send, recv, tx=partner).wait_send()


def store_kernel(y_v, k_v, v_v, y_h, ko_h, vo_h, y_sem, out_sem):
    copies = [pltpu.make_async_copy(k_v.at[r], ko_h.at[r], out_sem.at[0, r]) for r in range(k_v.shape[0])]
    copies += [pltpu.make_async_copy(v_v.at[r], vo_h.at[r], out_sem.at[1, r]) for r in range(v_v.shape[0])]
    copies += [pltpu.make_async_copy(y_v, y_h, y_sem)]
    for c in copies:
        c.start()
    for c in copies:
        c.wait()


def solution(mesh):
    ny = mesh.shape["ty"]
    ntx = mesh.shape["tx"]
    nx = ntx // 2
    cache_spec = P(("dp", "ty", "tx"), None, None)
    vspec = pl.BlockSpec(memory_space=VMEM)
    hspec = pl.BlockSpec(memory_space=pltpu.HBM)
    sspec = pl.BlockSpec(memory_space=pltpu.SMEM)

    def layer_shard(x_blk, lens_part, k_blk, v_blk, gamma_blk, w_query, w_key, w_value, w_gate, w_up, w_out, w_down):
        rows, dl = x_blk.shape
        sb, ctx, hd = k_blk.shape
        qn = w_query.shape[1]
        lh = qn // hd
        qw = qn + 2 * hd
        fb = w_gate.shape[1] // ntx
        rb = rows // ntx
        yb = rows // ny

        natural = np.arange(rows)
        order = np.reshape(np.transpose(np.reshape(natural, (ny, ntx, sb)), (1, 0, 2)), (rows,))
        perm = jnp.asarray(order[:, None] == natural[None, :], dtype=BF16)
        part = np.arange(rows // 2)
        order = np.reshape(np.transpose(np.reshape(part, (nx, ny, sb)), (1, 0, 2)), (rows // 2,))
        back = jnp.asarray(order[:, None] == part[None, :], dtype=BF16)
        freqs = np.power(ROPE_BASE, -(np.arange(hd // 2, dtype=np.float32) * 2.0) / hd).astype(np.float32)
        freqs = jnp.asarray(np.tile(np.concatenate([freqs, freqs])[None, :], (8, 1)))

        y_vm, k_vm, v_vm = pl.pallas_call(
            functools.partial(step_kernel, ny, nx, dl * ntx),
            out_shape=(
                pltpu.VMEM((rows, dl), BF16),
                pltpu.VMEM(k_blk.shape, BF16),
                pltpu.VMEM(v_blk.shape, BF16),
            ),
            in_specs=[sspec] + [hspec] * 14,
            out_specs=(vspec,) * 3,
            scratch_shapes=[
                VMEM((rows, dl), BF16), VMEM((dl,), F32), VMEM((rows, rows), BF16), VMEM((rows // 2, rows // 2), BF16), VMEM((8, hd), F32),
                VMEM((dl, qw), BF16), VMEM((ntx, dl, 2 * fb), BF16), VMEM((qn, dl), BF16), VMEM((ntx, fb, dl), BF16),
                VMEM((rows + 16, dl), BF16), VMEM((8, rows), F32), VMEM((ntx, 8, rows), F32),
                VMEM((16, hd), BF16), VMEM((ntx, 16, hd), BF16), VMEM((ntx, 16, hd), BF16), VMEM((ntx, 16, hd), BF16), VMEM((rows, rows), F32),
                VMEM((ntx, rb, qw), F32), VMEM((nx, rb, qw), BF16), VMEM((nx, rb, qw), BF16),
                VMEM((2 * sb, hd), F32), VMEM((nx, rb, qw), BF16), VMEM((nx, rb, qw), BF16), VMEM((rb, qw), F32), VMEM((2, rb, hd), F32),
                VMEM((ny, sb * lh, hd), F32), VMEM((ny, sb * lh, hd), F32),
                VMEM((nx, rows, 2 * fb), F32), VMEM((nx, rows, 2 * fb), BF16), VMEM((nx, rows, 2 * fb), BF16),
                VMEM((nx - 1, rows, 2 * fb), BF16), VMEM((nx - 1, rows, 2 * fb), BF16),
                VMEM((2, 8, hd), F32), VMEM((ny * lh, hd), F32), VMEM((ny * lh, ctx), F32), VMEM((ny, sb * lh, hd), F32),
                VMEM((ny, sb * lh, hd), BF16), VMEM((ny, sb * lh, hd), BF16), VMEM((lh, rb, hd), F32),
                VMEM((ntx, lh, rb, hd), BF16), VMEM((ntx, rows, fb), BF16), VMEM((rows, dl), F32),
                VMEM((2, ny, yb // 2, dl), BF16), VMEM((2, ny, yb // 2, dl), BF16), VMEM((2, ny, yb // 2, dl), BF16),
                DMA((5,)), DMA, DMA((ntx,)), DMA((2,)), DMA, DMA,
                DMA, DMA, DMA, DMA, DMA, DMA, DMA, DMA, DMA, DMA, DMA, DMA,
                DMA, DMA((nx,)), DMA, DMA((nx - 1, SUBS)),
                DMA, DMA, DMA, DMA((nx - 1,)), DMA, DMA,
                DMA, DMA((nx - 1, SUBS)), DMA, DMA((nx,)), DMA((2,)), DMA((2,)), DMA((2,)), DMA((2,)),
            ],
            compiler_params=pltpu.CompilerParams(collective_id=0, has_side_effects=True, vmem_limit_bytes=52 * 1024 * 1024),
            name="step",
        )(lens_part, x_blk, gamma_blk, perm, back, freqs, w_query, w_key, w_value, w_gate, w_up, k_blk, v_blk, w_out, w_down)

        return pl.pallas_call(
            store_kernel,
            out_shape=(
                jax.ShapeDtypeStruct((rows, dl), BF16),
                jax.ShapeDtypeStruct(k_blk.shape, BF16),
                jax.ShapeDtypeStruct(v_blk.shape, BF16),
            ),
            in_specs=[vspec] * 3,
            out_specs=(hspec,) * 3,
            scratch_shapes=[DMA, DMA((2, sb))],
            compiler_params=pltpu.CompilerParams(vmem_limit_bytes=4 * 1024 * 1024),
            name="store",
        )(y_vm, k_vm, v_vm)

    in_specs = (P("dp", "tx"), P("dp"), cache_spec, cache_spec, P("tx"), P("tx", "ty"), P("tx", None), P("tx", None), P("tx", "ty"), P("tx", "ty"), P("ty", "tx"), P("ty", "tx"))
    out_specs = (P("dp", "tx"), cache_spec, cache_spec)
    return jax.shard_map(layer_shard, mesh=mesh, in_specs=in_specs, out_specs=out_specs, check_vma=False)
```
